128 devices in a mesh: local: 16 (over z, y), data: 8 (over x, core).
Axes of the slice: x: 4, y: 4, z: 4, core: 2. Of those that a mesh axis runs over, the one named last changes fastest.
Arguments:
- tokens: bfloat16 [16384, 2048], P(('local', 'data'))
- cotangent: bfloat16 [16384, 2048], P(('local', 'data'))
- w_in: bfloat16 [2, 2048, 8192], P(None, 'local')
- w_out: bfloat16 [2, 8192, 2048], P(None, 'local')
Outputs:
- output 1: bfloat16 [16384, 2048], P(('local', 'data'))
- output 2: float32 [2, 2048, 8192], P(None, 'local')
- output 3: float32 [2, 8192, 2048], P(None, 'local')
- output 4: bfloat16 [16384, 2048], P(('local', 'data'))
All inputs are finite; a program needn't handle non-finite values.
Results may differ from the reference program's by a relative error of at most 0.0134477.
Values are sent between devices in bfloat16 or wider.
A program may use at most 1 GiB of HBM per device.

```python
import jax
import jax.numpy as jnp
from jax import lax

HIDDEN = 2048
FFN_WIDTH = 8192
LAYERS = 2
TOKENS_DEV = 128
DEVICES = 128
TOKENS = TOKENS_DEV * DEVICES
EPSILON = 1e-6


def setup_inputs(seed: int = 0) -> dict:
    base_key = jax.random.key(seed)
    key_tok, key_cot, key_in, key_out = jax.random.split(base_key, 4)
    tokens = jax.random.normal(key_tok, (TOKENS, HIDDEN), jnp.float32)
    cotangent = jax.random.normal(key_cot, (TOKENS, HIDDEN), jnp.float32)
    w_in = jax.random.normal(key_in, (LAYERS, HIDDEN, FFN_WIDTH), jnp.float32) * (HIDDEN ** -0.5)
    w_out = jax.random.normal(key_out, (LAYERS, FFN_WIDTH, HIDDEN), jnp.float32) * (1.5 * FFN_WIDTH ** -0.5)
    return {'tokens': tokens.astype(jnp.bfloat16), 'cotangent': cotangent.astype(jnp.bfloat16), 'w_in': w_in.astype(jnp.bfloat16), 'w_out': w_out.astype(jnp.bfloat16)}


def norm_rows(x_f):
    return x_f * lax.rsqrt(jnp.mean(x_f * x_f, axis=-1, keepdims=True) + EPSILON)


def layer_forward(x_in, w_first, w_second):
    normed = norm_rows(x_in.astype(jnp.float32)).astype(jnp.bfloat16)
    pre_act = jnp.dot(normed, w_first, preferred_element_type=jnp.float32).astype(jnp.bfloat16)
    hidden = jax.nn.gelu(pre_act.astype(jnp.float32)).astype(jnp.bfloat16)
    branch = jnp.dot(hidden, w_second, preferred_element_type=jnp.float32)
    return (x_in.astype(jnp.float32) + branch).astype(jnp.bfloat16), pre_act


def layer_backward(grad_next, x_in, pre_act, w_first, w_second):
    normed_f, norm_vjp = jax.vjp(norm_rows, x_in.astype(jnp.float32))
    normed = normed_f.astype(jnp.bfloat16)
    hidden_f, gelu_vjp = jax.vjp(jax.nn.gelu, pre_act.astype(jnp.float32))
    hidden = hidden_f.astype(jnp.bfloat16)
    grad_b = grad_next.astype(jnp.bfloat16)
    grad_second = jnp.dot(hidden.T, grad_b, preferred_element_type=jnp.float32)
    grad_hidden = jnp.dot(grad_b, w_second.T, preferred_element_type=jnp.float32)
    grad_pre = gelu_vjp(grad_hidden)[0].astype(jnp.bfloat16)
    grad_first = jnp.dot(normed.T, grad_pre, preferred_element_type=jnp.float32)
    grad_normed = jnp.dot(grad_pre, w_first.T, preferred_element_type=jnp.float32)
    grad_x = grad_next + norm_vjp(grad_normed)[0]
    return grad_x, grad_first, grad_second


def reference(tokens, cotangent, w_in, w_out):
    tok_blocks = tokens.reshape(DEVICES, TOKENS_DEV, HIDDEN)
    cot_blocks = cotangent.reshape(DEVICES, TOKENS_DEV, HIDDEN)

    def block_step(acc_pair, block_in):
        x_blk, g_blk = block_in

        def fwd_step(current, weights):
            next_act, pre_act = layer_forward(current, weights[0], weights[1])
            return next_act, (current, pre_act)

        out_blk, saved_acts = lax.scan(fwd_step, x_blk, (w_in, w_out))

        def bwd_step(grad_up, layer_items):
            grad_prev, grad_first, grad_second = layer_backward(grad_up, layer_items[0], layer_items[1], layer_items[2], layer_items[3])
            return grad_prev, (grad_first, grad_second)

        grad_blk, layer_grads = lax.scan(bwd_step, g_blk.astype(jnp.float32), (saved_acts[0], saved_acts[1], w_in, w_out), reverse=True)
        return (acc_pair[0] + layer_grads[0], acc_pair[1] + layer_grads[1]), (out_blk, grad_blk.astype(jnp.bfloat16))

    zero_grads = (jnp.zeros((LAYERS, HIDDEN, FFN_WIDTH), jnp.float32), jnp.zeros((LAYERS, FFN_WIDTH, HIDDEN), jnp.float32))
    grad_sums, block_outs = lax.scan(block_step, zero_grads, (tok_blocks, cot_blocks))
    return (block_outs[0].reshape(TOKENS, HIDDEN), grad_sums[0], grad_sums[1], block_outs[1].reshape(TOKENS, HIDDEN))
```

```python
import functools

import jax
import jax.numpy as jnp
from jax import lax
from jax.experimental import pallas as pl
from jax.experimental.pallas import tpu as pltpu
from jax.sharding import PartitionSpec as P

EPSILON = 1e-6
GELU_SCALE = 0.7978845608028654
GELU_CUBE = 0.044715
BF16 = jnp.bfloat16
F32 = jnp.float32
MESH = pl.DeviceIdType.MESH
HBM = pltpu.HBM
VMEM = pltpu.VMEM


class Comm:
    def __init__(self, send_sems, recv_sems):
        l = lax.axis_index('local')
        d = lax.axis_index('data')
        self.l, self.d = l, d
        self.z, self.y, self.x, self.c = l // 4, l % 4, d // 2, d % 2
        self.send_sems, self.recv_sems = send_sems, recv_sems
        self.count = 0
        self.open_sends = []
        self.partner = (l, self.x * 2 + 1 - self.c)

    def pos(self, axis):
        return {'x': self.x, 'y': self.y, 'z': self.z}[axis]

    def neighbor(self, axis, delta):
        p = (self.pos(axis) + delta) % 4
        if axis == 'x':
            return (self.l, p * 2 + self.c)
        if axis == 'y':
            return (self.z * 4 + p, self.d)
        return (p * 4 + self.y, self.d)

    def barrier(self, axes):
        sem = pltpu.get_barrier_semaphore()
        devices = [self.partner]
        for axis in axes:
            devices += [self.neighbor(axis, 1), self.neighbor(axis, 3)]
        for device in devices:
            pl.semaphore_signal(sem, inc=1, device_id=device, device_id_type=MESH)
        pl.semaphore_wait(sem, len(devices))

    def send(self, src, dst, device):
        k = self.count
        self.count += 1
        copy = pltpu.make_async_remote_copy(
            src_ref=src, dst_ref=dst, send_sem=self.send_sems.at[k], recv_sem=self.recv_sems.at[k],
            device_id=device, device_id_type=MESH)
        copy.start()
        self.open_sends.append((k, copy))
        return k

    def wait_recv(self, k, ref, device):
        pltpu.make_async_remote_copy(
            src_ref=ref, dst_ref=ref, send_sem=self.send_sems.at[k], recv_sem=self.recv_sems.at[k],
            device_id=device, device_id_type=MESH).wait_recv()

    def wait_sends(self, keys=None):
        rest = []
        for k, copy in self.open_sends:
            if keys is None or k in keys:
                copy.wait_send()
            else:
                rest.append((k, copy))
        self.open_sends = rest


class RingGather:
    def __init__(self, comm, axis, own, slot):
        self.comm, self.own, self.slot = comm, own, slot
        self.me = comm.pos(axis)
        self.right, self.left = (self.me + 1) % 4, (self.me + 3) % 4
        self.far = (self.me + 2) % 4
        self.to_right, self.to_left = comm.neighbor(axis, 1), comm.neighbor(axis, 3)

    def start(self):
        send, own, slot, me = self.comm.send, self.own, self.slot, self.me
        self.r0 = send(own(0), slot(me, 0), self.to_right)
        self.l0 = send(own(1), slot(me, 1), self.to_left)
        self.r1 = send(own(1), slot(me, 1), self.to_right)
        self.l1 = send(own(0), slot(me, 0), self.to_left)

    def forward(self):
        c, slot = self.comm, self.slot
        c.wait_recv(self.r0, slot(self.left, 0), self.to_left)
        self.r2 = c.send(slot(self.left, 0), slot(self.left, 0), self.to_right)
        c.wait_recv(self.l0, slot(self.right, 1), self.to_right)
        self.l2 = c.send(slot(self.right, 1), slot(self.right, 1), self.to_left)

    def near(self):
        c, slot = self.comm, self.slot
        c.wait_recv(self.r1, slot(self.left, 1), self.to_left)
        c.wait_recv(self.l1, slot(self.right, 0), self.to_right)

    def finish(self):
        c, slot = self.comm, self.slot
        c.wait_recv(self.r2, slot(self.far, 0), self.to_left)
        c.wait_recv(self.l2, slot(self.far, 1), self.to_right)


class RingReduce:
    def __init__(self, comm, axis, part, landing):
        self.comm, self.part, self.landing = comm, part, landing
        self.me = comm.pos(axis)
        self.right, self.left = (self.me + 1) % 4, (self.me + 3) % 4
        self.far = (self.me + 2) % 4
        self.to_right, self.to_left = comm.neighbor(axis, 1), comm.neighbor(axis, 3)

    def send_far(self, half):
        ref = self.part(self.far, half)
        if half == 0:
            self.r0 = self.comm.send(ref, self.landing.at[0], self.to_right)
        else:
            self.l0 = self.comm.send(ref, self.landing.at[3], self.to_left)

    def send_near(self, half):
        if half == 1:
            self.r1 = self.comm.send(self.part(self.right, 1), self.landing.at[1], self.to_right)
        else:
            self.l1 = self.comm.send(self.part(self.left, 0), self.landing.at[4], self.to_left)

    def start(self):
        self.send_far(0)
        self.send_far(1)
        self.send_near(1)
        self.send_near(0)

    def middle(self, add):
        c, landing = self.comm, self.landing
        c.wait_recv(self.r0, landing.at[0], self.to_left)
        add(landing.at[0], self.right, 0)
        self.r2 = c.send(landing.at[0], landing.at[2], self.to_right)
        c.wait_recv(self.l0, landing.at[3], self.to_right)
        add(landing.at[3], self.left, 1)
        self.l2 = c.send(landing.at[3], landing.at[5], self.to_left)

    def finish(self):
        c, landing = self.comm, self.landing
        c.wait_recv(self.r1, landing.at[1], self.to_left)
        c.wait_recv(self.l1, landing.at[4], self.to_right)
        c.wait_recv(self.r2, landing.at[2], self.to_left)
        c.wait_recv(self.l2, landing.at[5], self.to_right)


def add_from(part):
    def add(ref, pos, half):
        ref[...] = ref[...] + part(pos, half)[...]
    return add


class WeightGather:
    def __init__(self, comm, first, second, full, own):
        self.comm, self.full, self.second = comm, full, second
        c = comm.c
        b = comm.pos(second)
        half_rows = full.shape[3] // 2
        rows = lambda h: pl.ds(h * half_rows, half_rows)
        self.b = b
        self.ring1 = RingGather(comm, first, own=lambda h: own.at[rows(h)],
                                slot=lambda p, h: full.at[p, b, c, rows(h)])
        pair = lambda p, h: full.at[pl.ds(2 * h, 2), p, c]
        self.ring2 = RingGather(comm, second, own=lambda h: pair(b, h), slot=pair)
        self.pushed = []

    def start1(self):
        self.ring1.start()

    def forward1(self):
        self.ring1.forward()

    def start2(self):
        self.ring1.near()
        self.ring1.finish()
        self.ring2.start()
        self.push(self.b)

    def push(self, p):
        c = self.comm
        mine = self.full.at[:, p, c.c]
        self.pushed.append((p, c.send(mine, mine, c.partner)))

    def forward2(self):
        self.ring2.forward()
        self.ring2.near()
        self.push(self.ring2.left)
        self.push(self.ring2.right)

    def finish2(self):
        self.ring2.finish()
        self.push(self.ring2.far)

    def arrived(self):
        c = self.comm
        for p, k in self.pushed:
            c.wait_recv(k, self.full.at[:, p, 1 - c.c], c.partner)


def start_local(copies, sems, first):
    out = []
    for i, (src, dst) in enumerate(copies):
        copy = pltpu.make_async_copy(src, dst, sems.at[first + i])
        copy.start()
        out.append(copy)
    return out


def wait_local(copies):
    for copy in copies:
        copy.wait()


def w1_strips(comm, w_in, layer, dst, rows):
    width = w_in.shape[2] // 64
    out = []
    for y in range(4):
        for z in range(4):
            start = (4 * z + y) * 4 * width + comm.x * width
            out.append((w_in.at[layer, pl.ds(comm.c * rows, rows), pl.ds(pl.multiple_of(start, width), width)],
                        dst.at[:, pl.ds((4 * y + z) * width, width)]))
    return out


def w2_rows(comm, w_out, layer, rows):
    start = (comm.x * 2 + comm.c) * rows
    return w_out.at[layer, pl.ds(pl.multiple_of(start, rows), rows)]


def norm_rows(x):
    return x * lax.rsqrt(jnp.mean(x * x, axis=-1, keepdims=True) + EPSILON)


def norm_rows_vjp(x, g):
    r = lax.rsqrt(jnp.mean(x * x, axis=-1, keepdims=True) + EPSILON)
    dot = jnp.mean(x * g, axis=-1, keepdims=True)
    return r * g - x * (r * r * r * dot)


def gelu(x):
    t = jnp.tanh(GELU_SCALE * (x + GELU_CUBE * (x * x * x)))
    return x * (0.5 * (1.0 + t))


def gelu_grad(x):
    x2 = x * x
    t = jnp.tanh(GELU_SCALE * (x + GELU_CUBE * (x2 * x)))
    return 0.5 * (1.0 + t) + (0.5 * x) * (1.0 - t * t) * (GELU_SCALE * (1.0 + (3.0 * GELU_CUBE) * x2))


def dot(a, b):
    return lax.dot_general(a, b, (((1,), (0,)), ((), ())), preferred_element_type=F32)


def dot_bt(a, b):
    return lax.dot_general(a, b, (((1,), (1,)), ((), ())), preferred_element_type=F32)


def dot_at(a, b):
    return lax.dot_general(a, b, (((0,), (0,)), ((), ())), preferred_element_type=F32)


def flat(value):
    return value.reshape(-1, value.shape[-1])


def tile_of(n):
    return min(256, n)


def forward_acts(u, w1, a, s):
    width = a.shape[1]
    t = tile_of(width)

    def step(i, _):
        cols = pl.ds(pl.multiple_of(i * t, t), t)
        acc = dot(flat(u[...]), flat(w1[:, :, :, :, cols])).astype(BF16)
        a[:, cols] = acc
        s[:, cols] = gelu(acc.astype(F32)).astype(BF16)
        return 0

    lax.fori_loop(0, width // t, step, 0)


def forward_part(s, w2, part, half):
    width = part.shape[1] // 2
    t = tile_of(width)

    def step(i, _):
        cols = pl.ds(pl.multiple_of(half * width + i * t, t), t)
        part[:, cols] = dot(s[...], flat(w2[:, :, :, :, cols]))
        return 0

    lax.fori_loop(0, width // t, step, 0)


def backward_acts(d, w2, a, q):
    rows = 2 * w2.shape[2] * w2.shape[3]

    def step(i, _):
        cols = pl.ds(pl.multiple_of(i * rows, rows), rows)
        w = flat(w2[i // 2, pl.ds((i % 2) * 2, 2)])
        c = dot_bt(flat(d[...]), w)
        q[:, cols] = (c * gelu_grad(a[:, cols].astype(F32))).astype(BF16)
        return 0

    lax.fori_loop(0, 8, step, 0)


def backward_part(q, w1, part, half):
    rows = 2 * w1.shape[2] * w1.shape[3]

    def step(j, _):
        i = half * 4 + j
        cols = pl.ds(pl.multiple_of(i * rows, rows), rows)
        w = flat(w1[i // 2, pl.ds((i % 2) * 2, 2)])
        part[:, cols] = dot_bt(q[...], w)
        return 0

    lax.fori_loop(0, 4, step, 0)


def part_block(part, tokens):
    width = part.shape[1] // 2
    return lambda pos, half: part.at[pl.ds(pl.multiple_of(pos * tokens, tokens), tokens),
                                     pl.ds(half * width, width)]


def reduced(part, ring, tokens):
    block = part_block(part, tokens)
    landing = ring.landing
    left = block(ring.me, 0)[...] + landing[2] + landing[4]
    right = block(ring.me, 1)[...] + landing[1] + landing[5]
    return jnp.concatenate([left, right], axis=1)


def forward_first(x0, cot, w_in, w_out,
                  x1, u1, u_all, s_all, a_out, cot_all, w1_next, w2_next,
                  w1, w2, uf, a, s, part, landing, stage1, stage2, send_sems, recv_sems, local_sems):
    comm = Comm(send_sems, recv_sems)
    tokens = x0.shape[0]
    rows1, rows2 = w1.shape[3], w2.shape[3]
    z, y, x, c = comm.z, comm.y, comm.x, comm.c

    own1, own2 = w1.at[z, y, c], w2.at[y, z, c]
    strips = start_local(w1_strips(comm, w_in, 0, own1, rows1), local_sems, 0)
    strips += start_local([(w2_rows(comm, w_out, 0, rows2), own2)], local_sems, 16)
    strips1 = start_local(w1_strips(comm, w_in, 1, stage1, rows1), local_sems, 17)
    strips1 += start_local([(w2_rows(comm, w_out, 1, rows2), stage2)], local_sems, 33)

    uf[x] = norm_rows(x0[...].astype(F32)).astype(BF16)
    comm.barrier('xyz')

    half_tokens = tokens // 2
    half_of = lambda h: pl.ds(h * half_tokens, half_tokens)
    gather_u = RingGather(comm, 'x', own=lambda h: uf.at[x, half_of(h)], slot=lambda p, h: uf.at[p, half_of(h)])
    gather_cot = RingGather(comm, 'x', own=lambda h: cot.at[half_of(h)], slot=lambda p, h: cot_all.at[p, half_of(h)])
    wait_local(strips)
    g1 = WeightGather(comm, 'z', 'y', w1, own1)
    g2 = WeightGather(comm, 'y', 'z', w2, own2)
    g1.start1()
    g2.start1()
    gather_u.start()
    g1.forward1()
    g2.forward1()
    gather_u.forward()
    gather_cot.start()
    g1.start2()
    g2.start2()

    wait_local(strips1)
    n1 = WeightGather(comm, 'z', 'y', w1_next, stage1)
    n2 = WeightGather(comm, 'y', 'z', w2_next, stage2)
    keep = start_local([(stage1, w1_next.at[z, y, c]), (stage2, w2_next.at[y, z, c])], local_sems, 34)

    gather_u.near()
    gather_u.finish()
    push_u = comm.send(uf, u_all.at[1], comm.partner)
    keep_u = start_local([(uf, u_all.at[0])], local_sems, 36)
    gather_cot.forward()
    g1.forward2()
    g2.forward2()
    wait_local(keep)
    n1.start1()
    n2.start1()
    gather_cot.near()
    gather_cot.finish()
    g1.finish2()
    g2.finish2()
    g1.arrived()
    n1.forward1()
    n2.forward1()
    forward_acts(uf, w1, a, s)
    g2.arrived()
    block = part_block(part, tokens)
    ring = RingReduce(comm, 'x', block, landing)
    forward_part(s, w2, part, 0)
    ring.send_far(0)
    ring.send_near(0)
    n1.start2()
    n2.start2()
    forward_part(s, w2, part, 1)
    ring.send_far(1)
    ring.send_near(1)
    push_s = comm.send(s, s_all.at[1], comm.partner)
    keep_s = start_local([(s, s_all.at[0]), (a, a_out)], local_sems, 37)
    ring.middle(add_from(block))
    n1.forward2()
    n2.forward2()
    ring.finish()
    x_next = (x0[...].astype(F32) + reduced(part, ring, tokens)).astype(BF16)
    x1[...] = x_next
    u1[...] = norm_rows(x_next.astype(F32)).astype(BF16)
    n1.finish2()
    n2.finish2()
    n1.arrived()
    n2.arrived()
    comm.wait_recv(push_u, u_all.at[1], comm.partner)
    comm.wait_recv(push_s, s_all.at[1], comm.partner)
    wait_local(keep_u)
    wait_local(keep_s)
    comm.wait_sends()


def sds(shape, dtype):
    return jax.ShapeDtypeStruct(shape, dtype)


def sems(n):
    return pltpu.SemaphoreType.DMA((n,))


def hbm():
    return pl.BlockSpec(memory_space=HBM)


def vmem():
    return pl.BlockSpec(memory_space=VMEM)


def params(collective_id):
    return pltpu.CompilerParams(collective_id=collective_id, has_side_effects=True,
                                vmem_limit_bytes=67043328)


def call_forward_first(x0, cot, w_in, w_out):
    tokens, width = x0.shape
    inner = w_in.shape[2]
    group = 4 * tokens
    slice_ = inner // 4
    w1_shape = (4, 4, 2, width // 32, slice_)
    w2_shape = (4, 4, 2, inner // 128, width)
    return pl.pallas_call(
        forward_first,
        name='forward_first',
        out_shape=(sds((tokens, width), BF16), sds((tokens, width), BF16),
                   sds((2, 4, tokens, width), BF16), sds((2, group, slice_), BF16), sds((group, slice_), BF16),
                   sds((4, tokens, width), BF16), sds(w1_shape, BF16), sds(w2_shape, BF16)),
        in_specs=[vmem(), hbm(), hbm(), hbm()],
        out_specs=(vmem(), vmem(), hbm(), hbm(), hbm(), hbm(), hbm(), hbm()),
        scratch_shapes=[VMEM(w1_shape, BF16), VMEM(w2_shape, BF16), VMEM((4, tokens, width), BF16),
                        VMEM((group, slice_), BF16), VMEM((group, slice_), BF16), VMEM((group, width), F32),
                        VMEM((6, tokens, width // 2), F32), VMEM(w1_shape[3:], BF16), VMEM(w2_shape[3:], BF16),
                        sems(96), sems(96), sems(40)],
        compiler_params=params(1),
        cost_estimate=pl.CostEstimate(flops=4 * group * width * slice_, bytes_accessed=1 << 24, transcendentals=0),
    )(x0, cot, w_in, w_out)


def top_layer(x1, u1, cot, cot_all, w1_fwd, w2_fwd, w_in, w_out,
              x2, e1, d0, u_all, s_all, q_half, d_half, w1_back, w2_back, w1_next, w2_next,
              w1, w2, uf, df, a, s, q, part, part_e, landing, landing_e, stages1, stages2,
              send_sems, recv_sems, local_sems):
    comm = Comm(send_sems, recv_sems)
    tokens = x1.shape[0]
    rows1, rows2 = w1.shape[3], w2.shape[3]
    z, y, x, c = comm.z, comm.y, comm.x, comm.c

    strips = start_local(w1_strips(comm, w_in, 1, stages1.at[0], rows1), local_sems, 0)
    strips += start_local([(w2_rows(comm, w_out, 1, rows2), stages2.at[0])], local_sems, 16)
    load1 = start_local([(w1_fwd, w1)], local_sems, 17)
    load2 = start_local([(w2_fwd, w2)], local_sems, 18)
    strips0 = start_local(w1_strips(comm, w_in, 0, stages1.at[1], rows1), local_sems, 19)
    strips0 += start_local([(w2_rows(comm, w_out, 0, rows2), stages2.at[1])], local_sems, 35)
    others = [(x + k) % 4 for k in (1, 2, 3)]
    load_d = start_local([(cot_all.at[p], df.at[p]) for p in others], local_sems, 36)
    df[x] = cot[...]
    uf[x] = u1[...]
    wait_local(strips)
    keep = start_local([(stages1.at[0], w1_back.at[z, y, c]), (stages2.at[0], w2_back.at[y, z, c])], local_sems, 39)
    comm.barrier('xyz')

    half_tokens = tokens // 2
    half_of = lambda h: pl.ds(h * half_tokens, half_tokens)
    gather_u = RingGather(comm, 'x', own=lambda h: uf.at[x, half_of(h)], slot=lambda p, h: uf.at[p, half_of(h)])
    g1 = WeightGather(comm, 'z', 'y', w1_back, stages1.at[0])
    g2 = WeightGather(comm, 'y', 'z', w2_back, stages2.at[0])
    gather_u.start()
    g1.start1()
    g2.start1()
    g1.forward1()
    g2.forward1()
    gather_u.forward()
    wait_local(keep)
    g1.start2()
    g2.start2()
    gather_u.near()
    gather_u.finish()
    push_u = comm.send(uf, u_all.at[1], comm.partner)
    keep_u = start_local([(uf, u_all.at[0])], local_sems, 41)
    wait_local(load1)
    forward_acts(uf, w1, a, s)
    wait_local(load2)
    block = part_block(part, tokens)
    ring = RingReduce(comm, 'x', block, landing)
    forward_part(s, w2, part, 0)
    ring.send_far(0)
    ring.send_near(0)
    g1.forward2()
    g2.forward2()
    forward_part(s, w2, part, 1)
    ring.send_far(1)
    ring.send_near(1)
    push_s = comm.send(s, s_all.at[1], comm.partner)
    keep_s = start_local([(s, s_all.at[0])], local_sems, 42)
    wait_local(load_d)
    mine = lambda ref, k: ref.at[..., pl.ds(pl.multiple_of(k * (ref.shape[-1] // 2), ref.shape[-1] // 2),
                                            ref.shape[-1] // 2)]
    push_d = comm.send(mine(df, 1 - c), d_half.at[1], comm.partner)
    keep_d = start_local([(mine(df, c), d_half.at[0])], local_sems, 43)

    wait_local(strips0)
    keep0 = start_local([(stages1.at[1], w1_next.at[z, y, c]), (stages2.at[1], w2_next.at[y, z, c])], local_sems, 44)
    n1 = WeightGather(comm, 'z', 'y', w1_next, stages1.at[1])
    n2 = WeightGather(comm, 'y', 'z', w2_next, stages2.at[1])
    n1.start1()
    n2.start1()
    ring.middle(add_from(block))
    g2.finish2()
    g1.finish2()
    g2.arrived()
    load2 = start_local([(w2_back, w2)], local_sems, 46)
    g1.arrived()
    load1 = start_local([(w1_back, w1)], local_sems, 47)
    n1.forward1()
    n2.forward1()
    wait_local(load2)
    backward_acts(df, w2, a, q)
    wait_local(keep0)
    n1.start2()
    n2.start2()
    wait_local(load1)
    block_e = part_block(part_e, tokens)
    ring_e = RingReduce(comm, 'x', block_e, landing_e)
    backward_part(q, w1, part_e, 0)
    ring_e.send_far(0)
    ring_e.send_near(0)
    backward_part(q, w1, part_e, 1)
    ring_e.send_far(1)
    ring_e.send_near(1)
    push_q = comm.send(mine(q, 1 - c), q_half.at[1], comm.partner)
    keep_q = start_local([(mine(q, c), q_half.at[0])], local_sems, 48)
    ring.finish()
    xf = x1[...].astype(F32)
    x2[...] = (xf + reduced(part, ring, tokens)).astype(BF16)
    ring_e.middle(add_from(block_e))
    n1.forward2()
    n2.forward2()
    ring_e.finish()
    e = cot[...].astype(F32) + norm_rows_vjp(x1[...].astype(F32), reduced(part_e, ring_e, tokens))
    e1[...] = e
    d0[...] = e.astype(BF16)
    n1.finish2()
    n2.finish2()
    n1.arrived()
    n2.arrived()
    for k, ref in ((push_u, u_all), (push_s, s_all), (push_d, d_half), (push_q, q_half)):
        comm.wait_recv(k, ref.at[1], comm.partner)
    wait_local(keep_u + keep_s + keep_d + keep_q)
    comm.wait_sends()


def call_top_layer(x1, u1, cot, cot_all, w1_fwd, w2_fwd, w_in, w_out):
    tokens, width = x1.shape
    group = 4 * tokens
    slice_ = w_in.shape[2] // 4
    w1_shape, w2_shape = w1_fwd.shape, w2_fwd.shape
    acts = VMEM((group, slice_), BF16)
    parts = VMEM((group, width), F32)
    landing = VMEM((6, tokens, width // 2), F32)
    return pl.pallas_call(
        top_layer,
        name='top_layer',
        out_shape=(sds((tokens, width), BF16), sds((tokens, width), F32), sds((tokens, width), BF16),
                   sds((2, 4, tokens, width), BF16), sds((2, group, slice_), BF16),
                   sds((2, group, slice_ // 2), BF16), sds((2, 4, tokens, width // 2), BF16),
                   sds(w1_shape, BF16), sds(w2_shape, BF16), sds(w1_shape, BF16), sds(w2_shape, BF16)),
        in_specs=[vmem(), vmem(), vmem()] + [hbm()] * 5,
        out_specs=(vmem(), vmem(), vmem()) + (hbm(),) * 8,
        scratch_shapes=[VMEM(w1_shape, BF16), VMEM(w2_shape, BF16), VMEM((4, tokens, width), BF16),
                        VMEM((4, tokens, width), BF16), acts, acts, acts, parts, parts, landing, landing,
                        VMEM((2,) + w1_shape[3:], BF16), VMEM((2,) + w2_shape[3:], BF16),
                        sems(96), sems(96), sems(52)],
        compiler_params=params(2),
        cost_estimate=pl.CostEstimate(flops=8 * group * width * slice_, bytes_accessed=1 << 24, transcendentals=0),
    )(x1, u1, cot, cot_all, w1_fwd, w2_fwd, w_in, w_out)


class GradReduce:
    def __init__(self, comm, axis1, axis2, a, b, first_column, sends, landing1, landing2, result):
        self.comm, self.axis1, self.axis2 = comm, axis1, axis2
        self.a, self.b, self.first_column = a, b, first_column
        self.sends, self.landing2, self.result = sends, landing2, result
        self.half = sends.shape[2]
        self.rows = sends.shape[1]
        self.ring = RingReduce(comm, axis1, None, landing1)

    def product(self, pos, half):
        rows = pl.ds(pl.multiple_of(pos * self.rows, self.rows), self.rows)
        cols = pl.ds(self.first_column + half * self.half, self.half)
        return dot_at(flat(self.a[..., rows]), flat(self.b[..., cols]))

    def start(self):
        ring, sends = self.ring, self.sends
        plan = ((ring.far, 0), (ring.far, 1), (ring.right, 1), (ring.left, 0))
        ring.part = lambda pos, half: sends.at[self.slot]
        for self.slot, (pos, half) in enumerate(plan):
            sends[self.slot] = self.product(pos, half)
            if self.slot < 2:
                ring.send_far(half)
            else:
                ring.send_near(half)

    def middle(self):
        def add(ref, pos, half):
            ref[...] = ref[...] + self.product(pos, half)
        self.ring.middle(add)

    def turn(self):
        ring, sends, landing = self.ring, self.sends, self.ring.landing
        ring.finish()
        self.comm.wait_sends((ring.r0, ring.l0))
        sends[0] = self.product(ring.me, 0) + landing[2] + landing[4]
        sends[1] = self.product(ring.me, 1) + landing[1] + landing[5]
        rows = self.rows // 4
        self.block = lambda pos, half: sends.at[half, pl.ds(pl.multiple_of(pos * rows, rows), rows)]
        self.ring2 = RingReduce(self.comm, self.axis2, self.block, self.landing2)
        self.ring2.start()

    def middle2(self):
        self.ring2.middle(add_from(self.block))

    def finish(self):
        ring, landing, w = self.ring2, self.landing2, self.half
        ring.finish()
        self.result[:, 0:w] = self.block(ring.me, 0)[...] + landing[2] + landing[4]
        self.result[:, w:2 * w] = self.block(ring.me, 1)[...] + landing[1] + landing[5]


CHUNKS = 2


def grad_scratch(width, slice_):
    out = []
    for rows, cols in ((width // 4, slice_ // 2), (slice_ // 4, width // 2)):
        w = cols // CHUNKS // 2
        out += [VMEM((CHUNKS, 4, rows, w), F32), VMEM((CHUNKS, 6, rows, w), F32), VMEM((CHUNKS, 6, rows // 4, w), F32)]
    return out


def grad_reduces(comm, u, q, s, d, bufs, results):
    out = []
    for k in range(CHUNKS):
        for (axis1, axis2, a, b), (sends, land1, land2), result in zip(
                (('z', 'y', u, q), ('y', 'z', s, d)), (bufs[:3], bufs[3:]), results):
            first = k * 2 * sends.shape[3]
            out.append(GradReduce(comm, axis1, axis2, a, b, first, sends.at[k], land1.at[k], land2.at[k], result.at[k]))
    return out


def bottom_layer(x0, e1, d0, w1_hbm, w2_hbm, a_hbm, u_top, s_top, q_top, d_top,
                 grad, q_half, d_half, res_in, res_out,
                 w, df, a, q, part, landing, gu, gs, gq, gd, *rest):
    bufs, (send_sems, recv_sems, local_sems) = rest[:6], rest[6:]
    comm = Comm(send_sems, recv_sems)
    tokens = x0.shape[0]
    x, c = comm.x, comm.c
    loads = start_local([(u_top, gu), (q_top, gq), (s_top, gs), (d_top, gd)], local_sems, 0)
    load2 = start_local([(w2_hbm, w), (a_hbm, a)], local_sems, 4)
    df[x] = d0[...]
    comm.barrier('xyz')

    half_tokens = tokens // 2
    half_of = lambda h: pl.ds(h * half_tokens, half_tokens)
    gather_d = RingGather(comm, 'x', own=lambda h: df.at[x, half_of(h)], slot=lambda p, h: df.at[p, half_of(h)])
    gather_d.start()
    wait_local(loads)
    top = grad_reduces(comm, gu, gq, gs, gd, bufs, (res_in, res_out))
    first, second = top[:2], top[2:]
    for g in first:
        g.start()
    gather_d.forward()
    for g in second:
        g.start()
    gather_d.near()
    gather_d.finish()
    wait_local(load2)
    backward_acts(df, w, a, q)
    load1 = start_local([(w1_hbm, w)], local_sems, 6)
    mine = lambda ref, k: ref.at[..., pl.ds(pl.multiple_of(k * (ref.shape[-1] // 2), ref.shape[-1] // 2),
                                            ref.shape[-1] // 2)]
    push_d = comm.send(mine(df, 1 - c), d_half.at[1], comm.partner)
    push_q = comm.send(mine(q, 1 - c), q_half.at[1], comm.partner)
    keep = start_local([(mine(df, c), d_half.at[0]), (mine(q, c), q_half.at[0])], local_sems, 7)
    for g in first:
        g.middle()
    wait_local(load1)
    block = part_block(part, tokens)
    ring = RingReduce(comm, 'x', block, landing)
    backward_part(q, w, part, 0)
    ring.send_far(0)
    ring.send_near(0)
    backward_part(q, w, part, 1)
    ring.send_far(1)
    ring.send_near(1)
    for g in first:
        g.turn()
    for g in second:
        g.middle()
    ring.middle(add_from(block))
    for g in first:
        g.middle2()
    for g in second:
        g.turn()
    for g in first:
        g.finish()
    ring.finish()
    grad[...] = (e1[...] + norm_rows_vjp(x0[...].astype(F32), reduced(part, ring, tokens))).astype(BF16)
    for g in second:
        g.middle2()
    for g in second:
        g.finish()
    comm.wait_recv(push_d, d_half.at[1], comm.partner)
    comm.wait_recv(push_q, q_half.at[1], comm.partner)
    wait_local(keep)
    comm.wait_sends()


def result_shapes(width, slice_):
    return ((CHUNKS, width // 16, slice_ // 2 // CHUNKS), (CHUNKS, slice_ // 16, width // 2 // CHUNKS))


def call_bottom_layer(x0, e1, d0, w1_hbm, w2_hbm, a_hbm, u_top, s_top, q_top, d_top):
    tokens, width = x0.shape
    group, slice_ = a_hbm.shape
    acts = VMEM((group, slice_), BF16)
    shapes = result_shapes(width, slice_)
    return pl.pallas_call(
        bottom_layer,
        name='bottom_layer',
        out_shape=(sds((tokens, width), BF16), sds(q_top.shape, BF16), sds(d_top.shape, BF16),
                   sds(shapes[0], F32), sds(shapes[1], F32)),
        in_specs=[vmem()] * 3 + [hbm()] * 7,
        out_specs=(vmem(), hbm(), hbm(), vmem(), vmem()),
        scratch_shapes=[VMEM(w1_hbm.shape, BF16), VMEM((4, tokens, width), BF16), acts, acts, VMEM((group, width), F32),
                        VMEM((6, tokens, width // 2), F32), VMEM(u_top.shape, BF16), VMEM(s_top.shape, BF16),
                        VMEM(q_top.shape, BF16), VMEM(d_top.shape, BF16)] + grad_scratch(width, slice_)
        + [sems(80), sems(80), sems(10)],
        compiler_params=params(3),
        cost_estimate=pl.CostEstimate(flops=8 * group * width * slice_, bytes_accessed=1 << 24, transcendentals=0),
    )(x0, e1, d0, w1_hbm, w2_hbm, a_hbm, u_top, s_top, q_top, d_top)


class BlockGather:
    def __init__(self, comm, own, out):
        self.comm, self.own, self.out = comm, own, out
        c = comm.c
        rows = own.shape[0] // 2
        half = lambda h: pl.ds(h * rows, rows)
        self.ring = RingGather(comm, 'x', own=lambda h: own.at[half(h)], slot=lambda p, h: out.at[p, c, half(h)])
        self.pushed = []

    def push(self, pos, src):
        c = self.comm
        self.pushed.append((pos, c.send(src, self.out.at[pos, c.c], c.partner)))

    def start(self):
        self.ring.start()
        self.push(self.ring.me, self.own)

    def forward(self):
        self.ring.forward()

    def near(self):
        ring, c = self.ring, self.comm.c
        ring.near()
        self.push(ring.left, self.out.at[ring.left, c])
        self.push(ring.right, self.out.at[ring.right, c])

    def finish(self):
        ring, c = self.ring, self.comm.c
        ring.finish()
        self.push(ring.far, self.out.at[ring.far, c])

    def arrived(self):
        c = self.comm
        for pos, k in self.pushed:
            c.wait_recv(k, self.out.at[pos, 1 - c.c], c.partner)


def last_grads(u_hbm, q_hbm, s_hbm, d_hbm, top_in, top_out, all_in, all_out,
               gu, gs, gq, gd, res_in, res_out, *rest):
    bufs, (send_sems, recv_sems, local_sems) = rest[:6], rest[6:]
    comm = Comm(send_sems, recv_sems)
    x, c = comm.x, comm.c
    loads = start_local([(u_hbm, gu), (q_hbm, gq), (s_hbm, gs), (d_hbm, gd)], local_sems, 0)
    keep = start_local([(top_in.at[k], all_in.at[1, k, x, c]) for k in range(CHUNKS)]
                       + [(top_out.at[k], all_out.at[1, k, x, c]) for k in range(CHUNKS)], local_sems, 4)
    comm.barrier('xyz')
    wait_local(loads)
    grads = grad_reduces(comm, gu, gq, gs, gd, bufs, (res_in, res_out))
    first, second = grads[:2], grads[2:]
    for g in first:
        g.start()
    for g in second:
        g.start()
    top = []
    for k in range(CHUNKS):
        top += [BlockGather(comm, top_in.at[k], all_in.at[1, k]), BlockGather(comm, top_out.at[k], all_out.at[1, k])]
    for b in top:
        b.start()
    for g in first:
        g.middle()
    for b in top:
        b.forward()
    for b in top:
        b.near()
    for g in first:
        g.turn()
    for g in second:
        g.middle()
    for b in top:
        b.finish()
    for g in first:
        g.middle2()
    for g in second:
        g.turn()
    for g in first:
        g.finish()
    low = [BlockGather(comm, res.at[k], out.at[0, k]) for k in range(CHUNKS)
           for res, out in ((res_in, all_in), (res_out, all_out))]
    for b in low[:2]:
        b.start()
    for g in second:
        g.middle2()
    for b in low[:2]:
        b.forward()
    for g in second:
        g.finish()
    for b in low[2:]:
        b.start()
    keep += start_local([(res_in.at[k], all_in.at[0, k, x, c]) for k in range(CHUNKS)]
                        + [(res_out.at[k], all_out.at[0, k, x, c]) for k in range(CHUNKS)], local_sems, 4 + 2 * CHUNKS)
    for b in low[:2]:
        b.near()
    for b in low[2:]:
        b.forward()
    for b in low[:2]:
        b.finish()
    for b in low[2:]:
        b.near()
    for b in low[2:]:
        b.finish()
    for b in top + low:
        b.arrived()
    wait_local(keep)
    comm.wait_sends()


def call_last_grads(u_hbm, q_hbm, s_hbm, d_hbm, top_in, top_out):
    slice_ = s_hbm.shape[2]
    width = u_hbm.shape[3]
    shapes = result_shapes(width, slice_)
    outs = [sds((2, CHUNKS, 4, 2) + shape[1:], F32) for shape in shapes]
    return pl.pallas_call(
        last_grads,
        name='last_grads',
        out_shape=tuple(outs),
        in_specs=[hbm()] * 4 + [vmem()] * 2,
        out_specs=(hbm(), hbm()),
        scratch_shapes=[VMEM(r.shape, BF16) for r in (u_hbm, s_hbm, q_hbm, d_hbm)] + [VMEM(s, F32) for s in shapes]
        + grad_scratch(width, slice_) + [sems(144), sems(144), sems(4 + 4 * CHUNKS)],
        compiler_params=params(4),
        cost_estimate=pl.CostEstimate(flops=8 * 8 * width * slice_ * 64, bytes_accessed=1 << 24, transcendentals=0),
    )(u_hbm, q_hbm, s_hbm, d_hbm, top_in, top_out)


def solution(mesh):
    tok_spec = P(('local', 'data'), None)
    w_spec = P(None, 'local', None)

    def device_step(tokens, cotangent, w_in, w_out):
        x1, u1, u0_all, s0_all, a0, cot_all, w1_top, w2_top = call_forward_first(tokens, cotangent, w_in, w_out)
        (x2, e1, d0, u1_all, s1_all, q1_half, d1_half, _, _, w1_low, w2_low) = call_top_layer(
            x1, u1, cotangent, cot_all, w1_top, w2_top, w_in, w_out)
        grad, q0_half, d0_half, top_in, top_out = call_bottom_layer(
            tokens, e1, d0, w1_low, w2_low, a0, u1_all, s1_all, q1_half, d1_half)
        all_in, all_out = call_last_grads(u0_all, q0_half, s0_all, d0_half, top_in, top_out)
        rows = w_in.shape[1]
        strip = w_in.shape[2] // 64
        per = 2 // CHUNKS
        grad_in = all_in.reshape(2, CHUNKS, 4, 2, rows, per, 4, strip)
        grad_in = grad_in.transpose(0, 4, 6, 3, 1, 5, 2, 7).reshape(w_in.shape)
        grad_out = all_out.transpose(0, 2, 4, 3, 1, 5).reshape(w_out.shape)
        return x2, grad_in, grad_out, grad

    return jax.shard_map(device_step, mesh=mesh, in_specs=(tok_spec, tok_spec, w_spec, w_spec),
                         out_specs=(tok_spec, w_spec, w_spec, tok_spec), check_vma=False)
```

```python
import functools

import jax
import jax.numpy as jnp
from jax import lax
from jax.experimental import pallas as pl
from jax.experimental.pallas import tpu as pltpu
from jax.sharding import PartitionSpec as P

EPSILON = 1e-6
GELU_SCALE = 0.7978845608028654
GELU_CUBE = 0.044715
BF16 = jnp.bfloat16
F32 = jnp.float32
MESH = pl.DeviceIdType.MESH
HBM = pltpu.HBM
VMEM = pltpu.VMEM


class Comm:
    def __init__(self, send_sems, recv_sems):
        l = lax.axis_index('local')
        d = lax.axis_index('data')
        self.l, self.d = l, d
        self.z, self.y, self.x, self.c = l // 4, l % 4, d // 2, d % 2
        self.send_sems, self.recv_sems = send_sems, recv_sems
        self.count = 0
        self.open_sends = []
        self.partner = (l, self.x * 2 + 1 - self.c)

    def pos(self, axis):
        return {'x': self.x, 'y': self.y, 'z': self.z}[axis]

    def neighbor(self, axis, delta):
        p = (self.pos(axis) + delta) % 4
        if axis == 'x':
            return (self.l, p * 2 + self.c)
        if axis == 'y':
            return (self.z * 4 + p, self.d)
        return (p * 4 + self.y, self.d)

    def barrier(self, axes):
        sem = pltpu.get_barrier_semaphore()
        devices = [self.partner]
        for axis in axes:
            devices += [self.neighbor(axis, 1), self.neighbor(axis, 3)]
        for device in devices:
            pl.semaphore_signal(sem, inc=1, device_id=device, device_id_type=MESH)
        pl.semaphore_wait(sem, len(devices))

    def send(self, src, dst, device):
        k = self.count
        self.count += 1
        copy = pltpu.make_async_remote_copy(
            src_ref=src, dst_ref=dst, send_sem=self.send_sems.at[k], recv_sem=self.recv_sems.at[k],
            device_id=device, device_id_type=MESH)
        copy.start()
        self.open_sends.append((k, copy))
        return k

    def wait_recv(self, k, ref, device):
        pltpu.make_async_remote_copy(
            src_ref=ref, dst_ref=ref, send_sem=self.send_sems.at[k], recv_sem=self.recv_sems.at[k],
            device_id=device, device_id_type=MESH).wait_recv()

    def wait_sends(self, keys=None):
        rest = []
        for k, copy in self.open_sends:
            if keys is None or k in keys:
                copy.wait_send()
            else:
                rest.append((k, copy))
        self.open_sends = rest


class RingGather:
    def __init__(self, comm, axis, own, slot):
        self.comm, self.own, self.slot = comm, own, slot
        self.me = comm.pos(axis)
        self.right, self.left = (self.me + 1) % 4, (self.me + 3) % 4
        self.far = (self.me + 2) % 4
        self.to_right, self.to_left = comm.neighbor(axis, 1), comm.neighbor(axis, 3)

    def start(self):
        send, own, slot, me = self.comm.send, self.own, self.slot, self.me
        self.r0 = send(own(0), slot(me, 0), self.to_right)
        self.l0 = send(own(1), slot(me, 1), self.to_left)
        self.r1 = send(own(1), slot(me, 1), self.to_right)
        self.l1 = send(own(0), slot(me, 0), self.to_left)

    def forward(self):
        c, slot = self.comm, self.slot
        c.wait_recv(self.r0, slot(self.left, 0), self.to_left)
        self.r2 = c.send(slot(self.left, 0), slot(self.left, 0), self.to_right)
        c.wait_recv(self.l0, slot(self.right, 1), self.to_right)
        self.l2 = c.send(slot(self.right, 1), slot(self.right, 1), self.to_left)

    def near(self):
        c, slot = self.comm, self.slot
        c.wait_recv(self.r1, slot(self.left, 1), self.to_left)
        c.wait_recv(self.l1, slot(self.right, 0), self.to_right)

    def finish(self):
        c, slot = self.comm, self.slot
        c.wait_recv(self.r2, slot(self.far, 0), self.to_left)
        c.wait_recv(self.l2, slot(self.far, 1), self.to_right)


class RingReduce:
    def __init__(self, comm, axis, part, landing):
        self.comm, self.part, self.landing = comm, part, landing
        self.me = comm.pos(axis)
        self.right, self.left = (self.me + 1) % 4, (self.me + 3) % 4
        self.far = (self.me + 2) % 4
        self.to_right, self.to_left = comm.neighbor(axis, 1), comm.neighbor(axis, 3)

    def send_far(self, half):
        ref = self.part(self.far, half)
        if half == 0:
            self.r0 = self.comm.send(ref, self.landing.at[0], self.to_right)
        else:
            self.l0 = self.comm.send(ref, self.landing.at[3], self.to_left)

    def send_near(self, half):
        if half == 1:
            self.r1 = self.comm.send(self.part(self.right, 1), self.landing.at[1], self.to_right)
        else:
            self.l1 = self.comm.send(self.part(self.left, 0), self.landing.at[4], self.to_left)

    def start(self):
        self.send_far(0)
        self.send_far(1)
        self.send_near(1)
        self.send_near(0)

    def middle_right(self, add):
        c, landing = self.comm, self.landing
        c.wait_recv(self.r0, landing.at[0], self.to_left)
        add(landing.at[0], self.right, 0)
        self.r2 = c.send(landing.at[0], landing.at[2], self.to_right)

    def middle_left(self, add):
        c, landing = self.comm, self.landing
        c.wait_recv(self.l0, landing.at[3], self.to_right)
        add(landing.at[3], self.left, 1)
        self.l2 = c.send(landing.at[3], landing.at[5], self.to_left)

    def middle(self, add):
        self.middle_right(add)
        self.middle_left(add)

    def finish(self):
        c, landing = self.comm, self.landing
        c.wait_recv(self.r1, landing.at[1], self.to_left)
        c.wait_recv(self.l1, landing.at[4], self.to_right)
        c.wait_recv(self.r2, landing.at[2], self.to_left)
        c.wait_recv(self.l2, landing.at[5], self.to_right)


def add_from(part):
    def add(ref, pos, half):
        ref[...] = ref[...] + part(pos, half)[...]
    return add


class HalfGather:
    def __init__(self, comm, dims, first, full, own, part):
        self.comm, self.full = comm, full
        c = comm.c
        lead = dims[0] == first
        second = dims[1] if lead else dims[0]
        b = comm.pos(second)
        half_rows, width = full.shape[3] // 2, full.shape[4] // 2
        rows = lambda h: pl.ds(h * half_rows, half_rows)
        self.cols = cols = pl.ds(part * width, width)
        self.b, self.lead = b, lead
        if lead:
            slot1 = lambda p, h: full.at[p, b, c, rows(h), cols]
            slot2 = lambda p, h: full.at[pl.ds(2 * h, 2), p, c, :, cols]
        else:
            slot1 = lambda p, h: full.at[b, p, c, rows(h), cols]
            slot2 = lambda p, h: full.at[p, pl.ds(2 * h, 2), c, :, cols]
        self.ring1 = RingGather(comm, first, own=lambda h: own.at[rows(h), cols], slot=slot1)
        self.ring2 = RingGather(comm, second, own=lambda h: slot2(b, h), slot=slot2)
        self.pushed = []

    def line(self, p, core):
        return self.full.at[:, p, core, :, self.cols] if self.lead else self.full.at[p, :, core, :, self.cols]

    def push(self, p):
        c = self.comm
        mine = self.line(p, c.c)
        self.pushed.append((p, c.send(mine, mine, c.partner)))

    def start1(self):
        self.ring1.start()

    def forward1(self):
        self.ring1.forward()

    def start2(self):
        self.ring1.near()
        self.ring1.finish()
        self.ring2.start()
        self.push(self.b)

    def forward2(self):
        self.ring2.forward()
        self.ring2.near()
        self.push(self.ring2.left)
        self.push(self.ring2.right)

    def finish2(self):
        self.ring2.finish()
        self.push(self.ring2.far)

    def arrived(self):
        c = self.comm
        for p, k in self.pushed:
            c.wait_recv(k, self.line(p, 1 - c.c), c.partner)


class WeightGather:
    def __init__(self, comm, dims, full, own):
        self.halves = [HalfGather(comm, dims, dims[k], full, own, k) for k in (0, 1)]

    def __getattr__(self, step):
        def run():
            for half in self.halves:
                getattr(half, step)()
        return run


def start_local(copies, sems, first):
    out = []
    for i, (src, dst) in enumerate(copies):
        copy = pltpu.make_async_copy(src, dst, sems.at[first + i])
        copy.start()
        out.append(copy)
    return out


def wait_local(copies):
    for copy in copies:
        copy.wait()


def w1_strips(comm, w_in, layer, dst, rows):
    width = w_in.shape[2] // 64
    out = []
    for y in range(4):
        for z in range(4):
            start = (4 * z + y) * 4 * width + comm.x * width
            out.append((w_in.at[layer, pl.ds(comm.c * rows, rows), pl.ds(pl.multiple_of(start, width), width)],
                        dst.at[:, pl.ds((4 * y + z) * width, width)]))
    return out


def w2_rows(comm, w_out, layer, rows):
    start = (comm.x * 2 + comm.c) * rows
    return w_out.at[layer, pl.ds(pl.multiple_of(start, rows), rows)]


def norm_rows(x):
    return x * lax.rsqrt(jnp.mean(x * x, axis=-1, keepdims=True) + EPSILON)


def norm_rows_vjp(x, g):
    r = lax.rsqrt(jnp.mean(x * x, axis=-1, keepdims=True) + EPSILON)
    dot = jnp.mean(x * g, axis=-1, keepdims=True)
    return r * g - x * (r * r * r * dot)


def gelu(x):
    t = jnp.tanh(GELU_SCALE * (x + GELU_CUBE * (x * x * x)))
    return x * (0.5 * (1.0 + t))


def gelu_grad(x):
    x2 = x * x
    t = jnp.tanh(GELU_SCALE * (x + GELU_CUBE * (x2 * x)))
    return 0.5 * (1.0 + t) + (0.5 * x) * (1.0 - t * t) * (GELU_SCALE * (1.0 + (3.0 * GELU_CUBE) * x2))


def dot(a, b):
    return lax.dot_general(a, b, (((1,), (0,)), ((), ())), preferred_element_type=F32)


def dot_bt(a, b):
    return lax.dot_general(a, b, (((1,), (1,)), ((), ())), preferred_element_type=F32)


def dot_at(a, b):
    return lax.dot_general(a, b, (((0,), (0,)), ((), ())), preferred_element_type=F32)


def flat(value):
    return value.reshape(-1, value.shape[-1])


def tile_of(n):
    return min(256, n)


def forward_acts(u, w1, a, s):
    width = a.shape[1]
    t = tile_of(width)

    def step(i, _):
        cols = pl.ds(pl.multiple_of(i * t, t), t)
        acc = dot(flat(u[...]), flat(w1[:, :, :, :, cols])).astype(BF16)
        a[:, cols] = acc
        s[:, cols] = gelu(acc.astype(F32)).astype(BF16)
        return 0

    lax.fori_loop(0, width // t, step, 0)


def forward_part(s, w2, part, half):
    width = part.shape[1] // 2
    t = tile_of(width)

    def step(i, _):
        cols = pl.ds(pl.multiple_of(half * width + i * t, t), t)
        part[:, cols] = dot(s[...], flat(w2[:, :, :, :, cols]))
        return 0

    lax.fori_loop(0, width // t, step, 0)


def backward_acts(d, w2, a, q):
    rows = 2 * w2.shape[2] * w2.shape[3]

    def step(i, _):
        cols = pl.ds(pl.multiple_of(i * rows, rows), rows)
        w = flat(w2[i // 2, pl.ds((i % 2) * 2, 2)])
        c = dot_bt(flat(d[...]), w)
        q[:, cols] = (c * gelu_grad(a[:, cols].astype(F32))).astype(BF16)
        return 0

    lax.fori_loop(0, 8, step, 0)


def backward_part(q, w1, part, half):
    rows = 2 * w1.shape[2] * w1.shape[3]

    def step(j, _):
        i = half * 4 + j
        cols = pl.ds(pl.multiple_of(i * rows, rows), rows)
        w = flat(w1[i // 2, pl.ds((i % 2) * 2, 2)])
        part[:, cols] = dot_bt(q[...], w)
        return 0

    lax.fori_loop(0, 4, step, 0)


def part_block(part, tokens):
    width = part.shape[1] // 2
    return lambda pos, half: part.at[pl.ds(pl.multiple_of(pos * tokens, tokens), tokens),
                                     pl.ds(half * width, width)]


def reduced(part, ring, tokens):
    block = part_block(part, tokens)
    landing = ring.landing
    left = block(ring.me, 0)[...] + landing[2] + landing[4]
    right = block(ring.me, 1)[...] + landing[1] + landing[5]
    return jnp.concatenate([left, right], axis=1)


def forward_first(x0, cot, w_in, w_out,
                  x1, u1, u_all, s_all, a_out, cot_all, w1_next, w2_next,
                  w1, w2, uf, a, s, part, landing, stage1, stage2, send_sems, recv_sems, local_sems):
    comm = Comm(send_sems, recv_sems)
    tokens = x0.shape[0]
    rows1, rows2 = w1.shape[3], w2.shape[3]
    z, y, x, c = comm.z, comm.y, comm.x, comm.c

    own1, own2 = w1.at[z, y, c], w2.at[y, z, c]
    strips = start_local(w1_strips(comm, w_in, 0, own1, rows1), local_sems, 0)
    strips += start_local([(w2_rows(comm, w_out, 0, rows2), own2)], local_sems, 16)
    strips1 = start_local(w1_strips(comm, w_in, 1, stage1, rows1), local_sems, 17)
    strips1 += start_local([(w2_rows(comm, w_out, 1, rows2), stage2)], local_sems, 33)
    uf[x] = norm_rows(x0[...].astype(F32)).astype(BF16)
    comm.barrier('xyz')

    half_tokens = tokens // 2
    half_of = lambda h: pl.ds(h * half_tokens, half_tokens)
    gather_u = RingGather(comm, 'x', own=lambda h: uf.at[x, half_of(h)], slot=lambda p, h: uf.at[p, half_of(h)])
    gather_cot = RingGather(comm, 'x', own=lambda h: cot.at[half_of(h)], slot=lambda p, h: cot_all.at[p, half_of(h)])
    wait_local(strips)
    g1 = WeightGather(comm, 'zy', w1, own1)
    g2 = WeightGather(comm, 'yz', w2, own2)
    n1 = WeightGather(comm, 'zy', w1_next, stage1)
    n2 = WeightGather(comm, 'yz', w2_next, stage2)
    g1.start1()
    gather_u.start()
    g2.start1()
    wait_local(strips1)
    keep = start_local([(stage1, w1_next.at[z, y, c]), (stage2, w2_next.at[y, z, c])], local_sems, 34)
    g1.forward1()
    gather_u.forward()
    gather_cot.start()
    g2.forward1()
    g1.start2()
    g1.forward2()
    g2.start2()
    gather_u.near()
    gather_u.finish()
    push_u = comm.send(uf, u_all.at[1], comm.partner)
    keep_u = start_local([(uf, u_all.at[0])], local_sems, 36)
    gather_cot.forward()
    n1.start1()
    n2.start1()
    g1.finish2()
    g1.arrived()
    forward_acts(uf, w1, a, s)
    g2.forward2()
    gather_cot.near()
    gather_cot.finish()
    push_s = comm.send(s, s_all.at[1], comm.partner)
    keep_s = start_local([(s, s_all.at[0]), (a, a_out)], local_sems, 37)
    n1.forward1()
    n2.forward1()
    g2.finish2()
    g2.arrived()
    block = part_block(part, tokens)
    ring = RingReduce(comm, 'x', block, landing)
    forward_part(s, w2, part, 0)
    ring.send_far(0)
    ring.send_near(0)
    wait_local(keep)
    n1.start2()
    forward_part(s, w2, part, 1)
    ring.send_far(1)
    ring.send_near(1)
    n1.forward2()
    n2.start2()
    ring.middle_right(add_from(block))
    n1.finish2()
    n2.forward2()
    ring.middle_left(add_from(block))
    ring.finish()
    x_next = (x0[...].astype(F32) + reduced(part, ring, tokens)).astype(BF16)
    x1[...] = x_next
    u1[...] = norm_rows(x_next.astype(F32)).astype(BF16)
    n2.finish2()
    n1.arrived()
    n2.arrived()
    comm.wait_recv(push_u, u_all.at[1], comm.partner)
    comm.wait_recv(push_s, s_all.at[1], comm.partner)
    wait_local(keep_u)
    wait_local(keep_s)
    comm.wait_sends()


def sds(shape, dtype):
    return jax.ShapeDtypeStruct(shape, dtype)


def sems(n):
    return pltpu.SemaphoreType.DMA((n,))


def hbm():
    return pl.BlockSpec(memory_space=HBM)


def vmem():
    return pl.BlockSpec(memory_space=VMEM)


def params(collective_id):
    return pltpu.CompilerParams(collective_id=collective_id, has_side_effects=True,
                                vmem_limit_bytes=67043328)


def call_forward_first(x0, cot, w_in, w_out):
    tokens, width = x0.shape
    inner = w_in.shape[2]
    group = 4 * tokens
    slice_ = inner // 4
    w1_shape = (4, 4, 2, width // 32, slice_)
    w2_shape = (4, 4, 2, inner // 128, width)
    return pl.pallas_call(
        forward_first,
        name='forward_first',
        out_shape=(sds((tokens, width), BF16), sds((tokens, width), BF16),
                   sds((2, 4, tokens, width), BF16), sds((2, group, slice_), BF16), sds((group, slice_), BF16),
                   sds((4, tokens, width), BF16), sds(w1_shape, BF16), sds(w2_shape, BF16)),
        in_specs=[vmem(), hbm(), hbm(), hbm()],
        out_specs=(vmem(), vmem(), hbm(), hbm(), hbm(), hbm(), hbm(), hbm()),
        scratch_shapes=[VMEM(w1_shape, BF16), VMEM(w2_shape, BF16), VMEM((4, tokens, width), BF16),
                        VMEM((group, slice_), BF16), VMEM((group, slice_), BF16), VMEM((group, width), F32),
                        VMEM((6, tokens, width // 2), F32), VMEM(w1_shape[3:], BF16), VMEM(w2_shape[3:], BF16),
                        sems(160), sems(160), sems(40)],
        compiler_params=params(1),
        cost_estimate=pl.CostEstimate(flops=4 * group * width * slice_, bytes_accessed=1 << 24, transcendentals=0),
    )(x0, cot, w_in, w_out)


def last_dim_half(ref, k):
    width = ref.shape[-1] // 2
    return ref.at[..., pl.ds(pl.multiple_of(k * width, width), width)]


def top_layer(x1, u1, cot, cot_all, w1_fwd, w2_fwd, w_in, w_out,
              e1, d0, part_out, u_all, s_all, q_half, d_half, w1_next, w2_next,
              w1, w2, w1_back, w2_back, uf, df, a, s, q, part, landing, stage1, stage2,
              send_sems, recv_sems, local_sems):
    comm = Comm(send_sems, recv_sems)
    tokens = x1.shape[0]
    rows1, rows2 = w1.shape[3], w2.shape[3]
    z, y, x, c = comm.z, comm.y, comm.x, comm.c

    own1, own2 = w1_back.at[z, y, c], w2_back.at[y, z, c]
    strips = start_local(w1_strips(comm, w_in, 1, own1, rows1), local_sems, 0)
    strips += start_local([(w2_rows(comm, w_out, 1, rows2), own2)], local_sems, 16)
    load1 = start_local([(w1_fwd, w1)], local_sems, 17)
    others = [(x + k) % 4 for k in (1, 2, 3)]
    load_d = start_local([(cot_all.at[p], df.at[p]) for p in others], local_sems, 36)
    load2 = start_local([(w2_fwd, w2)], local_sems, 18)
    strips0 = start_local(w1_strips(comm, w_in, 0, stage1, rows1), local_sems, 19)
    strips0 += start_local([(w2_rows(comm, w_out, 0, rows2), stage2)], local_sems, 35)
    df[x] = cot[...]
    uf[x] = u1[...]
    comm.barrier('xyz')

    half_tokens = tokens // 2
    half_of = lambda h: pl.ds(h * half_tokens, half_tokens)
    gather_u = RingGather(comm, 'x', own=lambda h: uf.at[x, half_of(h)], slot=lambda p, h: uf.at[p, half_of(h)])
    g1 = WeightGather(comm, 'zy', w1_back, own1)
    g2 = WeightGather(comm, 'yz', w2_back, own2)
    n1 = WeightGather(comm, 'zy', w1_next, stage1)
    n2 = WeightGather(comm, 'yz', w2_next, stage2)
    gather_u.start()
    wait_local(strips)
    g2.start1()
    g1.start1()
    g2.forward1()
    gather_u.forward()
    g1.forward1()
    g2.start2()
    wait_local(strips0)
    keep = start_local([(stage1, w1_next.at[z, y, c]), (stage2, w2_next.at[y, z, c])], local_sems, 39)
    g2.forward2()
    g1.start2()
    gather_u.near()
    gather_u.finish()
    push_u = comm.send(uf, u_all.at[1], comm.partner)
    keep_u = start_local([(uf, u_all.at[0])], local_sems, 41)
    wait_local(load1)
    forward_acts(uf, w1, a, s)
    n2.start1()
    n1.start1()
    g2.finish2()
    push_s = comm.send(s, s_all.at[1], comm.partner)
    keep_s = start_local([(s, s_all.at[0])], local_sems, 42)
    wait_local(load_d)
    push_d = comm.send(last_dim_half(df, 1 - c), d_half.at[1], comm.partner)
    keep_d = start_local([(last_dim_half(df, c), d_half.at[0])], local_sems, 43)
    g2.arrived()
    backward_acts(df, w2_back, a, q)
    g1.forward2()
    n2.forward1()
    n1.forward1()
    wait_local(load2)
    forward_part(s, w2, part, 0)
    forward_part(s, w2, part, 1)
    keep_part = start_local([(part, part_out)], local_sems, 44)
    push_q = comm.send(last_dim_half(q, 1 - c), q_half.at[1], comm.partner)
    keep_q = start_local([(last_dim_half(q, c), q_half.at[0])], local_sems, 45)
    wait_local(keep)
    g1.finish2()
    n2.start2()
    g1.arrived()
    wait_local(keep_part)
    block = part_block(part, tokens)
    ring = RingReduce(comm, 'x', block, landing)
    backward_part(q, w1_back, part, 0)
    ring.send_far(0)
    ring.send_near(0)
    backward_part(q, w1_back, part, 1)
    ring.send_far(1)
    ring.send_near(1)
    n2.forward2()
    n1.start2()
    ring.middle_right(add_from(block))
    n2.finish2()
    n1.forward2()
    ring.middle_left(add_from(block))
    ring.finish()
    e = cot[...].astype(F32) + norm_rows_vjp(x1[...].astype(F32), reduced(part, ring, tokens))
    e1[...] = e
    d0[...] = e.astype(BF16)
    n1.finish2()
    n2.arrived()
    n1.arrived()
    for k, ref in ((push_u, u_all), (push_s, s_all), (push_d, d_half), (push_q, q_half)):
        comm.wait_recv(k, ref.at[1], comm.partner)
    wait_local(keep_u + keep_s + keep_d + keep_q)
    comm.wait_sends()


def call_top_layer(x1, u1, cot, cot_all, w1_fwd, w2_fwd, w_in, w_out):
    tokens, width = x1.shape
    group = 4 * tokens
    slice_ = w_in.shape[2] // 4
    w1_shape, w2_shape = w1_fwd.shape, w2_fwd.shape
    acts = VMEM((group, slice_), BF16)
    return pl.pallas_call(
        top_layer,
        name='top_layer',
        out_shape=(sds((tokens, width), F32), sds((tokens, width), BF16), sds((group, width), F32),
                   sds((2, 4, tokens, width), BF16), sds((2, group, slice_), BF16),
                   sds((2, group, slice_ // 2), BF16), sds((2, 4, tokens, width // 2), BF16),
                   sds(w1_shape, BF16), sds(w2_shape, BF16)),
        in_specs=[vmem(), vmem(), vmem()] + [hbm()] * 5,
        out_specs=(vmem(), vmem()) + (hbm(),) * 7,
        scratch_shapes=[VMEM(w1_shape, BF16), VMEM(w2_shape, BF16), VMEM(w1_shape, BF16), VMEM(w2_shape, BF16),
                        VMEM((4, tokens, width), BF16), VMEM((4, tokens, width), BF16), acts, acts, acts,
                        VMEM((group, width), F32), VMEM((6, tokens, width // 2), F32),
                        VMEM(w1_shape[3:], BF16), VMEM(w2_shape[3:], BF16),
                        sems(160), sems(160), sems(48)],
        compiler_params=params(2),
        cost_estimate=pl.CostEstimate(flops=8 * group * width * slice_, bytes_accessed=1 << 24, transcendentals=0),
    )(x1, u1, cot, cot_all, w1_fwd, w2_fwd, w_in, w_out)


class GradReduce:
    def __init__(self, comm, axis1, axis2, a, b, first_column, sends, landing1, landing2, result):
        self.comm, self.axis1, self.axis2 = comm, axis1, axis2
        self.a, self.b, self.first_column = a, b, first_column
        self.sends, self.landing2, self.result = sends, landing2, result
        self.half = sends.shape[2]
        self.rows = sends.shape[1]
        self.ring = RingReduce(comm, axis1, None, landing1)

    def product(self, ref, pos, half, landed=()):
        t = tile_of(self.rows)
        cols = pl.ds(pl.multiple_of(self.first_column + half * self.half, self.half), self.half)

        def step(i, _):
            rows = pl.ds(pl.multiple_of(i * t, t), t)
            columns = pl.ds(pl.multiple_of(pos * self.rows + i * t, t), t)
            value = dot_at(flat(self.a[..., columns]), flat(self.b[..., cols]))
            for other in landed:
                value = value + other[rows]
            ref[rows] = value
            return 0

        lax.fori_loop(0, self.rows // t, step, 0)

    def start(self):
        ring, sends = self.ring, self.sends
        for self.slot, (pos, half) in enumerate(((ring.far, 0), (ring.far, 1), (ring.right, 1), (ring.left, 0))):
            self.product(sends.at[self.slot], pos, half)
            ring.part = lambda pos, half: sends.at[self.slot]
            if self.slot < 2:
                ring.send_far(half)
            else:
                ring.send_near(half)

    def middle(self):
        self.ring.middle(lambda ref, pos, half: self.product(ref, pos, half, (ref,)))

    def turn(self):
        ring, sends, landing = self.ring, self.sends, self.ring.landing
        ring.finish()
        self.comm.wait_sends((ring.r0, ring.l0))
        self.product(sends.at[0], ring.me, 0, (landing.at[2], landing.at[4]))
        self.product(sends.at[1], ring.me, 1, (landing.at[1], landing.at[5]))
        rows = self.rows // 4
        self.block = lambda pos, half: sends.at[half, pl.ds(pl.multiple_of(pos * rows, rows), rows)]
        self.ring2 = RingReduce(self.comm, self.axis2, self.block, self.landing2)
        self.ring2.start()

    def middle2(self):
        self.ring2.middle(add_from(self.block))

    def finish(self):
        ring, landing, w = self.ring2, self.landing2, self.half
        ring.finish()
        self.result[:, 0:w] = self.block(ring.me, 0)[...] + landing[2] + landing[4]
        self.result[:, w:2 * w] = self.block(ring.me, 1)[...] + landing[1] + landing[5]


TOP_CHUNKS = 2
LOW_CHUNKS = 4


def grad_scratch(width, slice_, chunks):
    out = []
    for rows, cols in ((width // 4, slice_ // 2), (slice_ // 4, width // 2)):
        w = cols // chunks // 2
        out += [VMEM((chunks, 4, rows, w), F32), VMEM((chunks, 6, rows, w), F32), VMEM((chunks, 6, rows // 4, w), F32)]
    return out


class GradPair:
    def __init__(self, comm, k, u, q, s, d, bufs, results):
        self.both = []
        for axes, a, b, (sends, land1, land2), result in zip(('zy', 'yz'), (u, s), (q, d), (bufs[:3], bufs[3:]), results):
            first = k * 2 * sends.shape[3]
            self.both.append(GradReduce(comm, axes[0], axes[1], a, b, first,
                                        sends.at[k], land1.at[k], land2.at[k], result.at[k]))

    def __getattr__(self, step):
        def run():
            for grad in self.both:
                getattr(grad, step)()
        return run


def bottom_layer(x0, e1, d0, w1_hbm, w2_hbm, a_hbm, u_top, s_top, q_top, d_top,
                 grad, q_half, d_half, res_in, res_out,
                 w, df, a, q, part, landing, gu, gs, gq, gd, *rest):
    bufs, (send_sems, recv_sems, local_sems) = rest[:6], rest[6:]
    comm = Comm(send_sems, recv_sems)
    tokens = x0.shape[0]
    x, c = comm.x, comm.c
    loads = start_local([(u_top, gu), (q_top, gq), (s_top, gs), (d_top, gd)], local_sems, 0)
    load2 = start_local([(w2_hbm, w), (a_hbm, a)], local_sems, 4)
    df[x] = d0[...]
    comm.barrier('xyz')

    half_tokens = tokens // 2
    half_of = lambda h: pl.ds(h * half_tokens, half_tokens)
    gather_d = RingGather(comm, 'x', own=lambda h: df.at[x, half_of(h)], slot=lambda p, h: df.at[p, half_of(h)])
    gather_d.start()
    wait_local(loads)
    t0, t1 = [GradPair(comm, k, gu, gq, gs, gd, bufs, (res_in, res_out)) for k in range(TOP_CHUNKS)]
    t0.start()
    gather_d.forward()
    t1.start()
    gather_d.near()
    gather_d.finish()
    wait_local(load2)
    backward_acts(df, w, a, q)
    load1 = start_local([(w1_hbm, w)], local_sems, 6)
    push_d = comm.send(last_dim_half(df, 1 - c), d_half.at[1], comm.partner)
    push_q = comm.send(last_dim_half(q, 1 - c), q_half.at[1], comm.partner)
    keep = start_local([(last_dim_half(df, c), d_half.at[0]), (last_dim_half(q, c), q_half.at[0])], local_sems, 7)
    t0.middle()
    wait_local(load1)
    block = part_block(part, tokens)
    ring = RingReduce(comm, 'x', block, landing)
    backward_part(q, w, part, 0)
    ring.send_far(0)
    ring.send_near(0)
    backward_part(q, w, part, 1)
    ring.send_far(1)
    ring.send_near(1)
    t1.middle()
    ring.middle(add_from(block))
    t0.turn()
    t0.middle2()
    ring.finish()
    grad[...] = (e1[...] + norm_rows_vjp(x0[...].astype(F32), reduced(part, ring, tokens))).astype(BF16)
    t0.finish()
    t1.turn()
    t1.middle2()
    t1.finish()
    comm.wait_recv(push_d, d_half.at[1], comm.partner)
    comm.wait_recv(push_q, q_half.at[1], comm.partner)
    wait_local(keep)
    comm.wait_sends()


def result_shapes(width, slice_, chunks):
    return ((chunks, width // 16, slice_ // 2 // chunks), (chunks, slice_ // 16, width // 2 // chunks))


def call_bottom_layer(x0, e1, d0, w1_hbm, w2_hbm, a_hbm, u_top, s_top, q_top, d_top):
    tokens, width = x0.shape
    group, slice_ = a_hbm.shape
    acts = VMEM((group, slice_), BF16)
    shapes = result_shapes(width, slice_, TOP_CHUNKS)
    return pl.pallas_call(
        bottom_layer,
        name='bottom_layer',
        out_shape=(sds((tokens, width), BF16), sds(q_top.shape, BF16), sds(d_top.shape, BF16),
                   sds(shapes[0], F32), sds(shapes[1], F32)),
        in_specs=[vmem()] * 3 + [hbm()] * 7,
        out_specs=(vmem(), hbm(), hbm(), vmem(), vmem()),
        scratch_shapes=[VMEM(w1_hbm.shape, BF16), VMEM((4, tokens, width), BF16), acts, acts, VMEM((group, width), F32),
                        VMEM((6, tokens, width // 2), F32), VMEM(u_top.shape, BF16), VMEM(s_top.shape, BF16),
                        VMEM(q_top.shape, BF16), VMEM(d_top.shape, BF16)] + grad_scratch(width, slice_, TOP_CHUNKS)
        + [sems(80), sems(80), sems(10)],
        compiler_params=params(3),
        cost_estimate=pl.CostEstimate(flops=8 * group * width * slice_, bytes_accessed=1 << 24, transcendentals=0),
    )(x0, e1, d0, w1_hbm, w2_hbm, a_hbm, u_top, s_top, q_top, d_top)


class BlockGather:
    def __init__(self, comm, own, out):
        self.comm, self.own, self.out = comm, own, out
        c = comm.c
        rows = own.shape[0] // 2
        half = lambda h: pl.ds(h * rows, rows)
        self.ring = RingGather(comm, 'x', own=lambda h: own.at[half(h)], slot=lambda p, h: out.at[p, c, half(h)])
        self.pushed = []

    def push(self, pos, src):
        c = self.comm
        self.pushed.append((pos, c.send(src, self.out.at[pos, c.c], c.partner)))

    def start(self):
        self.ring.start()
        self.push(self.ring.me, self.own)

    def forward(self):
        self.ring.forward()

    def near(self):
        ring, c = self.ring, self.comm.c
        ring.near()
        self.push(ring.left, self.out.at[ring.left, c])
        self.push(ring.right, self.out.at[ring.right, c])

    def finish(self):
        ring, c = self.ring, self.comm.c
        ring.finish()
        self.push(ring.far, self.out.at[ring.far, c])

    def arrived(self):
        c = self.comm
        for pos, k in self.pushed:
            c.wait_recv(k, self.out.at[pos, 1 - c.c], c.partner)


class PairGather:
    def __init__(self, comm, k, results, outs):
        self.both = [BlockGather(comm, res.at[k], out.at[k]) for res, out in zip(results, outs)]

    def __getattr__(self, step):
        def run():
            for block in self.both:
                getattr(block, step)()
        return run


def last_grads(u_hbm, q_hbm, s_hbm, d_hbm, top_in, top_out, x1, part_hbm,
               x2, top_all_in, top_all_out, low_all_in, low_all_out,
               gu, gs, gq, gd, part, landing, res_in, res_out, *rest):
    bufs, (send_sems, recv_sems, local_sems) = rest[:6], rest[6:]
    comm = Comm(send_sems, recv_sems)
    tokens = x1.shape[0]
    x, c = comm.x, comm.c
    loads = start_local([(u_hbm, gu), (q_hbm, gq), (s_hbm, gs), (d_hbm, gd)], local_sems, 0)
    load_part = start_local([(part_hbm, part)], local_sems, 4)
    keep = start_local([(res.at[k], out.at[k, x, c]) for k in range(TOP_CHUNKS)
                        for res, out in ((top_in, top_all_in), (top_out, top_all_out))], local_sems, 5)
    comm.barrier('xyz')
    wait_local(loads)
    g = [GradPair(comm, k, gu, gq, gs, gd, bufs, (res_in, res_out)) for k in range(LOW_CHUNKS)]
    top = [PairGather(comm, k, (top_in, top_out), (top_all_in, top_all_out)) for k in range(TOP_CHUNKS)]
    low = [PairGather(comm, k, (res_in, res_out), (low_all_in, low_all_out)) for k in range(LOW_CHUNKS)]
    g[0].start()
    wait_local(load_part)
    block = part_block(part, tokens)
    ring = RingReduce(comm, 'x', block, landing)
    ring.start()
    g[1].start()
    top[0].start()
    g[0].middle()
    ring.middle(add_from(block))
    top[1].start()
    g[2].start()
    g[1].middle()
    g[0].turn()
    g[3].start()
    ring.finish()
    x2[...] = (x1[...].astype(F32) + reduced(part, ring, tokens)).astype(BF16)
    top[0].forward()
    g[0].middle2()
    g[2].middle()
    top[0].near()
    top[1].forward()
    g[1].turn()
    g[0].finish()
    low[0].start()
    top[0].finish()
    g[1].middle2()
    g[3].middle()
    top[1].near()
    g[1].finish()
    low[1].start()
    low[0].forward()
    top[1].finish()
    g[2].turn()
    low[0].near()
    g[2].middle2()
    low[1].forward()
    low[0].finish()
    g[3].turn()
    g[2].finish()
    low[2].start()
    g[3].middle2()
    low[1].near()
    low[2].forward()
    low[1].finish()
    g[3].finish()
    low[3].start()
    keep += start_local([(res.at[k], out.at[k, x, c]) for k in range(LOW_CHUNKS)
                         for res, out in ((res_in, low_all_in), (res_out, low_all_out))], local_sems, 5 + 2 * TOP_CHUNKS)
    low[2].near()
    low[3].forward()
    low[2].finish()
    low[3].near()
    low[3].finish()
    for pair in top + low:
        pair.arrived()
    wait_local(keep)
    comm.wait_sends()


def call_last_grads(u_hbm, q_hbm, s_hbm, d_hbm, top_in, top_out, x1, part_hbm):
    slice_ = s_hbm.shape[2]
    tokens, width = x1.shape
    low = result_shapes(width, slice_, LOW_CHUNKS)
    outs = [sds((shape[0], 4, 2) + shape[1:], F32) for shape in (top_in.shape, top_out.shape) + low]
    return pl.pallas_call(
        last_grads,
        name='last_grads',
        out_shape=(sds((tokens, width), BF16),) + tuple(outs),
        in_specs=[hbm()] * 4 + [vmem()] * 3 + [hbm()],
        out_specs=(vmem(),) + (hbm(),) * 4,
        scratch_shapes=[VMEM(r.shape, BF16) for r in (u_hbm, s_hbm, q_hbm, d_hbm)]
        + [VMEM(part_hbm.shape, F32), VMEM((6, tokens, width // 2), F32)] + [VMEM(s, F32) for s in low]
        + grad_scratch(width, slice_, LOW_CHUNKS) + [sems(240), sems(240), sems(5 + 2 * TOP_CHUNKS + 2 * LOW_CHUNKS)],
        compiler_params=params(4),
        cost_estimate=pl.CostEstimate(flops=64 * tokens * width * slice_, bytes_accessed=1 << 24, transcendentals=0),
    )(u_hbm, q_hbm, s_hbm, d_hbm, top_in, top_out, x1, part_hbm)


def assemble(top_in, top_out, low_in, low_out, grad_in, grad_out, v_top_in, v_top_out, v_low_in, v_low_out,
             load_sems, store_sems):
    loads = []
    for i, (src, dst) in enumerate(((low_in, v_low_in), (low_out, v_low_out), (top_in, v_top_in), (top_out, v_top_out))):
        copy = pltpu.make_async_copy(src, dst, load_sems.at[i])
        copy.start()
        loads.append(copy)
    strip = grad_in.shape[2] // 64
    for i, ref in enumerate((v_low_in, v_low_out, v_top_in, v_top_out)):
        loads[i].wait()
        layer = i // 2
        chunks, rows, width = ref.shape[0], ref.shape[3], ref.shape[4]
        for k in range(chunks):
            for x in range(4):
                for c in range(2):
                    if i % 2:
                        dst = grad_out.at[layer, pl.ds(x * rows, rows), pl.ds((c * chunks + k) * width, width)]
                        pltpu.make_async_copy(ref.at[k, x, c], dst, store_sems.at[1]).start()
                        continue
                    for j in range(width // strip):
                        t = k * (width // strip) + j
                        y, z = 2 * c + t // 4, t % 4
                        dst = grad_in.at[layer, :, pl.ds(((4 * z + y) * 4 + x) * strip, strip)]
                        pltpu.make_async_copy(ref.at[k, x, c, :, pl.ds(j * strip, strip)], dst, store_sems.at[0]).start()
    pltpu.make_async_copy(grad_in, grad_in, store_sems.at[0]).wait()
    pltpu.make_async_copy(grad_out, grad_out, store_sems.at[1]).wait()


def call_assemble(top_in, top_out, low_in, low_out, in_shape, out_shape):
    ins = (top_in, top_out, low_in, low_out)
    return pl.pallas_call(
        assemble,
        name='assemble',
        out_shape=(sds(in_shape, F32), sds(out_shape, F32)),
        in_specs=[hbm()] * 4,
        out_specs=(hbm(), hbm()),
        scratch_shapes=[VMEM(r.shape, F32) for r in ins] + [sems(4), sems(2)],
        compiler_params=pltpu.CompilerParams(vmem_limit_bytes=67043328),
        cost_estimate=pl.CostEstimate(flops=1 << 30, bytes_accessed=1 << 25, transcendentals=0),
    )(*ins)


def solution(mesh):
    tok_spec = P(('local', 'data'), None)
    w_spec = P(None, 'local', None)

    def device_step(tokens, cotangent, w_in, w_out):
        x1, u1, u0_all, s0_all, a0, cot_all, w1_top, w2_top = call_forward_first(tokens, cotangent, w_in, w_out)
        e1, d0, part_out, u1_all, s1_all, q1_half, d1_half, w1_low, w2_low = call_top_layer(
            x1, u1, cotangent, cot_all, w1_top, w2_top, w_in, w_out)
        grad, q0_half, d0_half, res_in, res_out = call_bottom_layer(
            tokens, e1, d0, w1_low, w2_low, a0, u1_all, s1_all, q1_half, d1_half)
        x2, top_in, top_out, low_in, low_out = call_last_grads(
            u0_all, q0_half, s0_all, d0_half, res_in, res_out, x1, part_out)
        grad_in, grad_out = call_assemble(top_in, top_out, low_in, low_out, w_in.shape, w_out.shape)
        return x2, grad_in, grad_out, grad

    return jax.shard_map(device_step, mesh=mesh, in_specs=(tok_spec, tok_spec, w_spec, w_spec),
                         out_specs=(tok_spec, w_spec, w_spec, tok_spec), check_vma=False)
```

```python
import functools

import jax
import jax.numpy as jnp
from jax import lax
from jax.experimental import pallas as pl
from jax.experimental.pallas import tpu as pltpu
from jax.sharding import PartitionSpec as P

EPSILON = 1e-6
GELU_SCALE = 0.7978845608028654
GELU_CUBE = 0.044715
BF16 = jnp.bfloat16
F32 = jnp.float32
MESH = pl.DeviceIdType.MESH
HBM = pltpu.HBM
VMEM = pltpu.VMEM
VMEM_BYTES = 67043328
UPPER = (67, 147)
LOWER = (59, 99, 34)


class Comm:
    def __init__(self, send_sems, recv_sems, local_sems):
        l = lax.axis_index('local')
        d = lax.axis_index('data')
        self.l, self.d = l, d
        self.z, self.y, self.x, self.c = l // 4, l % 4, d // 2, d % 2
        self.send_sems, self.recv_sems, self.local_sems = send_sems, recv_sems, local_sems
        self.sends = self.recvs = self.local_count = 0
        self.groups = []
        self.partner = (l, self.x * 2 + 1 - self.c)

    def pos(self, axis):
        return {'x': self.x, 'y': self.y, 'z': self.z}[axis]

    def neighbor(self, axis, delta):
        p = (self.pos(axis) + delta) % 4
        if axis == 'x':
            return (self.l, p * 2 + self.c)
        if axis == 'y':
            return (self.z * 4 + p, self.d)
        return (p * 4 + self.y, self.d)

    def peers(self, axes):
        out = [self.partner] if 'c' in axes else []
        for axis in axes.replace('c', ''):
            out += [self.neighbor(axis, 1), self.neighbor(axis, 3)]
        return out

    def signal(self, sem, axes):
        for device in self.peers(axes):
            pl.semaphore_signal(sem, inc=1, device_id=device, device_id_type=MESH)

    def wait(self, sem, axes):
        pl.semaphore_wait(sem, len(self.peers(axes)))

    def barrier(self, axes):
        sem = pltpu.get_barrier_semaphore()
        self.signal(sem, axes)
        self.wait(sem, axes)

    def send_sem(self):
        self.sends += 1
        return self.send_sems.at[self.sends - 1]

    def recv_sem(self):
        self.recvs += 1
        return self.recv_sems.at[self.recvs - 1]

    def copy(self, src, dst, device, send_sem, recv_sem):
        return pltpu.make_async_remote_copy(src_ref=src, dst_ref=dst, send_sem=send_sem, recv_sem=recv_sem,
                                            device_id=device, device_id_type=MESH)

    def send(self, src, dst, device, group, recv_sem):
        self.copy(src, dst, device, group.sem, recv_sem).start()

    def wait_recv(self, ref, recv_sem):
        self.copy(ref, ref, self.partner, self.send_sems.at[0], recv_sem).wait_recv()

    def push(self, src, dst):
        group, recv_sem = Sends(self, src), self.recv_sem()
        self.send(src, dst, self.partner, group, recv_sem)
        return group, lambda: self.wait_recv(dst, recv_sem)

    def local(self, *pairs):
        out = []
        for src, dst in pairs:
            copy = pltpu.make_async_copy(src, dst, self.local_sems.at[self.local_count])
            copy.start()
            self.local_count += 1
            out.append(copy)
        return out

    def end(self):
        for group in self.groups:
            group.wait()


class Sends:
    def __init__(self, comm, ref, sem=None):
        self.comm, self.ref, self.sem = comm, ref, sem or comm.send_sem()
        self.waited = False
        comm.groups.append(self)

    def wait(self):
        if not self.waited:
            self.waited = True
            c = self.comm
            c.copy(self.ref, self.ref, c.partner, self.sem, c.recv_sems.at[0]).wait_send()


def done(copies):
    for copy in copies:
        copy.wait()


class Every:
    def __init__(self, things):
        self.things = things

    def __getattr__(self, step):
        def run(*args):
            for thing in self.things:
                getattr(thing, step)(*args)
        return run


class RingGather:
    def __init__(self, comm, axis, own, slot, block, three):
        self.comm, self.own, self.slot, self.block = comm, own, slot, block
        self.me = comm.pos(axis)
        self.right, self.far, self.left = [(self.me + k) % 4 for k in (1, 2, 3)]
        self.to_right, self.to_left = comm.neighbor(axis, 1), comm.neighbor(axis, 3)
        self.group = Sends(comm, three)
        self.sems = [comm.recv_sem() for _ in range(3)]

    def both(self, k, right, right_slot, left, left_slot):
        self.comm.send(right, right_slot, self.to_right, self.group, self.sems[k])
        self.comm.send(left, left_slot, self.to_left, self.group, self.sems[k])

    def start(self):
        own, slot, me = self.own, self.slot, self.me
        self.both(0, own(0), slot(me, 0), own(1), slot(me, 1))
        self.both(1, own(1), slot(me, 1), own(0), slot(me, 0))

    def forward(self):
        self.comm.wait_recv(self.block, self.sems[0])
        right, left = self.slot(self.left, 0), self.slot(self.right, 1)
        self.both(2, right, right, left, left)

    def near(self):
        self.comm.wait_recv(self.block, self.sems[1])

    def finish(self):
        self.comm.wait_recv(self.block, self.sems[2])

    def sent(self):
        self.group.wait()


class RingReduce:
    def __init__(self, comm, axis, part, landing, before=None):
        self.comm, self.part, self.landing = comm, part, landing
        self.me = comm.pos(axis)
        self.right, self.far, self.left = [(self.me + k) % 4 for k in (1, 2, 3)]
        self.to_right, self.to_left = comm.neighbor(axis, 1), comm.neighbor(axis, 3)
        self.first = Sends(comm, landing.at[pl.ds(0, 2)], before and before.first.sem)
        self.rest = Sends(comm, landing.at[pl.ds(0, 4)], before and before.rest.sem)
        self.sems = before.sems if before else [comm.recv_sem() for _ in range(3)]

    def right_to(self, k, src, group, sem):
        self.comm.send(src, self.landing.at[k], self.to_right, group, sem)

    def left_to(self, k, src, group, sem):
        self.comm.send(src, self.landing.at[k], self.to_left, group, sem)

    def start(self, far0, far1, right1, left0):
        self.right_to(0, far0, self.first, self.sems[0])
        self.left_to(3, far1, self.first, self.sems[1])
        self.right_to(1, right1, self.rest, self.sems[2])
        self.left_to(4, left0, self.rest, self.sems[2])

    def start_all(self):
        part = self.part
        self.start(part(self.far, 0), part(self.far, 1), part(self.right, 1), part(self.left, 0))

    def start_half(self, half):
        if half == 0:
            self.right_to(0, self.part(self.far, 0), self.first, self.sems[0])
            self.left_to(4, self.part(self.left, 0), self.rest, self.sems[2])
        else:
            self.left_to(3, self.part(self.far, 1), self.first, self.sems[1])
            self.right_to(1, self.part(self.right, 1), self.rest, self.sems[2])

    def wait_right(self):
        self.comm.wait_recv(self.landing.at[0], self.sems[0])

    def wait_left(self):
        self.comm.wait_recv(self.landing.at[3], self.sems[1])

    def pass_right(self):
        self.right_to(2, self.landing.at[0], self.rest, self.sems[2])

    def pass_left(self):
        self.left_to(5, self.landing.at[3], self.rest, self.sems[2])

    def middle_right(self):
        landing = self.landing
        self.wait_right()
        landing[0] = landing[0] + self.part(self.right, 0)[...]
        self.pass_right()

    def middle_left(self):
        landing = self.landing
        self.wait_left()
        landing[3] = landing[3] + self.part(self.left, 1)[...]
        self.pass_left()

    def finish(self):
        self.comm.wait_recv(self.landing.at[pl.ds(0, 4)], self.sems[2])

    def sent(self):
        self.first.wait()
        self.rest.wait()

    def sums(self):
        landing = self.landing
        return (self.part(self.me, 0)[...] + landing[2] + landing[4],
                self.part(self.me, 1)[...] + landing[1] + landing[5])


class PlaneGather:
    def __init__(self, comm, dims, first, full, cols):
        self.comm = comm
        c = comm.c
        lead = dims[0] == first
        second = dims.replace(first, '')
        b = comm.pos(second)
        half_rows = full.shape[3] // 2
        rows = lambda h: pl.ds(h * half_rows, half_rows)
        pair = lambda h: pl.ds(2 * h, 2)
        self.b = b
        every, three, own = slice(None), pl.ds(0, 3), comm.pos(first)
        at = lambda p, q, r: full.at[(p, q, c, r, cols) if lead else (q, p, c, r, cols)]
        slot1 = lambda p, h: at(p, b, rows(h))
        slot2 = lambda p, h: at(pair(h), p, every)
        self.ring1 = RingGather(comm, first, lambda h: slot1(own, h), slot1, at(own, b, every), at(three, b, every))
        self.ring2 = RingGather(comm, second, lambda h: slot2(b, h), slot2, at(every, b, every), at(every, three, every))
        self.line = lambda p: at(every, p, every)
        whole = at(every, every, every)
        self.group, self.sem, self.whole = Sends(comm, whole), comm.recv_sem(), whole

    def push(self, p):
        self.comm.send(self.line(p), self.line(p), self.comm.partner, self.group, self.sem)

    def start1(self):
        self.ring1.start()

    def forward1(self):
        self.ring1.forward()

    def start2(self):
        self.ring1.near()
        self.ring1.finish()
        self.ring2.start()
        self.push(self.b)

    def forward2(self):
        self.ring2.forward()

    def near2(self):
        self.ring2.near()
        self.push(self.ring2.left)
        self.push(self.ring2.right)

    def finish2(self):
        self.ring2.finish()
        self.push(self.ring2.far)

    def arrived(self):
        self.comm.wait_recv(self.whole, self.sem)

    def sent(self):
        self.ring1.sent()
        self.ring2.sent()
        self.group.wait()


def gathers(comm, dims, full, pieces):
    width = full.shape[4] // pieces
    out = [PlaneGather(comm, dims, dims[k % 2], full, pl.ds(k * width, width)) for k in range(pieces)]
    return [Every(out[k:k + 2]) for k in range(0, pieces, 2)]


def own_blocks(comm, w_in, w_out, layer, w1, w2):
    z, y, x, c = comm.z, comm.y, comm.x, comm.c
    width = w_in.shape[2] // 64
    rows1, rows2 = w1.shape[3], w2.shape[3]
    own = w1.at[z, y, c]
    k = comm.local_count
    comm.local_count += 1
    for j in range(16):
        start = (4 * (j % 4) + j // 4) * 4 * width + x * width
        pltpu.make_async_copy(w_in.at[layer, pl.ds(c * rows1, rows1), pl.ds(pl.multiple_of(start, width), width)],
                              own.at[:, pl.ds(j * width, width)], comm.local_sems.at[k]).start()
    start = (x * 2 + c) * rows2
    copies = comm.local((w_out.at[layer, pl.ds(pl.multiple_of(start, rows2), rows2)], w2.at[y, z, c]))
    return [pltpu.make_async_copy(own, own, comm.local_sems.at[k])] + copies


def ring_of_tokens(comm, full):
    n = full.shape[1] // 2
    slot = lambda p, h: full.at[p, pl.ds(h * n, n)]
    return RingGather(comm, 'x', lambda h: slot(comm.x, h), slot, full.at[0], full.at[pl.ds(0, 3)])


def token_sums(comm, part, landing, tokens):
    width = part.shape[1] // 2
    block = lambda pos, half: part.at[pl.ds(pl.multiple_of(pos * tokens, tokens), tokens), pl.ds(half * width, width)]
    return RingReduce(comm, 'x', block, landing)


def norm_rows(x):
    return x * lax.rsqrt(jnp.mean(x * x, axis=-1, keepdims=True) + EPSILON)


def norm_rows_vjp(x, g):
    r = lax.rsqrt(jnp.mean(x * x, axis=-1, keepdims=True) + EPSILON)
    dot = jnp.mean(x * g, axis=-1, keepdims=True)
    return r * g - x * (r * r * r * dot)


def gelu(x):
    t = jnp.tanh(GELU_SCALE * (x + GELU_CUBE * (x * x * x)))
    return x * (0.5 * (1.0 + t))


def gelu_grad(x):
    x2 = x * x
    t = jnp.tanh(GELU_SCALE * (x + GELU_CUBE * (x2 * x)))
    return 0.5 * (1.0 + t) + (0.5 * x) * (1.0 - t * t) * (GELU_SCALE * (1.0 + (3.0 * GELU_CUBE) * x2))


def dot(a, b):
    return lax.dot_general(a, b, (((1,), (0,)), ((), ())), preferred_element_type=F32)


def dot_bt(a, b):
    return lax.dot_general(a, b, (((1,), (1,)), ((), ())), preferred_element_type=F32)


def flat(value):
    return value.reshape(-1, value.shape[-1])


def tiles(n, step, tile=256):
    t = min(tile, n)

    def run(i, _):
        step(pl.ds(pl.multiple_of(i * t, t), t))
        return 0

    lax.fori_loop(0, n // t, run, 0)


def forward_acts(u, w1, a, s, st):
    def step(cols):
        acc = dot(flat(u[...]), flat(w1[:, :, :, :, cols])).astype(BF16)
        a[:, cols] = acc
        value = gelu(acc.astype(F32)).astype(BF16)
        s[:, cols] = value
        st[cols, :] = value.T

    tiles(a.shape[1], step)


def transposed(u, ut):
    def step(cols):
        ut[cols, :] = flat(u[:, :, cols]).T

    tiles(ut.shape[0], step)


def forward_part(s, w2, part, half):
    width = part.shape[1] // 2
    t = min(256, width)

    def run(i, _):
        cols = pl.ds(pl.multiple_of(half * width + i * t, t), t)
        part[:, cols] = dot(s[...], flat(w2[:, :, :, :, cols]))
        return 0

    lax.fori_loop(0, width // t, run, 0)


def row_tile(w, i):
    return flat(w[i // 2, pl.ds((i % 2) * 2, 2)])


def backward_acts(d, tile_product, a, q):
    rows = a.shape[1] // 8

    def step(i, _):
        cols = pl.ds(pl.multiple_of(i * rows, rows), rows)
        q[:, cols] = (tile_product(i) * gelu_grad(a[:, cols].astype(F32))).astype(BF16)
        return 0

    lax.fori_loop(0, 8, step, 0)


def backward_part(tile_product, part, half):
    rows = part.shape[1] // 8

    def step(j, _):
        i = half * 4 + j
        part[:, pl.ds(pl.multiple_of(i * rows, rows), rows)] = tile_product(i)
        return 0

    lax.fori_loop(0, 4, step, 0)


def last_dim_half(ref, k):
    width = ref.shape[-1] // 2
    return ref.at[..., pl.ds(pl.multiple_of(k * width, width), width)]


def upper_half(x0, cot, w_in, w_out,
               x1, e1, d0, part_out, a_low, ut_low, st_low, ut_top, st_top, q_top, d_top, w1_low, w2_low,
               p1, p2, q1, q2, uf, df, a, s, q, ut, st, part, landing,
               send_sems, recv_sems, local_sems, credits):
    comm = Comm(send_sems, recv_sems, local_sems)
    tokens = x0.shape[0]
    x, c = comm.x, comm.c
    p_free, q_free = credits.at[0], credits.at[1]

    own0 = own_blocks(comm, w_in, w_out, 0, p1, p2)
    own1 = own_blocks(comm, w_in, w_out, 1, q1, q2)
    uf[x] = norm_rows(x0[...].astype(F32)).astype(BF16)
    df[x] = cot[...]
    comm.barrier('xyzc')

    gather_u = ring_of_tokens(comm, uf)
    gather_d = ring_of_tokens(comm, df)
    g1, = gathers(comm, 'zy', p1, 2)
    g2, g3 = gathers(comm, 'yz', p2, 4)
    n1, = gathers(comm, 'zy', q1, 2)
    n2, = gathers(comm, 'yz', q2, 2)
    done(own0)
    g1.start1()
    g2.start1()
    gather_u.start()
    g1.forward1()
    g3.start1()
    g2.forward1()
    g1.start2()
    gather_u.forward()
    gather_d.start()
    g1.forward2()
    g3.forward1()
    gather_u.near()
    g2.start2()
    done(own1)
    n1.start1()
    gather_u.finish()
    transposed(uf, ut)
    pushed = [comm.push(ut, ut_low.at[1])]
    kept = comm.local((ut, ut_low.at[0]))
    g1.near2()
    gather_d.forward()
    g1.finish2()
    g1.arrived()
    g2.forward2()
    g3.start2()
    forward_acts(uf, p1, a, s, st)
    g2.near2()
    g2.finish2()
    n1.forward1()
    g3.forward2()
    n2.start1()
    pushed += [comm.push(st, st_low.at[1])]
    kept += comm.local((st, st_low.at[0]), (a, a_low))
    g2.arrived()
    gather_u.sent()
    ring = token_sums(comm, part, landing, tokens)
    forward_part(s, p2, part, 0)
    ring.start_half(0)
    g3.near2()
    n1.start2()
    g3.finish2()
    g3.arrived()
    forward_part(s, p2, part, 1)
    ring.start_half(1)
    n2.forward1()
    gather_d.near()
    gather_d.finish()
    pushed += [comm.push(last_dim_half(df, 1 - c), d_top.at[1])]
    kept_d = comm.local((last_dim_half(df, c), d_top.at[0]))
    g1.sent()
    g2.sent()
    g3.sent()
    comm.signal(p_free, 'yzc')
    own2 = own_blocks(comm, w_in, w_out, 1, p1, p2)
    b1, = gathers(comm, 'zy', p1, 2)
    b2, = gathers(comm, 'yz', p2, 2)
    n1.forward2()
    ring.middle_right()
    n1.near2()
    n2.start2()
    done(own2)
    comm.wait(p_free, 'yzc')
    b2.start1()
    b1.start1()
    ring.middle_left()
    n1.finish2()
    n2.forward2()
    ring.finish()
    x_next = (x0[...].astype(F32) + jnp.concatenate(ring.sums(), axis=1)).astype(BF16)
    x1[...] = x_next
    uf[x] = norm_rows(x_next.astype(F32)).astype(BF16)
    ring.sent()
    gather_v = ring_of_tokens(comm, uf)
    gather_v.start()
    b2.forward1()
    b1.forward1()
    n2.near2()
    n1.arrived()
    b2.start2()
    n2.finish2()
    gather_v.forward()
    n2.arrived()
    done(kept)
    pushed[0][0].wait()
    pushed[1][0].wait()
    b2.forward2()
    gather_v.near()
    b1.start2()
    gather_v.finish()
    forward_acts(uf, q1, a, s, st)
    b2.near2()
    b2.finish2()
    forward_part(s, q2, part, 0)
    forward_part(s, q2, part, 1)
    keep_part = comm.local((part, part_out))
    n1.sent()
    n2.sent()
    comm.signal(q_free, 'yzc')
    own3 = own_blocks(comm, w_in, w_out, 0, q1, q2)
    l1, = gathers(comm, 'zy', q1, 2)
    l2, = gathers(comm, 'yz', q2, 2)
    b2.arrived()
    b1.forward2()
    transposed(uf, ut)
    pushed += [comm.push(ut, ut_top.at[1]), comm.push(st, st_top.at[1])]
    kept = kept_d + comm.local((ut, ut_top.at[0]), (st, st_top.at[0]))
    done(own3)
    comm.wait(q_free, 'yzc')
    l1.start1()
    b1.near2()
    backward_acts(df, lambda i: dot_bt(flat(df[...]), row_tile(p2, i)), a, q)
    b1.finish2()
    l1.forward1()
    l2.start1()
    b1.arrived()
    done(keep_part)
    ring = token_sums(comm, part, landing, tokens)
    product = lambda i: dot_bt(q[...], row_tile(p1, i))
    backward_part(product, part, 0)
    ring.start_half(0)
    l2.forward1()
    l1.start2()
    backward_part(product, part, 1)
    ring.start_half(1)
    pushed += [comm.push(last_dim_half(q, 1 - c), q_top.at[1])]
    kept += comm.local((last_dim_half(q, c), q_top.at[0]))
    l1.forward2()
    l2.start2()
    ring.middle_right()
    l1.near2()
    l1.finish2()
    l2.forward2()
    ring.middle_left()
    l1.arrived()
    kept += comm.local((q1, w1_low))
    l2.near2()
    l2.finish2()
    ring.finish()
    g = jnp.concatenate(ring.sums(), axis=1)
    e = cot[...].astype(F32) + norm_rows_vjp(x1[...].astype(F32), g)
    e1[...] = e
    d0[...] = e.astype(BF16)
    l2.arrived()
    kept += comm.local((q2, w2_low))
    for _, arrived in pushed:
        arrived()
    done(kept)
    comm.end()


def sds(shape, dtype):
    return jax.ShapeDtypeStruct(shape, dtype)


def sems(n):
    return pltpu.SemaphoreType.DMA((n,))


def spaces(kinds):
    return [pl.BlockSpec(memory_space=VMEM if k == 'v' else HBM) for k in kinds]


def call(kernel, ins, in_kinds, outs, out_kinds, scratch, copies, credits, collective_id, flops):
    return pl.pallas_call(
        kernel,
        name=kernel.__name__,
        out_shape=tuple(outs),
        in_specs=spaces(in_kinds),
        out_specs=tuple(spaces(out_kinds)),
        scratch_shapes=scratch + [sems(copies[0][0]), sems(copies[0][1]), sems(copies[1]),
                                  pltpu.SemaphoreType.REGULAR((credits,))],
        compiler_params=pltpu.CompilerParams(collective_id=collective_id, has_side_effects=True,
                                             vmem_limit_bytes=VMEM_BYTES),
        cost_estimate=pl.CostEstimate(flops=flops, bytes_accessed=1 << 24, transcendentals=0),
    )(*ins)


def call_upper_half(x0, cot, w_in, w_out):
    tokens, width = x0.shape
    inner = w_in.shape[2]
    group, slice_ = 4 * tokens, inner // 4
    w1 = (4, 4, 2, width // 32, slice_)
    w2 = (4, 4, 2, inner // 128, width)
    block = sds((tokens, width), BF16)
    acts = (group, slice_)
    ut, st = (width, group), (slice_, group)
    pair = lambda shape: sds((2,) + shape, BF16)
    outs = [block, sds((tokens, width), F32), block, sds((group, width), F32), sds(acts, BF16),
            pair(ut), pair(st), pair(ut), pair(st), pair((group, slice_ // 2)), pair((4, tokens, width // 2)),
            sds(w1, BF16), sds(w2, BF16)]
    tok = (4, tokens, width)
    scratch = [VMEM(shape, BF16) for shape in (w1, w2, w1, w2, tok, tok, acts, acts, acts, ut, st)]
    scratch += [VMEM((group, width), F32), VMEM((6, tokens, width // 2), F32)]
    return call(upper_half, (x0, cot, w_in, w_out), 'vvhh', outs, 'vvv' + 'h' * 10, scratch, (UPPER, 18), 2, 1,
                16 * group * width * slice_)


class GradReduce:
    def __init__(self, comm, axes, operands, column, sends, landing1, landing2, result, credits, before=None):
        self.comm, self.axes, self.operands, self.column = comm, axes, operands, column
        self.sends, self.landing1, self.landing2, self.result = sends, landing1, landing2, result
        self.credits, self.before = credits, before
        self.ring = RingReduce(comm, axes[0], None, landing1, before and before.ring)
        rows = sends.shape[1] // 2
        half = sends.shape[2] // 2
        self.block = lambda pos, h: sends.at[pos // 2, pl.ds(pl.multiple_of((pos % 2) * rows, rows), rows),
                                             pl.ds(h * half, half)]
        self.ring2 = RingReduce(comm, axes[1], self.block, landing2, before and before.ring2)

    def products(self, count, where, store):
        rows, width = self.sends.shape[1:]
        t = min(128, rows)
        per = rows // t

        def step(n, _):
            i, j = n // per, n % per
            pos, half = where(i)
            start = pl.multiple_of((pos * 2 + half) * rows + j * t, t)
            value = None
            for at, b in self.operands:
                term = dot(at[pl.ds(start, t)], b(pl.ds(self.column, width)))
                value = term if value is None else value + term
            store(i, pl.ds(pl.multiple_of(j * t, t), t), value)
            return 0

        lax.fori_loop(0, count * per, step, 0)

    def start(self):
        me, sends = self.ring.me, self.sends
        if self.before:
            self.before.sent()
            self.comm.wait(self.credits.at[0], self.axes[0])

        def where(i):
            return (me + jnp.where(i < 2, 2, 2 * i - 3)) % 4, ((i + 1) // 2) % 2

        def store(i, rows, value):
            sends[i, rows] = value

        self.products(4, where, store)
        self.ring.start(*[sends.at[k] for k in range(4)])

    def middle(self):
        me, landing = self.ring.me, self.landing1
        self.ring.wait_right()
        self.ring.wait_left()

        def store(i, rows, value):
            landing[3 * i, rows] = landing[3 * i, rows] + value

        self.products(2, lambda i: ((me + 1 + 2 * i) % 4, i), store)
        self.ring.pass_right()
        self.ring.pass_left()

    def turn(self):
        me, landing, sends = self.ring.me, self.landing1, self.sends
        self.ring.finish()
        self.ring.first.wait()

        def store(i, rows, value):
            sends[i, rows] = value + landing[2 - i, rows] + landing[4 + i, rows]

        self.products(2, lambda i: (me, i), store)
        if self.before:
            self.comm.wait(self.credits.at[1], self.axes[1])
        self.ring2.start_all()

    def free1(self):
        self.ring.sent()
        self.comm.signal(self.credits.at[0], self.axes[0])

    def middle2(self):
        self.ring2.middle_right()
        self.ring2.middle_left()

    def finish(self):
        self.ring2.finish()
        w = self.sends.shape[2] // 2
        self.result[:, 0:w], self.result[:, w:2 * w] = self.ring2.sums()

    def sent(self):
        self.ring2.sent()

    def free2(self):
        self.sent()
        self.comm.signal(self.credits.at[1], self.axes[1])


CHUNKS = 4


def grad_buffers(width, slice_):
    out = []
    for rows, cols in ((width // 8, slice_ // 2), (slice_ // 8, width // 2)):
        w = cols // CHUNKS
        out += [VMEM((CHUNKS, 4, rows, w), F32), VMEM((CHUNKS, 6, rows, w), F32),
                VMEM((CHUNKS, 6, rows // 2, w // 2), F32)]
    return out


def result_shapes(width, slice_):
    return [(CHUNKS, width // 16, slice_ // 2 // CHUNKS), (CHUNKS, slice_ // 16, width // 2 // CHUNKS)]


def grad_chunks(comm, operands, bufs, results, credits, before=None):
    out = []
    for k in range(CHUNKS):
        both = []
        for i, axes in enumerate(('zy', 'yz')):
            sends, land1, land2 = bufs[3 * i:3 * i + 3]
            both.append(GradReduce(comm, axes, operands[i], k * sends.shape[3], sends.at[k], land1.at[k], land2.at[k],
                                   results[i].at[k], credits.at[2 * k + i],
                                   before[k].things[i] if before else None))
        out.append(Every(both))
    return out


class BlockGather:
    def __init__(self, comm, own, out):
        self.comm, self.own, self.out = comm, own, out
        c = comm.c
        n = own.shape[0] // 2
        half = lambda h: pl.ds(h * n, n)
        self.ring = RingGather(comm, 'x', lambda h: own.at[half(h)], lambda p, h: out.at[p, c, half(h)],
                               own, out.at[pl.ds(0, 3), c])
        self.four = out.at[:, c]
        self.group, self.sem = Sends(comm, self.four), comm.recv_sem()

    def push(self, pos, src):
        c = self.comm
        c.send(src, self.out.at[pos, c.c], c.partner, self.group, self.sem)

    def start(self):
        self.ring.start()
        self.push(self.ring.me, self.own)
        self.kept = self.comm.local((self.own, self.out.at[self.ring.me, self.comm.c]))

    def forward(self):
        self.ring.forward()

    def near(self):
        ring, c = self.ring, self.comm.c
        ring.near()
        self.push(ring.left, self.out.at[ring.left, c])
        self.push(ring.right, self.out.at[ring.right, c])

    def finish(self):
        ring, c = self.ring, self.comm.c
        ring.finish()
        self.push(ring.far, self.out.at[ring.far, c])

    def arrived(self):
        self.comm.wait_recv(self.four, self.sem)
        done(self.kept)


def lower_half(x0, x1, e1, d0, part_hbm, w1_hbm, w2_hbm, a_hbm, ut_low, st_low, ut_top, st_top, q_top, d_top,
               grad, x2, q_low, d_low, top_all_in, top_all_out, low_all_in, low_all_out,
               w, df, a, q, part, landing, gut, gst, gq, gd, top_in, top_out, low_in, low_out, *rest):
    bufs, (send_sems, recv_sems, local_sems, credits, x_free) = rest[:6], rest[6:]
    comm = Comm(send_sems, recv_sems, local_sems)
    tokens = x0.shape[0]
    x, c = comm.x, comm.c
    group = a.shape[0]
    load_d = comm.local((d0, df.at[x]))
    loads = comm.local((ut_top, gut), (q_top, gq), (st_top, gst), (d_top, gd))
    columns = lambda ref, j: ref.at[:, pl.ds(j * group, group)]
    load_w = lambda ref: comm.local(*[(columns(ref, j), w.at[j]) for j in range(4)])
    load2 = load_w(w2_hbm) + comm.local((a_hbm, a))
    comm.barrier('xyzc')

    gather_d = ring_of_tokens(comm, df)
    done(load_d)
    gather_d.start()
    done(loads)
    own_b = lambda ref: lambda cols: flat(ref[..., cols])
    top = [[(gut.at[k], own_b(gq.at[k])) for k in (0, 1)], [(gst.at[k], own_b(gd.at[k])) for k in (0, 1)]]
    upper = grad_chunks(comm, top, bufs, (top_in, top_out), credits)
    t0, t1, t2, t3 = upper

    def by_columns(left):
        rows = w.shape[1] // 8

        def product(i):
            value = None
            for j in range(4):
                term = dot_bt(flat(left[..., j * group:(j + 1) * group]),
                              w[j, pl.ds(pl.multiple_of(i * rows, rows), rows)])
                value = term if value is None else value + term
            return value

        return product

    t0.start()
    t1.start()
    t2.start()
    gather_d.forward()
    t0.middle()
    gather_d.near()
    gather_d.finish()
    done(load2)
    backward_acts(df, by_columns(df), a, q)
    load1 = load_w(w1_hbm)
    _, d_arrived = comm.push(last_dim_half(df, 1 - c), d_low)
    _, q_arrived = comm.push(last_dim_half(q, 1 - c), q_low)
    done(load1)
    ring = token_sums(comm, part, landing, tokens)
    product = by_columns(q)
    backward_part(product, part, 0)
    ring.start_half(0)
    backward_part(product, part, 1)
    ring.start_half(1)
    d_arrived()
    q_arrived()
    half = a.shape[1] // 2
    loads = comm.local(*[(ut_low.at[k], w.at[k]) for k in (0, 1)], *[(st_low.at[k], w.at[2 + k]) for k in (0, 1)],
                       (q_low, a.at[:, pl.ds(0, half)]))
    loads += comm.local(*[(d_low.at[k], a.at[pl.ds(k * tokens, tokens), pl.ds(half, half)]) for k in range(4)])
    t1.middle()
    t3.start()
    t0.turn()
    t2.middle()
    ring.middle_right()
    t1.turn()
    t3.middle()
    ring.middle_left()
    t0.middle2()
    t2.turn()
    ring.finish()
    g = jnp.concatenate(ring.sums(), axis=1)
    grad[...] = (e1[...] + norm_rows_vjp(x0[...].astype(F32), g)).astype(BF16)
    ring.sent()
    comm.signal(x_free, 'x')
    load_part = comm.local((part_hbm, part))
    t1.middle2()
    t0.free1()
    t1.free1()
    comm.wait(x_free, 'x')
    done(load_part)
    ring = token_sums(comm, part, landing, tokens)
    ring.start_all()
    t3.turn()
    t0.finish()
    t0.free2()
    t2.middle2()
    done(loads)
    mine = lambda ref: lambda cols: flat(ref[..., pl.ds(pl.multiple_of(c * half + cols.start, cols.size), cols.size)])
    other = lambda first: lambda cols: a[:, pl.ds(first + cols.start, cols.size)]
    low = [[(w.at[0], mine(q)), (w.at[1], other(0))], [(w.at[2], mine(df)), (w.at[3], other(half))]]
    g0, g1, g2, g3 = grad_chunks(comm, low, bufs, (low_in, low_out), credits, upper)
    g0.start()
    t1.finish()
    t1.free2()
    t2.free1()
    t3.middle2()
    t2.finish()
    t2.free2()
    t3.free1()
    ring.middle_right()
    ring.middle_left()
    g0.middle()
    g1.start()
    t3.finish()
    t3.free2()
    top = Every([BlockGather(comm, top_in, top_all_in), BlockGather(comm, top_out, top_all_out)])
    low = [Every([BlockGather(comm, low_in.at[k], low_all_in.at[k]), BlockGather(comm, low_out.at[k], low_all_out.at[k])])
           for k in range(CHUNKS)]
    low0, low1, low2, low3 = low
    top.start()
    g0.turn()
    g1.middle()
    ring.finish()
    x2[...] = (x1[...].astype(F32) + jnp.concatenate(ring.sums(), axis=1)).astype(BF16)
    g0.middle2()
    g2.start()
    g1.turn()
    g0.finish()
    top.forward()
    low0.start()
    g2.middle()
    top.near()
    g1.middle2()
    g3.start()
    g2.turn()
    g1.finish()
    low1.start()
    top.finish()
    low0.forward()
    low0.near()
    g3.middle()
    low1.forward()
    low1.near()
    low0.finish()
    g2.middle2()
    low1.finish()
    g3.turn()
    g2.finish()
    low2.start()
    g3.middle2()
    low2.forward()
    g3.finish()
    low3.start()
    low2.near()
    low2.finish()
    low3.forward()
    low3.near()
    low3.finish()
    for pair in [top] + low:
        pair.arrived()
    comm.end()


def call_lower_half(x0, x1, e1, d0, part_hbm, w1_hbm, w2_hbm, a_hbm, ut_low, st_low, ut_top, st_top, q_top, d_top):
    tokens, width = x0.shape
    group, slice_ = a_hbm.shape
    shapes = result_shapes(width, slice_)
    tops = [(4, 2) + shape for shape in shapes]
    lows = [(CHUNKS, 4, 2) + shape[1:] for shape in shapes]
    block = sds((tokens, width), BF16)
    outs = [block, block, sds(q_top.shape[1:], BF16), sds(d_top.shape[1:], BF16)] + [sds(s, F32) for s in tops + lows]
    acts = VMEM((group, slice_), BF16)
    scratch = [VMEM((4, width, group), BF16), VMEM((4, tokens, width), BF16), acts, acts, VMEM((group, width), F32),
               VMEM((6, tokens, width // 2), F32)]
    scratch += [VMEM(r.shape, BF16) for r in (ut_top, st_top, q_top, d_top)] + [VMEM(s, F32) for s in shapes + shapes]
    scratch += grad_buffers(width, slice_)
    ins = (x0, x1, e1, d0, part_hbm, w1_hbm.reshape(width, slice_), w2_hbm.reshape(slice_, width), a_hbm,
           ut_low, st_low, ut_top, st_top, q_top, d_top)
    return pl.pallas_call(
        lower_half,
        name='lower_half',
        out_shape=tuple(outs),
        in_specs=spaces('vvv' + 'h' * 11),
        out_specs=tuple(spaces('vv' + 'h' * 6)),
        scratch_shapes=scratch + [sems(LOWER[0]), sems(LOWER[1]), sems(LOWER[2]), pltpu.SemaphoreType.REGULAR((2 * CHUNKS, 2)),
                                  pltpu.SemaphoreType.REGULAR],
        compiler_params=pltpu.CompilerParams(collective_id=2, has_side_effects=True, vmem_limit_bytes=VMEM_BYTES),
        cost_estimate=pl.CostEstimate(flops=16 * group * width * slice_, bytes_accessed=1 << 24, transcendentals=0),
    )(*ins)


def assemble(top_in, top_out, low_in, low_out, grad_in, grad_out, v_top_in, v_top_out, v_low_in, v_low_out,
             load_sems, store_sems):
    loads = []
    refs = (v_low_in, v_low_out, v_top_in, v_top_out)
    for i, src in enumerate((low_in, low_out, top_in, top_out)):
        copy = pltpu.make_async_copy(src, refs[i], load_sems.at[i])
        copy.start()
        loads.append(copy)
    strip = grad_in.shape[2] // 64
    rows, width = low_in.shape[3:]
    width_out = low_out.shape[4]
    per = width // strip
    for i, ref in enumerate(refs):
        loads[i].wait()
        layer = i // 2
        for k in range(CHUNKS):
            for x in range(4):
                for c in range(2):
                    src = ref.at[x, c, k] if layer else ref.at[k, x, c]
                    if i % 2:
                        dst = grad_out.at[layer, pl.ds(x * src.shape[0], src.shape[0]),
                                          pl.ds((c * CHUNKS + k) * width_out, width_out)]
                        pltpu.make_async_copy(src, dst, store_sems.at[1]).start()
                        continue
                    for j in range(per):
                        y, z = (c * 8 + k * per + j) // 4, (k * per + j) % 4
                        dst = grad_in.at[layer, :, pl.ds(((4 * z + y) * 4 + x) * strip, strip)]
                        pltpu.make_async_copy(src.at[:, pl.ds(j * strip, strip)], dst, store_sems.at[0]).start()
    pltpu.make_async_copy(grad_in, grad_in, store_sems.at[0]).wait()
    pltpu.make_async_copy(grad_out, grad_out, store_sems.at[1]).wait()


def call_assemble(ins, in_shape, out_shape):
    return pl.pallas_call(
        assemble,
        name='assemble',
        out_shape=(sds(in_shape, F32), sds(out_shape, F32)),
        in_specs=spaces('hhhh'),
        out_specs=tuple(spaces('hh')),
        scratch_shapes=[VMEM(r.shape, F32) for r in ins] + [sems(4), sems(2)],
        compiler_params=pltpu.CompilerParams(vmem_limit_bytes=VMEM_BYTES),
        cost_estimate=pl.CostEstimate(flops=1 << 30, bytes_accessed=1 << 25, transcendentals=0),
    )(*ins)


def solution(mesh):
    tok_spec = P(('local', 'data'), None)
    w_spec = P(None, 'local', None)

    def device_step(tokens, cotangent, w_in, w_out):
        (x1, e1, d0, part_out, a_low, ut_low, st_low, ut_top, st_top, q_top, d_top, w1_low, w2_low) = call_upper_half(
            tokens, cotangent, w_in, w_out)
        grad, x2, _, _, *gathered = call_lower_half(
            tokens, x1, e1, d0, part_out, w1_low, w2_low, a_low, ut_low, st_low, ut_top, st_top, q_top, d_top)
        grad_in, grad_out = call_assemble(gathered, w_in.shape, w_out.shape)
        return x2, grad_in, grad_out, grad

    return jax.shard_map(device_step, mesh=mesh, in_specs=(tok_spec, tok_spec, w_spec, w_spec),
                         out_specs=(tok_spec, w_spec, w_spec, tok_spec), check_vma=False)
```

```python
import functools

import jax
import jax.numpy as jnp
from jax import lax
from jax.experimental import pallas as pl
from jax.experimental.pallas import tpu as pltpu
from jax.sharding import PartitionSpec as P

EPSILON = 1e-6
GELU_SCALE = 0.7978845608028654
GELU_CUBE = 0.044715
BF16 = jnp.bfloat16
F32 = jnp.float32
MESH = pl.DeviceIdType.MESH
HBM = pltpu.HBM
VMEM = pltpu.VMEM
VMEM_BYTES = 67043328
UPPER = (40, 95)
LOWER = (69, 116, 41)


class Comm:
    def __init__(self, send_sems, recv_sems, local_sems):
        l = lax.axis_index('local')
        d = lax.axis_index('data')
        self.l, self.d = l, d
        self.z, self.y, self.x, self.c = l // 4, l % 4, d // 2, d % 2
        self.send_sems, self.recv_sems, self.local_sems = send_sems, recv_sems, local_sems
        self.sends = self.recvs = self.local_count = 0
        self.groups = []
        self.partner = (l, self.x * 2 + 1 - self.c)

    def pos(self, axis):
        return {'x': self.x, 'y': self.y, 'z': self.z}[axis]

    def neighbor(self, axis, delta):
        p = (self.pos(axis) + delta) % 4
        if axis == 'x':
            return (self.l, p * 2 + self.c)
        if axis == 'y':
            return (self.z * 4 + p, self.d)
        return (p * 4 + self.y, self.d)

    def peers(self, axes):
        out = [self.partner] if 'c' in axes else []
        for axis in axes.replace('c', ''):
            out += [self.neighbor(axis, 1), self.neighbor(axis, 3)]
        return out

    def signal(self, sem, axes):
        for device in self.peers(axes):
            pl.semaphore_signal(sem, inc=1, device_id=device, device_id_type=MESH)

    def wait(self, sem, axes):
        pl.semaphore_wait(sem, len(self.peers(axes)))

    def arrive(self, axes):
        self.signal(pltpu.get_barrier_semaphore(), axes)

    def meet(self, axes):
        self.wait(pltpu.get_barrier_semaphore(), axes)

    def send_sem(self):
        self.sends += 1
        return self.send_sems.at[self.sends - 1]

    def recv_sem(self):
        self.recvs += 1
        return self.recv_sems.at[self.recvs - 1]

    def copy(self, src, dst, device, send_sem, recv_sem):
        return pltpu.make_async_remote_copy(src_ref=src, dst_ref=dst, send_sem=send_sem, recv_sem=recv_sem,
                                            device_id=device, device_id_type=MESH)

    def send(self, src, dst, device, group, recv_sem):
        self.copy(src, dst, device, group.sem, recv_sem).start()

    def wait_recv(self, ref, recv_sem):
        self.copy(ref, ref, self.partner, self.send_sems.at[0], recv_sem).wait_recv()

    def push(self, src, dst):
        group, recv_sem = Sends(self, src), self.recv_sem()
        self.send(src, dst, self.partner, group, recv_sem)
        return group, lambda: self.wait_recv(dst, recv_sem)

    def local(self, *pairs):
        out = []
        for src, dst in pairs:
            copy = pltpu.make_async_copy(src, dst, self.local_sems.at[self.local_count])
            copy.start()
            self.local_count += 1
            out.append(copy)
        return out

    def end(self):
        for group in self.groups:
            group.wait()


class Sends:
    def __init__(self, comm, ref, sem=None):
        self.comm, self.ref, self.sem = comm, ref, sem or comm.send_sem()
        self.waited = False
        comm.groups.append(self)

    def wait(self):
        if not self.waited:
            self.waited = True
            c = self.comm
            c.copy(self.ref, self.ref, c.partner, self.sem, c.recv_sems.at[0]).wait_send()


def done(copies):
    for copy in copies:
        copy.wait()


class Every:
    def __init__(self, things):
        self.things = things

    def __getattr__(self, step):
        def run(*args):
            for thing in self.things:
                getattr(thing, step)(*args)
        return run


class RingGather:
    def __init__(self, comm, axis, own, slot, block, three, before=None):
        self.comm, self.own, self.slot, self.block = comm, own, slot, block
        self.me = comm.pos(axis)
        self.right, self.far, self.left = [(self.me + k) % 4 for k in (1, 2, 3)]
        self.to_right, self.to_left = comm.neighbor(axis, 1), comm.neighbor(axis, 3)
        self.group = Sends(comm, three, before and before.group.sem)
        self.sems = before.sems if before else [comm.recv_sem() for _ in range(3)]

    def both(self, k, right, right_slot, left, left_slot):
        self.comm.send(right, right_slot, self.to_right, self.group, self.sems[k])
        self.comm.send(left, left_slot, self.to_left, self.group, self.sems[k])

    def start(self):
        own, slot, me = self.own, self.slot, self.me
        self.both(0, own(0), slot(me, 0), own(1), slot(me, 1))
        self.both(1, own(1), slot(me, 1), own(0), slot(me, 0))

    def forward(self):
        self.comm.wait_recv(self.block, self.sems[0])
        right, left = self.slot(self.left, 0), self.slot(self.right, 1)
        self.both(2, right, right, left, left)

    def near(self):
        self.comm.wait_recv(self.block, self.sems[1])

    def finish(self):
        self.comm.wait_recv(self.block, self.sems[2])

    def sent(self):
        self.group.wait()


class RingReduce:
    def __init__(self, comm, axis, part, landing, before=None):
        self.comm, self.part, self.landing = comm, part, landing
        self.me = comm.pos(axis)
        self.right, self.far, self.left = [(self.me + k) % 4 for k in (1, 2, 3)]
        self.to_right, self.to_left = comm.neighbor(axis, 1), comm.neighbor(axis, 3)
        self.first = Sends(comm, landing.at[pl.ds(0, 2)], before and before.first.sem)
        self.rest = Sends(comm, landing.at[pl.ds(0, 4)], before and before.rest.sem)
        self.sems = before.sems if before else [comm.recv_sem() for _ in range(3)]

    def right_to(self, k, src, group, sem):
        self.comm.send(src, self.landing.at[k], self.to_right, group, sem)

    def left_to(self, k, src, group, sem):
        self.comm.send(src, self.landing.at[k], self.to_left, group, sem)

    def start(self, far0, far1, right1, left0):
        self.right_to(0, far0, self.first, self.sems[0])
        self.left_to(3, far1, self.first, self.sems[1])
        self.right_to(1, right1, self.rest, self.sems[2])
        self.left_to(4, left0, self.rest, self.sems[2])

    def start_all(self):
        part = self.part
        self.start(part(self.far, 0), part(self.far, 1), part(self.right, 1), part(self.left, 0))

    def start_half(self, half):
        if half == 0:
            self.right_to(0, self.part(self.far, 0), self.first, self.sems[0])
            self.left_to(4, self.part(self.left, 0), self.rest, self.sems[2])
        else:
            self.left_to(3, self.part(self.far, 1), self.first, self.sems[1])
            self.right_to(1, self.part(self.right, 1), self.rest, self.sems[2])

    def wait_right(self):
        self.comm.wait_recv(self.landing.at[0], self.sems[0])

    def wait_left(self):
        self.comm.wait_recv(self.landing.at[3], self.sems[1])

    def pass_right(self):
        self.right_to(2, self.landing.at[0], self.rest, self.sems[2])

    def pass_left(self):
        self.left_to(5, self.landing.at[3], self.rest, self.sems[2])

    def middle_right(self):
        landing = self.landing
        self.wait_right()
        landing[0] = landing[0] + self.part(self.right, 0)[...]
        self.pass_right()

    def middle_left(self):
        landing = self.landing
        self.wait_left()
        landing[3] = landing[3] + self.part(self.left, 1)[...]
        self.pass_left()

    def finish(self):
        self.comm.wait_recv(self.landing.at[pl.ds(0, 4)], self.sems[2])

    def sent(self):
        self.first.wait()
        self.rest.wait()

    def sums(self):
        landing = self.landing
        return (self.part(self.me, 0)[...] + landing[2] + landing[4],
                self.part(self.me, 1)[...] + landing[1] + landing[5])


class PlaneGather:
    def __init__(self, comm, dims, first, full, cols, before=None):
        self.comm = comm
        c = comm.c
        lead = dims[0] == first
        second = dims.replace(first, '')
        b = comm.pos(second)
        half_rows = full.shape[3] // 2
        rows = lambda h: pl.ds(h * half_rows, half_rows)
        pair = lambda h: pl.ds(2 * h, 2)
        self.b = b
        every, three, own = slice(None), pl.ds(0, 3), comm.pos(first)
        at = lambda p, q, r: full.at[(p, q, c, r, cols) if lead else (q, p, c, r, cols)]
        slot1 = lambda p, h: at(p, b, rows(h))
        slot2 = lambda p, h: at(pair(h), p, every)
        self.ring1 = RingGather(comm, first, lambda h: slot1(own, h), slot1, at(own, b, every), at(three, b, every),
                                before and before.ring1)
        self.ring2 = RingGather(comm, second, lambda h: slot2(b, h), slot2, at(every, b, every), at(every, three, every),
                                before and before.ring2)
        self.line = lambda p: at(every, p, every)
        self.both_cores = lambda p, ref: ref.at[(every, p, every, every, cols) if lead else (p, every, every, every, cols)]
        self.whole, self.near_lines = at(every, every, every), at(every, three, every)
        self.group = Sends(comm, self.whole, before and before.group.sem)
        self.sems = before.sems if before else [comm.recv_sem(), comm.recv_sem()]
        self.full = full

    def push(self, p, k=0):
        self.comm.send(self.line(p), self.line(p), self.comm.partner, self.group, self.sems[k])

    def start1(self):
        self.ring1.start()

    def forward1(self):
        self.ring1.forward()

    def start2(self):
        self.ring1.near()
        self.ring1.finish()
        self.ring2.start()
        self.push(self.b)

    def forward2(self):
        self.ring2.forward()

    def near2(self):
        self.ring2.near()
        self.push(self.ring2.left)
        self.push(self.ring2.right)

    def finish2(self):
        self.ring2.finish()
        self.push(self.ring2.far, 1)

    def arrived_near(self):
        self.comm.wait_recv(self.near_lines, self.sems[0])

    def arrived_far(self):
        self.comm.wait_recv(self.line(self.b), self.sems[1])

    def arrived(self):
        self.arrived_near()
        self.arrived_far()

    def copy_out(self, out, positions, kept):
        both = self.both_cores
        kept += self.comm.local(*[(both(p, self.full), both(p, out)) for p in positions])

    def near_out(self, out, kept):
        self.arrived_near()
        self.copy_out(out, (self.b, self.ring2.left, self.ring2.right), kept)

    def far_out(self, out, kept):
        self.arrived_far()
        self.copy_out(out, (self.ring2.far,), kept)

    def sent(self):
        self.ring1.sent()
        self.ring2.sent()
        self.group.wait()


def gathers(comm, dims, full, pieces, before=None):
    width = full.shape[4] // pieces
    out = [PlaneGather(comm, dims, dims[k % 2], full, pl.ds(k * width, width), before and before.things[k])
           for k in range(pieces)]
    return [Every(out[k:k + 2]) for k in range(0, pieces, 2)]


def own_blocks(comm, w_in, w_out, layer, w1, w2):
    z, y, x, c = comm.z, comm.y, comm.x, comm.c
    width = w_in.shape[2] // 64
    rows1, rows2 = w1.shape[3], w2.shape[3]
    own = w1.at[z, y, c]
    k = comm.local_count
    comm.local_count += 1
    for j in range(16):
        start = (4 * (j % 4) + j // 4) * 4 * width + x * width
        pltpu.make_async_copy(w_in.at[layer, pl.ds(c * rows1, rows1), pl.ds(pl.multiple_of(start, width), width)],
                              own.at[:, pl.ds(j * width, width)], comm.local_sems.at[k]).start()
    start = (x * 2 + c) * rows2
    copies = comm.local((w_out.at[layer, pl.ds(pl.multiple_of(start, rows2), rows2)], w2.at[y, z, c]))
    return [pltpu.make_async_copy(own, own, comm.local_sems.at[k])] + copies


def ring_of_tokens(comm, full, before=None):
    n = full.shape[1] // 2
    slot = lambda p, h: full.at[p, pl.ds(h * n, n)]
    return RingGather(comm, 'x', lambda h: slot(comm.x, h), slot, full.at[0], full.at[pl.ds(0, 3)], before)


def token_sums(comm, part, landing, tokens, before=None):
    width = part.shape[1] // 2
    block = lambda pos, half: part.at[pl.ds(pl.multiple_of(pos * tokens, tokens), tokens), pl.ds(half * width, width)]
    return RingReduce(comm, 'x', block, landing, before)


def norm_rows(x):
    return x * lax.rsqrt(jnp.mean(x * x, axis=-1, keepdims=True) + EPSILON)


def norm_rows_vjp(x, g):
    r = lax.rsqrt(jnp.mean(x * x, axis=-1, keepdims=True) + EPSILON)
    dot = jnp.mean(x * g, axis=-1, keepdims=True)
    return r * g - x * (r * r * r * dot)


def gelu(x):
    t = jnp.tanh(GELU_SCALE * (x + GELU_CUBE * (x * x * x)))
    return x * (0.5 * (1.0 + t))


def gelu_grad(x):
    x2 = x * x
    t = jnp.tanh(GELU_SCALE * (x + GELU_CUBE * (x2 * x)))
    return 0.5 * (1.0 + t) + (0.5 * x) * (1.0 - t * t) * (GELU_SCALE * (1.0 + (3.0 * GELU_CUBE) * x2))


def dot(a, b):
    return lax.dot_general(a, b, (((1,), (0,)), ((), ())), preferred_element_type=F32)


def dot_bt(a, b):
    return lax.dot_general(a, b, (((1,), (1,)), ((), ())), preferred_element_type=F32)


def flat(value):
    return value.reshape(-1, value.shape[-1])


def tiles(n, step, tile=256):
    t = min(tile, n)

    def run(i, _):
        step(pl.ds(pl.multiple_of(i * t, t), t))
        return 0

    lax.fori_loop(0, n // t, run, 0)


def forward_acts(u, w1, a, s, st):
    def step(cols):
        acc = dot(flat(u[...]), flat(w1[:, :, :, :, cols])).astype(BF16)
        a[:, cols] = acc
        value = gelu(acc.astype(F32)).astype(BF16)
        s[:, cols] = value
        st[cols, :] = value.T

    tiles(a.shape[1], step)


def transposed(u, ut):
    def step(cols):
        ut[cols, :] = flat(u[:, :, cols]).T

    tiles(ut.shape[0], step)


def forward_part(s, w2, part, half):
    width = part.shape[1] // 2
    t = min(256, width)

    def run(i, _):
        cols = pl.ds(pl.multiple_of(half * width + i * t, t), t)
        part[:, cols] = dot(s[...], flat(w2[:, :, :, :, cols]))
        return 0

    lax.fori_loop(0, width // t, run, 0)


def row_tile(w, i):
    return flat(w[i // 2, pl.ds((i % 2) * 2, 2)])


def backward_acts(d, tile_product, a, q):
    rows = a.shape[1] // 8

    def step(i, _):
        cols = pl.ds(pl.multiple_of(i * rows, rows), rows)
        q[:, cols] = (tile_product(i) * gelu_grad(a[:, cols].astype(F32))).astype(BF16)
        return 0

    lax.fori_loop(0, 8, step, 0)


def backward_part(tile_product, part, half):
    rows = part.shape[1] // 8

    def step(j, _):
        i = half * 4 + j
        part[:, pl.ds(pl.multiple_of(i * rows, rows), rows)] = tile_product(i)
        return 0

    lax.fori_loop(0, 4, step, 0)


def last_dim_half(ref, k):
    width = ref.shape[-1] // 2
    return ref.at[..., pl.ds(pl.multiple_of(k * width, width), width)]


def upper_half(x0, cot, w_in, w_out,
               x1_out, e1_out, d0_out, part_out, a_low, ut_low, st_low, ut_top, st_top, q_top, d_top, w1_low, w2_low,
               p1, p2, q1, q2, uf, df, a, s, q, ut, st, x1, d0, part, landing, e1,
               send_sems, recv_sems, local_sems, credits):
    comm = Comm(send_sems, recv_sems, local_sems)
    tokens = x0.shape[0]
    x, c = comm.x, comm.c
    p_free, q_free = credits.at[0], credits.at[1]

    own0 = own_blocks(comm, w_in, w_out, 0, p1, p2)
    own1 = own_blocks(comm, w_in, w_out, 1, q1, q2)
    comm.arrive('xyzc')
    uf[x] = norm_rows(x0[...].astype(F32)).astype(BF16)
    df[x] = cot[...]
    comm.meet('xyzc')

    gather_u = ring_of_tokens(comm, uf)
    gather_d = ring_of_tokens(comm, df)
    g1, = gathers(comm, 'zy', p1, 2)
    g2, g3 = gathers(comm, 'yz', p2, 4)
    n1, = gathers(comm, 'zy', q1, 2)
    n2, = gathers(comm, 'yz', q2, 2)
    done(own0)
    g2.start1()
    gather_u.start()
    gather_d.start()
    done(own1)
    g1.start1()
    g2.forward1()
    g3.start1()
    g1.forward1()
    g2.start2()
    gather_u.forward()
    g3.forward1()
    g1.start2()
    gather_u.near()
    gather_d.forward()
    g1.forward2()
    g2.forward2()
    n1.start1()
    g3.start2()
    n2.start1()
    g2.near2()
    gather_d.near()
    g1.near2()
    g1.finish2()
    gather_u.finish()
    transposed(uf, ut)
    pushed = [comm.push(ut, ut_low.at[1])]
    kept = comm.local((ut, ut_low.at[0]))
    gather_d.finish()
    g2.finish2()
    g1.arrived()
    forward_acts(uf, p1, a, s, st)
    g2.arrived()
    n1.forward1()
    g3.forward2()
    gather_u.sent()
    ring = token_sums(comm, part, landing, tokens)
    forward_part(s, p2, part, 0)
    ring.start_half(0)
    g3.near2()
    pushed += [comm.push(st, st_low.at[1])]
    kept += comm.local((st, st_low.at[0]), (a, a_low))
    pushed += [comm.push(last_dim_half(df, 1 - c), d_top.at[1])]
    kept_d = comm.local((last_dim_half(df, c), d_top.at[0]))
    n2.forward1()
    n1.start2()
    g3.finish2()
    g3.arrived()
    forward_part(s, p2, part, 1)
    ring.start_half(1)
    g1.sent()
    g2.sent()
    g3.sent()
    comm.signal(p_free, 'yzc')
    own2 = own_blocks(comm, w_in, w_out, 1, p1, p2)
    b1, = gathers(comm, 'zy', p1, 2, g1)
    b2, = gathers(comm, 'yz', p2, 2, g2)
    done(own2)
    comm.wait(p_free, 'yzc')
    b2.start1()
    n1.forward2()
    n2.start2()
    b1.start1()
    ring.middle_right()
    n1.near2()
    ring.middle_left()
    n1.finish2()
    b2.forward1()
    n2.forward2()
    n1.arrived()
    n2.near2()
    b1.forward1()
    ring.finish()
    x_next = (x0[...].astype(F32) + jnp.concatenate(ring.sums(), axis=1)).astype(BF16)
    x1[...] = x_next
    keep_x = comm.local((x1, x1_out))
    uf[x] = norm_rows(x_next.astype(F32)).astype(BF16)
    ring.sent()
    gather_v = ring_of_tokens(comm, uf, gather_u)
    gather_v.start()
    done(kept)
    pushed[0][0].wait()
    pushed[1][0].wait()
    b2.start2()
    n2.finish2()
    gather_v.forward()
    b2.forward2()
    gather_v.near()
    b1.start2()
    n2.arrived()
    b2.near2()
    gather_v.finish()
    forward_acts(uf, q1, a, s, st)
    b2.finish2()
    forward_part(s, q2, part, 0)
    forward_part(s, q2, part, 1)
    keep_part = comm.local((part, part_out))
    b1.forward2()
    n1.sent()
    n2.sent()
    comm.signal(q_free, 'yzc')
    own3 = own_blocks(comm, w_in, w_out, 0, q1, q2)
    l1, = gathers(comm, 'zy', q1, 2, n1)
    l2, = gathers(comm, 'yz', q2, 2, n2)
    b2.arrived()
    done(own3)
    comm.wait(q_free, 'yzc')
    l1.start1()
    b1.near2()
    backward_acts(df, lambda i: dot_bt(flat(df[...]), row_tile(p2, i)), a, q)
    b1.finish2()
    l1.forward1()
    transposed(uf, ut)
    pushed += [comm.push(ut, ut_top.at[1]), comm.push(st, st_top.at[1])]
    kept = kept_d + comm.local((ut, ut_top.at[0]), (st, st_top.at[0]))
    l2.start1()
    b1.arrived()
    done(keep_part)
    ring = token_sums(comm, part, landing, tokens, ring)
    product = lambda i: dot_bt(q[...], row_tile(p1, i))
    backward_part(product, part, 0)
    ring.start_half(0)
    l2.forward1()
    l1.start2()
    backward_part(product, part, 1)
    ring.start_half(1)
    pushed += [comm.push(last_dim_half(q, 1 - c), q_top.at[1])]
    kept += comm.local((last_dim_half(q, c), q_top.at[0]))
    l2.start2()
    l1.forward2()
    l1.near2()
    ring.middle_right()
    l1.near_out(w1_low, kept)
    l2.forward2()
    ring.middle_left()
    l2.near2()
    l1.finish2()
    l2.near_out(w2_low, kept)
    l1.far_out(w1_low, kept)
    l2.finish2()
    ring.finish()
    g = jnp.concatenate(ring.sums(), axis=1)
    e = cot[...].astype(F32) + norm_rows_vjp(x1[...].astype(F32), g)
    e1[...] = e
    d0[...] = e.astype(BF16)
    kept += keep_x + comm.local((e1, e1_out), (d0, d0_out))
    l2.far_out(w2_low, kept)
    for _, arrived in pushed:
        arrived()
    done(kept)
    comm.end()


def sds(shape, dtype):
    return jax.ShapeDtypeStruct(shape, dtype)


def sems(n):
    return pltpu.SemaphoreType.DMA((n,))


def spaces(kinds):
    return [pl.BlockSpec(memory_space=VMEM if k == 'v' else HBM) for k in kinds]


def call(kernel, ins, in_kinds, outs, out_kinds, scratch, copies, credits, collective_id, flops):
    return pl.pallas_call(
        kernel,
        name=kernel.__name__,
        out_shape=tuple(outs),
        in_specs=spaces(in_kinds),
        out_specs=tuple(spaces(out_kinds)),
        scratch_shapes=scratch + [sems(copies[0][0]), sems(copies[0][1]), sems(copies[1]),
                                  pltpu.SemaphoreType.REGULAR((credits,))],
        compiler_params=pltpu.CompilerParams(collective_id=collective_id, has_side_effects=True,
                                             vmem_limit_bytes=VMEM_BYTES),
        cost_estimate=pl.CostEstimate(flops=flops, bytes_accessed=1 << 24, transcendentals=0),
    )(*ins)


def call_upper_half(x0, cot, w_in, w_out):
    tokens, width = x0.shape
    inner = w_in.shape[2]
    group, slice_ = 4 * tokens, inner // 4
    w1 = (4, 4, 2, width // 32, slice_)
    w2 = (4, 4, 2, inner // 128, width)
    block = sds((tokens, width), BF16)
    acts = (group, slice_)
    ut, st = (width, group), (slice_, group)
    pair = lambda shape: sds((2,) + shape, BF16)
    outs = [block, sds((tokens, width), F32), block, sds((group, width), F32), sds(acts, BF16),
            pair(ut), pair(st), pair(ut), pair(st), pair((group, slice_ // 2)), pair((4, tokens, width // 2)),
            sds(w1, BF16), sds(w2, BF16)]
    tok = (4, tokens, width)
    scratch = [VMEM(shape, BF16) for shape in (w1, w2, w1, w2, tok, tok, acts, acts, acts, ut, st, block.shape,
                                            block.shape)]
    scratch += [VMEM((group, width), F32), VMEM((6, tokens, width // 2), F32), VMEM(block.shape, F32)]
    return call(upper_half, (x0, cot, w_in, w_out), 'vvhh', outs, 'h' * 13, scratch, (UPPER, 35), 2, 1,
                16 * group * width * slice_)


class GradReduce:
    def __init__(self, comm, axes, operands, column, sends, landing1, landing2, result, credits, before=None):
        self.comm, self.axes, self.operands, self.column = comm, axes, operands, column
        self.sends, self.landing1, self.landing2, self.result = sends, landing1, landing2, result
        self.credits, self.before = credits, before
        self.ring = RingReduce(comm, axes[0], None, landing1, before and before.ring)
        rows = sends.shape[1] // 4
        self.block = lambda pos, h: sends.at[pos // 2, pl.ds(pl.multiple_of(((pos % 2) * 2 + h) * rows, rows), rows)]
        self.ring2 = RingReduce(comm, axes[1], self.block, landing2, before and before.ring2)

    def products(self, count, where, store):
        rows, width = self.sends.shape[1:]
        t = min(128, rows)
        per = rows // t

        def step(n, _):
            i, j = n // per, n % per
            pos, half = where(i)
            start = pl.multiple_of((pos * 2 + half) * rows + j * t, t)
            value = None
            for at, b in self.operands:
                term = dot(at[pl.ds(start, t)], b(pl.ds(self.column, width)))
                value = term if value is None else value + term
            store(i, pl.ds(pl.multiple_of(j * t, t), t), value)
            return 0

        lax.fori_loop(0, count * per, step, 0)

    def start(self):
        me, sends = self.ring.me, self.sends
        if self.before:
            self.before.sent()
            self.comm.wait(self.credits.at[0], self.axes[0])

        def where(i):
            return (me + jnp.where(i < 2, 2, 2 * i - 3)) % 4, ((i + 1) // 2) % 2

        def store(i, rows, value):
            sends[i, rows] = value

        self.products(4, where, store)
        self.ring.start(*[sends.at[k] for k in range(4)])

    def middle(self):
        me, landing = self.ring.me, self.landing1
        self.ring.wait_right()
        self.ring.wait_left()

        def store(i, rows, value):
            landing[3 * i, rows] = landing[3 * i, rows] + value

        self.products(2, lambda i: ((me + 1 + 2 * i) % 4, i), store)
        self.ring.pass_right()
        self.ring.pass_left()

    def turn(self):
        me, landing, sends = self.ring.me, self.landing1, self.sends
        self.ring.finish()
        self.ring.first.wait()

        def store(i, rows, value):
            sends[i, rows] = value + landing[2 - i, rows] + landing[4 + i, rows]

        self.products(2, lambda i: (me, i), store)
        if self.before:
            self.comm.wait(self.credits.at[1], self.axes[1])
        self.ring2.start_all()

    def free1(self):
        self.ring.sent()
        self.comm.signal(self.credits.at[0], self.axes[0])

    def middle2(self):
        self.ring2.middle_right()
        self.ring2.middle_left()

    def finish(self):
        self.ring2.finish()
        n = self.result.shape[0] // 2
        self.result[0:n], self.result[n:2 * n] = self.ring2.sums()

    def sent(self):
        self.ring2.sent()

    def free2(self):
        self.sent()
        self.comm.signal(self.credits.at[1], self.axes[1])


CHUNKS = 4


def grad_buffers(width, slice_):
    out = []
    for rows, cols in ((width // 8, slice_ // 2), (slice_ // 8, width // 2)):
        w = cols // CHUNKS
        out += [VMEM((CHUNKS, 4, rows, w), F32), VMEM((CHUNKS, 6, rows, w), F32),
                VMEM((CHUNKS, 6, rows // 4, w), F32)]
    return out


def result_shapes(width, slice_):
    return [(CHUNKS, width // 16, slice_ // 2 // CHUNKS), (CHUNKS, slice_ // 16, width // 2 // CHUNKS)]


def grad_chunks(comm, operands, bufs, results, credits, before=None):
    out = []
    for k in range(CHUNKS):
        pieces = 2 if before and k == CHUNKS - 1 else 1
        for piece in range(pieces):
            both = []
            for i, axes in enumerate(('zy', 'yz')):
                width = bufs[3 * i].shape[3] // pieces
                cols = pl.ds(piece * width, width)
                sends, land1, land2 = [ref.at[k, :, :, cols] for ref in bufs[3 * i:3 * i + 3]]
                both.append(GradReduce(comm, axes, operands[i], (k * pieces + piece) * width, sends, land1, land2,
                                       results[i].at[k, :, cols], credits.at[2 * k + i],
                                       before[k].things[i] if before and piece == 0 else None))
            out.append(Every(both))
    return out


class BlockGather:
    def __init__(self, comm, own, out):
        self.comm, self.own, self.out = comm, own, out
        c = comm.c
        n = own.shape[0] // 2
        half = lambda h: pl.ds(h * n, n)
        self.ring = RingGather(comm, 'x', lambda h: own.at[half(h)], lambda p, h: out.at[p, c, half(h)],
                               own, out.at[pl.ds(0, 3), c])
        self.four = out.at[:, c]
        self.group, self.sem = Sends(comm, self.four), comm.recv_sem()

    def push(self, pos, src):
        c = self.comm
        c.send(src, self.out.at[pos, c.c], c.partner, self.group, self.sem)

    def start(self):
        self.ring.start()
        self.push(self.ring.me, self.own)
        self.kept = self.comm.local((self.own, self.out.at[self.ring.me, self.comm.c]))

    def forward(self):
        self.ring.forward()

    def near(self):
        ring, c = self.ring, self.comm.c
        ring.near()
        self.push(ring.left, self.out.at[ring.left, c])
        self.push(ring.right, self.out.at[ring.right, c])

    def finish(self):
        ring, c = self.ring, self.comm.c
        ring.finish()
        self.push(ring.far, self.out.at[ring.far, c])

    def arrived(self):
        self.comm.wait_recv(self.four, self.sem)
        done(self.kept)


def lower_half(x0_hbm, x1_hbm, e1_hbm, d0, part_hbm, w1_hbm, w2_hbm, a_hbm, ut_low, st_low, ut_top, st_top, q_top, d_top,
               grad_out, x2_out, q_low, d_low, top_all_in, top_all_out, low_all_in, low_all_out,
               w, df, a, q, x0, x1, grad, x2, e1, part, landing, gut, gst, gq, gd,
               top_in, top_out, low_in, low_out, *rest):
    bufs, (send_sems, recv_sems, local_sems, credits, x_free) = rest[:6], rest[6:]
    comm = Comm(send_sems, recv_sems, local_sems)
    tokens = x0.shape[0]
    x, c = comm.x, comm.c
    group = a.shape[0]
    load_d = comm.local((d0, df.at[x]))
    loads_in = comm.local((ut_top, gut), (q_top, gq))
    comm.arrive('xyzc')
    loads_out = comm.local((st_top, gst), (d_top, gd))
    columns = lambda ref, j: ref.at[:, pl.ds(j * group, group)]
    load_w = lambda ref: comm.local(*[(columns(ref, j), w.at[j]) for j in range(4)])
    comm.meet('xyzc')

    gather_d = ring_of_tokens(comm, df)
    done(load_d)
    gather_d.start()
    load2 = load_w(w2_hbm) + comm.local((a_hbm, a))
    load_x = comm.local((x0_hbm, x0), (e1_hbm, e1), (x1_hbm, x1))
    own_b = lambda ref: lambda cols: flat(ref[..., cols])
    top = [[(gut.at[k], own_b(gq.at[k])) for k in (0, 1)], [(gst.at[k], own_b(gd.at[k])) for k in (0, 1)]]
    upper = grad_chunks(comm, top, bufs, (top_in, top_out), credits)
    t0, t1, t2, t3 = upper

    def by_columns(left):
        rows = w.shape[1] // 8

        def product(i):
            value = None
            for j in range(4):
                term = dot_bt(flat(left[..., j * group:(j + 1) * group]),
                              w[j, pl.ds(pl.multiple_of(i * rows, rows), rows)])
                value = term if value is None else value + term
            return value

        return product

    done(loads_in)
    t0.things[0].start()
    done(loads_out)
    t0.things[1].start()
    top = Every([BlockGather(comm, top_in, top_all_in), BlockGather(comm, top_out, top_all_out)])
    w_in, w_out = low_in.shape[2] // 2, low_out.shape[2] // 2
    low = [(k, slice(None), slice(None)) for k in range(CHUNKS - 1)]
    low += [(CHUNKS - 1, pl.ds(h * w_in, w_in), pl.ds(h * w_out, w_out)) for h in (0, 1)]
    low = [Every([BlockGather(comm, low_in.at[k, :, i], low_all_in.at[k, :, :, :, i]),
                  BlockGather(comm, low_out.at[k, :, o], low_all_out.at[k, :, :, :, o])]) for k, i, o in low]
    low0, low1, low2, low3, low4 = low
    t1.start()
    gather_d.forward()
    t0.middle()
    gather_d.near()
    t2.start()
    gather_d.finish()
    done(load2)
    backward_acts(df, by_columns(df), a, q)
    load1 = load_w(w1_hbm)
    _, d_arrived = comm.push(last_dim_half(df, 1 - c), d_low)
    _, q_arrived = comm.push(last_dim_half(q, 1 - c), q_low)
    done(load1)
    ring = token_sums(comm, part, landing, tokens)
    product = by_columns(q)
    backward_part(product, part, 0)
    ring.start_half(0)
    backward_part(product, part, 1)
    ring.start_half(1)
    d_arrived()
    q_arrived()
    half = a.shape[1] // 2
    loads = comm.local(*[(ut_low.at[k], w.at[k]) for k in (0, 1)], *[(st_low.at[k], w.at[2 + k]) for k in (0, 1)],
                       (q_low, a.at[:, pl.ds(0, half)]))
    loads += comm.local(*[(d_low.at[k], a.at[pl.ds(k * tokens, tokens), pl.ds(half, half)]) for k in range(4)])
    done(loads)
    mine = lambda ref: lambda cols: flat(ref[..., pl.ds(pl.multiple_of(c * half + cols.start, cols.size), cols.size)])
    other = lambda first: lambda cols: a[:, pl.ds(first + cols.start, cols.size)]
    operands = [[(w.at[0], mine(q)), (w.at[1], other(0))], [(w.at[2], mine(df)), (w.at[3], other(half))]]
    g0, g1, g2, g3, g4 = grad_chunks(comm, operands, bufs, (low_in, low_out), credits, upper)
    t0.turn()
    t0.free1()
    t2.middle()
    ring.middle_right()
    t0.middle2()
    t1.middle()
    t3.start()
    t2.turn()
    t0.finish()
    ring.middle_left()
    t0.free2()
    t2.free1()
    t1.turn()
    t1.free1()
    t3.middle()
    ring.finish()
    g = jnp.concatenate(ring.sums(), axis=1)
    done(load_x)
    grad[...] = (e1[...] + norm_rows_vjp(x0[...].astype(F32), g)).astype(BF16)
    keep = comm.local((grad, grad_out))
    ring.sent()
    comm.signal(x_free, 'x')
    load_part = comm.local((part_hbm, part))
    comm.wait(x_free, 'x')
    done(load_part)
    ring = token_sums(comm, part, landing, tokens, ring)
    ring.start_all()
    t2.middle2()
    t1.middle2()
    g0.start()
    t3.turn()
    t3.free1()
    t1.finish()
    t2.finish()
    ring.middle_left()
    ring.middle_right()
    g0.middle()
    t1.free2()
    t2.free2()
    t3.middle2()
    g1.start()
    t3.finish()
    top.start()
    t3.free2()
    g0.turn()
    ring.finish()
    x2[...] = (x1[...].astype(F32) + jnp.concatenate(ring.sums(), axis=1)).astype(BF16)
    keep += comm.local((x2, x2_out))
    g1.middle()
    g0.middle2()
    g2.start()
    top.forward()
    g0.finish()
    top.near()
    low0.start()
    g1.turn()
    g2.middle()
    g1.middle2()
    g3.start()
    top.finish()
    low0.forward()
    g2.turn()
    g1.finish()
    low1.start()
    g4.start()
    low0.near()
    g2.middle2()
    g3.middle()
    low1.forward()
    low1.near()
    g4.middle()
    low0.finish()
    low1.finish()
    g2.finish()
    low2.start()
    g3.turn()
    g4.turn()
    g3.middle2()
    low2.forward()
    low2.near()
    g4.middle2()
    g3.finish()
    low3.start()
    low2.finish()
    g4.finish()
    low4.start()
    low3.forward()
    low3.near()
    low4.forward()
    low4.near()
    low3.finish()
    low4.finish()
    for pair in [top] + low:
        pair.arrived()
    done(keep)
    comm.end()


def call_lower_half(x0, x1, e1, d0, part_hbm, w1_hbm, w2_hbm, a_hbm, ut_low, st_low, ut_top, st_top, q_top, d_top):
    tokens, width = x0.shape
    group, slice_ = a_hbm.shape
    shapes = result_shapes(width, slice_)
    tops = [(4, 2) + shape for shape in shapes]
    lows = [(CHUNKS, 4, 2) + shape[1:] for shape in shapes]
    block = sds((tokens, width), BF16)
    outs = [block, block, sds(q_top.shape[1:], BF16), sds(d_top.shape[1:], BF16)] + [sds(s, F32) for s in tops + lows]
    acts = VMEM((group, slice_), BF16)
    scratch = [VMEM((4, width, group), BF16), VMEM((4, tokens, width), BF16), acts, acts]
    scratch += [VMEM(block.shape, BF16) for _ in range(4)] + [VMEM(block.shape, F32), VMEM((group, width), F32),
                                                              VMEM((6, tokens, width // 2), F32)]
    scratch += [VMEM(r.shape, BF16) for r in (ut_top, st_top, q_top, d_top)] + [VMEM(s, F32) for s in shapes + shapes]
    scratch += grad_buffers(width, slice_)
    ins = (x0, x1, e1, d0, part_hbm, w1_hbm.reshape(width, slice_), w2_hbm.reshape(slice_, width), a_hbm,
           ut_low, st_low, ut_top, st_top, q_top, d_top)
    return pl.pallas_call(
        lower_half,
        name='lower_half',
        out_shape=tuple(outs),
        in_specs=spaces('h' * 14),
        out_specs=tuple(spaces('h' * 8)),
        scratch_shapes=scratch + [sems(LOWER[0]), sems(LOWER[1]), sems(LOWER[2]), pltpu.SemaphoreType.REGULAR((2 * CHUNKS, 2)),
                                  pltpu.SemaphoreType.REGULAR],
        compiler_params=pltpu.CompilerParams(collective_id=2, has_side_effects=True, vmem_limit_bytes=VMEM_BYTES),
        cost_estimate=pl.CostEstimate(flops=16 * group * width * slice_, bytes_accessed=1 << 24, transcendentals=0),
    )(*ins)


def assemble(top_in, top_out, low_in, low_out, grad_in, grad_out, v_top_in, v_top_out, v_low_in, v_low_out,
             load_sems, store_sems):
    loads = []
    refs = (v_low_in, v_low_out, v_top_in, v_top_out)
    for i, src in enumerate((low_in, low_out, top_in, top_out)):
        copy = pltpu.make_async_copy(src, refs[i], load_sems.at[i])
        copy.start()
        loads.append(copy)
    strip = grad_in.shape[2] // 64
    rows, width = low_in.shape[3:]
    width_out = low_out.shape[4]
    per = width // strip
    for i, ref in enumerate(refs):
        loads[i].wait()
        layer = i // 2
        for k in range(CHUNKS):
            for x in range(4):
                for c in range(2):
                    src = ref.at[x, c, k] if layer else ref.at[k, x, c]
                    if i % 2:
                        dst = grad_out.at[layer, pl.ds(x * src.shape[0], src.shape[0]),
                                          pl.ds((c * CHUNKS + k) * width_out, width_out)]
                        pltpu.make_async_copy(src, dst, store_sems.at[1]).start()
                        continue
                    for j in range(per):
                        y, z = (c * 8 + k * per + j) // 4, (k * per + j) % 4
                        dst = grad_in.at[layer, :, pl.ds(((4 * z + y) * 4 + x) * strip, strip)]
                        pltpu.make_async_copy(src.at[:, pl.ds(j * strip, strip)], dst, store_sems.at[0]).start()
    pltpu.make_async_copy(grad_in, grad_in, store_sems.at[0]).wait()
    pltpu.make_async_copy(grad_out, grad_out, store_sems.at[1]).wait()


def call_assemble(ins, in_shape, out_shape):
    return pl.pallas_call(
        assemble,
        name='assemble',
        out_shape=(sds(in_shape, F32), sds(out_shape, F32)),
        in_specs=spaces('hhhh'),
        out_specs=tuple(spaces('hh')),
        scratch_shapes=[VMEM(r.shape, F32) for r in ins] + [sems(4), sems(2)],
        compiler_params=pltpu.CompilerParams(vmem_limit_bytes=VMEM_BYTES),
        cost_estimate=pl.CostEstimate(flops=1 << 30, bytes_accessed=1 << 25, transcendentals=0),
    )(*ins)


def solution(mesh):
    tok_spec = P(('local', 'data'), None)
    w_spec = P(None, 'local', None)

    def device_step(tokens, cotangent, w_in, w_out):
        (x1, e1, d0, part_out, a_low, ut_low, st_low, ut_top, st_top, q_top, d_top, w1_low, w2_low) = call_upper_half(
            tokens, cotangent, w_in, w_out)
        grad, x2, _, _, *gathered = call_lower_half(
            tokens, x1, e1, d0, part_out, w1_low, w2_low, a_low, ut_low, st_low, ut_top, st_top, q_top, d_top)
        grad_in, grad_out = call_assemble(gathered, w_in.shape, w_out.shape)
        return x2, grad_in, grad_out, grad

    return jax.shard_map(device_step, mesh=mesh, in_specs=(tok_spec, tok_spec, w_spec, w_spec),
                         out_specs=(tok_spec, w_spec, w_spec, tok_spec), check_vma=False)
```

```python
import functools

import jax
import jax.numpy as jnp
from jax import lax
from jax.experimental import pallas as pl
from jax.experimental.pallas import tpu as pltpu
from jax.sharding import PartitionSpec as P

EPSILON = 1e-6
GELU_SCALE = 0.7978845608028654
GELU_CUBE = 0.044715
BF16 = jnp.bfloat16
F32 = jnp.float32
MESH = pl.DeviceIdType.MESH
HBM = pltpu.HBM
VMEM = pltpu.VMEM
VMEM_BYTES = 67043328
UPPER = (40, 95)
LOWER = (69, 116, 41)


class Comm:
    def __init__(self, send_sems, recv_sems, local_sems):
        l = lax.axis_index('local')
        d = lax.axis_index('data')
        self.l, self.d = l, d
        self.z, self.y, self.x, self.c = l // 4, l % 4, d // 2, d % 2
        self.send_sems, self.recv_sems, self.local_sems = send_sems, recv_sems, local_sems
        self.sends = self.recvs = self.local_count = 0
        self.groups = []
        self.partner = (l, self.x * 2 + 1 - self.c)

    def pos(self, axis):
        return {'x': self.x, 'y': self.y, 'z': self.z}[axis]

    def neighbor(self, axis, delta):
        p = (self.pos(axis) + delta) % 4
        if axis == 'x':
            return (self.l, p * 2 + self.c)
        if axis == 'y':
            return (self.z * 4 + p, self.d)
        return (p * 4 + self.y, self.d)

    def peers(self, axes):
        out = [self.partner] if 'c' in axes else []
        for axis in axes.replace('c', ''):
            out += [self.neighbor(axis, 1), self.neighbor(axis, 3)]
        return out

    def signal(self, sem, axes):
        for device in self.peers(axes):
            pl.semaphore_signal(sem, inc=1, device_id=device, device_id_type=MESH)

    def wait(self, sem, axes):
        pl.semaphore_wait(sem, len(self.peers(axes)))

    def arrive(self, axes):
        self.signal(pltpu.get_barrier_semaphore(), axes)

    def meet(self, axes):
        self.wait(pltpu.get_barrier_semaphore(), axes)

    def send_sem(self):
        self.sends += 1
        return self.send_sems.at[self.sends - 1]

    def recv_sem(self):
        self.recvs += 1
        return self.recv_sems.at[self.recvs - 1]

    def copy(self, src, dst, device, send_sem, recv_sem):
        return pltpu.make_async_remote_copy(src_ref=src, dst_ref=dst, send_sem=send_sem, recv_sem=recv_sem,
                                            device_id=device, device_id_type=MESH)

    def send(self, src, dst, device, group, recv_sem):
        self.copy(src, dst, device, group.sem, recv_sem).start()

    def wait_recv(self, ref, recv_sem):
        self.copy(ref, ref, self.partner, self.send_sems.at[0], recv_sem).wait_recv()

    def push(self, src, dst):
        group, recv_sem = Sends(self, src), self.recv_sem()
        self.send(src, dst, self.partner, group, recv_sem)
        return group, lambda: self.wait_recv(dst, recv_sem)

    def local(self, *pairs):
        out = []
        for src, dst in pairs:
            copy = pltpu.make_async_copy(src, dst, self.local_sems.at[self.local_count])
            copy.start()
            self.local_count += 1
            out.append(copy)
        return out

    def end(self):
        for group in self.groups:
            group.wait()


class Sends:
    def __init__(self, comm, ref, sem=None):
        self.comm, self.ref, self.sem = comm, ref, sem or comm.send_sem()
        self.waited = False
        comm.groups.append(self)

    def wait(self):
        if not self.waited:
            self.waited = True
            c = self.comm
            c.copy(self.ref, self.ref, c.partner, self.sem, c.recv_sems.at[0]).wait_send()


def done(copies):
    for copy in copies:
        copy.wait()


class Every:
    def __init__(self, things):
        self.things = things

    def __getattr__(self, step):
        def run(*args):
            for thing in self.things:
                getattr(thing, step)(*args)
        return run


class RingGather:
    def __init__(self, comm, axis, own, slot, block, three, before=None):
        self.comm, self.own, self.slot, self.block = comm, own, slot, block
        self.me = comm.pos(axis)
        self.right, self.far, self.left = [(self.me + k) % 4 for k in (1, 2, 3)]
        self.to_right, self.to_left = comm.neighbor(axis, 1), comm.neighbor(axis, 3)
        self.group = Sends(comm, three, before and before.group.sem)
        self.sems = before.sems if before else [comm.recv_sem() for _ in range(3)]

    def both(self, k, right, right_slot, left, left_slot):
        self.comm.send(right, right_slot, self.to_right, self.group, self.sems[k])
        self.comm.send(left, left_slot, self.to_left, self.group, self.sems[k])

    def start(self):
        own, slot, me = self.own, self.slot, self.me
        self.both(0, own(0), slot(me, 0), own(1), slot(me, 1))
        self.both(1, own(1), slot(me, 1), own(0), slot(me, 0))

    def forward(self):
        self.comm.wait_recv(self.block, self.sems[0])
        right, left = self.slot(self.left, 0), self.slot(self.right, 1)
        self.both(2, right, right, left, left)

    def near(self):
        self.comm.wait_recv(self.block, self.sems[1])

    def finish(self):
        self.comm.wait_recv(self.block, self.sems[2])

    def sent(self):
        self.group.wait()


class RingReduce:
    def __init__(self, comm, axis, part, landing, before=None):
        self.comm, self.part, self.landing = comm, part, landing
        self.me = comm.pos(axis)
        self.right, self.far, self.left = [(self.me + k) % 4 for k in (1, 2, 3)]
        self.to_right, self.to_left = comm.neighbor(axis, 1), comm.neighbor(axis, 3)
        self.first = Sends(comm, landing.at[pl.ds(0, 2)], before and before.first.sem)
        self.rest = Sends(comm, landing.at[pl.ds(0, 4)], before and before.rest.sem)
        self.sems = before.sems if before else [comm.recv_sem() for _ in range(3)]

    def right_to(self, k, src, group, sem):
        self.comm.send(src, self.landing.at[k], self.to_right, group, sem)

    def left_to(self, k, src, group, sem):
        self.comm.send(src, self.landing.at[k], self.to_left, group, sem)

    def start_far(self, far0, far1):
        self.right_to(0, far0, self.first, self.sems[0])
        self.left_to(3, far1, self.first, self.sems[1])

    def start_near(self, right1, left0):
        self.right_to(1, right1, self.rest, self.sems[2])
        self.left_to(4, left0, self.rest, self.sems[2])

    def start_all(self):
        part = self.part
        self.start_far(part(self.far, 0), part(self.far, 1))
        self.start_near(part(self.right, 1), part(self.left, 0))

    def start_half(self, half):
        if half == 0:
            self.right_to(0, self.part(self.far, 0), self.first, self.sems[0])
            self.left_to(4, self.part(self.left, 0), self.rest, self.sems[2])
        else:
            self.left_to(3, self.part(self.far, 1), self.first, self.sems[1])
            self.right_to(1, self.part(self.right, 1), self.rest, self.sems[2])

    def wait_right(self):
        self.comm.wait_recv(self.landing.at[0], self.sems[0])

    def wait_left(self):
        self.comm.wait_recv(self.landing.at[3], self.sems[1])

    def pass_right(self):
        self.right_to(2, self.landing.at[0], self.rest, self.sems[2])

    def pass_left(self):
        self.left_to(5, self.landing.at[3], self.rest, self.sems[2])

    def middle_right(self):
        landing = self.landing
        self.wait_right()
        landing[0] = landing[0] + self.part(self.right, 0)[...]
        self.pass_right()

    def middle_left(self):
        landing = self.landing
        self.wait_left()
        landing[3] = landing[3] + self.part(self.left, 1)[...]
        self.pass_left()

    def finish(self):
        self.comm.wait_recv(self.landing.at[pl.ds(0, 4)], self.sems[2])

    def sent(self):
        self.first.wait()
        self.rest.wait()

    def sums(self):
        landing = self.landing
        return (self.part(self.me, 0)[...] + landing[2] + landing[4],
                self.part(self.me, 1)[...] + landing[1] + landing[5])


class PlaneGather:
    def __init__(self, comm, dims, first, full, cols, before=None):
        self.comm = comm
        c = comm.c
        lead = dims[0] == first
        second = dims.replace(first, '')
        b = comm.pos(second)
        half_rows = full.shape[3] // 2
        rows = lambda h: pl.ds(h * half_rows, half_rows)
        pair = lambda h: pl.ds(2 * h, 2)
        self.b = b
        every, three, own = slice(None), pl.ds(0, 3), comm.pos(first)
        at = lambda p, q, r: full.at[(p, q, c, r, cols) if lead else (q, p, c, r, cols)]
        slot1 = lambda p, h: at(p, b, rows(h))
        slot2 = lambda p, h: at(pair(h), p, every)
        self.ring1 = RingGather(comm, first, lambda h: slot1(own, h), slot1, at(own, b, every), at(three, b, every),
                                before and before.ring1)
        self.ring2 = RingGather(comm, second, lambda h: slot2(b, h), slot2, at(every, b, every), at(every, three, every),
                                before and before.ring2)
        self.line = lambda p: at(every, p, every)
        self.both_cores = lambda p, ref: ref.at[(every, p, every, every, cols) if lead else (p, every, every, every, cols)]
        self.whole, self.near_lines = at(every, every, every), at(every, three, every)
        self.group = Sends(comm, self.whole, before and before.group.sem)
        self.sems = before.sems if before else [comm.recv_sem(), comm.recv_sem()]
        self.full = full

    def push(self, p, k=0):
        self.comm.send(self.line(p), self.line(p), self.comm.partner, self.group, self.sems[k])

    def start1(self):
        self.ring1.start()

    def forward1(self):
        self.ring1.forward()

    def start2(self):
        self.ring1.near()
        self.ring1.finish()
        self.ring2.start()
        self.push(self.b)

    def forward2(self):
        self.ring2.forward()

    def near2(self):
        self.ring2.near()
        self.push(self.ring2.left)
        self.push(self.ring2.right)

    def finish2(self):
        self.ring2.finish()
        self.push(self.ring2.far, 1)

    def arrived_near(self):
        self.comm.wait_recv(self.near_lines, self.sems[0])

    def arrived_far(self):
        self.comm.wait_recv(self.line(self.b), self.sems[1])

    def arrived(self):
        self.arrived_near()
        self.arrived_far()

    def copy_out(self, out, positions, kept):
        both = self.both_cores
        kept += self.comm.local(*[(both(p, self.full), both(p, out)) for p in positions])

    def near_out(self, out, kept):
        self.arrived_near()
        self.copy_out(out, (self.b, self.ring2.left, self.ring2.right), kept)

    def far_out(self, out, kept):
        self.arrived_far()
        self.copy_out(out, (self.ring2.far,), kept)

    def sent(self):
        self.ring1.sent()
        self.ring2.sent()
        self.group.wait()


def gathers(comm, dims, full, pieces, before=None):
    width = full.shape[4] // pieces
    out = [PlaneGather(comm, dims, dims[k % 2], full, pl.ds(k * width, width), before and before.things[k])
           for k in range(pieces)]
    return [Every(out[k:k + 2]) for k in range(0, pieces, 2)]


def own_blocks(comm, w_in, w_out, layer, w1, w2):
    z, y, x, c = comm.z, comm.y, comm.x, comm.c
    width = w_in.shape[2] // 64
    rows1, rows2 = w1.shape[3], w2.shape[3]
    own = w1.at[z, y, c]
    k = comm.local_count
    comm.local_count += 1
    for j in range(16):
        start = (4 * (j % 4) + j // 4) * 4 * width + x * width
        pltpu.make_async_copy(w_in.at[layer, pl.ds(c * rows1, rows1), pl.ds(pl.multiple_of(start, width), width)],
                              own.at[:, pl.ds(j * width, width)], comm.local_sems.at[k]).start()
    start = (x * 2 + c) * rows2
    copies = comm.local((w_out.at[layer, pl.ds(pl.multiple_of(start, rows2), rows2)], w2.at[y, z, c]))
    return [pltpu.make_async_copy(own, own, comm.local_sems.at[k])] + copies


def ring_of_tokens(comm, full, before=None):
    n = full.shape[1] // 2
    slot = lambda p, h: full.at[p, pl.ds(h * n, n)]
    return RingGather(comm, 'x', lambda h: slot(comm.x, h), slot, full.at[0], full.at[pl.ds(0, 3)], before)


def token_sums(comm, part, landing, tokens, before=None):
    width = part.shape[1] // 2
    block = lambda pos, half: part.at[pl.ds(pl.multiple_of(pos * tokens, tokens), tokens), pl.ds(half * width, width)]
    return RingReduce(comm, 'x', block, landing, before)


def norm_rows(x):
    return x * lax.rsqrt(jnp.mean(x * x, axis=-1, keepdims=True) + EPSILON)


def norm_rows_vjp(x, g):
    r = lax.rsqrt(jnp.mean(x * x, axis=-1, keepdims=True) + EPSILON)
    dot = jnp.mean(x * g, axis=-1, keepdims=True)
    return r * g - x * (r * r * r * dot)


def gelu(x):
    t = jnp.tanh(GELU_SCALE * (x + GELU_CUBE * (x * x * x)))
    return x * (0.5 * (1.0 + t))


def gelu_grad(x):
    x2 = x * x
    t = jnp.tanh(GELU_SCALE * (x + GELU_CUBE * (x2 * x)))
    return 0.5 * (1.0 + t) + (0.5 * x) * (1.0 - t * t) * (GELU_SCALE * (1.0 + (3.0 * GELU_CUBE) * x2))


def dot(a, b):
    return lax.dot_general(a, b, (((1,), (0,)), ((), ())), preferred_element_type=F32)


def dot_bt(a, b):
    return lax.dot_general(a, b, (((1,), (1,)), ((), ())), preferred_element_type=F32)


def flat(value):
    return value.reshape(-1, value.shape[-1])


def tiles(n, step, tile=256):
    t = min(tile, n)

    def run(i, _):
        step(pl.ds(pl.multiple_of(i * t, t), t))
        return 0

    lax.fori_loop(0, n // t, run, 0)


def forward_acts(u, w1, a, s, st):
    def step(cols):
        acc = dot(flat(u[...]), flat(w1[:, :, :, :, cols])).astype(BF16)
        a[:, cols] = acc
        value = gelu(acc.astype(F32)).astype(BF16)
        s[:, cols] = value
        st[cols, :] = value.T

    tiles(a.shape[1], step)


def transposed(u, ut):
    def step(cols):
        ut[cols, :] = flat(u[:, :, cols]).T

    tiles(ut.shape[0], step)


def forward_part(s, w2, part, half):
    width = part.shape[1] // 2
    t = min(256, width)

    def run(i, _):
        cols = pl.ds(pl.multiple_of(half * width + i * t, t), t)
        part[:, cols] = dot(s[...], flat(w2[:, :, :, :, cols]))
        return 0

    lax.fori_loop(0, width // t, run, 0)


def row_tile(w, i):
    return flat(w[i // 2, pl.ds((i % 2) * 2, 2)])


def backward_acts(d, tile_product, a, q):
    rows = a.shape[1] // 8

    def step(i, _):
        cols = pl.ds(pl.multiple_of(i * rows, rows), rows)
        q[:, cols] = (tile_product(i) * gelu_grad(a[:, cols].astype(F32))).astype(BF16)
        return 0

    lax.fori_loop(0, 8, step, 0)


def backward_part(tile_product, part, half):
    rows = part.shape[1] // 8

    def step(j, _):
        i = half * 4 + j
        part[:, pl.ds(pl.multiple_of(i * rows, rows), rows)] = tile_product(i)
        return 0

    lax.fori_loop(0, 4, step, 0)


def last_dim_half(ref, k):
    width = ref.shape[-1] // 2
    return ref.at[..., pl.ds(pl.multiple_of(k * width, width), width)]


def upper_half(x0, cot, w_in, w_out,
               x1_out, e1_out, d0_out, part_out, a_low, ut_low, st_low, ut_top, st_top, q_top, d_top, w1_low, w2_low,
               p1, p2, q1, q2, uf, df, a, s, q, ut, st, x1, d0, part, landing, e1,
               send_sems, recv_sems, local_sems, credits):
    comm = Comm(send_sems, recv_sems, local_sems)
    tokens = x0.shape[0]
    x, c = comm.x, comm.c
    p_free, q_free = credits.at[0], credits.at[1]

    own0 = own_blocks(comm, w_in, w_out, 0, p1, p2)
    own1 = own_blocks(comm, w_in, w_out, 1, q1, q2)
    comm.arrive('xyzc')
    uf[x] = norm_rows(x0[...].astype(F32)).astype(BF16)
    df[x] = cot[...]
    comm.meet('xyzc')

    gather_u = ring_of_tokens(comm, uf)
    gather_d = ring_of_tokens(comm, df)
    g1, = gathers(comm, 'zy', p1, 2)
    g2, g3 = gathers(comm, 'yz', p2, 4)
    n1, = gathers(comm, 'zy', q1, 2)
    n2, = gathers(comm, 'yz', q2, 2)
    done(own0)
    g2.start1()
    gather_u.start()
    gather_d.start()
    done(own1)
    g1.start1()
    g2.forward1()
    g3.start1()
    g1.forward1()
    g2.start2()
    gather_u.forward()
    g3.forward1()
    g1.start2()
    gather_u.near()
    gather_d.forward()
    g1.forward2()
    g2.forward2()
    n1.start1()
    g3.start2()
    n2.start1()
    g2.near2()
    gather_d.near()
    g1.near2()
    g1.finish2()
    gather_u.finish()
    transposed(uf, ut)
    pushed = [comm.push(ut, ut_low.at[1])]
    kept = comm.local((ut, ut_low.at[0]))
    gather_d.finish()
    g2.finish2()
    g1.arrived()
    forward_acts(uf, p1, a, s, st)
    g2.arrived()
    n1.forward1()
    g3.forward2()
    gather_u.sent()
    ring = token_sums(comm, part, landing, tokens)
    forward_part(s, p2, part, 0)
    ring.start_half(0)
    g3.near2()
    pushed += [comm.push(st, st_low.at[1])]
    kept += comm.local((st, st_low.at[0]), (a, a_low))
    pushed += [comm.push(last_dim_half(df, 1 - c), d_top.at[1])]
    kept_d = comm.local((last_dim_half(df, c), d_top.at[0]))
    n2.forward1()
    n1.start2()
    g3.finish2()
    g3.arrived()
    forward_part(s, p2, part, 1)
    ring.start_half(1)
    g1.sent()
    g2.sent()
    g3.sent()
    comm.signal(p_free, 'yzc')
    own2 = own_blocks(comm, w_in, w_out, 1, p1, p2)
    b1, = gathers(comm, 'zy', p1, 2, g1)
    b2, = gathers(comm, 'yz', p2, 2, g2)
    done(own2)
    comm.wait(p_free, 'yzc')
    b2.start1()
    n1.forward2()
    n2.start2()
    b1.start1()
    ring.middle_right()
    n1.near2()
    ring.middle_left()
    n1.finish2()
    b2.forward1()
    n2.forward2()
    n1.arrived()
    n2.near2()
    b1.forward1()
    ring.finish()
    x_next = (x0[...].astype(F32) + jnp.concatenate(ring.sums(), axis=1)).astype(BF16)
    x1[...] = x_next
    keep_x = comm.local((x1, x1_out))
    uf[x] = norm_rows(x_next.astype(F32)).astype(BF16)
    ring.sent()
    gather_v = ring_of_tokens(comm, uf, gather_u)
    gather_v.start()
    done(kept)
    pushed[0][0].wait()
    pushed[1][0].wait()
    b2.start2()
    n2.finish2()
    gather_v.forward()
    b2.forward2()
    gather_v.near()
    b1.start2()
    n2.arrived()
    b2.near2()
    gather_v.finish()
    forward_acts(uf, q1, a, s, st)
    b2.finish2()
    forward_part(s, q2, part, 0)
    forward_part(s, q2, part, 1)
    keep_part = comm.local((part, part_out))
    b1.forward2()
    n1.sent()
    n2.sent()
    comm.signal(q_free, 'yzc')
    own3 = own_blocks(comm, w_in, w_out, 0, q1, q2)
    l1, = gathers(comm, 'zy', q1, 2, n1)
    l2, = gathers(comm, 'yz', q2, 2, n2)
    b2.arrived()
    done(own3)
    comm.wait(q_free, 'yzc')
    l1.start1()
    b1.near2()
    backward_acts(df, lambda i: dot_bt(flat(df[...]), row_tile(p2, i)), a, q)
    b1.finish2()
    l1.forward1()
    transposed(uf, ut)
    pushed += [comm.push(ut, ut_top.at[1]), comm.push(st, st_top.at[1])]
    kept = kept_d + comm.local((ut, ut_top.at[0]), (st, st_top.at[0]))
    l2.start1()
    b1.arrived()
    done(keep_part)
    ring = token_sums(comm, part, landing, tokens, ring)
    product = lambda i: dot_bt(q[...], row_tile(p1, i))
    backward_part(product, part, 0)
    ring.start_half(0)
    l2.forward1()
    l1.start2()
    backward_part(product, part, 1)
    ring.start_half(1)
    pushed += [comm.push(last_dim_half(q, 1 - c), q_top.at[1])]
    kept += comm.local((last_dim_half(q, c), q_top.at[0]))
    l2.start2()
    l1.forward2()
    l1.near2()
    ring.middle_right()
    l1.near_out(w1_low, kept)
    l2.forward2()
    ring.middle_left()
    l2.near2()
    l1.finish2()
    l2.near_out(w2_low, kept)
    l1.far_out(w1_low, kept)
    l2.finish2()
    ring.finish()
    g = jnp.concatenate(ring.sums(), axis=1)
    e = cot[...].astype(F32) + norm_rows_vjp(x1[...].astype(F32), g)
    e1[...] = e
    d0[...] = e.astype(BF16)
    kept += keep_x + comm.local((e1, e1_out), (d0, d0_out))
    l2.far_out(w2_low, kept)
    for _, arrived in pushed:
        arrived()
    done(kept)
    comm.end()


def sds(shape, dtype):
    return jax.ShapeDtypeStruct(shape, dtype)


def sems(n):
    return pltpu.SemaphoreType.DMA((n,))


def spaces(kinds):
    return [pl.BlockSpec(memory_space=VMEM if k == 'v' else HBM) for k in kinds]


def call(kernel, ins, in_kinds, outs, out_kinds, scratch, copies, credits, collective_id, flops):
    return pl.pallas_call(
        kernel,
        name=kernel.__name__,
        out_shape=tuple(outs),
        in_specs=spaces(in_kinds),
        out_specs=tuple(spaces(out_kinds)),
        scratch_shapes=scratch + [sems(copies[0][0]), sems(copies[0][1]), sems(copies[1]),
                                  pltpu.SemaphoreType.REGULAR((credits,))],
        compiler_params=pltpu.CompilerParams(collective_id=collective_id, has_side_effects=True,
                                             vmem_limit_bytes=VMEM_BYTES),
        cost_estimate=pl.CostEstimate(flops=flops, bytes_accessed=1 << 24, transcendentals=0),
    )(*ins)


def call_upper_half(x0, cot, w_in, w_out):
    tokens, width = x0.shape
    inner = w_in.shape[2]
    group, slice_ = 4 * tokens, inner // 4
    w1 = (4, 4, 2, width // 32, slice_)
    w2 = (4, 4, 2, inner // 128, width)
    block = sds((tokens, width), BF16)
    acts = (group, slice_)
    ut, st = (width, group), (slice_, group)
    pair = lambda shape: sds((2,) + shape, BF16)
    outs = [block, sds((tokens, width), F32), block, sds((group, width), F32), sds(acts, BF16),
            pair(ut), pair(st), pair(ut), pair(st), pair((group, slice_ // 2)), pair((4, tokens, width // 2)),
            sds(w1, BF16), sds(w2, BF16)]
    tok = (4, tokens, width)
    scratch = [VMEM(shape, BF16) for shape in (w1, w2, w1, w2, tok, tok, acts, acts, acts, ut, st, block.shape,
                                            block.shape)]
    scratch += [VMEM((group, width), F32), VMEM((6, tokens, width // 2), F32), VMEM(block.shape, F32)]
    return call(upper_half, (x0, cot, w_in, w_out), 'vvhh', outs, 'h' * 13, scratch, (UPPER, 35), 2, 1,
                16 * group * width * slice_)


class GradReduce:
    def __init__(self, comm, axes, operands, column, sends, landing1, landing2, result, credits, before=None):
        self.comm, self.axes, self.operands, self.column = comm, axes, operands, column
        self.sends, self.landing1, self.landing2, self.result = sends, landing1, landing2, result
        self.credits, self.before = credits, before
        self.ring = RingReduce(comm, axes[0], None, landing1, before and before.ring)
        rows = sends.shape[1] // 4
        self.block = lambda pos, h: sends.at[pos // 2, pl.ds(pl.multiple_of(((pos % 2) * 2 + h) * rows, rows), rows)]
        self.ring2 = RingReduce(comm, axes[1], self.block, landing2, before and before.ring2)

    def products(self, count, where, store):
        rows, width = self.sends.shape[1:]
        t = min(128, rows)
        per = rows // t

        def step(n, _):
            i, j = n // per, n % per
            pos, half = where(i)
            start = pl.multiple_of((pos * 2 + half) * rows + j * t, t)
            value = None
            for at, b in self.operands:
                term = dot(at[pl.ds(start, t)], b(pl.ds(self.column, width)))
                value = term if value is None else value + term
            store(i, pl.ds(pl.multiple_of(j * t, t), t), value)
            return 0

        lax.fori_loop(0, count * per, step, 0)

    def start_far(self):
        me, sends = self.ring.me, self.sends
        if self.before:
            self.before.sent()
            self.comm.wait(self.credits.at[0], self.axes[0])

        def store(i, rows, value):
            sends[i, rows] = value

        self.products(2, lambda i: ((me + 2) % 4, i), store)
        self.ring.start_far(sends.at[0], sends.at[1])

    def start_near(self):
        me, sends = self.ring.me, self.sends

        def store(i, rows, value):
            sends[2 + i, rows] = value

        self.products(2, lambda i: ((me + 1 + 2 * i) % 4, 1 - i), store)
        self.ring.start_near(sends.at[2], sends.at[3])

    def start(self):
        self.start_far()
        self.start_near()

    def middle(self):
        me, landing = self.ring.me, self.landing1
        self.ring.wait_right()
        self.ring.wait_left()

        def store(i, rows, value):
            landing[3 * i, rows] = landing[3 * i, rows] + value

        self.products(2, lambda i: ((me + 1 + 2 * i) % 4, i), store)
        self.ring.pass_right()
        self.ring.pass_left()

    def turn(self):
        me, landing, sends = self.ring.me, self.landing1, self.sends
        self.ring.finish()
        self.ring.first.wait()

        def store(i, rows, value):
            sends[i, rows] = value + landing[2 - i, rows] + landing[4 + i, rows]

        self.products(2, lambda i: (me, i), store)
        if self.before:
            self.comm.wait(self.credits.at[1], self.axes[1])
        self.ring2.start_all()

    def free1(self):
        self.ring.sent()
        self.comm.signal(self.credits.at[0], self.axes[0])

    def middle2(self):
        self.ring2.middle_right()
        self.ring2.middle_left()

    def finish(self):
        self.ring2.finish()
        n = self.result.shape[0] // 2
        self.result[0:n], self.result[n:2 * n] = self.ring2.sums()

    def sent(self):
        self.ring2.sent()

    def free2(self):
        self.sent()
        self.comm.signal(self.credits.at[1], self.axes[1])


CHUNKS = 4


def grad_buffers(width, slice_):
    out = []
    for rows, cols in ((width // 8, slice_ // 2), (slice_ // 8, width // 2)):
        w = cols // CHUNKS
        out += [VMEM((CHUNKS, 4, rows, w), F32), VMEM((CHUNKS, 6, rows, w), F32),
                VMEM((CHUNKS, 6, rows // 4, w), F32)]
    return out


def result_shapes(width, slice_):
    return [(CHUNKS, width // 16, slice_ // 2 // CHUNKS), (CHUNKS, slice_ // 16, width // 2 // CHUNKS)]


def grad_chunks(comm, operands, bufs, results, credits, before=None):
    out = []
    for k in range(CHUNKS):
        pieces = 2 if before and k == CHUNKS - 1 else 1
        for piece in range(pieces):
            both = []
            for i, axes in enumerate(('zy', 'yz')):
                width = bufs[3 * i].shape[3] // pieces
                cols = pl.ds(piece * width, width)
                sends, land1, land2 = [ref.at[k, :, :, cols] for ref in bufs[3 * i:3 * i + 3]]
                both.append(GradReduce(comm, axes, operands[i], (k * pieces + piece) * width, sends, land1, land2,
                                       results[i].at[k, :, cols], credits.at[2 * k + i],
                                       before[k].things[i] if before and piece == 0 else None))
            out.append(Every(both))
    return out


class BlockGather:
    def __init__(self, comm, own, out):
        self.comm, self.own, self.out = comm, own, out
        c = comm.c
        n = own.shape[0] // 2
        half = lambda h: pl.ds(h * n, n)
        self.ring = RingGather(comm, 'x', lambda h: own.at[half(h)], lambda p, h: out.at[p, c, half(h)],
                               own, out.at[pl.ds(0, 3), c])
        self.four = out.at[:, c]
        self.group, self.sem = Sends(comm, self.four), comm.recv_sem()

    def push(self, pos, src):
        c = self.comm
        c.send(src, self.out.at[pos, c.c], c.partner, self.group, self.sem)

    def start(self):
        self.ring.start()
        self.push(self.ring.me, self.own)
        self.kept = self.comm.local((self.own, self.out.at[self.ring.me, self.comm.c]))

    def forward(self):
        self.ring.forward()

    def near(self):
        ring, c = self.ring, self.comm.c
        ring.near()
        self.push(ring.left, self.out.at[ring.left, c])
        self.push(ring.right, self.out.at[ring.right, c])

    def finish(self):
        ring, c = self.ring, self.comm.c
        ring.finish()
        self.push(ring.far, self.out.at[ring.far, c])

    def arrived(self):
        self.comm.wait_recv(self.four, self.sem)
        done(self.kept)


def lower_half(x0_hbm, x1_hbm, e1_hbm, d0, part_hbm, w1_hbm, w2_hbm, a_hbm, ut_low, st_low, ut_top, st_top, q_top, d_top,
               grad_out, x2_out, q_low, d_low, top_all_in, top_all_out, low_all_in, low_all_out,
               w, df, a, q, x0, x1, grad, x2, e1, part, landing, gut, gst, gq, gd,
               top_in, top_out, low_in, low_out, *rest):
    bufs, (send_sems, recv_sems, local_sems, credits, x_free) = rest[:6], rest[6:]
    comm = Comm(send_sems, recv_sems, local_sems)
    tokens = x0.shape[0]
    x, c = comm.x, comm.c
    group = a.shape[0]
    load_d = comm.local((d0, df.at[x]))
    loads_in = comm.local((ut_top, gut), (q_top, gq))
    comm.arrive('xyzc')
    loads_out = comm.local((st_top, gst), (d_top, gd))
    columns = lambda ref, j: ref.at[:, pl.ds(j * group, group)]
    load_w = lambda ref: comm.local(*[(columns(ref, j), w.at[j]) for j in range(4)])
    comm.meet('xyzc')

    gather_d = ring_of_tokens(comm, df)
    done(load_d)
    gather_d.start()
    load2 = load_w(w2_hbm) + comm.local((a_hbm, a))
    load_x = comm.local((x0_hbm, x0), (e1_hbm, e1), (x1_hbm, x1))
    own_b = lambda ref: lambda cols: flat(ref[..., cols])
    top = [[(gut.at[k], own_b(gq.at[k])) for k in (0, 1)], [(gst.at[k], own_b(gd.at[k])) for k in (0, 1)]]
    upper = grad_chunks(comm, top, bufs, (top_in, top_out), credits)
    (t0i, t0o), (t1i, t1o), (t2i, t2o), (t3i, t3o) = [pair.things for pair in upper]

    def by_columns(left):
        rows = w.shape[1] // 8

        def product(i):
            value = None
            for j in range(4):
                term = dot_bt(flat(left[..., j * group:(j + 1) * group]),
                              w[j, pl.ds(pl.multiple_of(i * rows, rows), rows)])
                value = term if value is None else value + term
            return value

        return product

    done(loads_in)
    t0i.start_far()
    done(loads_out)
    t0o.start_far()
    t0i.start_near()
    t0o.start_near()
    top = Every([BlockGather(comm, top_in, top_all_in), BlockGather(comm, top_out, top_all_out)])
    w_in, w_out = low_in.shape[2] // 2, low_out.shape[2] // 2
    low = [(k, slice(None), slice(None)) for k in range(CHUNKS - 1)]
    low += [(CHUNKS - 1, pl.ds(h * w_in, w_in), pl.ds(h * w_out, w_out)) for h in (0, 1)]
    low = [Every([BlockGather(comm, low_in.at[k, :, i], low_all_in.at[k, :, :, :, i]),
                  BlockGather(comm, low_out.at[k, :, o], low_all_out.at[k, :, :, :, o])]) for k, i, o in low]
    (low0i, low0o), (low1i, low1o), (low2i, low2o), (low3i, low3o), (low4i, low4o) = [pair.things for pair in low]
    t3i.start()
    t1i.start()
    gather_d.forward()
    t1o.start()
    t0o.middle()
    t0i.middle()
    t3o.start()
    gather_d.near()
    t2o.start()
    gather_d.finish()
    done(load2)
    backward_acts(df, by_columns(df), a, q)
    load1 = load_w(w1_hbm)
    _, d_arrived = comm.push(last_dim_half(df, 1 - c), d_low)
    _, q_arrived = comm.push(last_dim_half(q, 1 - c), q_low)
    done(load1)
    ring = token_sums(comm, part, landing, tokens)
    product = by_columns(q)
    backward_part(product, part, 0)
    ring.start_half(0)
    backward_part(product, part, 1)
    ring.start_half(1)
    t1o.middle()
    t0o.turn()
    d_arrived()
    q_arrived()
    half = a.shape[1] // 2
    loads = comm.local(*[(ut_low.at[k], w.at[k]) for k in (0, 1)], *[(st_low.at[k], w.at[2 + k]) for k in (0, 1)],
                       (q_low, a.at[:, pl.ds(0, half)]))
    loads += comm.local(*[(d_low.at[k], a.at[pl.ds(k * tokens, tokens), pl.ds(half, half)]) for k in range(4)])
    done(loads)
    mine = lambda ref: lambda cols: flat(ref[..., pl.ds(pl.multiple_of(c * half + cols.start, cols.size), cols.size)])
    other = lambda first: lambda cols: a[:, pl.ds(first + cols.start, cols.size)]
    operands = [[(w.at[0], mine(q)), (w.at[1], other(0))], [(w.at[2], mine(df)), (w.at[3], other(half))]]
    lower = grad_chunks(comm, operands, bufs, (low_in, low_out), credits, upper)
    (g0i, g0o), (g1i, g1o), (g2i, g2o), (g3i, g3o), (g4i, g4o) = [pair.things for pair in lower]
    t0o.free1()
    t2i.start()
    t1i.middle()
    t0i.turn()
    t0i.free1()
    t3o.middle()
    t0o.middle2()
    ring.middle_right()
    t2i.middle()
    t3i.middle()
    t2o.middle()
    ring.middle_left()
    t0i.middle2()
    t1i.turn()
    t1o.turn()
    t0o.finish()
    t1i.free1()
    t1o.free1()
    t3o.turn()
    t2i.turn()
    t2i.free1()
    ring.finish()
    g = jnp.concatenate(ring.sums(), axis=1)
    done(load_x)
    grad[...] = (e1[...] + norm_rows_vjp(x0[...].astype(F32), g)).astype(BF16)
    keep = comm.local((grad, grad_out))
    ring.sent()
    comm.signal(x_free, 'x')
    load_part = comm.local((part_hbm, part))
    comm.wait(x_free, 'x')
    done(load_part)
    ring = token_sums(comm, part, landing, tokens, ring)
    ring.start_all()
    t2o.turn()
    t0i.finish()
    t0i.free2()
    t3i.turn()
    t0o.free2()
    t3i.free1()
    t2o.free1()
    t1i.middle2()
    t3o.middle2()
    t1o.middle2()
    t2i.middle2()
    t2o.middle2()
    t3o.free1()
    g0i.start()
    t3i.middle2()
    t3o.finish()
    g0o.start()
    t1i.finish()
    t2i.finish()
    t2o.finish()
    t2o.free2()
    t1o.finish()
    t3o.free2()
    t2i.free2()
    t1i.free2()
    t3i.finish()
    t3i.free2()
    t1o.free2()
    ring.middle_right()
    ring.middle_left()
    g0i.middle()
    top.start()
    g0o.middle()
    g2o.start()
    g2i.start()
    g0i.turn()
    g0o.turn()
    g1i.start()
    g1o.start()
    g0o.middle2()
    ring.finish()
    x2[...] = (x1[...].astype(F32) + jnp.concatenate(ring.sums(), axis=1)).astype(BF16)
    keep += comm.local((x2, x2_out))
    g0i.middle2()
    g2o.middle()
    g2i.middle()
    g1i.middle()
    g1o.middle()
    g3i.start()
    g0o.finish()
    low0o.start()
    g0i.finish()
    low0i.start()
    top.forward()
    top.near()
    low0o.forward()
    g2o.turn()
    g2i.turn()
    low0i.forward()
    g1i.turn()
    low0o.near()
    low0i.near()
    g2i.middle2()
    g1o.turn()
    g1i.middle2()
    g3o.start()
    g2o.middle2()
    g1i.finish()
    g2i.finish()
    low2i.start()
    g1o.middle2()
    low1i.start()
    g4i.start()
    g3o.middle()
    g2o.finish()
    g1o.finish()
    g4o.start()
    low1o.start()
    low0o.finish()
    g3i.middle()
    top.finish()
    low2o.start()
    low0i.finish()
    low2i.forward()
    low2i.near()
    low1i.forward()
    low1i.near()
    g4i.middle()
    g3o.turn()
    low1o.forward()
    g4o.middle()
    g3i.turn()
    low2o.forward()
    low2o.near()
    g4i.turn()
    g3o.middle2()
    g4o.turn()
    g3i.middle2()
    g4i.middle2()
    g3o.finish()
    low3o.start()
    low2i.finish()
    g4o.middle2()
    g3i.finish()
    low1o.near()
    low3i.start()
    g4i.finish()
    low4i.start()
    g4o.finish()
    low4o.start()
    low3o.forward()
    low3o.near()
    low2o.finish()
    low3i.forward()
    low3i.near()
    low4i.forward()
    low1i.finish()
    low4i.near()
    low1o.finish()
    low4o.forward()
    low3o.finish()
    low3i.finish()
    low4i.finish()
    low4o.near()
    low4o.finish()
    for pair in [top] + low:
        pair.arrived()
    done(keep)
    comm.end()


def call_lower_half(x0, x1, e1, d0, part_hbm, w1_hbm, w2_hbm, a_hbm, ut_low, st_low, ut_top, st_top, q_top, d_top):
    tokens, width = x0.shape
    group, slice_ = a_hbm.shape
    shapes = result_shapes(width, slice_)
    tops = [(4, 2) + shape for shape in shapes]
    lows = [(CHUNKS, 4, 2) + shape[1:] for shape in shapes]
    block = sds((tokens, width), BF16)
    outs = [block, block, sds(q_top.shape[1:], BF16), sds(d_top.shape[1:], BF16)] + [sds(s, F32) for s in tops + lows]
    acts = VMEM((group, slice_), BF16)
    scratch = [VMEM((4, width, group), BF16), VMEM((4, tokens, width), BF16), acts, acts]
    scratch += [VMEM(block.shape, BF16) for _ in range(4)] + [VMEM(block.shape, F32), VMEM((group, width), F32),
                                                              VMEM((6, tokens, width // 2), F32)]
    scratch += [VMEM(r.shape, BF16) for r in (ut_top, st_top, q_top, d_top)] + [VMEM(s, F32) for s in shapes + shapes]
    scratch += grad_buffers(width, slice_)
    ins = (x0, x1, e1, d0, part_hbm, w1_hbm.reshape(width, slice_), w2_hbm.reshape(slice_, width), a_hbm,
           ut_low, st_low, ut_top, st_top, q_top, d_top)
    return pl.pallas_call(
        lower_half,
        name='lower_half',
        out_shape=tuple(outs),
        in_specs=spaces('h' * 14),
        out_specs=tuple(spaces('h' * 8)),
        scratch_shapes=scratch + [sems(LOWER[0]), sems(LOWER[1]), sems(LOWER[2]), pltpu.SemaphoreType.REGULAR((2 * CHUNKS, 2)),
                                  pltpu.SemaphoreType.REGULAR],
        compiler_params=pltpu.CompilerParams(collective_id=2, has_side_effects=True, vmem_limit_bytes=VMEM_BYTES),
        cost_estimate=pl.CostEstimate(flops=16 * group * width * slice_, bytes_accessed=1 << 24, transcendentals=0),
    )(*ins)


def assemble(top_in, top_out, low_in, low_out, grad_in, grad_out, v_top_in, v_top_out, v_low_in, v_low_out,
             load_sems, store_sems):
    loads = []
    refs = (v_low_in, v_low_out, v_top_in, v_top_out)
    for i, src in enumerate((low_in, low_out, top_in, top_out)):
        copy = pltpu.make_async_copy(src, refs[i], load_sems.at[i])
        copy.start()
        loads.append(copy)
    strip = grad_in.shape[2] // 64
    rows, width = low_in.shape[3:]
    width_out = low_out.shape[4]
    per = width // strip
    for i, ref in enumerate(refs):
        loads[i].wait()
        layer = i // 2
        for k in range(CHUNKS):
            for x in range(4):
                for c in range(2):
                    src = ref.at[x, c, k] if layer else ref.at[k, x, c]
                    if i % 2:
                        dst = grad_out.at[layer, pl.ds(x * src.shape[0], src.shape[0]),
                                          pl.ds((c * CHUNKS + k) * width_out, width_out)]
                        pltpu.make_async_copy(src, dst, store_sems.at[1]).start()
                        continue
                    for j in range(per):
                        y, z = (c * 8 + k * per + j) // 4, (k * per + j) % 4
                        dst = grad_in.at[layer, :, pl.ds(((4 * z + y) * 4 + x) * strip, strip)]
                        pltpu.make_async_copy(src.at[:, pl.ds(j * strip, strip)], dst, store_sems.at[0]).start()
    pltpu.make_async_copy(grad_in, grad_in, store_sems.at[0]).wait()
    pltpu.make_async_copy(grad_out, grad_out, store_sems.at[1]).wait()


def call_assemble(ins, in_shape, out_shape):
    return pl.pallas_call(
        assemble,
        name='assemble',
        out_shape=(sds(in_shape, F32), sds(out_shape, F32)),
        in_specs=spaces('hhhh'),
        out_specs=tuple(spaces('hh')),
        scratch_shapes=[VMEM(r.shape, F32) for r in ins] + [sems(4), sems(2)],
        compiler_params=pltpu.CompilerParams(vmem_limit_bytes=VMEM_BYTES),
        cost_estimate=pl.CostEstimate(flops=1 << 30, bytes_accessed=1 << 25, transcendentals=0),
    )(*ins)


def solution(mesh):
    tok_spec = P(('local', 'data'), None)
    w_spec = P(None, 'local', None)

    def device_step(tokens, cotangent, w_in, w_out):
        (x1, e1, d0, part_out, a_low, ut_low, st_low, ut_top, st_top, q_top, d_top, w1_low, w2_low) = call_upper_half(
            tokens, cotangent, w_in, w_out)
        grad, x2, _, _, *gathered = call_lower_half(
            tokens, x1, e1, d0, part_out, w1_low, w2_low, a_low, ut_low, st_low, ut_top, st_top, q_top, d_top)
        grad_in, grad_out = call_assemble(gathered, w_in.shape, w_out.shape)
        return x2, grad_in, grad_out, grad

    return jax.shard_map(device_step, mesh=mesh, in_specs=(tok_spec, tok_spec, w_spec, w_spec),
                         out_specs=(tok_spec, w_spec, w_spec, tok_spec), check_vma=False)
```

```python
import functools

import jax
import jax.numpy as jnp
from jax import lax
from jax.experimental import pallas as pl
from jax.experimental.pallas import tpu as pltpu
from jax.sharding import PartitionSpec as P

EPSILON = 1e-6
GELU_SCALE = 0.7978845608028654
GELU_CUBE = 0.044715
BF16 = jnp.bfloat16
F32 = jnp.float32
MESH = pl.DeviceIdType.MESH
HBM = pltpu.HBM
VMEM = pltpu.VMEM
VMEM_BYTES = 67043328
UPPER = (40, 95)
LOWER = (69, 116, 49)


class Comm:
    def __init__(self, send_sems, recv_sems, local_sems):
        l = lax.axis_index('local')
        d = lax.axis_index('data')
        self.l, self.d = l, d
        self.z, self.y, self.x, self.c = l // 4, l % 4, d // 2, d % 2
        self.send_sems, self.recv_sems, self.local_sems = send_sems, recv_sems, local_sems
        self.sends = self.recvs = self.local_count = 0
        self.groups = []
        self.partner = (l, self.x * 2 + 1 - self.c)

    def pos(self, axis):
        return {'x': self.x, 'y': self.y, 'z': self.z}[axis]

    def neighbor(self, axis, delta):
        p = (self.pos(axis) + delta) % 4
        if axis == 'x':
            return (self.l, p * 2 + self.c)
        if axis == 'y':
            return (self.z * 4 + p, self.d)
        return (p * 4 + self.y, self.d)

    def peers(self, axes):
        out = [self.partner] if 'c' in axes else []
        for axis in axes.replace('c', ''):
            out += [self.neighbor(axis, 1), self.neighbor(axis, 3)]
        return out

    def signal(self, sem, axes):
        for device in self.peers(axes):
            pl.semaphore_signal(sem, inc=1, device_id=device, device_id_type=MESH)

    def wait(self, sem, axes):
        pl.semaphore_wait(sem, len(self.peers(axes)))

    def arrive(self, axes):
        self.signal(pltpu.get_barrier_semaphore(), axes)

    def meet(self, axes):
        self.wait(pltpu.get_barrier_semaphore(), axes)

    def send_sem(self):
        self.sends += 1
        return self.send_sems.at[self.sends - 1]

    def recv_sem(self):
        self.recvs += 1
        return self.recv_sems.at[self.recvs - 1]

    def copy(self, src, dst, device, send_sem, recv_sem):
        return pltpu.make_async_remote_copy(src_ref=src, dst_ref=dst, send_sem=send_sem, recv_sem=recv_sem,
                                            device_id=device, device_id_type=MESH)

    def send(self, src, dst, device, group, recv_sem):
        self.copy(src, dst, device, group.sem, recv_sem).start()

    def wait_recv(self, ref, recv_sem):
        self.copy(ref, ref, self.partner, self.send_sems.at[0], recv_sem).wait_recv()

    def push(self, src, dst):
        group, recv_sem = Sends(self, src), self.recv_sem()
        self.send(src, dst, self.partner, group, recv_sem)
        return group, lambda: self.wait_recv(dst, recv_sem)

    def local(self, *pairs):
        out = []
        for src, dst in pairs:
            copy = pltpu.make_async_copy(src, dst, self.local_sems.at[self.local_count])
            copy.start()
            self.local_count += 1
            out.append(copy)
        return out

    def end(self):
        for group in self.groups:
            group.wait()


class Sends:
    def __init__(self, comm, ref, sem=None):
        self.comm, self.ref, self.sem = comm, ref, sem or comm.send_sem()
        self.waited = False
        comm.groups.append(self)

    def wait(self):
        if not self.waited:
            self.waited = True
            c = self.comm
            c.copy(self.ref, self.ref, c.partner, self.sem, c.recv_sems.at[0]).wait_send()


def done(copies):
    for copy in copies:
        copy.wait()


class Every:
    def __init__(self, things):
        self.things = things

    def __getattr__(self, step):
        def run(*args):
            for thing in self.things:
                getattr(thing, step)(*args)
        return run


class RingGather:
    def __init__(self, comm, axis, own, slot, block, three, before=None):
        self.comm, self.own, self.slot, self.block = comm, own, slot, block
        self.me = comm.pos(axis)
        self.right, self.far, self.left = [(self.me + k) % 4 for k in (1, 2, 3)]
        self.to_right, self.to_left = comm.neighbor(axis, 1), comm.neighbor(axis, 3)
        self.group = Sends(comm, three, before and before.group.sem)
        self.sems = before.sems if before else [comm.recv_sem() for _ in range(3)]

    def both(self, k, right, right_slot, left, left_slot):
        self.comm.send(right, right_slot, self.to_right, self.group, self.sems[k])
        self.comm.send(left, left_slot, self.to_left, self.group, self.sems[k])

    def start(self):
        own, slot, me = self.own, self.slot, self.me
        self.both(0, own(0), slot(me, 0), own(1), slot(me, 1))
        self.both(1, own(1), slot(me, 1), own(0), slot(me, 0))

    def forward(self):
        self.comm.wait_recv(self.block, self.sems[0])
        right, left = self.slot(self.left, 0), self.slot(self.right, 1)
        self.both(2, right, right, left, left)

    def near(self):
        self.comm.wait_recv(self.block, self.sems[1])

    def finish(self):
        self.comm.wait_recv(self.block, self.sems[2])

    def sent(self):
        self.group.wait()


class RingReduce:
    def __init__(self, comm, axis, part, landing, before=None):
        self.comm, self.part, self.landing = comm, part, landing
        self.me = comm.pos(axis)
        self.right, self.far, self.left = [(self.me + k) % 4 for k in (1, 2, 3)]
        self.to_right, self.to_left = comm.neighbor(axis, 1), comm.neighbor(axis, 3)
        self.first = Sends(comm, landing.at[pl.ds(0, 2)], before and before.first.sem)
        self.rest = Sends(comm, landing.at[pl.ds(0, 4)], before and before.rest.sem)
        self.sems = before.sems if before else [comm.recv_sem() for _ in range(3)]

    def right_to(self, k, src, group, sem):
        self.comm.send(src, self.landing.at[k], self.to_right, group, sem)

    def left_to(self, k, src, group, sem):
        self.comm.send(src, self.landing.at[k], self.to_left, group, sem)

    def start_far(self, far0, far1):
        self.right_to(0, far0, self.first, self.sems[0])
        self.left_to(3, far1, self.first, self.sems[1])

    def start_near(self, right1, left0):
        self.right_to(1, right1, self.rest, self.sems[2])
        self.left_to(4, left0, self.rest, self.sems[2])

    def start_all(self):
        part = self.part
        self.start_far(part(self.far, 0), part(self.far, 1))
        self.start_near(part(self.right, 1), part(self.left, 0))

    def start_half(self, half):
        if half == 0:
            self.right_to(0, self.part(self.far, 0), self.first, self.sems[0])
            self.left_to(4, self.part(self.left, 0), self.rest, self.sems[2])
        else:
            self.left_to(3, self.part(self.far, 1), self.first, self.sems[1])
            self.right_to(1, self.part(self.right, 1), self.rest, self.sems[2])

    def wait_right(self):
        self.comm.wait_recv(self.landing.at[0], self.sems[0])

    def wait_left(self):
        self.comm.wait_recv(self.landing.at[3], self.sems[1])

    def pass_right(self):
        self.right_to(2, self.landing.at[0], self.rest, self.sems[2])

    def pass_left(self):
        self.left_to(5, self.landing.at[3], self.rest, self.sems[2])

    def middle_right(self):
        landing = self.landing
        self.wait_right()
        landing[0] = landing[0] + self.part(self.right, 0)[...]
        self.pass_right()

    def middle_left(self):
        landing = self.landing
        self.wait_left()
        landing[3] = landing[3] + self.part(self.left, 1)[...]
        self.pass_left()

    def finish(self):
        self.comm.wait_recv(self.landing.at[pl.ds(0, 4)], self.sems[2])

    def sent(self):
        self.first.wait()
        self.rest.wait()

    def sums(self):
        landing = self.landing
        return (self.part(self.me, 0)[...] + landing[2] + landing[4],
                self.part(self.me, 1)[...] + landing[1] + landing[5])


class PlaneGather:
    def __init__(self, comm, dims, first, full, cols, before=None, out=None):
        self.comm, self.out, self.kept = comm, out, []
        c = comm.c
        lead = dims[0] == first
        second = dims.replace(first, '')
        b = comm.pos(second)
        half_rows = full.shape[3] // 2
        rows = lambda h: pl.ds(h * half_rows, half_rows)
        pair = lambda h: pl.ds(2 * h, 2)
        self.b = b
        every, three, own = slice(None), pl.ds(0, 3), comm.pos(first)
        at = lambda p, q, r: full.at[(p, q, c, r, cols) if lead else (q, p, c, r, cols)]
        slot1 = lambda p, h: at(p, b, rows(h))
        slot2 = lambda p, h: at(pair(h), p, every)
        self.ring1 = RingGather(comm, first, lambda h: slot1(own, h), slot1, at(own, b, every), at(three, b, every),
                                before and before.ring1)
        self.ring2 = RingGather(comm, second, lambda h: slot2(b, h), slot2, at(every, b, every), at(every, three, every),
                                before and before.ring2)
        self.line = lambda p, ref=full: ref.at[(every, p, c, every, cols) if lead else (p, every, c, every, cols)]
        self.whole, self.near_lines = at(every, every, every), at(every, three, every)
        self.group = Sends(comm, self.whole, before and before.group.sem)
        self.sems = before.sems if before else [comm.recv_sem(), comm.recv_sem()]

    def push(self, p, k=0):
        line = self.line(p)
        target = line if self.out is None else self.line(p, self.out)
        self.comm.send(line, target, self.comm.partner, self.group, self.sems[k])
        if self.out is not None:
            self.kept += self.comm.local((line, target))

    def start1(self):
        self.ring1.start()

    def forward1(self):
        self.ring1.forward()

    def start2(self):
        self.ring1.near()
        self.ring1.finish()
        self.ring2.start()
        self.push(self.b)

    def forward2(self):
        self.ring2.forward()

    def near2(self):
        self.ring2.near()
        self.push(self.ring2.left)
        self.push(self.ring2.right)

    def finish2(self):
        self.ring2.finish()
        self.push(self.ring2.far, 1)

    def arrived(self):
        self.comm.wait_recv(self.near_lines, self.sems[0])
        self.comm.wait_recv(self.line(self.b), self.sems[1])
        done(self.kept)

    def sent(self):
        self.ring1.sent()
        self.ring2.sent()
        self.group.wait()


def gathers(comm, dims, full, pieces, before=None, out=None):
    width = full.shape[4] // pieces
    out = [PlaneGather(comm, dims, dims[k % 2], full, pl.ds(k * width, width), before and before.things[k], out)
           for k in range(pieces)]
    return [Every(out[k:k + 2]) for k in range(0, pieces, 2)]


def own_blocks(comm, w_in, w_out, layer, w1, w2):
    z, y, x, c = comm.z, comm.y, comm.x, comm.c
    width = w_in.shape[2] // 64
    rows1, rows2 = w1.shape[3], w2.shape[3]
    own = w1.at[z, y, c]
    k = comm.local_count
    comm.local_count += 1
    for j in range(16):
        start = (4 * (j % 4) + j // 4) * 4 * width + x * width
        pltpu.make_async_copy(w_in.at[layer, pl.ds(c * rows1, rows1), pl.ds(pl.multiple_of(start, width), width)],
                              own.at[:, pl.ds(j * width, width)], comm.local_sems.at[k]).start()
    start = (x * 2 + c) * rows2
    copies = comm.local((w_out.at[layer, pl.ds(pl.multiple_of(start, rows2), rows2)], w2.at[y, z, c]))
    return [pltpu.make_async_copy(own, own, comm.local_sems.at[k])] + copies


def ring_of_tokens(comm, full, before=None):
    n = full.shape[1] // 2
    slot = lambda p, h: full.at[p, pl.ds(h * n, n)]
    return RingGather(comm, 'x', lambda h: slot(comm.x, h), slot, full.at[0], full.at[pl.ds(0, 3)], before)


def token_sums(comm, part, landing, tokens, before=None):
    width = part.shape[1] // 2
    block = lambda pos, half: part.at[pl.ds(pl.multiple_of(pos * tokens, tokens), tokens), pl.ds(half * width, width)]
    return RingReduce(comm, 'x', block, landing, before)


def norm_rows(x):
    return x * lax.rsqrt(jnp.mean(x * x, axis=-1, keepdims=True) + EPSILON)


def norm_rows_vjp(x, g):
    r = lax.rsqrt(jnp.mean(x * x, axis=-1, keepdims=True) + EPSILON)
    dot = jnp.mean(x * g, axis=-1, keepdims=True)
    return r * g - x * (r * r * r * dot)


def gelu(x):
    t = jnp.tanh(GELU_SCALE * (x + GELU_CUBE * (x * x * x)))
    return x * (0.5 * (1.0 + t))


def gelu_grad(x):
    x2 = x * x
    t = jnp.tanh(GELU_SCALE * (x + GELU_CUBE * (x2 * x)))
    return 0.5 * (1.0 + t) + (0.5 * x) * (1.0 - t * t) * (GELU_SCALE * (1.0 + (3.0 * GELU_CUBE) * x2))


def dot(a, b):
    return lax.dot_general(a, b, (((1,), (0,)), ((), ())), preferred_element_type=F32)


def dot_bt(a, b):
    return lax.dot_general(a, b, (((1,), (1,)), ((), ())), preferred_element_type=F32)


def flat(value):
    return value.reshape(-1, value.shape[-1])


def tiles(n, step, tile=256):
    t = min(tile, n)

    def run(i, _):
        step(pl.ds(pl.multiple_of(i * t, t), t))
        return 0

    lax.fori_loop(0, n // t, run, 0)


def forward_acts(u, w1, a, s, st):
    def step(cols):
        acc = dot(flat(u[...]), flat(w1[:, :, :, :, cols])).astype(BF16)
        a[:, cols] = acc
        value = gelu(acc.astype(F32)).astype(BF16)
        s[:, cols] = value
        st[cols, :] = value.T

    tiles(a.shape[1], step)


def transposed(u, ut):
    def step(cols):
        ut[cols, :] = flat(u[:, :, cols]).T

    tiles(ut.shape[0], step)


def forward_part(s, w2, part, half):
    width = part.shape[1] // 2
    t = min(256, width)

    def run(i, _):
        cols = pl.ds(pl.multiple_of(half * width + i * t, t), t)
        part[:, cols] = dot(s[...], flat(w2[:, :, :, :, cols]))
        return 0

    lax.fori_loop(0, width // t, run, 0)


def row_tile(w, i):
    return flat(w[i // 2, pl.ds((i % 2) * 2, 2)])


def backward_acts(d, tile_product, a, q):
    rows = a.shape[1] // 8

    def step(i, _):
        cols = pl.ds(pl.multiple_of(i * rows, rows), rows)
        q[:, cols] = (tile_product(i) * gelu_grad(a[:, cols].astype(F32))).astype(BF16)
        return 0

    lax.fori_loop(0, 8, step, 0)


def backward_part(tile_product, part, half):
    rows = part.shape[1] // 8

    def step(j, _):
        i = half * 4 + j
        part[:, pl.ds(pl.multiple_of(i * rows, rows), rows)] = tile_product(i)
        return 0

    lax.fori_loop(0, 4, step, 0)


def last_dim_half(ref, k):
    width = ref.shape[-1] // 2
    return ref.at[..., pl.ds(pl.multiple_of(k * width, width), width)]


def upper_half(x0_hbm, cot, w_in, w_out,
               x1_out, e1_out, d0_out, part_out, a_low, ut_low, st_low, ut_top, st_top, q_top, d_top, w1_low, w2_low,
               p1, p2, q1, q2, uf, df, a, s, q, ut, st, x0, x1, d0, part, landing, e1,
               send_sems, recv_sems, local_sems, credits):
    comm = Comm(send_sems, recv_sems, local_sems)
    tokens = x0.shape[0]
    x, c = comm.x, comm.c
    p_free, q_free = credits.at[0], credits.at[1]

    comm.arrive('xyzc')
    load_x = comm.local((x0_hbm, x0))
    own0 = own_blocks(comm, w_in, w_out, 0, p1, p2)
    load_d = comm.local((cot, df.at[x]))
    own1 = own_blocks(comm, w_in, w_out, 1, q1, q2)
    done(load_x)
    uf[x] = norm_rows(x0[...].astype(F32)).astype(BF16)
    comm.meet('xyzc')

    gather_u = ring_of_tokens(comm, uf)
    gather_d = ring_of_tokens(comm, df)
    g1, = gathers(comm, 'zy', p1, 2)
    g2, g3 = gathers(comm, 'yz', p2, 4)
    n1, = gathers(comm, 'zy', q1, 2)
    n2, = gathers(comm, 'yz', q2, 2)
    done(own0 + load_d)
    g2.start1()
    gather_u.start()
    g1.start1()
    done(own1)
    g2.forward1()
    g3.start1()
    g1.forward1()
    g2.start2()
    g3.forward1()
    gather_u.forward()
    gather_d.start()
    g1.start2()
    gather_u.near()
    gather_u.finish()
    g1.forward2()
    g2.forward2()
    n2.start1()
    g2.near2()
    g3.start2()
    gather_d.forward()
    n1.start1()
    transposed(uf, ut)
    pushed = [comm.push(ut, ut_low.at[1])]
    kept = comm.local((ut, ut_low.at[0]))
    g1.near2()
    gather_d.near()
    g1.finish2()
    g2.finish2()
    gather_d.finish()
    g1.arrived()
    forward_acts(uf, p1, a, s, st)
    n2.forward1()
    g3.forward2()
    g2.arrived()
    gather_u.sent()
    ring = token_sums(comm, part, landing, tokens)
    forward_part(s, p2, part, 0)
    ring.start_half(0)
    n1.forward1()
    pushed += [comm.push(st, st_low.at[1])]
    kept += comm.local((st, st_low.at[0]), (a, a_low))
    g3.near2()
    pushed += [comm.push(last_dim_half(df, 1 - c), d_top.at[1])]
    kept_d = comm.local((last_dim_half(df, c), d_top.at[0]))
    n2.start2()
    g3.finish2()
    g3.arrived()
    forward_part(s, p2, part, 1)
    ring.start_half(1)
    g1.sent()
    g2.sent()
    g3.sent()
    comm.signal(p_free, 'yzc')
    own2 = own_blocks(comm, w_in, w_out, 1, p1, p2)
    b1, = gathers(comm, 'zy', p1, 2, g1)
    b2, = gathers(comm, 'yz', p2, 2, g2)
    done(own2)
    comm.wait(p_free, 'yzc')
    b1.start1()
    b2.start1()
    n1.start2()
    n2.forward2()
    ring.middle_right()
    n2.near2()
    b2.forward1()
    b1.forward1()
    ring.middle_left()
    n1.forward2()
    n1.near2()
    ring.finish()
    x_next = (x0[...].astype(F32) + jnp.concatenate(ring.sums(), axis=1)).astype(BF16)
    x1[...] = x_next
    keep_x = comm.local((x1, x1_out))
    uf[x] = norm_rows(x_next.astype(F32)).astype(BF16)
    ring.sent()
    gather_v = ring_of_tokens(comm, uf, gather_u)
    gather_v.start()
    n2.finish2()
    done(kept)
    pushed[0][0].wait()
    pushed[1][0].wait()
    b2.start2()
    n2.arrived()
    n1.finish2()
    gather_v.forward()
    n1.arrived()
    b2.forward2()
    gather_v.near()
    b1.start2()
    b2.near2()
    gather_v.finish()
    forward_acts(uf, q1, a, s, st)
    b2.finish2()
    forward_part(s, q2, part, 0)
    forward_part(s, q2, part, 1)
    keep_part = comm.local((part, part_out))
    b1.forward2()
    n1.sent()
    n2.sent()
    comm.signal(q_free, 'yzc')
    own3 = own_blocks(comm, w_in, w_out, 0, q1, q2)
    l1, = gathers(comm, 'zy', q1, 2, n1, w1_low)
    l2, = gathers(comm, 'yz', q2, 2, n2, w2_low)
    b2.arrived()
    done(own3)
    comm.wait(q_free, 'yzc')
    l2.start1()
    b1.near2()
    backward_acts(df, lambda i: dot_bt(flat(df[...]), row_tile(p2, i)), a, q)
    b1.finish2()
    l2.forward1()
    l1.start1()
    transposed(uf, ut)
    pushed += [comm.push(ut, ut_top.at[1]), comm.push(st, st_top.at[1])]
    kept = kept_d + comm.local((ut, ut_top.at[0]), (st, st_top.at[0]))
    pushed += [comm.push(last_dim_half(q, 1 - c), q_top.at[1])]
    kept += comm.local((last_dim_half(q, c), q_top.at[0]))
    b1.arrived()
    done(keep_part)
    ring = token_sums(comm, part, landing, tokens, ring)
    product = lambda i: dot_bt(q[...], row_tile(p1, i))
    backward_part(product, part, 0)
    ring.start_half(0)
    l1.forward1()
    l2.start2()
    backward_part(product, part, 1)
    ring.start_half(1)
    l2.forward2()
    l1.start2()
    ring.middle_right()
    l2.near2()
    l2.finish2()
    ring.middle_left()
    l1.forward2()
    l2.arrived()
    l1.near2()
    l1.finish2()
    ring.finish()
    g = jnp.concatenate(ring.sums(), axis=1)
    e = df[x].astype(F32) + norm_rows_vjp(x1[...].astype(F32), g)
    e1[...] = e
    d0[...] = e.astype(BF16)
    kept += keep_x + comm.local((e1, e1_out), (d0, d0_out))
    l1.arrived()
    for _, arrived in pushed:
        arrived()
    done(kept)
    comm.end()


def sds(shape, dtype):
    return jax.ShapeDtypeStruct(shape, dtype)


def sems(n):
    return pltpu.SemaphoreType.DMA((n,))


def spaces(kinds):
    return [pl.BlockSpec(memory_space=VMEM if k == 'v' else HBM) for k in kinds]


def call(kernel, ins, in_kinds, outs, out_kinds, scratch, copies, credits, collective_id, flops):
    return pl.pallas_call(
        kernel,
        name=kernel.__name__,
        out_shape=tuple(outs),
        in_specs=spaces(in_kinds),
        out_specs=tuple(spaces(out_kinds)),
        scratch_shapes=scratch + [sems(copies[0][0]), sems(copies[0][1]), sems(copies[1]),
                                  pltpu.SemaphoreType.REGULAR((credits,))],
        compiler_params=pltpu.CompilerParams(collective_id=collective_id, has_side_effects=True,
                                             vmem_limit_bytes=VMEM_BYTES),
        cost_estimate=pl.CostEstimate(flops=flops, bytes_accessed=1 << 24, transcendentals=0),
    )(*ins)


def call_upper_half(x0, cot, w_in, w_out):
    tokens, width = x0.shape
    inner = w_in.shape[2]
    group, slice_ = 4 * tokens, inner // 4
    w1 = (4, 4, 2, width // 32, slice_)
    w2 = (4, 4, 2, inner // 128, width)
    block = sds((tokens, width), BF16)
    acts = (group, slice_)
    ut, st = (width, group), (slice_, group)
    pair = lambda shape: sds((2,) + shape, BF16)
    outs = [block, sds((tokens, width), F32), block, sds((group, width), F32), sds(acts, BF16),
            pair(ut), pair(st), pair(ut), pair(st), pair((group, slice_ // 2)), pair((4, tokens, width // 2)),
            sds(w1, BF16), sds(w2, BF16)]
    tok = (4, tokens, width)
    scratch = [VMEM(shape, BF16) for shape in (w1, w2, w1, w2, tok, tok, acts, acts, acts, ut, st, block.shape,
                                            block.shape, block.shape)]
    scratch += [VMEM((group, width), F32), VMEM((6, tokens, width // 2), F32), VMEM(block.shape, F32)]
    return call(upper_half, (x0, cot, w_in, w_out), 'hhhh', outs, 'h' * 13, scratch, (UPPER, 37), 2, 1,
                16 * group * width * slice_)


class GradReduce:
    def __init__(self, comm, axes, operands, column, sends, landing1, landing2, result, credits, before=None):
        self.comm, self.axes, self.operands, self.column = comm, axes, operands, column
        self.sends, self.landing1, self.landing2, self.result = sends, landing1, landing2, result
        self.credits, self.before = credits, before
        self.ring = RingReduce(comm, axes[0], None, landing1, before and before.ring)
        rows = sends.shape[1] // 4
        self.block = lambda pos, h: sends.at[pos // 2, pl.ds(pl.multiple_of(((pos % 2) * 2 + h) * rows, rows), rows)]
        self.ring2 = RingReduce(comm, axes[1], self.block, landing2, before and before.ring2)

    def products(self, count, where, store):
        rows, width = self.sends.shape[1:]
        t = min(128, rows)
        per = rows // t

        def step(n, _):
            i, j = n // per, n % per
            pos, half = where(i)
            start = pl.multiple_of((pos * 2 + half) * rows + j * t, t)
            value = None
            for at, b in self.operands:
                term = dot(at[pl.ds(start, t)], b(pl.ds(self.column, width)))
                value = term if value is None else value + term
            store(i, pl.ds(pl.multiple_of(j * t, t), t), value)
            return 0

        lax.fori_loop(0, count * per, step, 0)

    def start_far(self):
        me, sends = self.ring.me, self.sends
        if self.before:
            self.before.sent()
            self.comm.wait(self.credits.at[0], self.axes[0])

        def store(i, rows, value):
            sends[i, rows] = value

        self.products(2, lambda i: ((me + 2) % 4, i), store)
        self.ring.start_far(sends.at[0], sends.at[1])

    def start_near(self):
        me, sends = self.ring.me, self.sends

        def store(i, rows, value):
            sends[2 + i, rows] = value

        self.products(2, lambda i: ((me + 1 + 2 * i) % 4, 1 - i), store)
        self.ring.start_near(sends.at[2], sends.at[3])

    def start(self):
        self.start_far()
        self.start_near()

    def middle(self):
        me, landing = self.ring.me, self.landing1
        self.ring.wait_right()
        self.ring.wait_left()

        def store(i, rows, value):
            landing[3 * i, rows] = landing[3 * i, rows] + value

        self.products(2, lambda i: ((me + 1 + 2 * i) % 4, i), store)
        self.ring.pass_right()
        self.ring.pass_left()

    def turn(self):
        me, landing, sends = self.ring.me, self.landing1, self.sends
        self.ring.finish()
        self.ring.first.wait()

        def store(i, rows, value):
            sends[i, rows] = value + landing[2 - i, rows] + landing[4 + i, rows]

        self.products(2, lambda i: (me, i), store)
        if self.before:
            self.comm.wait(self.credits.at[1], self.axes[1])
        self.ring2.start_all()

    def free1(self):
        self.ring.sent()
        self.comm.signal(self.credits.at[0], self.axes[0])

    def middle2(self):
        self.ring2.middle_right()
        self.ring2.middle_left()

    def finish(self):
        self.ring2.finish()
        n = self.result.shape[0] // 2
        self.result[0:n], self.result[n:2 * n] = self.ring2.sums()

    def sent(self):
        self.ring2.sent()

    def free2(self):
        self.sent()
        self.comm.signal(self.credits.at[1], self.axes[1])


CHUNKS = 4


def grad_buffers(width, slice_):
    out = []
    for rows, cols in ((width // 8, slice_ // 2), (slice_ // 8, width // 2)):
        w = cols // CHUNKS
        out += [VMEM((CHUNKS, 4, rows, w), F32), VMEM((CHUNKS, 6, rows, w), F32),
                VMEM((CHUNKS, 6, rows // 4, w), F32)]
    return out


def result_shapes(width, slice_):
    return [(CHUNKS, width // 16, slice_ // 2 // CHUNKS), (CHUNKS, slice_ // 16, width // 2 // CHUNKS)]


def grad_chunks(comm, operands, bufs, results, credits, before=None):
    out = []
    for k in range(CHUNKS):
        pieces = 2 if before and k == CHUNKS - 1 else 1
        for piece in range(pieces):
            both = []
            for i, axes in enumerate(('zy', 'yz')):
                width = bufs[3 * i].shape[3] // pieces
                cols = pl.ds(piece * width, width)
                sends, land1, land2 = [ref.at[k, :, :, cols] for ref in bufs[3 * i:3 * i + 3]]
                both.append(GradReduce(comm, axes, operands[i], (k * pieces + piece) * width, sends, land1, land2,
                                       results[i].at[k, :, cols], credits.at[2 * k + i],
                                       before[k].things[i] if before and piece == 0 else None))
            out.append(Every(both))
    return out


class BlockGather:
    def __init__(self, comm, own, out):
        self.comm, self.own, self.out = comm, own, out
        c = comm.c
        n = own.shape[0] // 2
        half = lambda h: pl.ds(h * n, n)
        self.ring = RingGather(comm, 'x', lambda h: own.at[half(h)], lambda p, h: out.at[p, c, half(h)],
                               own, out.at[pl.ds(0, 3), c])
        self.four = out.at[:, c]
        self.group, self.sem = Sends(comm, self.four), comm.recv_sem()

    def push(self, pos, src):
        c = self.comm
        c.send(src, self.out.at[pos, c.c], c.partner, self.group, self.sem)

    def start(self):
        self.ring.start()
        self.push(self.ring.me, self.own)
        self.kept = self.comm.local((self.own, self.out.at[self.ring.me, self.comm.c]))

    def forward(self):
        self.ring.forward()

    def near(self):
        ring, c = self.ring, self.comm.c
        ring.near()
        self.push(ring.left, self.out.at[ring.left, c])
        self.push(ring.right, self.out.at[ring.right, c])

    def finish(self):
        ring, c = self.ring, self.comm.c
        ring.finish()
        self.push(ring.far, self.out.at[ring.far, c])

    def arrived(self):
        self.comm.wait_recv(self.four, self.sem)
        done(self.kept)


def rows_from(src, dst, first):
    n = src.shape[1] // 4
    rows = [pl.ds(pl.multiple_of((first + k) % 4 * n, n), n) for k in range(4)]
    pairs = [(src.at[:, r], dst.at[:, r]) for r in rows]
    return pairs[0], pairs[1:]


def columns_from(src, dst):
    n = src.shape[-1] // CHUNKS
    return [(src.at[..., cols], dst.at[..., cols]) for cols in (pl.ds(0, n), pl.ds(n, src.shape[-1] - n))]


def lower_half(x0_hbm, x1_hbm, e1_hbm, d0, part_hbm, w1_hbm, w2_hbm, a_hbm, ut_low, st_low, ut_top, st_top, q_top, d_top,
               grad_out, x2_out, q_low, d_low, top_all_in, top_all_out, low_all_in, low_all_out,
               w, df, a, q, x0, x1, grad, x2, e1, part, landing, gut, gst, gq, gd,
               top_in, top_out, low_in, low_out, *rest):
    bufs, (send_sems, recv_sems, local_sems, credits, x_free) = rest[:6], rest[6:]
    comm = Comm(send_sems, recv_sems, local_sems)
    tokens = x0.shape[0]
    x, c = comm.x, comm.c
    group = a.shape[0]
    load_d = comm.local((d0, df.at[x]))
    far_in, rest_in = rows_from(ut_top, gut, comm.z + 2)
    far_out, rest_out = rows_from(st_top, gst, comm.y + 2)
    q_first, q_rest = columns_from(q_top, gq)
    d_first, d_rest = columns_from(d_top, gd)
    loads_in = comm.local(far_in, q_first)
    loads_out = comm.local(far_out, d_first)
    comm.arrive('xyzc')
    loads_rest = comm.local(q_rest, d_rest, *rest_in, *rest_out)
    columns = lambda ref, j: ref.at[:, pl.ds(j * group, group)]
    load_w = lambda ref: comm.local(*[(columns(ref, j), w.at[j]) for j in range(4)])
    comm.meet('xyzc')

    gather_d = ring_of_tokens(comm, df)
    done(load_d)
    gather_d.start()
    load2 = load_w(w2_hbm) + comm.local((a_hbm, a))
    load_x = comm.local((x0_hbm, x0), (e1_hbm, e1), (x1_hbm, x1))
    own_b = lambda ref: lambda cols: flat(ref[..., cols])
    top = [[(gut.at[k], own_b(gq.at[k])) for k in (0, 1)], [(gst.at[k], own_b(gd.at[k])) for k in (0, 1)]]
    upper = grad_chunks(comm, top, bufs, (top_in, top_out), credits)
    (t0i, t0o), (t1i, t1o), (t2i, t2o), (t3i, t3o) = [pair.things for pair in upper]

    def by_columns(left):
        rows = w.shape[1] // 8

        def product(i):
            value = None
            for j in range(4):
                term = dot_bt(flat(left[..., j * group:(j + 1) * group]),
                              w[j, pl.ds(pl.multiple_of(i * rows, rows), rows)])
                value = term if value is None else value + term
            return value

        return product

    done(loads_in)
    t0i.start_far()
    done(loads_out)
    t0o.start_far()
    done(loads_rest)
    t0i.start_near()
    t0o.start_near()
    top = Every([BlockGather(comm, top_in, top_all_in), BlockGather(comm, top_out, top_all_out)])
    w_in, w_out = low_in.shape[2] // 2, low_out.shape[2] // 2
    low = [(k, slice(None), slice(None)) for k in range(CHUNKS - 1)]
    low += [(CHUNKS - 1, pl.ds(h * w_in, w_in), pl.ds(h * w_out, w_out)) for h in (0, 1)]
    low = [Every([BlockGather(comm, low_in.at[k, :, i], low_all_in.at[k, :, :, :, i]),
                  BlockGather(comm, low_out.at[k, :, o], low_all_out.at[k, :, :, :, o])]) for k, i, o in low]
    (low0i, low0o), (low1i, low1o), (low2i, low2o), (low3i, low3o), (low4i, low4o) = [pair.things for pair in low]
    t3i.start()
    t1i.start()
    gather_d.forward()
    t1o.start()
    t0o.middle()
    t0i.middle()
    t3o.start()
    gather_d.near()
    t2o.start()
    gather_d.finish()
    done(load2)
    backward_acts(df, by_columns(df), a, q)
    load1 = load_w(w1_hbm)
    _, d_arrived = comm.push(last_dim_half(df, 1 - c), d_low)
    _, q_arrived = comm.push(last_dim_half(q, 1 - c), q_low)
    done(load1)
    ring = token_sums(comm, part, landing, tokens)
    product = by_columns(q)
    backward_part(product, part, 0)
    ring.start_half(0)
    backward_part(product, part, 1)
    ring.start_half(1)
    t1o.middle()
    t0o.turn()
    d_arrived()
    q_arrived()
    half = a.shape[1] // 2
    loads = comm.local(*[(ut_low.at[k], w.at[k]) for k in (0, 1)], *[(st_low.at[k], w.at[2 + k]) for k in (0, 1)],
                       (q_low, a.at[:, pl.ds(0, half)]))
    loads += comm.local(*[(d_low.at[k], a.at[pl.ds(k * tokens, tokens), pl.ds(half, half)]) for k in range(4)])
    done(loads)
    mine = lambda ref: lambda cols: flat(ref[..., pl.ds(pl.multiple_of(c * half + cols.start, cols.size), cols.size)])
    other = lambda first: lambda cols: a[:, pl.ds(first + cols.start, cols.size)]
    operands = [[(w.at[0], mine(q)), (w.at[1], other(0))], [(w.at[2], mine(df)), (w.at[3], other(half))]]
    lower = grad_chunks(comm, operands, bufs, (low_in, low_out), credits, upper)
    (g0i, g0o), (g1i, g1o), (g2i, g2o), (g3i, g3o), (g4i, g4o) = [pair.things for pair in lower]
    t0o.free1()
    t2i.start()
    t1i.middle()
    t0i.turn()
    t0i.free1()
    t3o.middle()
    t0o.middle2()
    ring.middle_right()
    t2i.middle()
    t3i.middle()
    t2o.middle()
    ring.middle_left()
    t0i.middle2()
    t1i.turn()
    t1o.turn()
    t0o.finish()
    t1i.free1()
    t1o.free1()
    t3o.turn()
    t2i.turn()
    t2i.free1()
    ring.finish()
    g = jnp.concatenate(ring.sums(), axis=1)
    done(load_x)
    grad[...] = (e1[...] + norm_rows_vjp(x0[...].astype(F32), g)).astype(BF16)
    keep = comm.local((grad, grad_out))
    ring.sent()
    comm.signal(x_free, 'x')
    load_part = comm.local((part_hbm, part))
    comm.wait(x_free, 'x')
    done(load_part)
    ring = token_sums(comm, part, landing, tokens, ring)
    ring.start_all()
    t2o.turn()
    t0i.finish()
    t0i.free2()
    t3i.turn()
    t0o.free2()
    t3i.free1()
    t2o.free1()
    t1i.middle2()
    t3o.middle2()
    t1o.middle2()
    t2i.middle2()
    t2o.middle2()
    t3o.free1()
    g0i.start()
    t3i.middle2()
    t3o.finish()
    g0o.start()
    t1i.finish()
    t2i.finish()
    t2o.finish()
    t2o.free2()
    t1o.finish()
    t3o.free2()
    t2i.free2()
    t1i.free2()
    t3i.finish()
    t3i.free2()
    t1o.free2()
    ring.middle_right()
    ring.middle_left()
    g0i.middle()
    top.start()
    g0o.middle()
    g2o.start()
    g2i.start()
    g0i.turn()
    g0o.turn()
    g1i.start()
    g1o.start()
    g0o.middle2()
    ring.finish()
    x2[...] = (x1[...].astype(F32) + jnp.concatenate(ring.sums(), axis=1)).astype(BF16)
    keep += comm.local((x2, x2_out))
    g0i.middle2()
    g2o.middle()
    g2i.middle()
    g1i.middle()
    g1o.middle()
    g3i.start()
    g0o.finish()
    low0o.start()
    g0i.finish()
    low0i.start()
    top.forward()
    top.near()
    low0o.forward()
    g2o.turn()
    g2i.turn()
    low0i.forward()
    g1i.turn()
    low0o.near()
    low0i.near()
    g2i.middle2()
    g1o.turn()
    g1i.middle2()
    g3o.start()
    g2o.middle2()
    g1i.finish()
    g2i.finish()
    low2i.start()
    g1o.middle2()
    low1i.start()
    g4i.start()
    g3o.middle()
    g2o.finish()
    g1o.finish()
    g4o.start()
    low1o.start()
    low0o.finish()
    g3i.middle()
    top.finish()
    low2o.start()
    low0i.finish()
    low2i.forward()
    low2i.near()
    low1i.forward()
    low1i.near()
    g4i.middle()
    g3o.turn()
    low1o.forward()
    g4o.middle()
    g3i.turn()
    low2o.forward()
    low2o.near()
    g4i.turn()
    g3o.middle2()
    g4o.turn()
    g3i.middle2()
    g4i.middle2()
    g3o.finish()
    low3o.start()
    low2i.finish()
    g4o.middle2()
    g3i.finish()
    low1o.near()
    low3i.start()
    g4i.finish()
    low4i.start()
    g4o.finish()
    low4o.start()
    low3o.forward()
    low3o.near()
    low2o.finish()
    low3i.forward()
    low3i.near()
    low4i.forward()
    low1i.finish()
    low4i.near()
    low1o.finish()
    low4o.forward()
    low3o.finish()
    low3i.finish()
    low4i.finish()
    low4o.near()
    low4o.finish()
    for pair in [top] + low:
        pair.arrived()
    done(keep)
    comm.end()


def call_lower_half(x0, x1, e1, d0, part_hbm, w1_hbm, w2_hbm, a_hbm, ut_low, st_low, ut_top, st_top, q_top, d_top):
    tokens, width = x0.shape
    group, slice_ = a_hbm.shape
    shapes = result_shapes(width, slice_)
    tops = [(4, 2) + shape for shape in shapes]
    lows = [(CHUNKS, 4, 2) + shape[1:] for shape in shapes]
    block = sds((tokens, width), BF16)
    outs = [block, block, sds(q_top.shape[1:], BF16), sds(d_top.shape[1:], BF16)] + [sds(s, F32) for s in tops + lows]
    acts = VMEM((group, slice_), BF16)
    scratch = [VMEM((4, width, group), BF16), VMEM((4, tokens, width), BF16), acts, acts]
    scratch += [VMEM(block.shape, BF16) for _ in range(4)] + [VMEM(block.shape, F32), VMEM((group, width), F32),
                                                              VMEM((6, tokens, width // 2), F32)]
    scratch += [VMEM(r.shape, BF16) for r in (ut_top, st_top, q_top, d_top)] + [VMEM(s, F32) for s in shapes + shapes]
    scratch += grad_buffers(width, slice_)
    ins = (x0, x1, e1, d0, part_hbm, w1_hbm.reshape(width, slice_), w2_hbm.reshape(slice_, width), a_hbm,
           ut_low, st_low, ut_top, st_top, q_top, d_top)
    return pl.pallas_call(
        lower_half,
        name='lower_half',
        out_shape=tuple(outs),
        in_specs=spaces('h' * 14),
        out_specs=tuple(spaces('h' * 8)),
        scratch_shapes=scratch + [sems(LOWER[0]), sems(LOWER[1]), sems(LOWER[2]), pltpu.SemaphoreType.REGULAR((2 * CHUNKS, 2)),
                                  pltpu.SemaphoreType.REGULAR],
        compiler_params=pltpu.CompilerParams(collective_id=2, has_side_effects=True, vmem_limit_bytes=VMEM_BYTES),
        cost_estimate=pl.CostEstimate(flops=16 * group * width * slice_, bytes_accessed=1 << 24, transcendentals=0),
    )(*ins)


def assemble(top_in, top_out, low_in, low_out, grad_in, grad_out, v_top_in, v_top_out, v_low_in, v_low_out,
             load_sems, store_sems):
    loads = []
    refs = (v_low_in, v_low_out, v_top_in, v_top_out)
    for i, src in enumerate((low_in, low_out, top_in, top_out)):
        copy = pltpu.make_async_copy(src, refs[i], load_sems.at[i])
        copy.start()
        loads.append(copy)
    strip = grad_in.shape[2] // 64
    rows, width = low_in.shape[3:]
    width_out = low_out.shape[4]
    per = width // strip
    for i, ref in enumerate(refs):
        loads[i].wait()
        layer = i // 2
        for k in range(CHUNKS):
            for x in range(4):
                for c in range(2):
                    src = ref.at[x, c, k] if layer else ref.at[k, x, c]
                    if i % 2:
                        dst = grad_out.at[layer, pl.ds(x * src.shape[0], src.shape[0]),
                                          pl.ds((c * CHUNKS + k) * width_out, width_out)]
                        pltpu.make_async_copy(src, dst, store_sems.at[1]).start()
                        continue
                    for j in range(per):
                        y, z = (c * 8 + k * per + j) // 4, (k * per + j) % 4
                        dst = grad_in.at[layer, :, pl.ds(((4 * z + y) * 4 + x) * strip, strip)]
                        pltpu.make_async_copy(src.at[:, pl.ds(j * strip, strip)], dst, store_sems.at[0]).start()
    pltpu.make_async_copy(grad_in, grad_in, store_sems.at[0]).wait()
    pltpu.make_async_copy(grad_out, grad_out, store_sems.at[1]).wait()


def call_assemble(ins, in_shape, out_shape):
    return pl.pallas_call(
        assemble,
        name='assemble',
        out_shape=(sds(in_shape, F32), sds(out_shape, F32)),
        in_specs=spaces('hhhh'),
        out_specs=tuple(spaces('hh')),
        scratch_shapes=[VMEM(r.shape, F32) for r in ins] + [sems(4), sems(2)],
        compiler_params=pltpu.CompilerParams(vmem_limit_bytes=VMEM_BYTES),
        cost_estimate=pl.CostEstimate(flops=1 << 30, bytes_accessed=1 << 25, transcendentals=0),
    )(*ins)


def solution(mesh):
    tok_spec = P(('local', 'data'), None)
    w_spec = P(None, 'local', None)

    def device_step(tokens, cotangent, w_in, w_out):
        (x1, e1, d0, part_out, a_low, ut_low, st_low, ut_top, st_top, q_top, d_top, w1_low, w2_low) = call_upper_half(
            tokens, cotangent, w_in, w_out)
        grad, x2, _, _, *gathered = call_lower_half(
            tokens, x1, e1, d0, part_out, w1_low, w2_low, a_low, ut_low, st_low, ut_top, st_top, q_top, d_top)
        grad_in, grad_out = call_assemble(gathered, w_in.shape, w_out.shape)
        return x2, grad_in, grad_out, grad

    return jax.shard_map(device_step, mesh=mesh, in_specs=(tok_spec, tok_spec, w_spec, w_spec),
                         out_specs=(tok_spec, w_spec, w_spec, tok_spec), check_vma=False)
```

```python
import functools

import jax
import jax.numpy as jnp
from jax import lax
from jax.experimental import pallas as pl
from jax.experimental.pallas import tpu as pltpu
from jax.sharding import PartitionSpec as P

EPSILON = 1e-6
GELU_SCALE = 0.7978845608028654
GELU_CUBE = 0.044715
BF16 = jnp.bfloat16
F32 = jnp.float32
MESH = pl.DeviceIdType.MESH
HBM = pltpu.HBM
VMEM = pltpu.VMEM
VMEM_BYTES = 67043328
VMEM_KEPT = 33 << 19
UPPER = (40, 95)
LOWER = (69, 116, 38)


class Comm:
    def __init__(self, send_sems, recv_sems, local_sems):
        l = lax.axis_index('local')
        d = lax.axis_index('data')
        self.l, self.d = l, d
        self.z, self.y, self.x, self.c = l // 4, l % 4, d // 2, d % 2
        self.send_sems, self.recv_sems, self.local_sems = send_sems, recv_sems, local_sems
        self.sends = self.recvs = self.local_count = 0
        self.groups = []
        self.partner = (l, self.x * 2 + 1 - self.c)

    def pos(self, axis):
        return {'x': self.x, 'y': self.y, 'z': self.z}[axis]

    def neighbor(self, axis, delta):
        p = (self.pos(axis) + delta) % 4
        if axis == 'x':
            return (self.l, p * 2 + self.c)
        if axis == 'y':
            return (self.z * 4 + p, self.d)
        return (p * 4 + self.y, self.d)

    def peers(self, axes):
        out = [self.partner] if 'c' in axes else []
        for axis in axes.replace('c', ''):
            out += [self.neighbor(axis, 1), self.neighbor(axis, 3)]
        return out

    def signal(self, sem, axes):
        for device in self.peers(axes):
            pl.semaphore_signal(sem, inc=1, device_id=device, device_id_type=MESH)

    def wait(self, sem, axes):
        pl.semaphore_wait(sem, len(self.peers(axes)))

    def arrive(self, axes):
        self.signal(pltpu.get_barrier_semaphore(), axes)

    def meet(self, axes):
        self.wait(pltpu.get_barrier_semaphore(), axes)

    def send_sem(self):
        self.sends += 1
        return self.send_sems.at[self.sends - 1]

    def recv_sem(self):
        self.recvs += 1
        return self.recv_sems.at[self.recvs - 1]

    def copy(self, src, dst, device, send_sem, recv_sem):
        return pltpu.make_async_remote_copy(src_ref=src, dst_ref=dst, send_sem=send_sem, recv_sem=recv_sem,
                                            device_id=device, device_id_type=MESH)

    def send(self, src, dst, device, group, recv_sem):
        self.copy(src, dst, device, group.sem, recv_sem).start()

    def wait_recv(self, ref, recv_sem):
        self.copy(ref, ref, self.partner, self.send_sems.at[0], recv_sem).wait_recv()

    def push(self, src, dst):
        group, recv_sem = Sends(self, src), self.recv_sem()
        self.send(src, dst, self.partner, group, recv_sem)
        return group, lambda: self.wait_recv(dst, recv_sem)

    def local(self, *pairs):
        out = []
        for src, dst in pairs:
            copy = pltpu.make_async_copy(src, dst, self.local_sems.at[self.local_count])
            copy.start()
            self.local_count += 1
            out.append(copy)
        return out

    def end(self):
        for group in self.groups:
            group.wait()


class Sends:
    def __init__(self, comm, ref, sem=None):
        self.comm, self.ref, self.sem = comm, ref, sem or comm.send_sem()
        self.waited = False
        comm.groups.append(self)

    def wait(self):
        if not self.waited:
            self.waited = True
            c = self.comm
            c.copy(self.ref, self.ref, c.partner, self.sem, c.recv_sems.at[0]).wait_send()


def done(copies):
    for copy in copies:
        copy.wait()


class Every:
    def __init__(self, things):
        self.things = things

    def __getattr__(self, step):
        def run(*args):
            for thing in self.things:
                getattr(thing, step)(*args)
        return run


class RingGather:
    def __init__(self, comm, axis, own, slot, block, three, before=None):
        self.comm, self.own, self.slot, self.block = comm, own, slot, block
        self.me = comm.pos(axis)
        self.right, self.far, self.left = [(self.me + k) % 4 for k in (1, 2, 3)]
        self.to_right, self.to_left = comm.neighbor(axis, 1), comm.neighbor(axis, 3)
        self.group = Sends(comm, three, before and before.group.sem)
        self.sems = before.sems if before else [comm.recv_sem() for _ in range(3)]

    def both(self, k, right, right_slot, left, left_slot):
        self.comm.send(right, right_slot, self.to_right, self.group, self.sems[k])
        self.comm.send(left, left_slot, self.to_left, self.group, self.sems[k])

    def start(self):
        own, slot, me = self.own, self.slot, self.me
        self.both(0, own(0), slot(me, 0), own(1), slot(me, 1))
        self.both(1, own(1), slot(me, 1), own(0), slot(me, 0))

    def forward(self):
        self.comm.wait_recv(self.block, self.sems[0])
        right, left = self.slot(self.left, 0), self.slot(self.right, 1)
        self.both(2, right, right, left, left)

    def near(self):
        self.comm.wait_recv(self.block, self.sems[1])

    def finish(self):
        self.comm.wait_recv(self.block, self.sems[2])

    def sent(self):
        self.group.wait()


class RingReduce:
    def __init__(self, comm, axis, part, landing, before=None):
        self.comm, self.part, self.landing = comm, part, landing
        self.me = comm.pos(axis)
        self.right, self.far, self.left = [(self.me + k) % 4 for k in (1, 2, 3)]
        self.to_right, self.to_left = comm.neighbor(axis, 1), comm.neighbor(axis, 3)
        self.first = Sends(comm, landing.at[pl.ds(0, 2)], before and before.first.sem)
        self.rest = Sends(comm, landing.at[pl.ds(0, 4)], before and before.rest.sem)
        self.sems = before.sems if before else [comm.recv_sem() for _ in range(3)]
        self.right_sem, self.left_sem, self.rest_sem = self.sems
        self.pair, self.quad = landing.at[pl.ds(0, 2)], landing.at[pl.ds(0, 4)]

    def right_to(self, k, src, group, sem):
        self.comm.send(src, self.landing.at[k], self.to_right, group, sem)

    def left_to(self, k, src, group, sem):
        self.comm.send(src, self.landing.at[k], self.to_left, group, sem)

    def start_far(self, far0, far1):
        self.right_to(0, far0, self.first, self.right_sem)
        self.left_to(3, far1, self.first, self.left_sem)

    def start_near(self, right1, left0):
        self.right_to(1, right1, self.rest, self.rest_sem)
        self.left_to(4, left0, self.rest, self.rest_sem)

    def start_all(self):
        part = self.part
        self.start_far(part(self.far, 0), part(self.far, 1))
        self.start_near(part(self.right, 1), part(self.left, 0))

    def start_half(self, half):
        if half == 0:
            self.right_to(0, self.part(self.far, 0), self.first, self.right_sem)
            self.left_to(4, self.part(self.left, 0), self.rest, self.rest_sem)
        else:
            self.left_to(3, self.part(self.far, 1), self.first, self.left_sem)
            self.right_to(1, self.part(self.right, 1), self.rest, self.rest_sem)

    def wait_right(self):
        self.comm.wait_recv(self.landing.at[0], self.right_sem)

    def wait_left(self):
        self.comm.wait_recv(self.landing.at[3], self.left_sem)

    def pass_right(self):
        self.right_to(2, self.landing.at[0], self.rest, self.rest_sem)

    def pass_left(self):
        self.left_to(5, self.landing.at[3], self.rest, self.rest_sem)

    def middle_right(self):
        landing = self.landing
        self.wait_right()
        landing[0] = landing[0] + self.part(self.right, 0)[...]
        self.pass_right()

    def middle_left(self):
        landing = self.landing
        self.wait_left()
        landing[3] = landing[3] + self.part(self.left, 1)[...]
        self.pass_left()

    def finish(self):
        self.comm.wait_recv(self.quad, self.rest_sem)

    def sent(self):
        self.first.wait()
        self.rest.wait()

    def sums(self):
        landing = self.landing
        return (self.part(self.me, 0)[...] + landing[2] + landing[4],
                self.part(self.me, 1)[...] + landing[1] + landing[5])


class PlaneGather:
    def __init__(self, comm, dims, first, full, cols, before=None, out=None):
        self.comm, self.out, self.kept = comm, out, []
        c = comm.c
        lead = dims[0] == first
        second = dims.replace(first, '')
        b = comm.pos(second)
        half_rows = full.shape[3] // 2
        rows = lambda h: pl.ds(h * half_rows, half_rows)
        pair = lambda h: pl.ds(2 * h, 2)
        self.b = b
        every, three, own = slice(None), pl.ds(0, 3), comm.pos(first)
        at = lambda p, q, r: full.at[(p, q, c, r, cols) if lead else (q, p, c, r, cols)]
        slot1 = lambda p, h: at(p, b, rows(h))
        slot2 = lambda p, h: at(pair(h), p, every)
        self.ring1 = RingGather(comm, first, lambda h: slot1(own, h), slot1, at(own, b, every), at(three, b, every),
                                before and before.ring1)
        self.ring2 = RingGather(comm, second, lambda h: slot2(b, h), slot2, at(every, b, every), at(every, three, every),
                                before and before.ring2)
        self.line = lambda p, ref=full: ref.at[(every, p, c, every, cols) if lead else (p, every, c, every, cols)]
        self.whole, self.near_lines = at(every, every, every), at(every, three, every)
        self.group = Sends(comm, self.whole, before and before.group.sem)
        self.sems = before.sems if before else [comm.recv_sem(), comm.recv_sem()]

    def push(self, p, k=0):
        line = self.line(p)
        target = line if self.out is None else self.line(p, self.out)
        self.comm.send(line, target, self.comm.partner, self.group, self.sems[k])
        if self.out is not None:
            self.kept += self.comm.local((line, target))

    def start1(self):
        self.ring1.start()

    def forward1(self):
        self.ring1.forward()

    def start2(self):
        self.ring1.near()
        self.ring1.finish()
        self.ring2.start()
        self.push(self.b)

    def forward2(self):
        self.ring2.forward()

    def near2(self):
        self.ring2.near()
        self.push(self.ring2.left)
        self.push(self.ring2.right)

    def finish2(self):
        self.ring2.finish()
        self.push(self.ring2.far, 1)

    def arrived(self):
        self.comm.wait_recv(self.near_lines, self.sems[0])
        self.comm.wait_recv(self.line(self.b), self.sems[1])
        done(self.kept)

    def sent(self):
        self.ring1.sent()
        self.ring2.sent()
        self.group.wait()


def gathers(comm, dims, full, pieces, before=None, out=None):
    width = full.shape[4] // pieces
    out = [PlaneGather(comm, dims, dims[k % 2], full, pl.ds(k * width, width), before and before.things[k], out)
           for k in range(pieces)]
    return [Every(out[k:k + 2]) for k in range(0, pieces, 2)]


def own_blocks(comm, w_in, w_out, layer, w1, w2):
    z, y, x, c = comm.z, comm.y, comm.x, comm.c
    width = w_in.shape[2] // 64
    rows1, rows2 = w1.shape[3], w2.shape[3]
    own = w1.at[z, y, c]
    k = comm.local_count
    comm.local_count += 1
    for j in range(16):
        start = (4 * (j % 4) + j // 4) * 4 * width + x * width
        pltpu.make_async_copy(w_in.at[layer, pl.ds(c * rows1, rows1), pl.ds(pl.multiple_of(start, width), width)],
                              own.at[:, pl.ds(j * width, width)], comm.local_sems.at[k]).start()
    start = (x * 2 + c) * rows2
    copies = comm.local((w_out.at[layer, pl.ds(pl.multiple_of(start, rows2), rows2)], w2.at[y, z, c]))
    return [pltpu.make_async_copy(own, own, comm.local_sems.at[k])] + copies


def ring_of_tokens(comm, full, before=None):
    n = full.shape[1] // 2
    slot = lambda p, h: full.at[p, pl.ds(h * n, n)]
    return RingGather(comm, 'x', lambda h: slot(comm.x, h), slot, full.at[0], full.at[pl.ds(0, 3)], before)


def token_sums(comm, part, landing, tokens, before=None):
    width = part.shape[1] // 2
    block = lambda pos, half: part.at[pl.ds(pl.multiple_of(pos * tokens, tokens), tokens), pl.ds(half * width, width)]
    return RingReduce(comm, 'x', block, landing, before)


def norm_rows(x):
    return x * lax.rsqrt(jnp.mean(x * x, axis=-1, keepdims=True) + EPSILON)


def norm_rows_vjp(x, g):
    r = lax.rsqrt(jnp.mean(x * x, axis=-1, keepdims=True) + EPSILON)
    dot = jnp.mean(x * g, axis=-1, keepdims=True)
    return r * g - x * (r * r * r * dot)


def gelu(x):
    t = jnp.tanh(GELU_SCALE * (x + GELU_CUBE * (x * x * x)))
    return x * (0.5 * (1.0 + t))


def gelu_grad(x):
    x2 = x * x
    t = jnp.tanh(GELU_SCALE * (x + GELU_CUBE * (x2 * x)))
    return 0.5 * (1.0 + t) + (0.5 * x) * (1.0 - t * t) * (GELU_SCALE * (1.0 + (3.0 * GELU_CUBE) * x2))


def dot(a, b):
    return lax.dot_general(a, b, (((1,), (0,)), ((), ())), preferred_element_type=F32)


def dot_bt(a, b):
    return lax.dot_general(a, b, (((1,), (1,)), ((), ())), preferred_element_type=F32)


def flat(value):
    return value.reshape(-1, value.shape[-1])


def tiles(n, step, tile=256):
    t = min(tile, n)

    def run(i, _):
        step(pl.ds(pl.multiple_of(i * t, t), t))
        return 0

    lax.fori_loop(0, n // t, run, 0)


def forward_acts(u, w1, a, s, st):
    def step(cols):
        acc = dot(flat(u[...]), flat(w1[:, :, :, :, cols])).astype(BF16)
        a[:, cols] = acc
        value = gelu(acc.astype(F32)).astype(BF16)
        s[:, cols] = value
        st[cols, :] = value.T

    tiles(a.shape[1], step)


def transposed(u, ut):
    def step(cols):
        ut[cols, :] = flat(u[:, :, cols]).T

    tiles(ut.shape[0], step)


def forward_part(s, w2, part, half):
    width = part.shape[1] // 2
    t = min(256, width)

    def run(i, _):
        cols = pl.ds(pl.multiple_of(half * width + i * t, t), t)
        part[:, cols] = dot(s[...], flat(w2[:, :, :, :, cols]))
        return 0

    lax.fori_loop(0, width // t, run, 0)


def row_tile(w, i):
    return flat(w[i // 2, pl.ds((i % 2) * 2, 2)])


def backward_acts(d, tile_product, a, q):
    rows = a.shape[1] // 8

    def step(i, _):
        cols = pl.ds(pl.multiple_of(i * rows, rows), rows)
        q[:, cols] = (tile_product(i) * gelu_grad(a[:, cols].astype(F32))).astype(BF16)
        return 0

    lax.fori_loop(0, 8, step, 0)


def backward_part(tile_product, part, half):
    rows = part.shape[1] // 8

    def step(j, _):
        i = half * 4 + j
        part[:, pl.ds(pl.multiple_of(i * rows, rows), rows)] = tile_product(i)
        return 0

    lax.fori_loop(0, 4, step, 0)


def last_dim_half(ref, k):
    width = ref.shape[-1] // 2
    return ref.at[..., pl.ds(pl.multiple_of(k * width, width), width)]


def upper_half(x0_hbm, cot, w_in, w_out,
               x1_out, e1_out, d0_out, part_out, a_low, ut_low, st_low, ut_top, st_top, q_top, d_top, w1_low, w2_low,
               p1, p2, q1, q2, uf, df, a, s, q, ut, st, x0, x1, d0, part, landing, e1,
               send_sems, recv_sems, local_sems, credits):
    comm = Comm(send_sems, recv_sems, local_sems)
    tokens = x0.shape[0]
    x, c = comm.x, comm.c
    p_free, q_free = credits.at[0], credits.at[1]

    comm.arrive('xyzc')
    load_x = comm.local((x0_hbm, x0))
    own0 = own_blocks(comm, w_in, w_out, 0, p1, p2)
    load_d = comm.local((cot, df.at[x]))
    own1 = own_blocks(comm, w_in, w_out, 1, q1, q2)
    done(load_x)
    uf[x] = norm_rows(x0[...].astype(F32)).astype(BF16)
    comm.meet('xyzc')

    gather_u = ring_of_tokens(comm, uf)
    gather_d = ring_of_tokens(comm, df)
    g1, = gathers(comm, 'zy', p1, 2)
    g2, g3 = gathers(comm, 'yz', p2, 4)
    n1, = gathers(comm, 'zy', q1, 2)
    n2, = gathers(comm, 'yz', q2, 2)
    done(own0 + load_d)
    g2.start1()
    gather_u.start()
    g1.start1()
    done(own1)
    g2.forward1()
    g3.start1()
    g1.forward1()
    g2.start2()
    g3.forward1()
    gather_u.forward()
    gather_d.start()
    g1.start2()
    gather_u.near()
    gather_u.finish()
    g1.forward2()
    g2.forward2()
    n2.start1()
    g2.near2()
    g3.start2()
    gather_d.forward()
    n1.start1()
    transposed(uf, ut)
    pushed = [comm.push(ut, ut_low.at[1])]
    kept = comm.local((ut, ut_low.at[0]))
    g1.near2()
    gather_d.near()
    g1.finish2()
    g2.finish2()
    gather_d.finish()
    g1.arrived()
    forward_acts(uf, p1, a, s, st)
    n2.forward1()
    g3.forward2()
    g2.arrived()
    gather_u.sent()
    ring = token_sums(comm, part, landing, tokens)
    forward_part(s, p2, part, 0)
    ring.start_half(0)
    n1.forward1()
    pushed += [comm.push(st, st_low.at[1])]
    kept += comm.local((st, st_low.at[0]), (a, a_low))
    g3.near2()
    pushed += [comm.push(last_dim_half(df, 1 - c), d_top.at[1])]
    kept_d = comm.local((last_dim_half(df, c), d_top.at[0]))
    n2.start2()
    g3.finish2()
    g3.arrived()
    forward_part(s, p2, part, 1)
    ring.start_half(1)
    g1.sent()
    g2.sent()
    g3.sent()
    comm.signal(p_free, 'yzc')
    own2 = own_blocks(comm, w_in, w_out, 1, p1, p2)
    b1, = gathers(comm, 'zy', p1, 2, g1)
    b2, = gathers(comm, 'yz', p2, 2, g2)
    done(own2)
    comm.wait(p_free, 'yzc')
    b1.start1()
    b2.start1()
    n1.start2()
    n2.forward2()
    ring.middle_right()
    n2.near2()
    b2.forward1()
    b1.forward1()
    ring.middle_left()
    n1.forward2()
    n1.near2()
    ring.finish()
    x_next = (x0[...].astype(F32) + jnp.concatenate(ring.sums(), axis=1)).astype(BF16)
    x1[...] = x_next
    keep_x = comm.local((x1, x1_out))
    uf[x] = norm_rows(x_next.astype(F32)).astype(BF16)
    ring.sent()
    gather_v = ring_of_tokens(comm, uf, gather_u)
    gather_v.start()
    n2.finish2()
    done(kept)
    pushed[0][0].wait()
    pushed[1][0].wait()
    b2.start2()
    n2.arrived()
    n1.finish2()
    gather_v.forward()
    n1.arrived()
    b2.forward2()
    gather_v.near()
    b1.start2()
    b2.near2()
    gather_v.finish()
    forward_acts(uf, q1, a, s, st)
    b2.finish2()
    forward_part(s, q2, part, 0)
    forward_part(s, q2, part, 1)
    keep_part = comm.local((part, part_out))
    b1.forward2()
    n1.sent()
    n2.sent()
    comm.signal(q_free, 'yzc')
    own3 = own_blocks(comm, w_in, w_out, 0, q1, q2)
    l1, = gathers(comm, 'zy', q1, 2, n1, w1_low)
    l2, = gathers(comm, 'yz', q2, 2, n2, w2_low)
    b2.arrived()
    done(own3)
    comm.wait(q_free, 'yzc')
    l2.start1()
    b1.near2()
    backward_acts(df, lambda i: dot_bt(flat(df[...]), row_tile(p2, i)), a, q)
    b1.finish2()
    l2.forward1()
    l1.start1()
    transposed(uf, ut)
    pushed += [comm.push(ut, ut_top.at[1]), comm.push(st, st_top.at[1])]
    kept = kept_d + comm.local((ut, ut_top.at[0]), (st, st_top.at[0]))
    pushed += [comm.push(last_dim_half(q, 1 - c), q_top.at[1])]
    kept += comm.local((last_dim_half(q, c), q_top.at[0]))
    b1.arrived()
    done(keep_part)
    ring = token_sums(comm, part, landing, tokens, ring)
    product = lambda i: dot_bt(q[...], row_tile(p1, i))
    backward_part(product, part, 0)
    ring.start_half(0)
    l1.forward1()
    l2.start2()
    backward_part(product, part, 1)
    ring.start_half(1)
    l2.forward2()
    l1.start2()
    ring.middle_right()
    l2.near2()
    l2.finish2()
    ring.middle_left()
    l1.forward2()
    l2.arrived()
    l1.near2()
    l1.finish2()
    ring.finish()
    g = jnp.concatenate(ring.sums(), axis=1)
    e = df[x].astype(F32) + norm_rows_vjp(x1[...].astype(F32), g)
    e1[...] = e
    d0[...] = e.astype(BF16)
    kept += keep_x + comm.local((e1, e1_out), (d0, d0_out))
    l1.arrived()
    for _, arrived in pushed:
        arrived()
    done(kept)
    comm.end()


def sds(shape, dtype):
    return jax.ShapeDtypeStruct(shape, dtype)


def sems(n):
    return pltpu.SemaphoreType.DMA((n,))


def spaces(kinds):
    return [pl.BlockSpec(memory_space=VMEM if k == 'v' else HBM) for k in kinds]


def call(kernel, ins, in_kinds, outs, out_kinds, scratch, copies, credits, collective_id, flops):
    return pl.pallas_call(
        kernel,
        name=kernel.__name__,
        out_shape=tuple(outs),
        in_specs=spaces(in_kinds),
        out_specs=tuple(spaces(out_kinds)),
        scratch_shapes=scratch + [sems(copies[0][0]), sems(copies[0][1]), sems(copies[1]),
                                  pltpu.SemaphoreType.REGULAR((credits,))],
        compiler_params=pltpu.CompilerParams(collective_id=collective_id, has_side_effects=True,
                                             vmem_limit_bytes=VMEM_BYTES),
        cost_estimate=pl.CostEstimate(flops=flops, bytes_accessed=1 << 24, transcendentals=0),
    )(*ins)


def call_upper_half(x0, cot, w_in, w_out):
    tokens, width = x0.shape
    inner = w_in.shape[2]
    group, slice_ = 4 * tokens, inner // 4
    w1 = (4, 4, 2, width // 32, slice_)
    w2 = (4, 4, 2, inner // 128, width)
    block = sds((tokens, width), BF16)
    acts = (group, slice_)
    ut, st = (width, group), (slice_, group)
    pair = lambda shape: sds((2,) + shape, BF16)
    outs = [block, sds((tokens, width), F32), block, sds((group, width), F32), sds(acts, BF16),
            pair(ut), pair(st), pair(ut), pair(st), pair((group, slice_ // 2)), pair((4, tokens, width // 2)),
            sds(w1, BF16), sds(w2, BF16)]
    tok = (4, tokens, width)
    scratch = [VMEM(shape, BF16) for shape in (w1, w2, w1, w2, tok, tok, acts, acts, acts, ut, st, block.shape,
                                            block.shape, block.shape)]
    scratch += [VMEM((group, width), F32), VMEM((6, tokens, width // 2), F32), VMEM(block.shape, F32)]
    return call(upper_half, (x0, cot, w_in, w_out), 'hhhh', outs, 'h' * 13, scratch, (UPPER, 37), 2, 1,
                16 * group * width * slice_)


class GradReduce:
    def __init__(self, comm, axes, operands, column, sends, landing1, landing2, result, credits, before=None, unused=None):
        self.comm, self.axes, self.operands, self.column = comm, axes, operands, column
        self.sends, self.landing1, self.landing2, self.result = sends, landing1, landing2, result
        self.credits, self.before, self.unused = credits, before, unused
        self.ring = RingReduce(comm, axes[0], None, landing1, before and before.ring)
        half = sends.shape[2] // 2
        self.block = lambda pos, h: sends.at[pos // 2, pos % 2, pl.ds(h * half, half)]
        self.ring2 = RingReduce(comm, axes[1], self.block, landing2, before and before.ring2)

    def products(self, where, store):
        rows, width = self.sends.shape[2:]

        def step(n, _):
            i, j = n // 2, n % 2
            pos, half = where(i)
            start = pl.multiple_of(((pos * 2 + half) * 2 + j) * rows, rows)
            value = None
            for at, b in self.operands:
                term = dot(at[pl.ds(start, rows)], b(pl.ds(self.column, width)))
                value = term if value is None else value + term
            store(i, j, value)
            return 0

        lax.fori_loop(0, 4, step, 0)

    def start_far(self):
        me, sends = self.ring.me, self.sends
        if self.before:
            self.before.sent()
            self.comm.wait(self.credits.at[0], self.axes[0])

        def store(i, j, value):
            sends[i, j] = value

        self.products(lambda i: ((me + 2) % 4, i), store)
        self.ring.start_far(sends.at[0], sends.at[1])

    def start_near(self):
        me, sends = self.ring.me, self.sends

        def store(i, j, value):
            sends[2 + i, j] = value

        self.products(lambda i: ((me + 1 + 2 * i) % 4, 1 - i), store)
        self.ring.start_near(sends.at[2], sends.at[3])

    def start(self):
        self.start_far()
        self.start_near()

    def middle(self):
        me, landing = self.ring.me, self.landing1
        self.ring.wait_right()
        self.ring.wait_left()

        def store(i, j, value):
            landing[3 * i, j] = landing[3 * i, j] + value

        self.products(lambda i: ((me + 1 + 2 * i) % 4, i), store)
        self.ring.pass_right()
        self.ring.pass_left()

    def turn(self):
        me, landing, sends = self.ring.me, self.landing1, self.sends
        self.ring.finish()
        self.ring.first.wait()

        def store(i, j, value):
            sends[i, j] = value + landing[2 - i, j] + landing[4 + i, j]

        self.products(lambda i: (me, i), store)
        if self.before:
            self.comm.wait(self.credits.at[1], self.axes[1])
        self.ring2.start_all()
        if self.unused is not None:
            self.ring.sent()
            self.comm.signal(self.unused, 'xc')

    def free1(self):
        self.ring.sent()
        self.comm.signal(self.credits.at[0], self.axes[0])

    def middle2(self):
        self.ring2.middle_right()
        self.ring2.middle_left()

    def finish(self):
        self.ring2.finish()
        n = self.result.shape[0] // 2
        self.result[0:n], self.result[n:2 * n] = self.ring2.sums()

    def sent(self):
        self.ring2.sent()

    def free2(self):
        self.sent()
        self.comm.signal(self.credits.at[1], self.axes[1])


CHUNKS = 4


def grad_shapes(width, slice_):
    return (width // 16, slice_ // 2 // CHUNKS), (slice_ // 16, width // 2 // CHUNKS)


def grad_chunks(comm, operands, bufs, results, credits, before=None, unused=None):
    out = []
    for k in range(CHUNKS):
        pieces = 2 if before and k == CHUNKS - 1 else 1
        for piece in range(pieces):
            both = []
            for i, axes in enumerate(('zy', 'yz')):
                width = bufs[3 * i].shape[4] // pieces
                cols = pl.ds(piece * width, width)
                sends, land1 = [ref.at[k, :, :, :, cols] for ref in bufs[3 * i:3 * i + 2]]
                land2 = bufs[3 * i + 2].at[k, :, :, cols]
                both.append(GradReduce(comm, axes, operands[i], (k * pieces + piece) * width, sends, land1, land2,
                                       results(i, k, cols), credits.at[2 * k + i],
                                       before[k].things[i] if before and piece == 0 else None,
                                       unused.at[k + piece, i] if before else None))
            out.append(Every(both))
    return out


class BlockGather:
    def __init__(self, comm, own, view, count, unused=None):
        self.comm, self.own, self.view, self.unused = comm, own, view, unused
        c = comm.c
        n = own.shape[0] // 2
        half = lambda h: pl.ds(h * n, n)
        self.ring = RingGather(comm, 'x', lambda h: own.at[half(h)], lambda p, h: view(p, c).at[half(h)], own, count(3))
        self.four = count(4)
        self.group, self.sem = Sends(comm, self.four), comm.recv_sem()
        self.kept = []

    def push(self, pos, src):
        c = self.comm
        c.send(src, self.view(pos, c.c), c.partner, self.group, self.sem)

    def start(self):
        here = self.view(self.ring.me, self.comm.c)
        if self.unused is None:
            self.kept = self.comm.local((self.own, here))
        else:
            self.comm.wait(self.unused, 'xc')
            here[...] = self.own[...]
        self.ring.start()
        self.push(self.ring.me, self.own)

    def forward(self):
        self.ring.forward()

    def near(self):
        ring, c = self.ring, self.comm.c
        ring.near()
        self.push(ring.left, self.view(ring.left, c))
        self.push(ring.right, self.view(ring.right, c))

    def finish(self):
        ring, c = self.ring, self.comm.c
        ring.finish()
        self.push(ring.far, self.view(ring.far, c))

    def arrived(self):
        self.comm.wait_recv(self.four, self.sem)
        done(self.kept)


def rows_from(src, dst, first):
    n = src.shape[1] // 4
    rows = [pl.ds(pl.multiple_of((first + k) % 4 * n, n), n) for k in range(4)]
    pairs = [(src.at[:, r], dst.at[:, r]) for r in rows]
    return pairs[0], pairs[1:]


def columns_from(src, dst):
    n = src.shape[-1] // CHUNKS
    return [(src.at[..., cols], dst.at[..., cols]) for cols in (pl.ds(0, n), pl.ds(n, src.shape[-1] - n))]


def lower_half(x0_hbm, x1_hbm, e1_hbm, d0, part_hbm, w1_hbm, w2_hbm, a_hbm, ut_low, st_low, ut_top, st_top, q_top, d_top,
               grad_out, x2_out, q_low, d_low, top_all_in, landed_in, landed_out, part,
               w, df, a, q, x0, x1, grad, x2, e1, landing, gut, gst, gq, gd, top_in, top_out, low_in, low_out,
               sends_in, sends_out, landing2_in, landing2_out,
               send_sems, recv_sems, local_sems, credits, x_free, part_free, unused):
    bufs = sends_in, landed_in, landing2_in, sends_out, landed_out, landing2_out
    comm = Comm(send_sems, recv_sems, local_sems)
    tokens = x0.shape[0]
    x, c = comm.x, comm.c
    group = a.shape[0]
    load_d = comm.local((d0, df.at[x]))
    far_in, rest_in = rows_from(ut_top, gut, comm.z + 2)
    far_out, rest_out = rows_from(st_top, gst, comm.y + 2)
    q_first, q_rest = columns_from(q_top, gq)
    d_first, d_rest = columns_from(d_top, gd)
    loads_in = comm.local(far_in, q_first)
    loads_out = comm.local(far_out, d_first)
    comm.arrive('xyzc')
    loads_rest = comm.local(q_rest, d_rest, *rest_in, *rest_out)
    columns = lambda ref, j: ref.at[:, pl.ds(j * group, group)]
    load_w = lambda ref: comm.local(*[(columns(ref, j), w.at[j]) for j in range(4)])
    comm.meet('xyzc')

    gather_d = ring_of_tokens(comm, df)
    done(load_d)
    gather_d.start()
    load2 = load_w(w2_hbm) + comm.local((a_hbm, a))
    load_x = comm.local((x0_hbm, x0), (e1_hbm, e1), (x1_hbm, x1))
    own_b = lambda ref: lambda cols: flat(ref[..., cols])
    top = [[(gut.at[k], own_b(gq.at[k])) for k in (0, 1)], [(gst.at[k], own_b(gd.at[k])) for k in (0, 1)]]
    chunk_out = low_out.shape[2]
    top_results = lambda i, k, cols: top_out.at[:, pl.ds(k * chunk_out, chunk_out)] if i else top_in.at[k]
    upper = grad_chunks(comm, top, bufs, top_results, credits)
    (t0i, t0o), (t1i, t1o), (t2i, t2o), (t3i, t3o) = [pair.things for pair in upper]

    def by_columns(left):
        rows = w.shape[1] // 8

        def product(i):
            value = None
            for j in range(4):
                term = dot_bt(flat(left[..., j * group:(j + 1) * group]),
                              w[j, pl.ds(pl.multiple_of(i * rows, rows), rows)])
                value = term if value is None else value + term
            return value

        return product

    done(loads_in)
    t0i.start_far()
    done(loads_out)
    t0o.start_far()
    done(loads_rest)
    t0i.start_near()
    t0o.start_near()
    topi = BlockGather(comm, top_in, lambda p, core: top_all_in.at[p, core], lambda n: top_all_in.at[pl.ds(0, n), 0])
    rows, width = top_out.shape
    topo = BlockGather(comm, top_out, lambda p, core: part.at[pl.ds(pl.multiple_of(p * rows, rows), rows),
                                                              pl.ds(pl.multiple_of(core * width, width), width)],
                       lambda n: part.at[pl.ds(0, n * rows), pl.ds(0, width)], part_free)

    def low_gather(k, piece, pieces, i):
        res, landed = (low_out, landed_out) if i else (low_in, landed_in)
        n = res.shape[2] // pieces
        cols = pl.ds(piece * n, n)
        return BlockGather(comm, res.at[k, :, cols], lambda p, core: landed.at[k, p, core, :, cols],
                           lambda m: landed.at[k, pl.ds(0, m), 0, :, cols], unused.at[k + piece, i])

    last = CHUNKS - 1
    low = [(k, 0, 1) for k in range(last)] + [(last, 0, 2), (last, 1, 2)]
    low = [Every([low_gather(*piece, i) for i in (0, 1)]) for piece in low]
    (low0i, low0o), (low1i, low1o), (low2i, low2o), (low3i, low3o), (low4i, low4o) = [pair.things for pair in low]
    t3i.start()
    t1i.start()
    gather_d.forward()
    t1o.start()
    t0o.middle()
    t0i.middle()
    t3o.start()
    gather_d.near()
    t2o.start()
    gather_d.finish()
    done(load2)
    backward_acts(df, by_columns(df), a, q)
    load1 = load_w(w1_hbm)
    _, d_arrived = comm.push(last_dim_half(df, 1 - c), d_low)
    _, q_arrived = comm.push(last_dim_half(q, 1 - c), q_low)
    done(load1)
    ring = token_sums(comm, part, landing, tokens)
    product = by_columns(q)
    backward_part(product, part, 0)
    ring.start_half(0)
    backward_part(product, part, 1)
    ring.start_half(1)
    t1o.middle()
    t0o.turn()
    d_arrived()
    q_arrived()
    half = a.shape[1] // 2
    loads = comm.local(*[(ut_low.at[k], w.at[k]) for k in (0, 1)], *[(st_low.at[k], w.at[2 + k]) for k in (0, 1)],
                       (q_low, a.at[:, pl.ds(0, half)]))
    loads += comm.local(*[(d_low.at[k], a.at[pl.ds(k * tokens, tokens), pl.ds(half, half)]) for k in range(4)])
    done(loads)
    mine = lambda ref: lambda cols: flat(ref[..., pl.ds(pl.multiple_of(c * half + cols.start, cols.size), cols.size)])
    other = lambda first: lambda cols: a[:, pl.ds(first + cols.start, cols.size)]
    operands = [[(w.at[0], mine(q)), (w.at[1], other(0))], [(w.at[2], mine(df)), (w.at[3], other(half))]]
    low_results = lambda i, k, cols: (low_out if i else low_in).at[k, :, cols]
    lower = grad_chunks(comm, operands, bufs, low_results, credits, upper, unused)
    (g0i, g0o), (g1i, g1o), (g2i, g2o), (g3i, g3o), (g4i, g4o) = [pair.things for pair in lower]
    t0o.free1()
    t2i.start()
    t1i.middle()
    t0i.turn()
    t0i.free1()
    t3o.middle()
    t0o.middle2()
    ring.middle_right()
    t2i.middle()
    t3i.middle()
    t2o.middle()
    ring.middle_left()
    t0i.middle2()
    t1i.turn()
    t1o.turn()
    t0o.finish()
    t1i.free1()
    t1o.free1()
    t3o.turn()
    t2i.turn()
    t2i.free1()
    ring.finish()
    g = jnp.concatenate(ring.sums(), axis=1)
    done(load_x)
    grad[...] = (e1[...] + norm_rows_vjp(x0[...].astype(F32), g)).astype(BF16)
    keep = comm.local((grad, grad_out))
    ring.sent()
    comm.signal(x_free, 'x')
    load_part = comm.local((part_hbm, part))
    comm.wait(x_free, 'x')
    done(load_part)
    ring = token_sums(comm, part, landing, tokens, ring)
    ring.start_all()
    t2o.turn()
    t0i.finish()
    t0i.free2()
    t3i.turn()
    t0o.free2()
    t3i.free1()
    t2o.free1()
    t3o.free1()
    t1i.middle2()
    t3o.middle2()
    t1o.middle2()
    t2i.middle2()
    t2o.middle2()
    g0i.start()
    t3i.middle2()
    t3o.finish()
    g0o.start()
    t1i.finish()
    t2i.finish()
    t2o.finish()
    t2o.free2()
    t1o.finish()
    t3o.free2()
    t2i.free2()
    t1i.free2()
    t3i.finish()
    t3i.free2()
    t1o.free2()
    ring.middle_right()
    ring.middle_left()
    g0i.middle()
    topi.start()
    g0o.middle()
    g2o.start()
    g2i.start()
    g0i.turn()
    g0o.turn()
    g1i.start()
    g1o.start()
    g0o.middle2()
    ring.finish()
    x2[...] = (x1[...].astype(F32) + jnp.concatenate(ring.sums(), axis=1)).astype(BF16)
    keep += comm.local((x2, x2_out))
    ring.sent()
    comm.signal(part_free, 'xc')
    topo.start()
    g0i.middle2()
    g2o.middle()
    g2i.middle()
    g1i.middle()
    g1o.middle()
    g3i.start()
    g0o.finish()
    low0o.start()
    g0i.finish()
    low0i.start()
    topi.forward()
    topo.forward()
    topi.near()
    low0o.forward()
    topo.near()
    g2o.turn()
    g2i.turn()
    low0i.forward()
    g1i.turn()
    low0o.near()
    low0i.near()
    g2i.middle2()
    g1o.turn()
    g1i.middle2()
    g3o.start()
    g2o.middle2()
    g2i.finish()
    low2i.start()
    g1o.middle2()
    g1i.finish()
    low1i.start()
    g4i.start()
    g3o.middle()
    g2o.finish()
    g1o.finish()
    g4o.start()
    low1o.start()
    low0o.finish()
    g3i.middle()
    topi.finish()
    topo.finish()
    low2o.start()
    low0i.finish()
    low2i.forward()
    low2i.near()
    low1i.forward()
    low1i.near()
    g4i.middle()
    g3o.turn()
    low1o.forward()
    g4o.middle()
    g3i.turn()
    low2o.forward()
    low2o.near()
    g4i.turn()
    g3o.middle2()
    g4o.turn()
    g3i.middle2()
    g4i.middle2()
    g3o.finish()
    low3o.start()
    low2i.finish()
    g4o.middle2()
    g3i.finish()
    low1o.near()
    low3i.start()
    g4i.finish()
    low4i.start()
    g4o.finish()
    low4o.start()
    low3o.forward()
    low3o.near()
    low2o.finish()
    low3i.forward()
    low3i.near()
    low4i.forward()
    low1i.finish()
    low4i.near()
    low1o.finish()
    low4o.forward()
    low3o.finish()
    low3i.finish()
    low4i.finish()
    low4o.near()
    low4o.finish()
    for pair in [topi, topo] + low:
        pair.arrived()
    done(keep)
    comm.end()


def call_lower_half(x0, x1, e1, d0, part_hbm, w1_hbm, w2_hbm, a_hbm, ut_low, st_low, ut_top, st_top, q_top, d_top):
    tokens, width = x0.shape
    group, slice_ = a_hbm.shape
    block = sds((tokens, width), BF16)
    shapes = grad_shapes(width, slice_)
    landed = [VMEM((CHUNKS, 6, 2) + shape, F32) for shape in shapes]
    (rows_in, cols_in), (rows_out, cols_out) = shapes
    outs = [block, block, sds(q_top.shape[1:], BF16), sds(d_top.shape[1:], BF16),
            sds((4, 2, CHUNKS, rows_in, cols_in), F32)] + landed + [VMEM((group, width), F32)]
    acts = VMEM((group, slice_), BF16)
    scratch = [VMEM((4, width, group), BF16), VMEM((4, tokens, width), BF16), acts, acts]
    scratch += [VMEM(block.shape, BF16) for _ in range(4)] + [VMEM(block.shape, F32), VMEM((6, tokens, width // 2), F32)]
    scratch += [VMEM(r.shape, BF16) for r in (ut_top, st_top, q_top, d_top)]
    scratch += [VMEM(shape, F32) for shape in ((CHUNKS, rows_in, cols_in), (rows_out, CHUNKS * cols_out),
                                               (CHUNKS, rows_in, cols_in), (CHUNKS, rows_out, cols_out))]
    scratch += [VMEM((CHUNKS, 4, 2) + shape, F32) for shape in shapes]
    scratch += [VMEM((CHUNKS, 6, rows // 2, cols), F32) for rows, cols in shapes]
    ins = (x0, x1, e1, d0, part_hbm, w1_hbm.reshape(width, slice_), w2_hbm.reshape(slice_, width), a_hbm,
           ut_low, st_low, ut_top, st_top, q_top, d_top)
    return pl.pallas_call(
        lower_half,
        name='lower_half',
        out_shape=tuple(outs),
        in_specs=spaces('h' * 14),
        out_specs=tuple(spaces('hhhhhvvv')),
        scratch_shapes=scratch + [sems(LOWER[0]), sems(LOWER[1]), sems(LOWER[2]), pltpu.SemaphoreType.REGULAR((2 * CHUNKS, 2)),
                                  pltpu.SemaphoreType.REGULAR, pltpu.SemaphoreType.REGULAR,
                                  pltpu.SemaphoreType.REGULAR((CHUNKS + 1, 2))],
        compiler_params=pltpu.CompilerParams(collective_id=2, has_side_effects=True,
                                             vmem_limit_bytes=VMEM_BYTES - VMEM_KEPT),
        cost_estimate=pl.CostEstimate(flops=16 * group * width * slice_, bytes_accessed=1 << 24, transcendentals=0),
    )(*ins)


def assemble(landed_in, landed_out, part, top_in, grad_in, grad_out, v_top_in, load_sem, store_sems):
    load = pltpu.make_async_copy(top_in, v_top_in, load_sem)
    load.start()
    strip = grad_in.shape[2] // 64
    rows, width = landed_out.shape[-2:]
    per = landed_in.shape[-1] // strip

    def store_in(layer, block):
        for x in range(4):
            for n in range(2 * CHUNKS):
                c, k = n // CHUNKS, n % CHUNKS
                for j in range(per):
                    t = k * per + j
                    y, z = 2 * c + t // 4, t % 4
                    dst = grad_in.at[layer, :, pl.ds(((4 * z + y) * 4 + x) * strip, strip)]
                    pltpu.make_async_copy(block(x, c, k).at[:, pl.ds(j * strip, strip)], dst, store_sems.at[0]).start()

    pltpu.make_async_copy(part, grad_out.at[1], store_sems.at[1]).start()
    store_in(0, lambda x, c, k: landed_in.at[k, x, c])
    for x in range(4):
        for n in range(2 * CHUNKS):
            dst = grad_out.at[0, pl.ds(x * rows, rows), pl.ds(n * width, width)]
            pltpu.make_async_copy(landed_out.at[n % CHUNKS, x, n // CHUNKS], dst, store_sems.at[1]).start()
    load.wait()
    store_in(1, lambda x, c, k: v_top_in.at[x, c, k])
    pltpu.make_async_copy(grad_in, grad_in, store_sems.at[0]).wait()
    pltpu.make_async_copy(grad_out, grad_out, store_sems.at[1]).wait()


def call_assemble(top_in, kept, in_shape, out_shape):
    kept = [pltpu.with_memory_space_constraint(ref, VMEM) for ref in kept]
    return pl.pallas_call(
        assemble,
        name='assemble',
        out_shape=(sds(in_shape, F32), sds(out_shape, F32)),
        in_specs=spaces('vvvh'),
        out_specs=tuple(spaces('hh')),
        scratch_shapes=[VMEM(top_in.shape, F32), pltpu.SemaphoreType.DMA, sems(2)],
        compiler_params=pltpu.CompilerParams(vmem_limit_bytes=VMEM_BYTES - VMEM_KEPT),
        cost_estimate=pl.CostEstimate(flops=1 << 30, bytes_accessed=1 << 25, transcendentals=0),
    )(*kept, top_in)


def solution(mesh):
    tok_spec = P(('local', 'data'), None)
    w_spec = P(None, 'local', None)

    def device_step(tokens, cotangent, w_in, w_out):
        (x1, e1, d0, part_out, a_low, ut_low, st_low, ut_top, st_top, q_top, d_top, w1_low, w2_low) = call_upper_half(
            tokens, cotangent, w_in, w_out)
        grad, x2, _, _, top_in, *kept = call_lower_half(
            tokens, x1, e1, d0, part_out, w1_low, w2_low, a_low, ut_low, st_low, ut_top, st_top, q_top, d_top)
        grad_in, grad_out = call_assemble(top_in, kept, w_in.shape, w_out.shape)
        return x2, grad_in, grad_out, grad

    return jax.shard_map(device_step, mesh=mesh, in_specs=(tok_spec, tok_spec, w_spec, w_spec),
                         out_specs=(tok_spec, w_spec, w_spec, tok_spec), check_vma=False)
```

```python
import functools

import jax
import jax.numpy as jnp
from jax import lax
from jax.experimental import pallas as pl
from jax.experimental.pallas import tpu as pltpu
from jax.sharding import PartitionSpec as P

EPSILON = 1e-6
GELU_SCALE = 0.7978845608028654
GELU_CUBE = 0.044715
BF16 = jnp.bfloat16
F32 = jnp.float32
MESH = pl.DeviceIdType.MESH
HBM = pltpu.HBM
VMEM = pltpu.VMEM
VMEM_BYTES = 67043328
VMEM_KEPT = 169 << 17
UPPER = (40, 95)
LOWER = (69, 116, 35)


class Comm:
    def __init__(self, send_sems, recv_sems, local_sems):
        l = lax.axis_index('local')
        d = lax.axis_index('data')
        self.l, self.d = l, d
        self.z, self.y, self.x, self.c = l // 4, l % 4, d // 2, d % 2
        self.send_sems, self.recv_sems, self.local_sems = send_sems, recv_sems, local_sems
        self.sends = self.recvs = self.local_count = 0
        self.groups = []
        self.partner = (l, self.x * 2 + 1 - self.c)

    def pos(self, axis):
        return {'x': self.x, 'y': self.y, 'z': self.z}[axis]

    def neighbor(self, axis, delta):
        p = (self.pos(axis) + delta) % 4
        if axis == 'x':
            return (self.l, p * 2 + self.c)
        if axis == 'y':
            return (self.z * 4 + p, self.d)
        return (p * 4 + self.y, self.d)

    def peers(self, axes):
        out = [self.partner] if 'c' in axes else []
        for axis in axes.replace('c', ''):
            out += [self.neighbor(axis, 1), self.neighbor(axis, 3)]
        return out

    def signal(self, sem, axes):
        for device in self.peers(axes):
            pl.semaphore_signal(sem, inc=1, device_id=device, device_id_type=MESH)

    def wait(self, sem, axes):
        pl.semaphore_wait(sem, len(self.peers(axes)))

    def arrive(self, axes):
        self.signal(pltpu.get_barrier_semaphore(), axes)

    def meet(self, axes):
        self.wait(pltpu.get_barrier_semaphore(), axes)

    def send_sem(self):
        self.sends += 1
        return self.send_sems.at[self.sends - 1]

    def recv_sem(self):
        self.recvs += 1
        return self.recv_sems.at[self.recvs - 1]

    def copy(self, src, dst, device, send_sem, recv_sem):
        return pltpu.make_async_remote_copy(src_ref=src, dst_ref=dst, send_sem=send_sem, recv_sem=recv_sem,
                                            device_id=device, device_id_type=MESH)

    def send(self, src, dst, device, group, recv_sem):
        self.copy(src, dst, device, group.sem, recv_sem).start()

    def wait_recv(self, ref, recv_sem):
        self.copy(ref, ref, self.partner, self.send_sems.at[0], recv_sem).wait_recv()

    def push(self, src, dst):
        group, recv_sem = Sends(self, src), self.recv_sem()
        self.send(src, dst, self.partner, group, recv_sem)
        return group, lambda: self.wait_recv(dst, recv_sem)

    def local(self, *pairs):
        out = []
        for src, dst in pairs:
            copy = pltpu.make_async_copy(src, dst, self.local_sems.at[self.local_count])
            copy.start()
            self.local_count += 1
            out.append(copy)
        return out

    def end(self):
        for group in self.groups:
            group.wait()


class Sends:
    def __init__(self, comm, ref, sem=None):
        self.comm, self.ref, self.sem = comm, ref, sem or comm.send_sem()
        self.waited = False
        comm.groups.append(self)

    def wait(self):
        if not self.waited:
            self.waited = True
            c = self.comm
            c.copy(self.ref, self.ref, c.partner, self.sem, c.recv_sems.at[0]).wait_send()


def done(copies):
    for copy in copies:
        copy.wait()


class Every:
    def __init__(self, things):
        self.things = things

    def __getattr__(self, step):
        def run(*args):
            for thing in self.things:
                getattr(thing, step)(*args)
        return run


class RingGather:
    def __init__(self, comm, axis, own, slot, block, three, before=None):
        self.comm, self.own, self.slot, self.block = comm, own, slot, block
        self.me = comm.pos(axis)
        self.right, self.far, self.left = [(self.me + k) % 4 for k in (1, 2, 3)]
        self.to_right, self.to_left = comm.neighbor(axis, 1), comm.neighbor(axis, 3)
        self.group = Sends(comm, three, before and before.group.sem)
        self.sems = before.sems if before else [comm.recv_sem() for _ in range(3)]

    def both(self, k, right, right_slot, left, left_slot):
        self.comm.send(right, right_slot, self.to_right, self.group, self.sems[k])
        self.comm.send(left, left_slot, self.to_left, self.group, self.sems[k])

    def start(self):
        own, slot, me = self.own, self.slot, self.me
        self.both(0, own(0), slot(me, 0), own(1), slot(me, 1))
        self.both(1, own(1), slot(me, 1), own(0), slot(me, 0))

    def forward(self):
        self.comm.wait_recv(self.block, self.sems[0])
        right, left = self.slot(self.left, 0), self.slot(self.right, 1)
        self.both(2, right, right, left, left)

    def near(self):
        self.comm.wait_recv(self.block, self.sems[1])

    def finish(self):
        self.comm.wait_recv(self.block, self.sems[2])

    def sent(self):
        self.group.wait()


class RingReduce:
    def __init__(self, comm, axis, part, landing, before=None):
        self.comm, self.part, self.landing = comm, part, landing
        self.me = comm.pos(axis)
        self.right, self.far, self.left = [(self.me + k) % 4 for k in (1, 2, 3)]
        self.to_right, self.to_left = comm.neighbor(axis, 1), comm.neighbor(axis, 3)
        self.first = Sends(comm, landing.at[pl.ds(0, 2)], before and before.first.sem)
        self.rest = Sends(comm, landing.at[pl.ds(0, 4)], before and before.rest.sem)
        self.sems = before.sems if before else [comm.recv_sem() for _ in range(3)]
        self.right_sem, self.left_sem, self.rest_sem = self.sems
        self.pair, self.quad = landing.at[pl.ds(0, 2)], landing.at[pl.ds(0, 4)]

    def right_to(self, k, src, group, sem):
        self.comm.send(src, self.landing.at[k], self.to_right, group, sem)

    def left_to(self, k, src, group, sem):
        self.comm.send(src, self.landing.at[k], self.to_left, group, sem)

    def start_far(self, far0, far1):
        self.right_to(0, far0, self.first, self.right_sem)
        self.left_to(3, far1, self.first, self.left_sem)

    def start_near(self, right1, left0):
        self.right_to(1, right1, self.rest, self.rest_sem)
        self.left_to(4, left0, self.rest, self.rest_sem)

    def start_all(self):
        part = self.part
        self.start_far(part(self.far, 0), part(self.far, 1))
        self.start_near(part(self.right, 1), part(self.left, 0))

    def start_half(self, half):
        if half == 0:
            self.right_to(0, self.part(self.far, 0), self.first, self.right_sem)
            self.left_to(4, self.part(self.left, 0), self.rest, self.rest_sem)
        else:
            self.left_to(3, self.part(self.far, 1), self.first, self.left_sem)
            self.right_to(1, self.part(self.right, 1), self.rest, self.rest_sem)

    def wait_right(self):
        self.comm.wait_recv(self.landing.at[0], self.right_sem)

    def wait_left(self):
        self.comm.wait_recv(self.landing.at[3], self.left_sem)

    def pass_right(self):
        self.right_to(2, self.landing.at[0], self.rest, self.rest_sem)

    def pass_left(self):
        self.left_to(5, self.landing.at[3], self.rest, self.rest_sem)

    def middle_right(self):
        landing = self.landing
        self.wait_right()
        landing[0] = landing[0] + self.part(self.right, 0)[...]
        self.pass_right()

    def middle_left(self):
        landing = self.landing
        self.wait_left()
        landing[3] = landing[3] + self.part(self.left, 1)[...]
        self.pass_left()

    def finish(self):
        self.comm.wait_recv(self.quad, self.rest_sem)

    def sent(self):
        self.first.wait()
        self.rest.wait()

    def sums(self):
        landing = self.landing
        return (self.part(self.me, 0)[...] + landing[2] + landing[4],
                self.part(self.me, 1)[...] + landing[1] + landing[5])


class PlaneGather:
    def __init__(self, comm, dims, first, full, cols, before=None, out=None):
        self.comm, self.out, self.kept = comm, out, []
        c = comm.c
        lead = dims[0] == first
        second = dims.replace(first, '')
        b = comm.pos(second)
        half_rows = full.shape[3] // 2
        rows = lambda h: pl.ds(h * half_rows, half_rows)
        pair = lambda h: pl.ds(2 * h, 2)
        self.b = b
        every, three, own = slice(None), pl.ds(0, 3), comm.pos(first)
        at = lambda p, q, r: full.at[(p, q, c, r, cols) if lead else (q, p, c, r, cols)]
        slot1 = lambda p, h: at(p, b, rows(h))
        slot2 = lambda p, h: at(pair(h), p, every)
        self.ring1 = RingGather(comm, first, lambda h: slot1(own, h), slot1, at(own, b, every), at(three, b, every),
                                before and before.ring1)
        self.ring2 = RingGather(comm, second, lambda h: slot2(b, h), slot2, at(every, b, every), at(every, three, every),
                                before and before.ring2)
        self.line = lambda p, ref=full: ref.at[(every, p, c, every, cols) if lead else (p, every, c, every, cols)]
        self.whole, self.near_lines = at(every, every, every), at(every, three, every)
        self.group = Sends(comm, self.whole, before and before.group.sem)
        self.sems = before.sems if before else [comm.recv_sem(), comm.recv_sem()]

    def push(self, p, k=0):
        line = self.line(p)
        target = line if self.out is None else self.line(p, self.out)
        self.comm.send(line, target, self.comm.partner, self.group, self.sems[k])
        if self.out is not None:
            self.kept += self.comm.local((line, target))

    def start1(self):
        self.ring1.start()

    def forward1(self):
        self.ring1.forward()

    def start2(self):
        self.ring1.near()
        self.ring1.finish()
        self.ring2.start()
        self.push(self.b)

    def forward2(self):
        self.ring2.forward()

    def near2(self):
        self.ring2.near()
        self.push(self.ring2.left)
        self.push(self.ring2.right)

    def finish2(self):
        self.ring2.finish()
        self.push(self.ring2.far, 1)

    def arrived(self):
        self.comm.wait_recv(self.near_lines, self.sems[0])
        self.comm.wait_recv(self.line(self.b), self.sems[1])
        done(self.kept)

    def sent(self):
        self.ring1.sent()
        self.ring2.sent()
        self.group.wait()


def gathers(comm, dims, full, pieces, before=None, out=None):
    width = full.shape[4] // pieces
    out = [PlaneGather(comm, dims, dims[k % 2], full, pl.ds(k * width, width), before and before.things[k], out)
           for k in range(pieces)]
    return [Every(out[k:k + 2]) for k in range(0, pieces, 2)]


def own_blocks(comm, w_in, w_out, layer, w1, w2):
    z, y, x, c = comm.z, comm.y, comm.x, comm.c
    width = w_in.shape[2] // 64
    rows1, rows2 = w1.shape[3], w2.shape[3]
    own = w1.at[z, y, c]
    k = comm.local_count
    comm.local_count += 1
    for j in range(16):
        start = (4 * (j % 4) + j // 4) * 4 * width + x * width
        pltpu.make_async_copy(w_in.at[layer, pl.ds(c * rows1, rows1), pl.ds(pl.multiple_of(start, width), width)],
                              own.at[:, pl.ds(j * width, width)], comm.local_sems.at[k]).start()
    start = (x * 2 + c) * rows2
    copies = comm.local((w_out.at[layer, pl.ds(pl.multiple_of(start, rows2), rows2)], w2.at[y, z, c]))
    return [pltpu.make_async_copy(own, own, comm.local_sems.at[k])] + copies


def ring_of_tokens(comm, full, before=None):
    n = full.shape[1] // 2
    slot = lambda p, h: full.at[p, pl.ds(h * n, n)]
    return RingGather(comm, 'x', lambda h: slot(comm.x, h), slot, full.at[0], full.at[pl.ds(0, 3)], before)


def token_sums(comm, part, landing, tokens, before=None):
    width = part.shape[1] // 2
    block = lambda pos, half: part.at[pl.ds(pl.multiple_of(pos * tokens, tokens), tokens), pl.ds(half * width, width)]
    return RingReduce(comm, 'x', block, landing, before)


def norm_rows(x):
    return x * lax.rsqrt(jnp.mean(x * x, axis=-1, keepdims=True) + EPSILON)


def norm_rows_vjp(x, g):
    r = lax.rsqrt(jnp.mean(x * x, axis=-1, keepdims=True) + EPSILON)
    dot = jnp.mean(x * g, axis=-1, keepdims=True)
    return r * g - x * (r * r * r * dot)


def gelu(x):
    t = jnp.tanh(GELU_SCALE * (x + GELU_CUBE * (x * x * x)))
    return x * (0.5 * (1.0 + t))


def gelu_grad(x):
    x2 = x * x
    t = jnp.tanh(GELU_SCALE * (x + GELU_CUBE * (x2 * x)))
    return 0.5 * (1.0 + t) + (0.5 * x) * (1.0 - t * t) * (GELU_SCALE * (1.0 + (3.0 * GELU_CUBE) * x2))


def dot(a, b):
    return lax.dot_general(a, b, (((1,), (0,)), ((), ())), preferred_element_type=F32)


def dot_bt(a, b):
    return lax.dot_general(a, b, (((1,), (1,)), ((), ())), preferred_element_type=F32)


def flat(value):
    return value.reshape(-1, value.shape[-1])


def tiles(n, step, tile=256):
    t = min(tile, n)

    def run(i, _):
        step(pl.ds(pl.multiple_of(i * t, t), t))
        return 0

    lax.fori_loop(0, n // t, run, 0)


def forward_acts(u, w1, a, s, st):
    def step(cols):
        acc = dot(flat(u[...]), flat(w1[:, :, :, :, cols])).astype(BF16)
        a[:, cols] = acc
        value = gelu(acc.astype(F32)).astype(BF16)
        s[:, cols] = value
        st[cols, :] = value.T

    tiles(a.shape[1], step)


def transposed(u, ut):
    def step(cols):
        ut[cols, :] = flat(u[:, :, cols]).T

    tiles(ut.shape[0], step)


def forward_part(s, w2, part, half):
    width = part.shape[1] // 2
    t = min(256, width)

    def run(i, _):
        cols = pl.ds(pl.multiple_of(half * width + i * t, t), t)
        part[:, cols] = dot(s[...], flat(w2[:, :, :, :, cols]))
        return 0

    lax.fori_loop(0, width // t, run, 0)


def row_tile(w, i):
    return flat(w[i // 2, pl.ds((i % 2) * 2, 2)])


def backward_acts(d, tile_product, a, q):
    rows = a.shape[1] // 8

    def step(i, _):
        cols = pl.ds(pl.multiple_of(i * rows, rows), rows)
        q[:, cols] = (tile_product(i) * gelu_grad(a[:, cols].astype(F32))).astype(BF16)
        return 0

    lax.fori_loop(0, 8, step, 0)


def backward_part(tile_product, part, half):
    rows = part.shape[1] // 8

    def step(j, _):
        i = half * 4 + j
        part[:, pl.ds(pl.multiple_of(i * rows, rows), rows)] = tile_product(i)
        return 0

    lax.fori_loop(0, 4, step, 0)


def last_dim_half(ref, k):
    width = ref.shape[-1] // 2
    return ref.at[..., pl.ds(pl.multiple_of(k * width, width), width)]


def upper_half(x0_hbm, cot, w_in, w_out,
               x1_out, e1_out, d0_out, part_out, a_low, ut_low, st_low, ut_top, st_top, q_top, d_top, w1_low, w2_low,
               p1, p2, q1, q2, uf, df, a, s, q, ut, st, x0, x1, d0, part, landing, e1,
               send_sems, recv_sems, local_sems, credits):
    comm = Comm(send_sems, recv_sems, local_sems)
    tokens = x0.shape[0]
    x, c = comm.x, comm.c
    p_free, q_free = credits.at[0], credits.at[1]

    comm.arrive('xyzc')
    load_x = comm.local((x0_hbm, x0))
    own0 = own_blocks(comm, w_in, w_out, 0, p1, p2)
    load_d = comm.local((cot, df.at[x]))
    own1 = own_blocks(comm, w_in, w_out, 1, q1, q2)
    done(load_x)
    uf[x] = norm_rows(x0[...].astype(F32)).astype(BF16)
    comm.meet('xyzc')

    gather_u = ring_of_tokens(comm, uf)
    gather_d = ring_of_tokens(comm, df)
    g1, = gathers(comm, 'zy', p1, 2)
    g2, g3 = gathers(comm, 'yz', p2, 4)
    n1, = gathers(comm, 'zy', q1, 2)
    n2, = gathers(comm, 'yz', q2, 2)
    done(own0 + load_d)
    g2.start1()
    gather_u.start()
    g1.start1()
    done(own1)
    g2.forward1()
    g3.start1()
    g1.forward1()
    g2.start2()
    g3.forward1()
    gather_u.forward()
    gather_d.start()
    g1.start2()
    gather_u.near()
    gather_u.finish()
    g1.forward2()
    g2.forward2()
    n2.start1()
    g2.near2()
    g3.start2()
    gather_d.forward()
    n1.start1()
    transposed(uf, ut)
    pushed = [comm.push(ut, ut_low.at[1])]
    kept = comm.local((ut, ut_low.at[0]))
    g1.near2()
    gather_d.near()
    g1.finish2()
    g2.finish2()
    gather_d.finish()
    g1.arrived()
    forward_acts(uf, p1, a, s, st)
    n2.forward1()
    g3.forward2()
    g2.arrived()
    gather_u.sent()
    ring = token_sums(comm, part, landing, tokens)
    forward_part(s, p2, part, 0)
    ring.start_half(0)
    n1.forward1()
    pushed += [comm.push(st, st_low.at[1])]
    kept += comm.local((st, st_low.at[0]), (a, a_low))
    g3.near2()
    pushed += [comm.push(last_dim_half(df, 1 - c), d_top.at[1])]
    kept_d = comm.local((last_dim_half(df, c), d_top.at[0]))
    n2.start2()
    g3.finish2()
    g3.arrived()
    forward_part(s, p2, part, 1)
    ring.start_half(1)
    g1.sent()
    g2.sent()
    g3.sent()
    comm.signal(p_free, 'yzc')
    own2 = own_blocks(comm, w_in, w_out, 1, p1, p2)
    b1, = gathers(comm, 'zy', p1, 2, g1)
    b2, = gathers(comm, 'yz', p2, 2, g2)
    done(own2)
    comm.wait(p_free, 'yzc')
    b1.start1()
    b2.start1()
    n1.start2()
    n2.forward2()
    ring.middle_right()
    n2.near2()
    b2.forward1()
    b1.forward1()
    ring.middle_left()
    n1.forward2()
    n1.near2()
    ring.finish()
    x_next = (x0[...].astype(F32) + jnp.concatenate(ring.sums(), axis=1)).astype(BF16)
    x1[...] = x_next
    keep_x = comm.local((x1, x1_out))
    uf[x] = norm_rows(x_next.astype(F32)).astype(BF16)
    ring.sent()
    gather_v = ring_of_tokens(comm, uf, gather_u)
    gather_v.start()
    n2.finish2()
    done(kept)
    pushed[0][0].wait()
    pushed[1][0].wait()
    b2.start2()
    n2.arrived()
    n1.finish2()
    gather_v.forward()
    n1.arrived()
    b2.forward2()
    gather_v.near()
    b1.start2()
    b2.near2()
    gather_v.finish()
    forward_acts(uf, q1, a, s, st)
    b2.finish2()
    forward_part(s, q2, part, 0)
    forward_part(s, q2, part, 1)
    keep_part = comm.local((part, part_out))
    b1.forward2()
    n1.sent()
    n2.sent()
    comm.signal(q_free, 'yzc')
    own3 = own_blocks(comm, w_in, w_out, 0, q1, q2)
    l1, = gathers(comm, 'zy', q1, 2, n1, w1_low)
    l2, = gathers(comm, 'yz', q2, 2, n2, w2_low)
    b2.arrived()
    done(own3)
    comm.wait(q_free, 'yzc')
    l2.start1()
    b1.near2()
    backward_acts(df, lambda i: dot_bt(flat(df[...]), row_tile(p2, i)), a, q)
    b1.finish2()
    l2.forward1()
    l1.start1()
    transposed(uf, ut)
    pushed += [comm.push(ut, ut_top.at[1]), comm.push(st, st_top.at[1])]
    kept = kept_d + comm.local((ut, ut_top.at[0]), (st, st_top.at[0]))
    pushed += [comm.push(last_dim_half(q, 1 - c), q_top.at[1])]
    kept += comm.local((last_dim_half(q, c), q_top.at[0]))
    b1.arrived()
    done(keep_part)
    ring = token_sums(comm, part, landing, tokens, ring)
    product = lambda i: dot_bt(q[...], row_tile(p1, i))
    backward_part(product, part, 0)
    ring.start_half(0)
    l1.forward1()
    l2.start2()
    backward_part(product, part, 1)
    ring.start_half(1)
    l2.forward2()
    l1.start2()
    ring.middle_right()
    l2.near2()
    l2.finish2()
    ring.middle_left()
    l1.forward2()
    l2.arrived()
    l1.near2()
    l1.finish2()
    ring.finish()
    g = jnp.concatenate(ring.sums(), axis=1)
    e = df[x].astype(F32) + norm_rows_vjp(x1[...].astype(F32), g)
    e1[...] = e
    d0[...] = e.astype(BF16)
    kept += keep_x + comm.local((e1, e1_out), (d0, d0_out))
    l1.arrived()
    for _, arrived in pushed:
        arrived()
    done(kept)
    comm.end()


def sds(shape, dtype):
    return jax.ShapeDtypeStruct(shape, dtype)


def sems(n):
    return pltpu.SemaphoreType.DMA((n,))


def spaces(kinds):
    return [pl.BlockSpec(memory_space=VMEM if k == 'v' else HBM) for k in kinds]


def call(kernel, ins, in_kinds, outs, out_kinds, scratch, copies, credits, collective_id, flops):
    return pl.pallas_call(
        kernel,
        name=kernel.__name__,
        out_shape=tuple(outs),
        in_specs=spaces(in_kinds),
        out_specs=tuple(spaces(out_kinds)),
        scratch_shapes=scratch + [sems(copies[0][0]), sems(copies[0][1]), sems(copies[1]),
                                  pltpu.SemaphoreType.REGULAR((credits,))],
        compiler_params=pltpu.CompilerParams(collective_id=collective_id, has_side_effects=True,
                                             vmem_limit_bytes=VMEM_BYTES),
        cost_estimate=pl.CostEstimate(flops=flops, bytes_accessed=1 << 24, transcendentals=0),
    )(*ins)


def call_upper_half(x0, cot, w_in, w_out):
    tokens, width = x0.shape
    inner = w_in.shape[2]
    group, slice_ = 4 * tokens, inner // 4
    w1 = (4, 4, 2, width // 32, slice_)
    w2 = (4, 4, 2, inner // 128, width)
    block = sds((tokens, width), BF16)
    acts = (group, slice_)
    ut, st = (width, group), (slice_, group)
    pair = lambda shape: sds((2,) + shape, BF16)
    outs = [block, sds((tokens, width), F32), block, sds((group, width), F32), sds(acts, BF16),
            pair(ut), pair(st), pair(ut), pair(st), pair((group, slice_ // 2)), pair((4, tokens, width // 2)),
            sds(w1, BF16), sds(w2, BF16)]
    tok = (4, tokens, width)
    scratch = [VMEM(shape, BF16) for shape in (w1, w2, w1, w2, tok, tok, acts, acts, acts, ut, st, block.shape,
                                            block.shape, block.shape)]
    scratch += [VMEM((group, width), F32), VMEM((6, tokens, width // 2), F32), VMEM(block.shape, F32)]
    return call(upper_half, (x0, cot, w_in, w_out), 'hhhh', outs, 'h' * 13, scratch, (UPPER, 37), 2, 1,
                16 * group * width * slice_)


class GradReduce:
    def __init__(self, comm, axes, operands, column, sends, landing1, landing2, result, credits, before=None, unused=None):
        self.comm, self.axes, self.operands, self.column = comm, axes, operands, column
        self.sends, self.landing1, self.landing2, self.result = sends, landing1, landing2, result
        self.credits, self.before, self.unused = credits, before, unused
        self.ring = RingReduce(comm, axes[0], None, landing1, before and before.ring)
        half = sends.shape[2] // 2
        self.block = lambda pos, h: sends.at[pos // 2, pos % 2, pl.ds(h * half, half)]
        self.ring2 = RingReduce(comm, axes[1], self.block, landing2, before and before.ring2)

    def products(self, where, store):
        rows, width = self.sends.shape[2:]

        def step(n, _):
            i, j = n // 2, n % 2
            pos, half = where(i)
            start = pl.multiple_of(((pos * 2 + half) * 2 + j) * rows, rows)
            value = None
            for at, b in self.operands:
                term = dot(at[pl.ds(start, rows)], b(pl.ds(self.column, width)))
                value = term if value is None else value + term
            store(i, j, value)
            return 0

        lax.fori_loop(0, 4, step, 0)

    def start_far(self):
        me, sends = self.ring.me, self.sends
        if self.before:
            self.before.sent()
            self.comm.wait(self.credits.at[0], self.axes[0])

        def store(i, j, value):
            sends[i, j] = value

        self.products(lambda i: ((me + 2) % 4, i), store)
        self.ring.start_far(sends.at[0], sends.at[1])

    def start_near(self):
        me, sends = self.ring.me, self.sends

        def store(i, j, value):
            sends[2 + i, j] = value

        self.products(lambda i: ((me + 1 + 2 * i) % 4, 1 - i), store)
        self.ring.start_near(sends.at[2], sends.at[3])

    def start(self):
        self.start_far()
        self.start_near()

    def middle(self):
        me, landing = self.ring.me, self.landing1
        self.ring.wait_right()
        self.ring.wait_left()

        def store(i, j, value):
            landing[3 * i, j] = landing[3 * i, j] + value

        self.products(lambda i: ((me + 1 + 2 * i) % 4, i), store)
        self.ring.pass_right()
        self.ring.pass_left()

    def turn(self):
        me, landing, sends = self.ring.me, self.landing1, self.sends
        self.ring.finish()
        self.ring.first.wait()

        def store(i, j, value):
            sends[i, j] = value + landing[2 - i, j] + landing[4 + i, j]

        self.products(lambda i: (me, i), store)
        if self.before:
            self.comm.wait(self.credits.at[1], self.axes[1])
        self.ring2.start_all()
        if self.unused is not None:
            self.ring.sent()
            self.comm.signal(self.unused, 'xc')

    def free1(self):
        self.ring.sent()
        self.comm.signal(self.credits.at[0], self.axes[0])

    def middle2(self):
        self.ring2.middle_right()
        self.ring2.middle_left()

    def finish(self):
        self.ring2.finish()
        n = self.result.shape[0] // 2
        self.result[0:n], self.result[n:2 * n] = self.ring2.sums()

    def sent(self):
        self.ring2.sent()

    def free2(self):
        self.sent()
        self.comm.signal(self.credits.at[1], self.axes[1])


CHUNKS = 4


def grad_shapes(width, slice_):
    return (width // 16, slice_ // 2 // CHUNKS), (slice_ // 16, width // 2 // CHUNKS)


def grad_chunks(comm, operands, bufs, results, credits, before=None, unused=None):
    out = []
    for k in range(CHUNKS):
        pieces = 2 if before and k == CHUNKS - 1 else 1
        for piece in range(pieces):
            both = []
            for i, axes in enumerate(('zy', 'yz')):
                width = bufs[3 * i].shape[4] // pieces
                cols = pl.ds(piece * width, width)
                sends, land1 = [ref.at[k, :, :, :, cols] for ref in bufs[3 * i:3 * i + 2]]
                land2 = bufs[3 * i + 2].at[k, :, :, cols]
                both.append(GradReduce(comm, axes, operands[i], (k * pieces + piece) * width, sends, land1, land2,
                                       results(i, k, cols), credits.at[2 * k + i],
                                       before[k].things[i] if before and piece == 0 else None,
                                       unused.at[k + piece, i] if before else None))
            out.append(Every(both))
    return out


class BlockGather:
    def __init__(self, comm, own, view, count, unused=None):
        self.comm, self.own, self.view, self.unused = comm, own, view, unused
        c = comm.c
        n = own.shape[0] // 2
        half = lambda h: pl.ds(h * n, n)
        self.ring = RingGather(comm, 'x', lambda h: own.at[half(h)], lambda p, h: view(p, c).at[half(h)], own, count(3))
        self.four = count(4)
        self.group, self.sem = Sends(comm, self.four), comm.recv_sem()
        self.kept = []

    def push(self, pos, src):
        c = self.comm
        c.send(src, self.view(pos, c.c), c.partner, self.group, self.sem)

    def start(self):
        here = self.view(self.ring.me, self.comm.c)
        if self.unused is None:
            self.kept = self.comm.local((self.own, here))
        else:
            self.comm.wait(self.unused, 'xc')
            here[...] = self.own[...]
        self.ring.start()
        self.push(self.ring.me, self.own)

    def forward(self):
        self.ring.forward()

    def near(self):
        ring, c = self.ring, self.comm.c
        ring.near()
        self.push(ring.left, self.view(ring.left, c))
        self.push(ring.right, self.view(ring.right, c))

    def finish(self):
        ring, c = self.ring, self.comm.c
        ring.finish()
        self.push(ring.far, self.view(ring.far, c))

    def arrived(self):
        self.comm.wait_recv(self.four, self.sem)
        done(self.kept)


def rows_from(src, dst, first):
    n = src.shape[1] // 4
    rows = [pl.ds(pl.multiple_of((first + k) % 4 * n, n), n) for k in range(4)]
    pairs = [(src.at[:, r], dst.at[:, r]) for r in rows]
    return pairs[0], pairs[1:]


def columns_from(src, dst):
    n = src.shape[-1] // CHUNKS
    return [(src.at[..., cols], dst.at[..., cols]) for cols in (pl.ds(0, n), pl.ds(n, src.shape[-1] - n))]


def lower_half(x0_hbm, x1_hbm, e1_hbm, d0, part_hbm, w1_hbm, w2_hbm, a_hbm, ut_low, st_low, ut_top, st_top, q_top, d_top,
               q_low, d_low, grad, x2, landed_in, landed_out, part, landing,
               w, df, a, q, xv, e1, gut, gst, gq, gd, top_in, top_out, low_in, low_out,
               sends_in, sends_out, landing2_in, landing2_out,
               send_sems, recv_sems, local_sems, credits, x_free, in_free, out_free, unused):
    bufs = sends_in, landed_in, landing2_in, sends_out, landed_out, landing2_out
    comm = Comm(send_sems, recv_sems, local_sems)
    tokens = xv.shape[0]
    x, c = comm.x, comm.c
    group = a.shape[0]
    load_d = comm.local((d0, df.at[x]))
    far_in, rest_in = rows_from(ut_top, gut, comm.z + 2)
    far_out, rest_out = rows_from(st_top, gst, comm.y + 2)
    q_first, q_rest = columns_from(q_top, gq)
    d_first, d_rest = columns_from(d_top, gd)
    loads_in = comm.local(far_in, q_first)
    loads_out = comm.local(far_out, d_first)
    comm.arrive('xyzc')
    loads_rest = comm.local(q_rest, d_rest, *rest_in, *rest_out)
    columns = lambda ref, j: ref.at[:, pl.ds(j * group, group)]
    load_w = lambda ref: comm.local(*[(columns(ref, j), w.at[j]) for j in range(4)])
    comm.meet('xyzc')

    gather_d = ring_of_tokens(comm, df)
    done(load_d)
    gather_d.start()
    load2 = load_w(w2_hbm) + comm.local((a_hbm, a))
    load_x = comm.local((x0_hbm, xv), (e1_hbm, e1))
    own_b = lambda ref: lambda cols: flat(ref[..., cols])
    top = [[(gut.at[k], own_b(gq.at[k])) for k in (0, 1)], [(gst.at[k], own_b(gd.at[k])) for k in (0, 1)]]
    chunk_out = low_out.shape[2]
    top_results = lambda i, k, cols: (top_out if i else top_in).at[:, pl.ds(k * chunk_out, chunk_out)]
    upper = grad_chunks(comm, top, bufs, top_results, credits)
    (t0i, t0o), (t1i, t1o), (t2i, t2o), (t3i, t3o) = [pair.things for pair in upper]

    def by_columns(left):
        rows = w.shape[1] // 8

        def product(i):
            value = None
            for j in range(4):
                term = dot_bt(flat(left[..., j * group:(j + 1) * group]),
                              w[j, pl.ds(pl.multiple_of(i * rows, rows), rows)])
                value = term if value is None else value + term
            return value

        return product

    done(loads_in)
    t0i.start_far()
    done(loads_out)
    t0o.start_far()
    done(loads_rest)
    t0i.start_near()
    t0o.start_near()
    t2o.start()
    t1i.start()
    gather_d.forward()
    t2i.start()
    t0o.middle()
    gather_d.near()
    t1o.start()
    gather_d.finish()
    done(load2)
    backward_acts(df, by_columns(df), a, q)
    load1 = load_w(w1_hbm)
    _, d_arrived = comm.push(last_dim_half(df, 1 - c), d_low)
    _, q_arrived = comm.push(last_dim_half(q, 1 - c), q_low)
    done(load1)
    ring = token_sums(comm, part, landing, tokens)
    product = by_columns(q)
    backward_part(product, part, 0)
    ring.start_half(0)
    t2i.middle()
    t2o.middle()
    t0o.turn()
    t0o.free1()
    t0i.middle()
    backward_part(product, part, 1)
    ring.start_half(1)
    d_arrived()
    q_arrived()
    half = a.shape[1] // 2
    loads = comm.local(*[(ut_low.at[k], w.at[k]) for k in (0, 1)], *[(st_low.at[k], w.at[2 + k]) for k in (0, 1)],
                       (q_low, a.at[:, pl.ds(0, half)]))
    loads += comm.local(*[(d_low.at[k], a.at[pl.ds(k * tokens, tokens), pl.ds(half, half)]) for k in range(4)])
    t1o.middle()
    t2i.turn()
    t0o.middle2()
    t2i.free1()
    t3i.start()
    ring.middle_right()
    t2o.turn()
    topi = BlockGather(comm, top_in, lambda p, core: landing.at[p * 2 + core], lambda n: landing.at[pl.ds(0, n)], in_free)
    rows, width = top_out.shape
    topo = BlockGather(comm, top_out, lambda p, core: part.at[pl.ds(pl.multiple_of(p * rows, rows), rows),
                                                              pl.ds(pl.multiple_of(core * width, width), width)],
                       lambda n: part.at[pl.ds(0, n * rows), pl.ds(0, width)], out_free)

    def low_gather(k, piece, pieces, i):
        res, landed = (low_out, landed_out) if i else (low_in, landed_in)
        n = res.shape[2] // pieces
        cols = pl.ds(piece * n, n)
        return BlockGather(comm, res.at[k, :, cols], lambda p, core: landed.at[k, p, core, :, cols],
                           lambda m: landed.at[k, pl.ds(0, m), 0, :, cols], unused.at[k + piece, i])

    last = CHUNKS - 1
    low = [(k, 0, 1) for k in range(last)] + [(last, 0, 2), (last, 1, 2)]
    low = [Every([low_gather(*piece, i) for i in (0, 1)]) for piece in low]
    (low0i, low0o), (low1i, low1o), (low2i, low2o), (low3i, low3o), (low4i, low4o) = [pair.things for pair in low]
    t2o.free1()
    t0i.turn()
    t0i.free1()
    t1o.turn()
    t1o.free1()
    ring.middle_left()
    t2i.middle2()
    t3o.start()
    t0i.middle2()
    done(loads)
    mine = lambda ref: lambda cols: flat(ref[..., pl.ds(pl.multiple_of(c * half + cols.start, cols.size), cols.size)])
    other = lambda first: lambda cols: a[:, pl.ds(first + cols.start, cols.size)]
    operands = [[(w.at[0], mine(q)), (w.at[1], other(0))], [(w.at[2], mine(df)), (w.at[3], other(half))]]
    low_results = lambda i, k, cols: (low_out if i else low_in).at[k, :, cols]
    lower = grad_chunks(comm, operands, bufs, low_results, credits, upper, unused)
    (g0i, g0o), (g1i, g1o), (g2i, g2o), (g3i, g3o), (g4i, g4o) = [pair.things for pair in lower]
    t0o.finish()
    t0o.free2()
    t2i.finish()
    t1i.middle()
    t2o.middle2()
    t3o.middle()
    t1o.middle2()
    t3i.middle()
    ring.finish()
    g = jnp.concatenate(ring.sums(), axis=1)
    done(load_x)
    grad[...] = (e1[...] + norm_rows_vjp(xv[...].astype(F32), g)).astype(BF16)
    load_x = comm.local((x1_hbm, xv))
    ring.sent()
    comm.signal(x_free, 'x')
    load_part = comm.local((part_hbm, part))
    comm.wait(x_free, 'x')
    done(load_part)
    ring = token_sums(comm, part, landing, tokens, ring)
    ring.start_all()
    t0i.finish()
    t1i.turn()
    t1i.free1()
    t2i.free2()
    t2o.finish()
    g0o.start()
    t1o.finish()
    t1o.free2()
    g2i.start()
    t0i.free2()
    t3o.turn()
    t3o.free1()
    t3i.turn()
    t1i.middle2()
    ring.middle_left()
    t3i.free1()
    ring.middle_right()
    g0o.middle()
    g2i.middle()
    t3i.middle2()
    t3o.middle2()
    g0i.start()
    t1i.finish()
    g1o.start()
    t2o.free2()
    g2i.turn()
    g0o.turn()
    t3o.finish()
    t3i.finish()
    t3i.free2()
    t1i.free2()
    t3o.free2()
    ring.finish()
    done(load_x)
    x2[...] = (xv[...].astype(F32) + jnp.concatenate(ring.sums(), axis=1)).astype(BF16)
    ring.sent()
    comm.signal(in_free, 'xc')
    comm.signal(out_free, 'xc')
    topo.start()
    topi.start()
    g0i.middle()
    g1o.middle()
    topo.forward()
    g2i.middle2()
    g0o.middle2()
    g1i.start()
    g2o.start()
    topo.near()
    g0i.turn()
    g0o.finish()
    g1o.turn()
    low0o.start()
    g2i.finish()
    low2i.start()
    g1i.middle()
    topi.forward()
    g2o.middle()
    g1o.middle2()
    g3i.start()
    g0i.middle2()
    g3o.start()
    topo.finish()
    g1i.turn()
    low2i.forward()
    g2o.turn()
    low0o.forward()
    g0i.finish()
    low2i.near()
    g1o.finish()
    g4i.start()
    topi.near()
    g3i.middle()
    g3o.middle()
    low1o.start()
    low0i.start()
    low0o.near()
    low2i.finish()
    g2o.middle2()
    g1i.middle2()
    g4o.start()
    low1o.forward()
    low1o.near()
    low0o.finish()
    g4i.middle()
    g1i.finish()
    low1i.start()
    low0i.forward()
    g3o.turn()
    g4o.middle()
    g3i.turn()
    g2o.finish()
    low2o.start()
    low1i.forward()
    g4i.turn()
    g3o.middle2()
    low1o.finish()
    low0i.near()
    g4o.turn()
    low2o.forward()
    g3i.middle2()
    g4i.middle2()
    g3o.finish()
    low3o.start()
    g4o.middle2()
    g3i.finish()
    low2o.near()
    low3i.start()
    low1i.near()
    low2o.finish()
    g4i.finish()
    low4i.start()
    low0i.finish()
    g4o.finish()
    low4o.start()
    topi.finish()
    low1i.finish()
    low3i.forward()
    low4i.forward()
    low4i.near()
    low3o.forward()
    low4o.forward()
    low3i.near()
    low3o.near()
    low4o.near()
    low3o.finish()
    low3i.finish()
    low4i.finish()
    low4o.finish()
    for pair in [topi, topo] + low:
        pair.arrived()
    comm.end()


def call_lower_half(x0, x1, e1, d0, part_hbm, w1_hbm, w2_hbm, a_hbm, ut_low, st_low, ut_top, st_top, q_top, d_top):
    tokens, width = x0.shape
    group, slice_ = a_hbm.shape
    block = sds((tokens, width), BF16)
    shapes = grad_shapes(width, slice_)
    landed = [VMEM((CHUNKS, 6, 2) + shape, F32) for shape in shapes]
    (rows_in, cols_in), (rows_out, cols_out) = shapes
    kept = [VMEM(block.shape, BF16), VMEM(block.shape, BF16)] + landed
    kept += [VMEM((group, width), F32), VMEM((8, tokens, width // 2), F32)]
    outs = [sds(q_top.shape[1:], BF16), sds(d_top.shape[1:], BF16)] + kept
    acts = VMEM((group, slice_), BF16)
    scratch = [VMEM((4, width, group), BF16), VMEM((4, tokens, width), BF16), acts, acts]
    scratch += [VMEM(block.shape, BF16), VMEM(block.shape, F32)]
    scratch += [VMEM(r.shape, BF16) for r in (ut_top, st_top, q_top, d_top)]
    scratch += [VMEM(shape, F32) for shape in ((rows_in, CHUNKS * cols_in), (rows_out, CHUNKS * cols_out),
                                               (CHUNKS, rows_in, cols_in), (CHUNKS, rows_out, cols_out))]
    scratch += [VMEM((CHUNKS, 4, 2) + shape, F32) for shape in shapes]
    scratch += [VMEM((CHUNKS, 6, rows // 2, cols), F32) for rows, cols in shapes]
    ins = (x0, x1, e1, d0, part_hbm, w1_hbm.reshape(width, slice_), w2_hbm.reshape(slice_, width), a_hbm,
           ut_low, st_low, ut_top, st_top, q_top, d_top)
    return pl.pallas_call(
        lower_half,
        name='lower_half',
        out_shape=tuple(outs),
        in_specs=spaces('h' * 14),
        out_specs=tuple(spaces('hhvvvvvv')),
        scratch_shapes=scratch + [sems(LOWER[0]), sems(LOWER[1]), sems(LOWER[2]), pltpu.SemaphoreType.REGULAR((2 * CHUNKS, 2)),
                                  pltpu.SemaphoreType.REGULAR, pltpu.SemaphoreType.REGULAR, pltpu.SemaphoreType.REGULAR,
                                  pltpu.SemaphoreType.REGULAR((CHUNKS + 1, 2))],
        compiler_params=pltpu.CompilerParams(collective_id=2, has_side_effects=True,
                                             vmem_limit_bytes=VMEM_BYTES - VMEM_KEPT),
        cost_estimate=pl.CostEstimate(flops=16 * group * width * slice_, bytes_accessed=1 << 24, transcendentals=0),
    )(*ins)


def assemble(grad, x2, landed_in, landed_out, part, landing, grad_in, grad_out, tokens_grad, tokens_out, store_sems):
    strip = grad_in.shape[2] // 64
    rows, width = landed_out.shape[-2:]
    per = landed_in.shape[-1] // strip
    others = [pltpu.make_async_copy(grad, tokens_grad, store_sems.at[2]), pltpu.make_async_copy(x2, tokens_out, store_sems.at[3])]
    for copy in others:
        copy.start()
    pltpu.make_async_copy(part, grad_out.at[1], store_sems.at[1]).start()
    for x in range(4):
        for n in range(2 * CHUNKS):
            c, k = n // CHUNKS, n % CHUNKS
            dst = grad_out.at[0, pl.ds(x * rows, rows), pl.ds(n * width, width)]
            pltpu.make_async_copy(landed_out.at[k, x, c], dst, store_sems.at[1]).start()
            for j in range(per):
                t = k * per + j
                y, z = 2 * c + t // 4, t % 4
                cols = pl.ds(((4 * z + y) * 4 + x) * strip, strip)
                low = landed_in.at[k, x, c, :, pl.ds(j * strip, strip)]
                top = landing.at[2 * x + c, :, pl.ds(t * strip, strip)]
                pltpu.make_async_copy(low, grad_in.at[0, :, cols], store_sems.at[0]).start()
                pltpu.make_async_copy(top, grad_in.at[1, :, cols], store_sems.at[0]).start()
    pltpu.make_async_copy(grad_in, grad_in, store_sems.at[0]).wait()
    pltpu.make_async_copy(grad_out, grad_out, store_sems.at[1]).wait()
    done(others)


def call_assemble(kept, in_shape, out_shape):
    kept = [pltpu.with_memory_space_constraint(ref, VMEM) for ref in kept]
    block = sds(kept[0].shape, BF16)
    return pl.pallas_call(
        assemble,
        name='assemble',
        out_shape=(sds(in_shape, F32), sds(out_shape, F32), block, block),
        in_specs=spaces('vvvvvv'),
        out_specs=tuple(spaces('hhhh')),
        scratch_shapes=[sems(4)],
        compiler_params=pltpu.CompilerParams(vmem_limit_bytes=VMEM_BYTES - VMEM_KEPT),
        cost_estimate=pl.CostEstimate(flops=1 << 30, bytes_accessed=1 << 25, transcendentals=0),
    )(*kept)


def solution(mesh):
    tok_spec = P(('local', 'data'), None)
    w_spec = P(None, 'local', None)

    def device_step(tokens, cotangent, w_in, w_out):
        (x1, e1, d0, part_out, a_low, ut_low, st_low, ut_top, st_top, q_top, d_top, w1_low, w2_low) = call_upper_half(
            tokens, cotangent, w_in, w_out)
        _, _, *kept = call_lower_half(
            tokens, x1, e1, d0, part_out, w1_low, w2_low, a_low, ut_low, st_low, ut_top, st_top, q_top, d_top)
        grad_in, grad_out, grad, x2 = call_assemble(kept, w_in.shape, w_out.shape)
        return x2, grad_in, grad_out, grad

    return jax.shard_map(device_step, mesh=mesh, in_specs=(tok_spec, tok_spec, w_spec, w_spec),
                         out_specs=(tok_spec, w_spec, w_spec, tok_spec), check_vma=False)
```

```python
import functools

import jax
import jax.numpy as jnp
from jax import lax
from jax.experimental import pallas as pl
from jax.experimental.pallas import tpu as pltpu
from jax.sharding import PartitionSpec as P

EPSILON = 1e-6
GELU_SCALE = 0.7978845608028654
GELU_CUBE = 0.044715
BF16 = jnp.bfloat16
F32 = jnp.float32
MESH = pl.DeviceIdType.MESH
HBM = pltpu.HBM
VMEM = pltpu.VMEM
VMEM_BYTES = 67043328
VMEM_KEPT = 169 << 17
UPPER = (40, 95)
LOWER = (69, 116, 34)


class Comm:
    def __init__(self, send_sems, recv_sems, local_sems):
        l = lax.axis_index('local')
        d = lax.axis_index('data')
        self.l, self.d = l, d
        self.z, self.y, self.x, self.c = l // 4, l % 4, d // 2, d % 2
        self.send_sems, self.recv_sems, self.local_sems = send_sems, recv_sems, local_sems
        self.sends = self.recvs = self.local_count = 0
        self.groups = []
        self.partner = (l, self.x * 2 + 1 - self.c)

    def pos(self, axis):
        return {'x': self.x, 'y': self.y, 'z': self.z}[axis]

    def neighbor(self, axis, delta):
        p = (self.pos(axis) + delta) % 4
        if axis == 'x':
            return (self.l, p * 2 + self.c)
        if axis == 'y':
            return (self.z * 4 + p, self.d)
        return (p * 4 + self.y, self.d)

    def peers(self, axes):
        out = [self.partner] if 'c' in axes else []
        for axis in axes.replace('c', ''):
            out += [self.neighbor(axis, 1), self.neighbor(axis, 3)]
        return out

    def signal(self, sem, axes):
        for device in self.peers(axes):
            pl.semaphore_signal(sem, inc=1, device_id=device, device_id_type=MESH)

    def wait(self, sem, axes):
        pl.semaphore_wait(sem, len(self.peers(axes)))

    def arrive(self, axes):
        self.signal(pltpu.get_barrier_semaphore(), axes)

    def meet(self, axes):
        self.wait(pltpu.get_barrier_semaphore(), axes)

    def send_sem(self):
        self.sends += 1
        return self.send_sems.at[self.sends - 1]

    def recv_sem(self):
        self.recvs += 1
        return self.recv_sems.at[self.recvs - 1]

    def copy(self, src, dst, device, send_sem, recv_sem):
        return pltpu.make_async_remote_copy(src_ref=src, dst_ref=dst, send_sem=send_sem, recv_sem=recv_sem,
                                            device_id=device, device_id_type=MESH)

    def send(self, src, dst, device, group, recv_sem):
        self.copy(src, dst, device, group.sem, recv_sem).start()

    def wait_recv(self, ref, recv_sem):
        self.copy(ref, ref, self.partner, self.send_sems.at[0], recv_sem).wait_recv()

    def push(self, src, dst):
        group, recv_sem = Sends(self, src), self.recv_sem()
        self.send(src, dst, self.partner, group, recv_sem)
        return group, lambda: self.wait_recv(dst, recv_sem)

    def local(self, *pairs):
        out = []
        for src, dst in pairs:
            copy = pltpu.make_async_copy(src, dst, self.local_sems.at[self.local_count])
            copy.start()
            self.local_count += 1
            out.append(copy)
        return out

    def end(self):
        for group in self.groups:
            group.wait()


class Sends:
    def __init__(self, comm, ref, sem=None):
        self.comm, self.ref, self.sem = comm, ref, sem or comm.send_sem()
        self.waited = False
        comm.groups.append(self)

    def wait(self):
        if not self.waited:
            self.waited = True
            c = self.comm
            c.copy(self.ref, self.ref, c.partner, self.sem, c.recv_sems.at[0]).wait_send()


def done(copies):
    for copy in copies:
        copy.wait()


class Every:
    def __init__(self, things):
        self.things = things

    def __getattr__(self, step):
        def run(*args):
            for thing in self.things:
                getattr(thing, step)(*args)
        return run


class RingGather:
    def __init__(self, comm, axis, own, slot, block, three, before=None):
        self.comm, self.own, self.slot, self.block = comm, own, slot, block
        self.me = comm.pos(axis)
        self.right, self.far, self.left = [(self.me + k) % 4 for k in (1, 2, 3)]
        self.to_right, self.to_left = comm.neighbor(axis, 1), comm.neighbor(axis, 3)
        self.group = Sends(comm, three, before and before.group.sem)
        self.sems = before.sems if before else [comm.recv_sem() for _ in range(3)]

    def both(self, k, right, right_slot, left, left_slot):
        self.comm.send(right, right_slot, self.to_right, self.group, self.sems[k])
        self.comm.send(left, left_slot, self.to_left, self.group, self.sems[k])

    def start(self):
        own, slot, me = self.own, self.slot, self.me
        self.both(0, own(0), slot(me, 0), own(1), slot(me, 1))
        self.both(1, own(1), slot(me, 1), own(0), slot(me, 0))

    def forward(self):
        self.comm.wait_recv(self.block, self.sems[0])
        right, left = self.slot(self.left, 0), self.slot(self.right, 1)
        self.both(2, right, right, left, left)

    def near(self):
        self.comm.wait_recv(self.block, self.sems[1])

    def finish(self):
        self.comm.wait_recv(self.block, self.sems[2])

    def sent(self):
        self.group.wait()


class RingReduce:
    def __init__(self, comm, axis, part, landing, before=None):
        self.comm, self.part, self.landing = comm, part, landing
        self.me = comm.pos(axis)
        self.right, self.far, self.left = [(self.me + k) % 4 for k in (1, 2, 3)]
        self.to_right, self.to_left = comm.neighbor(axis, 1), comm.neighbor(axis, 3)
        self.first = Sends(comm, landing.at[pl.ds(0, 2)], before and before.first.sem)
        self.rest = Sends(comm, landing.at[pl.ds(0, 4)], before and before.rest.sem)
        self.sems = before.sems if before else [comm.recv_sem() for _ in range(3)]
        self.right_sem, self.left_sem, self.rest_sem = self.sems
        self.pair, self.quad = landing.at[pl.ds(0, 2)], landing.at[pl.ds(0, 4)]

    def right_to(self, k, src, group, sem):
        self.comm.send(src, self.landing.at[k], self.to_right, group, sem)

    def left_to(self, k, src, group, sem):
        self.comm.send(src, self.landing.at[k], self.to_left, group, sem)

    def start_far(self, far0, far1):
        self.right_to(0, far0, self.first, self.right_sem)
        self.left_to(3, far1, self.first, self.left_sem)

    def start_near(self, right1, left0):
        self.right_to(1, right1, self.rest, self.rest_sem)
        self.left_to(4, left0, self.rest, self.rest_sem)

    def start_all(self):
        part = self.part
        self.start_far(part(self.far, 0), part(self.far, 1))
        self.start_near(part(self.right, 1), part(self.left, 0))

    def start_half(self, half):
        if half == 0:
            self.right_to(0, self.part(self.far, 0), self.first, self.right_sem)
            self.left_to(4, self.part(self.left, 0), self.rest, self.rest_sem)
        else:
            self.left_to(3, self.part(self.far, 1), self.first, self.left_sem)
            self.right_to(1, self.part(self.right, 1), self.rest, self.rest_sem)

    def wait_right(self):
        self.comm.wait_recv(self.landing.at[0], self.right_sem)

    def wait_left(self):
        self.comm.wait_recv(self.landing.at[3], self.left_sem)

    def pass_right(self):
        self.right_to(2, self.landing.at[0], self.rest, self.rest_sem)

    def pass_left(self):
        self.left_to(5, self.landing.at[3], self.rest, self.rest_sem)

    def middle_right(self):
        landing = self.landing
        self.wait_right()
        landing[0] = landing[0] + self.part(self.right, 0)[...]
        self.pass_right()

    def middle_left(self):
        landing = self.landing
        self.wait_left()
        landing[3] = landing[3] + self.part(self.left, 1)[...]
        self.pass_left()

    def finish(self):
        self.comm.wait_recv(self.quad, self.rest_sem)

    def sent(self):
        self.first.wait()
        self.rest.wait()

    def sums(self):
        landing = self.landing
        return (self.part(self.me, 0)[...] + landing[2] + landing[4],
                self.part(self.me, 1)[...] + landing[1] + landing[5])


class PlaneGather:
    def __init__(self, comm, dims, first, full, cols, before=None, out=None):
        self.comm, self.out, self.kept = comm, out, []
        c = comm.c
        lead = dims[0] == first
        second = dims.replace(first, '')
        b = comm.pos(second)
        half_rows = full.shape[3] // 2
        rows = lambda h: pl.ds(h * half_rows, half_rows)
        pair = lambda h: pl.ds(2 * h, 2)
        self.b = b
        every, three, own = slice(None), pl.ds(0, 3), comm.pos(first)
        at = lambda p, q, r: full.at[(p, q, c, r, cols) if lead else (q, p, c, r, cols)]
        slot1 = lambda p, h: at(p, b, rows(h))
        slot2 = lambda p, h: at(pair(h), p, every)
        self.ring1 = RingGather(comm, first, lambda h: slot1(own, h), slot1, at(own, b, every), at(three, b, every),
                                before and before.ring1)
        self.ring2 = RingGather(comm, second, lambda h: slot2(b, h), slot2, at(every, b, every), at(every, three, every),
                                before and before.ring2)
        self.line = lambda p, ref=full: ref.at[(every, p, c, every, cols) if lead else (p, every, c, every, cols)]
        self.whole, self.near_lines = at(every, every, every), at(every, three, every)
        self.group = Sends(comm, self.whole, before and before.group.sem)
        self.sems = before.sems if before else [comm.recv_sem(), comm.recv_sem()]

    def push(self, p, k=0):
        line = self.line(p)
        target = line if self.out is None else self.line(p, self.out)
        self.comm.send(line, target, self.comm.partner, self.group, self.sems[k])
        if self.out is not None:
            self.kept += self.comm.local((line, target))

    def start1(self):
        self.ring1.start()

    def forward1(self):
        self.ring1.forward()

    def start2(self):
        self.ring1.near()
        self.ring1.finish()
        self.ring2.start()
        self.push(self.b)

    def forward2(self):
        self.ring2.forward()

    def near2(self):
        self.ring2.near()
        self.push(self.ring2.left)
        self.push(self.ring2.right)

    def finish2(self):
        self.ring2.finish()
        self.push(self.ring2.far, 1)

    def arrived(self):
        self.comm.wait_recv(self.near_lines, self.sems[0])
        self.comm.wait_recv(self.line(self.b), self.sems[1])
        done(self.kept)

    def sent(self):
        self.ring1.sent()
        self.ring2.sent()
        self.group.wait()


def gathers(comm, dims, full, pieces, before=None, out=None):
    width = full.shape[4] // pieces
    out = [PlaneGather(comm, dims, dims[k % 2], full, pl.ds(k * width, width), before and before.things[k], out)
           for k in range(pieces)]
    return [Every(out[k:k + 2]) for k in range(0, pieces, 2)]


def own_first(comm, w_in, layer, w1):
    width = w_in.shape[2] // 64
    rows = w1.shape[3]
    own = w1.at[comm.z, comm.y, comm.c]
    sem = comm.local_sems.at[comm.local_count]
    comm.local_count += 1
    for j in range(16):
        start = (4 * (j % 4) + j // 4) * 4 * width + comm.x * width
        pltpu.make_async_copy(w_in.at[layer, pl.ds(comm.c * rows, rows), pl.ds(pl.multiple_of(start, width), width)],
                              own.at[:, pl.ds(j * width, width)], sem).start()
    return [pltpu.make_async_copy(own, own, sem)]


def own_second(comm, w_out, layer, w2):
    rows = w2.shape[3]
    start = (comm.x * 2 + comm.c) * rows
    return comm.local((w_out.at[layer, pl.ds(pl.multiple_of(start, rows), rows)], w2.at[comm.y, comm.z, comm.c]))


def own_blocks(comm, w_in, w_out, layer, w1, w2):
    return own_first(comm, w_in, layer, w1) + own_second(comm, w_out, layer, w2)


def ring_of_tokens(comm, full, before=None):
    n = full.shape[1] // 2
    slot = lambda p, h: full.at[p, pl.ds(h * n, n)]
    return RingGather(comm, 'x', lambda h: slot(comm.x, h), slot, full.at[0], full.at[pl.ds(0, 3)], before)


def token_sums(comm, part, landing, tokens, before=None):
    width = part.shape[1] // 2
    block = lambda pos, half: part.at[pl.ds(pl.multiple_of(pos * tokens, tokens), tokens), pl.ds(half * width, width)]
    return RingReduce(comm, 'x', block, landing, before)


def norm_rows(x):
    return x * lax.rsqrt(jnp.mean(x * x, axis=-1, keepdims=True) + EPSILON)


def norm_rows_vjp(x, g):
    r = lax.rsqrt(jnp.mean(x * x, axis=-1, keepdims=True) + EPSILON)
    dot = jnp.mean(x * g, axis=-1, keepdims=True)
    return r * g - x * (r * r * r * dot)


def gelu(x):
    t = jnp.tanh(GELU_SCALE * (x + GELU_CUBE * (x * x * x)))
    return x * (0.5 * (1.0 + t))


def gelu_grad(x):
    x2 = x * x
    t = jnp.tanh(GELU_SCALE * (x + GELU_CUBE * (x2 * x)))
    return 0.5 * (1.0 + t) + (0.5 * x) * (1.0 - t * t) * (GELU_SCALE * (1.0 + (3.0 * GELU_CUBE) * x2))


def dot(a, b):
    return lax.dot_general(a, b, (((1,), (0,)), ((), ())), preferred_element_type=F32)


def dot_bt(a, b):
    return lax.dot_general(a, b, (((1,), (1,)), ((), ())), preferred_element_type=F32)


def flat(value):
    return value.reshape(-1, value.shape[-1])


def tiles(n, step, tile=256):
    t = min(tile, n)

    def run(i, _):
        step(pl.ds(pl.multiple_of(i * t, t), t))
        return 0

    lax.fori_loop(0, n // t, run, 0)


def forward_acts(u, w1, a, s, st):
    def step(cols):
        acc = dot(flat(u[...]), flat(w1[:, :, :, :, cols])).astype(BF16)
        a[:, cols] = acc
        value = gelu(acc.astype(F32)).astype(BF16)
        s[:, cols] = value
        st[cols, :] = value.T

    tiles(a.shape[1], step)


def transposed(u, ut):
    def step(cols):
        ut[cols, :] = flat(u[:, :, cols]).T

    tiles(ut.shape[0], step)


def forward_part(s, w2, part, half):
    width = part.shape[1] // 2
    t = min(256, width)

    def run(i, _):
        cols = pl.ds(pl.multiple_of(half * width + i * t, t), t)
        part[:, cols] = dot(s[...], flat(w2[:, :, :, :, cols]))
        return 0

    lax.fori_loop(0, width // t, run, 0)


def row_tile(w, i):
    return flat(w[i // 2, pl.ds((i % 2) * 2, 2)])


def backward_acts(d, tile_product, a, q):
    rows = a.shape[1] // 8

    def step(i, _):
        cols = pl.ds(pl.multiple_of(i * rows, rows), rows)
        q[:, cols] = (tile_product(i) * gelu_grad(a[:, cols].astype(F32))).astype(BF16)
        return 0

    lax.fori_loop(0, 8, step, 0)


def backward_part(tile_product, part, half, which=slice(None)):
    rows = part.shape[1] // 8

    def step(j, _):
        i = half * 4 + j
        part[which, pl.ds(pl.multiple_of(i * rows, rows), rows)] = tile_product(i)
        return 0

    lax.fori_loop(0, 4, step, 0)


def backward_rows(q, w1, part, pos, tokens, half):
    rows = pl.ds(pl.multiple_of(pos * tokens, tokens), tokens)
    tile_product = lambda i: dot_bt(q[rows], row_tile(w1, i))
    backward_part(tile_product, part, half, rows)


def last_dim_half(ref, k):
    width = ref.shape[-1] // 2
    return ref.at[..., pl.ds(pl.multiple_of(k * width, width), width)]


def upper_half(x0_hbm, cot, w_in, w_out,
               x1_out, e1_out, part_out, a_low, ut_low, st_low, ut_top, st_top, q_top, d_top, w1_low, w2_low,
               p1, p2, q1, q2, uf, df, a, s, q, ut, st, x0, x1, part, landing, e1,
               send_sems, recv_sems, local_sems, credits):
    comm = Comm(send_sems, recv_sems, local_sems)
    tokens = x0.shape[0]
    x, c = comm.x, comm.c
    p_free, q1_free, q2_free = [credits.at[k] for k in range(3)]

    comm.arrive('xyzc')
    load_x = comm.local((x0_hbm, x0))
    own0 = own_blocks(comm, w_in, w_out, 0, p1, p2)
    load_d = comm.local((cot, df.at[x]))
    own1 = own_blocks(comm, w_in, w_out, 1, q1, q2)
    done(load_x)
    uf[x] = norm_rows(x0[...].astype(F32)).astype(BF16)
    comm.meet('xyzc')

    gather_u = ring_of_tokens(comm, uf)
    gather_d = ring_of_tokens(comm, df)
    g1, = gathers(comm, 'zy', p1, 2)
    g2, g3 = gathers(comm, 'yz', p2, 4)
    n1, = gathers(comm, 'zy', q1, 2)
    n2, = gathers(comm, 'yz', q2, 2)
    done(own0 + load_d)
    g2.start1()
    gather_d.start()
    g1.start1()
    gather_u.start()
    g2.forward1()
    done(own1)
    g3.start1()
    g1.forward1()
    g2.start2()
    g3.forward1()
    gather_d.forward()
    g1.start2()
    gather_d.near()
    g1.forward2()
    g2.forward2()
    gather_u.forward()
    n2.start1()
    n1.start1()
    g2.near2()
    gather_u.near()
    g3.start2()
    g1.near2()
    gather_d.finish()
    g1.finish2()
    gather_u.finish()
    g2.finish2()
    g1.arrived()
    forward_acts(uf, p1, a, s, st)
    n1.forward1()
    n2.forward1()
    g2.arrived()
    gather_u.sent()
    ring = token_sums(comm, part, landing, tokens)
    forward_part(s, p2, part, 0)
    ring.start_half(0)
    g3.forward2()
    g3.near2()
    transposed(uf, ut)
    pushed = [comm.push(ut, ut_low.at[1])]
    kept = comm.local((ut, ut_low.at[0]))
    pushed += [comm.push(st, st_low.at[1])]
    kept += comm.local((st, st_low.at[0]), (a, a_low))
    n1.start2()
    g3.finish2()
    g3.arrived()
    forward_part(s, p2, part, 1)
    ring.start_half(1)
    g1.sent()
    g2.sent()
    g3.sent()
    comm.signal(p_free, 'yzc')
    own2 = own_blocks(comm, w_in, w_out, 1, p1, p2)
    b1, = gathers(comm, 'zy', p1, 2, g1)
    b2, = gathers(comm, 'yz', p2, 2, g2)
    n1.forward2()
    done(own2)
    comm.wait(p_free, 'yzc')
    ring.middle_right()
    pushed += [comm.push(last_dim_half(df, 1 - c), d_top.at[1])]
    kept_d = comm.local((last_dim_half(df, c), d_top.at[0]))
    b2.start1()
    b1.start1()
    n1.near2()
    n1.finish2()
    n2.start2()
    b2.forward1()
    ring.middle_left()
    n1.arrived()
    b1.forward1()
    n2.forward2()
    ring.finish()
    x_next = (x0[...].astype(F32) + jnp.concatenate(ring.sums(), axis=1)).astype(BF16)
    x1[...] = x_next
    keep_x = comm.local((x1, x1_out))
    uf[x] = norm_rows(x_next.astype(F32)).astype(BF16)
    ring.sent()
    gather_v = ring_of_tokens(comm, uf, gather_u)
    gather_v.start()
    n2.near2()
    done(kept)
    pushed[0][0].wait()
    pushed[1][0].wait()
    b2.start2()
    n2.finish2()
    gather_v.forward()
    n2.arrived()
    b2.forward2()
    gather_v.near()
    b1.start2()
    b2.near2()
    gather_v.finish()
    forward_acts(uf, q1, a, s, st)
    b2.finish2()
    n1.sent()
    comm.signal(q1_free, 'yzc')
    own4 = own_first(comm, w_in, 0, q1)
    l1, = gathers(comm, 'zy', q1, 2, n1, w1_low)
    done(own4)
    comm.wait(q1_free, 'yzc')
    l1.start1()
    forward_part(s, q2, part, 0)
    forward_part(s, q2, part, 1)
    keep_part = comm.local((part, part_out))
    b1.forward2()
    n2.sent()
    comm.signal(q2_free, 'yzc')
    own3 = own_second(comm, w_out, 0, q2)
    l2, = gathers(comm, 'yz', q2, 2, n2, w2_low)
    b2.arrived()
    done(own3)
    comm.wait(q2_free, 'yzc')
    b1.near2()
    l1.forward1()
    backward_acts(df, lambda i: dot_bt(flat(df[...]), row_tile(p2, i)), a, q)
    b1.finish2()
    l2.start1()
    l1.start2()
    transposed(uf, ut)
    pushed += [comm.push(ut, ut_top.at[1]), comm.push(st, st_top.at[1])]
    kept = kept_d + comm.local((ut, ut_top.at[0]), (st, st_top.at[0]))
    b1.arrived()
    done(keep_part)
    ring = token_sums(comm, part, landing, tokens, ring)
    left, right = halves = range(2)
    tiles_of = lambda pos, half: backward_rows(q, p1, part, pos, tokens, half)
    for half in halves:
        tiles_of(ring.far, half)
    ring.start_far(*[ring.part(ring.far, half) for half in halves])
    l2.forward1()
    pushed += [comm.push(last_dim_half(q, 1 - c), q_top.at[1])]
    kept += comm.local((last_dim_half(q, c), q_top.at[0]))
    tiles_of(ring.right, right)
    tiles_of(ring.left, left)
    ring.start_near(ring.part(ring.right, right), ring.part(ring.left, left))
    l1.forward2()
    tiles_of(ring.right, left)
    tiles_of(ring.left, right)
    for half in halves:
        tiles_of(ring.me, half)
    l1.near2()
    l2.start2()
    ring.middle_right()
    ring.middle_left()
    l1.finish2()
    l2.forward2()
    l1.arrived()
    l2.near2()
    l2.finish2()
    ring.finish()
    g = jnp.concatenate(ring.sums(), axis=1)
    e = df[x].astype(F32) + norm_rows_vjp(x1[...].astype(F32), g)
    e1[...] = e
    kept += keep_x + comm.local((e1, e1_out))
    l2.arrived()
    for _, arrived in pushed:
        arrived()
    done(kept)
    comm.end()


def sds(shape, dtype):
    return jax.ShapeDtypeStruct(shape, dtype)


def sems(n):
    return pltpu.SemaphoreType.DMA((n,))


def spaces(kinds):
    return [pl.BlockSpec(memory_space=VMEM if k == 'v' else HBM) for k in kinds]


def call(kernel, ins, in_kinds, outs, out_kinds, scratch, copies, credits, collective_id, flops):
    return pl.pallas_call(
        kernel,
        name=kernel.__name__,
        out_shape=tuple(outs),
        in_specs=spaces(in_kinds),
        out_specs=tuple(spaces(out_kinds)),
        scratch_shapes=scratch + [sems(copies[0][0]), sems(copies[0][1]), sems(copies[1]),
                                  pltpu.SemaphoreType.REGULAR((credits,))],
        compiler_params=pltpu.CompilerParams(collective_id=collective_id, has_side_effects=True,
                                             vmem_limit_bytes=VMEM_BYTES),
        cost_estimate=pl.CostEstimate(flops=flops, bytes_accessed=1 << 24, transcendentals=0),
    )(*ins)


def call_upper_half(x0, cot, w_in, w_out):
    tokens, width = x0.shape
    inner = w_in.shape[2]
    group, slice_ = 4 * tokens, inner // 4
    w1 = (4, 4, 2, width // 32, slice_)
    w2 = (4, 4, 2, inner // 128, width)
    block = sds((tokens, width), BF16)
    acts = (group, slice_)
    ut, st = (width, group), (slice_, group)
    pair = lambda shape: sds((2,) + shape, BF16)
    outs = [block, sds((tokens, width), F32), sds((group, width), F32), sds(acts, BF16),
            pair(ut), pair(st), pair(ut), pair(st), pair((group, slice_ // 2)), pair((4, tokens, width // 2)),
            sds(w1, BF16), sds(w2, BF16)]
    tok = (4, tokens, width)
    scratch = [VMEM(shape, BF16) for shape in (w1, w2, w1, w2, tok, tok, acts, acts, acts, ut, st, block.shape,
                                            block.shape)]
    scratch += [VMEM((group, width), F32), VMEM((6, tokens, width // 2), F32), VMEM(block.shape, F32)]
    return call(upper_half, (x0, cot, w_in, w_out), 'hhhh', outs, 'h' * 12, scratch, (UPPER, 36), 3, 1,
                16 * group * width * slice_)


class GradReduce:
    def __init__(self, comm, axes, operands, column, sends, landing1, landing2, result, credits, before=None, unused=None):
        self.comm, self.axes, self.operands, self.column = comm, axes, operands, column
        self.sends, self.landing1, self.landing2, self.result = sends, landing1, landing2, result
        self.credits, self.before, self.unused = credits, before, unused
        self.ring = RingReduce(comm, axes[0], None, landing1, before and before.ring)
        half = sends.shape[2] // 2
        self.block = lambda pos, h: sends.at[pos // 2, pos % 2, pl.ds(h * half, half)]
        self.ring2 = RingReduce(comm, axes[1], self.block, landing2, before and before.ring2)

    def products(self, where, store):
        rows, width = self.sends.shape[2:]

        def step(n, _):
            i, j = n // 2, n % 2
            pos, half = where(i)
            start = pl.multiple_of(((pos * 2 + half) * 2 + j) * rows, rows)
            value = None
            for at, b in self.operands:
                term = dot(at[pl.ds(start, rows)], b(pl.ds(self.column, width)))
                value = term if value is None else value + term
            store(i, j, value)
            return 0

        lax.fori_loop(0, 4, step, 0)

    def start_far(self):
        me, sends = self.ring.me, self.sends
        if self.before:
            self.before.sent()
            self.comm.wait(self.credits.at[0], self.axes[0])

        def store(i, j, value):
            sends[i, j] = value

        self.products(lambda i: ((me + 2) % 4, i), store)
        self.ring.start_far(sends.at[0], sends.at[1])

    def start_near(self):
        me, sends = self.ring.me, self.sends

        def store(i, j, value):
            sends[2 + i, j] = value

        self.products(lambda i: ((me + 1 + 2 * i) % 4, 1 - i), store)
        self.ring.start_near(sends.at[2], sends.at[3])

    def start(self):
        self.start_far()
        self.start_near()

    def middle(self):
        me, landing = self.ring.me, self.landing1
        self.ring.wait_right()
        self.ring.wait_left()

        def store(i, j, value):
            landing[3 * i, j] = landing[3 * i, j] + value

        self.products(lambda i: ((me + 1 + 2 * i) % 4, i), store)
        self.ring.pass_right()
        self.ring.pass_left()

    def turn(self):
        me, landing, sends = self.ring.me, self.landing1, self.sends
        self.ring.finish()
        self.ring.first.wait()

        def store(i, j, value):
            sends[i, j] = value + landing[2 - i, j] + landing[4 + i, j]

        self.products(lambda i: (me, i), store)
        if self.before:
            self.comm.wait(self.credits.at[1], self.axes[1])
        self.ring2.start_all()
        if self.unused is not None:
            self.ring.sent()
            self.comm.signal(self.unused, 'xc')

    def free1(self):
        self.ring.sent()
        self.comm.signal(self.credits.at[0], self.axes[0])

    def middle2(self):
        self.ring2.middle_right()
        self.ring2.middle_left()

    def finish(self):
        self.ring2.finish()
        n = self.result.shape[0] // 2
        self.result[0:n], self.result[n:2 * n] = self.ring2.sums()

    def sent(self):
        self.ring2.sent()

    def free2(self):
        self.sent()
        self.comm.signal(self.credits.at[1], self.axes[1])


CHUNKS = 4


def grad_shapes(width, slice_):
    return (width // 16, slice_ // 2 // CHUNKS), (slice_ // 16, width // 2 // CHUNKS)


def grad_chunks(comm, operands, bufs, results, credits, before=None, unused=None):
    out = []
    for k in range(CHUNKS):
        pieces = 2 if before and k == CHUNKS - 1 else 1
        for piece in range(pieces):
            both = []
            for i, axes in enumerate(('zy', 'yz')):
                width = bufs[3 * i].shape[4] // pieces
                cols = pl.ds(piece * width, width)
                sends, land1 = [ref.at[k, :, :, :, cols] for ref in bufs[3 * i:3 * i + 2]]
                land2 = bufs[3 * i + 2].at[k, :, :, cols]
                both.append(GradReduce(comm, axes, operands[i], (k * pieces + piece) * width, sends, land1, land2,
                                       results(i, k, cols), credits.at[2 * k + i],
                                       before[k].things[i] if before and piece == 0 else None,
                                       unused.at[k + piece, i] if before else None))
            out.append(Every(both))
    return out


class BlockGather:
    def __init__(self, comm, own, view, count, unused=None):
        self.comm, self.own, self.view, self.unused = comm, own, view, unused
        c = comm.c
        n = own.shape[0] // 2
        half = lambda h: pl.ds(h * n, n)
        self.ring = RingGather(comm, 'x', lambda h: own.at[half(h)], lambda p, h: view(p, c).at[half(h)], own, count(3))
        self.four = count(4)
        self.group, self.sem = Sends(comm, self.four), comm.recv_sem()
        self.kept = []

    def push(self, pos, src):
        c = self.comm
        c.send(src, self.view(pos, c.c), c.partner, self.group, self.sem)

    def start(self):
        here = self.view(self.ring.me, self.comm.c)
        if self.unused is None:
            self.kept = self.comm.local((self.own, here))
        else:
            self.comm.wait(self.unused, 'xc')
            here[...] = self.own[...]
        self.ring.start()
        self.push(self.ring.me, self.own)

    def forward(self):
        self.ring.forward()

    def near(self):
        ring, c = self.ring, self.comm.c
        ring.near()
        self.push(ring.left, self.view(ring.left, c))
        self.push(ring.right, self.view(ring.right, c))

    def finish(self):
        ring, c = self.ring, self.comm.c
        ring.finish()
        self.push(ring.far, self.view(ring.far, c))

    def arrived(self):
        self.comm.wait_recv(self.four, self.sem)
        done(self.kept)


def rows_from(src, dst, first):
    n = src.shape[1] // 4
    rows = [pl.ds(pl.multiple_of((first + k) % 4 * n, n), n) for k in range(4)]
    pairs = [(src.at[:, r], dst.at[:, r]) for r in rows]
    return pairs[0], pairs[1:]


def columns_from(src, dst):
    n = src.shape[-1] // CHUNKS
    return [(src.at[..., cols], dst.at[..., cols]) for cols in (pl.ds(0, n), pl.ds(n, src.shape[-1] - n))]


def lower_half(x0_hbm, x1_hbm, e1_hbm, part_hbm, w1_hbm, w2_hbm, a_hbm, ut_low, st_low, ut_top, st_top, q_top, d_top,
               q_low, d_low, grad, x2, landed_in, landed_out, part, landing,
               w, df, a, q, xv, e1, gut, gst, gq, gd, top_in, top_out, low_in, low_out,
               sends_in, sends_out, landing2_in, landing2_out,
               send_sems, recv_sems, local_sems, credits, x_free, in_free, out_free, unused):
    bufs = sends_in, landed_in, landing2_in, sends_out, landed_out, landing2_out
    comm = Comm(send_sems, recv_sems, local_sems)
    tokens = xv.shape[0]
    x, c = comm.x, comm.c
    group = a.shape[0]
    load_d = comm.local((e1_hbm, e1))
    far_in, rest_in = rows_from(ut_top, gut, comm.z + 2)
    far_out, rest_out = rows_from(st_top, gst, comm.y + 2)
    q_first, q_rest = columns_from(q_top, gq)
    d_first, d_rest = columns_from(d_top, gd)
    loads_in = comm.local(far_in, q_first)
    loads_out = comm.local(far_out, d_first)
    comm.arrive('xyzc')
    loads_rest = comm.local(q_rest, d_rest, *rest_in, *rest_out)
    columns = lambda ref, j: ref.at[:, pl.ds(j * group, group)]
    load_w = lambda ref: comm.local(*[(columns(ref, j), w.at[j]) for j in range(4)])
    comm.meet('xyzc')

    gather_d = ring_of_tokens(comm, df)
    done(load_d)
    df[x] = e1[...].astype(BF16)
    gather_d.start()
    load2 = load_w(w2_hbm) + comm.local((a_hbm, a))
    load_x = comm.local((x0_hbm, xv))
    own_b = lambda ref: lambda cols: flat(ref[..., cols])
    top = [[(gut.at[k], own_b(gq.at[k])) for k in (0, 1)], [(gst.at[k], own_b(gd.at[k])) for k in (0, 1)]]
    chunk_out = low_out.shape[2]
    top_results = lambda i, k, cols: (top_out if i else top_in).at[:, pl.ds(k * chunk_out, chunk_out)]
    upper = grad_chunks(comm, top, bufs, top_results, credits)
    (t0i, t0o), (t1i, t1o), (t2i, t2o), (t3i, t3o) = [pair.things for pair in upper]

    def by_columns(left):
        rows = w.shape[1] // 8

        def product(i):
            value = None
            for j in range(4):
                term = dot_bt(flat(left[..., j * group:(j + 1) * group]),
                              w[j, pl.ds(pl.multiple_of(i * rows, rows), rows)])
                value = term if value is None else value + term
            return value

        return product

    done(loads_in)
    t0i.start_far()
    done(loads_out)
    t0o.start_far()
    done(loads_rest)
    t0i.start_near()
    t0o.start_near()
    t2o.start()
    t1i.start()
    gather_d.forward()
    t2i.start()
    t0o.middle()
    gather_d.near()
    t1o.start()
    gather_d.finish()
    done(load2)
    backward_acts(df, by_columns(df), a, q)
    load1 = load_w(w1_hbm)
    _, d_arrived = comm.push(last_dim_half(df, 1 - c), d_low)
    _, q_arrived = comm.push(last_dim_half(q, 1 - c), q_low)
    done(load1)
    ring = token_sums(comm, part, landing, tokens)
    product = by_columns(q)
    backward_part(product, part, 0)
    ring.start_half(0)
    t2i.middle()
    t2o.middle()
    t0o.turn()
    t0o.free1()
    t0i.middle()
    backward_part(product, part, 1)
    ring.start_half(1)
    d_arrived()
    q_arrived()
    half = a.shape[1] // 2
    loads = comm.local(*[(ut_low.at[k], w.at[k]) for k in (0, 1)], *[(st_low.at[k], w.at[2 + k]) for k in (0, 1)],
                       (q_low, a.at[:, pl.ds(0, half)]))
    loads += comm.local(*[(d_low.at[k], a.at[pl.ds(k * tokens, tokens), pl.ds(half, half)]) for k in range(4)])
    t1o.middle()
    t2i.turn()
    t0o.middle2()
    t2i.free1()
    t3i.start()
    ring.middle_right()
    t2o.turn()
    topi = BlockGather(comm, top_in, lambda p, core: landing.at[p * 2 + core], lambda n: landing.at[pl.ds(0, n)], in_free)
    rows, width = top_out.shape
    topo = BlockGather(comm, top_out, lambda p, core: part.at[pl.ds(pl.multiple_of(p * rows, rows), rows),
                                                              pl.ds(pl.multiple_of(core * width, width), width)],
                       lambda n: part.at[pl.ds(0, n * rows), pl.ds(0, width)], out_free)

    def low_gather(k, piece, pieces, i):
        res, landed = (low_out, landed_out) if i else (low_in, landed_in)
        n = res.shape[2] // pieces
        cols = pl.ds(piece * n, n)
        return BlockGather(comm, res.at[k, :, cols], lambda p, core: landed.at[k, p, core, :, cols],
                           lambda m: landed.at[k, pl.ds(0, m), 0, :, cols], unused.at[k + piece, i])

    last = CHUNKS - 1
    low = [(k, 0, 1) for k in range(last)] + [(last, 0, 2), (last, 1, 2)]
    low = [Every([low_gather(*piece, i) for i in (0, 1)]) for piece in low]
    (low0i, low0o), (low1i, low1o), (low2i, low2o), (low3i, low3o), (low4i, low4o) = [pair.things for pair in low]
    t2o.free1()
    t0i.turn()
    t0i.free1()
    t1o.turn()
    t1o.free1()
    ring.middle_left()
    t2i.middle2()
    t3o.start()
    t0i.middle2()
    done(loads)
    mine = lambda ref: lambda cols: flat(ref[..., pl.ds(pl.multiple_of(c * half + cols.start, cols.size), cols.size)])
    other = lambda first: lambda cols: a[:, pl.ds(first + cols.start, cols.size)]
    operands = [[(w.at[0], mine(q)), (w.at[1], other(0))], [(w.at[2], mine(df)), (w.at[3], other(half))]]
    low_results = lambda i, k, cols: (low_out if i else low_in).at[k, :, cols]
    lower = grad_chunks(comm, operands, bufs, low_results, credits, upper, unused)
    (g0i, g0o), (g1i, g1o), (g2i, g2o), (g3i, g3o), (g4i, g4o) = [pair.things for pair in lower]
    t0o.finish()
    t0o.free2()
    t2i.finish()
    t1i.middle()
    t2o.middle2()
    t3o.middle()
    t1o.middle2()
    t3i.middle()
    ring.finish()
    g = jnp.concatenate(ring.sums(), axis=1)
    done(load_x)
    grad[...] = (e1[...] + norm_rows_vjp(xv[...].astype(F32), g)).astype(BF16)
    load_x = comm.local((x1_hbm, xv))
    ring.sent()
    comm.signal(x_free, 'x')
    load_part = comm.local((part_hbm, part))
    comm.wait(x_free, 'x')
    done(load_part)
    ring = token_sums(comm, part, landing, tokens, ring)
    ring.start_all()
    t0i.finish()
    t1i.turn()
    t1i.free1()
    t2i.free2()
    t2o.finish()
    g0o.start()
    t1o.finish()
    t1o.free2()
    g2i.start()
    t0i.free2()
    t3o.turn()
    t3o.free1()
    t3i.turn()
    t1i.middle2()
    ring.middle_left()
    t3i.free1()
    ring.middle_right()
    g0o.middle()
    g2i.middle()
    t3i.middle2()
    t3o.middle2()
    g0i.start()
    t1i.finish()
    g1o.start()
    t2o.free2()
    g2i.turn()
    g0o.turn()
    t3o.finish()
    t3i.finish()
    t3i.free2()
    t1i.free2()
    t3o.free2()
    ring.finish()
    done(load_x)
    x2[...] = (xv[...].astype(F32) + jnp.concatenate(ring.sums(), axis=1)).astype(BF16)
    ring.sent()
    comm.signal(in_free, 'xc')
    comm.signal(out_free, 'xc')
    topo.start()
    topi.start()
    g0i.middle()
    g1o.middle()
    topo.forward()
    g2i.middle2()
    g0o.middle2()
    g1i.start()
    g2o.start()
    topo.near()
    g0i.turn()
    g0o.finish()
    g1o.turn()
    low0o.start()
    g2i.finish()
    low2i.start()
    g1i.middle()
    topi.forward()
    g2o.middle()
    g1o.middle2()
    g3i.start()
    g0i.middle2()
    g3o.start()
    topo.finish()
    g1i.turn()
    low2i.forward()
    g2o.turn()
    low0o.forward()
    g0i.finish()
    low2i.near()
    g1o.finish()
    g4i.start()
    topi.near()
    g3i.middle()
    g3o.middle()
    low1o.start()
    low0i.start()
    low0o.near()
    low2i.finish()
    g2o.middle2()
    g1i.middle2()
    g4o.start()
    low1o.forward()
    low1o.near()
    low0o.finish()
    g4i.middle()
    g1i.finish()
    low1i.start()
    low0i.forward()
    g3o.turn()
    g4o.middle()
    g3i.turn()
    g2o.finish()
    low2o.start()
    low1i.forward()
    g4i.turn()
    g3o.middle2()
    low1o.finish()
    low0i.near()
    g4o.turn()
    low2o.forward()
    g3i.middle2()
    g4i.middle2()
    g3o.finish()
    low3o.start()
    g4o.middle2()
    g3i.finish()
    low2o.near()
    low3i.start()
    low1i.near()
    low2o.finish()
    g4i.finish()
    low4i.start()
    low0i.finish()
    g4o.finish()
    low4o.start()
    topi.finish()
    low1i.finish()
    low3i.forward()
    low4i.forward()
    low4i.near()
    low3o.forward()
    low4o.forward()
    low3i.near()
    low3o.near()
    low4o.near()
    low3o.finish()
    low3i.finish()
    low4i.finish()
    low4o.finish()
    for pair in [topi, topo] + low:
        pair.arrived()
    comm.end()


def call_lower_half(x0, x1, e1, part_hbm, w1_hbm, w2_hbm, a_hbm, ut_low, st_low, ut_top, st_top, q_top, d_top):
    tokens, width = x0.shape
    group, slice_ = a_hbm.shape
    block = sds((tokens, width), BF16)
    shapes = grad_shapes(width, slice_)
    landed = [VMEM((CHUNKS, 6, 2) + shape, F32) for shape in shapes]
    (rows_in, cols_in), (rows_out, cols_out) = shapes
    kept = [VMEM(block.shape, BF16), VMEM(block.shape, BF16)] + landed
    kept += [VMEM((group, width), F32), VMEM((8, tokens, width // 2), F32)]
    outs = [sds(q_top.shape[1:], BF16), sds(d_top.shape[1:], BF16)] + kept
    acts = VMEM((group, slice_), BF16)
    scratch = [VMEM((4, width, group), BF16), VMEM((4, tokens, width), BF16), acts, acts]
    scratch += [VMEM(block.shape, BF16), VMEM(block.shape, F32)]
    scratch += [VMEM(r.shape, BF16) for r in (ut_top, st_top, q_top, d_top)]
    scratch += [VMEM(shape, F32) for shape in ((rows_in, CHUNKS * cols_in), (rows_out, CHUNKS * cols_out),
                                               (CHUNKS, rows_in, cols_in), (CHUNKS, rows_out, cols_out))]
    scratch += [VMEM((CHUNKS, 4, 2) + shape, F32) for shape in shapes]
    scratch += [VMEM((CHUNKS, 6, rows // 2, cols), F32) for rows, cols in shapes]
    ins = (x0, x1, e1, part_hbm, w1_hbm.reshape(width, slice_), w2_hbm.reshape(slice_, width), a_hbm,
           ut_low, st_low, ut_top, st_top, q_top, d_top)
    return pl.pallas_call(
        lower_half,
        name='lower_half',
        out_shape=tuple(outs),
        in_specs=spaces('h' * 13),
        out_specs=tuple(spaces('hhvvvvvv')),
        scratch_shapes=scratch + [sems(LOWER[0]), sems(LOWER[1]), sems(LOWER[2]), pltpu.SemaphoreType.REGULAR((2 * CHUNKS, 2)),
                                  pltpu.SemaphoreType.REGULAR, pltpu.SemaphoreType.REGULAR, pltpu.SemaphoreType.REGULAR,
                                  pltpu.SemaphoreType.REGULAR((CHUNKS + 1, 2))],
        compiler_params=pltpu.CompilerParams(collective_id=2, has_side_effects=True,
                                             vmem_limit_bytes=VMEM_BYTES - VMEM_KEPT),
        cost_estimate=pl.CostEstimate(flops=16 * group * width * slice_, bytes_accessed=1 << 24, transcendentals=0),
    )(*ins)


def assemble(grad, x2, landed_in, landed_out, part, landing, grad_in, grad_out, tokens_grad, tokens_out, store_sems):
    strip = grad_in.shape[2] // 64
    rows, width = landed_out.shape[-2:]
    per = landed_in.shape[-1] // strip
    others = [pltpu.make_async_copy(grad, tokens_grad, store_sems.at[2]), pltpu.make_async_copy(x2, tokens_out, store_sems.at[3])]
    for copy in others:
        copy.start()
    pltpu.make_async_copy(part, grad_out.at[1], store_sems.at[1]).start()
    for x in range(4):
        for n in range(2 * CHUNKS):
            c, k = n // CHUNKS, n % CHUNKS
            dst = grad_out.at[0, pl.ds(x * rows, rows), pl.ds(n * width, width)]
            pltpu.make_async_copy(landed_out.at[k, x, c], dst, store_sems.at[1]).start()
            for j in range(per):
                t = k * per + j
                y, z = 2 * c + t // 4, t % 4
                cols = pl.ds(((4 * z + y) * 4 + x) * strip, strip)
                low = landed_in.at[k, x, c, :, pl.ds(j * strip, strip)]
                top = landing.at[2 * x + c, :, pl.ds(t * strip, strip)]
                pltpu.make_async_copy(low, grad_in.at[0, :, cols], store_sems.at[0]).start()
                pltpu.make_async_copy(top, grad_in.at[1, :, cols], store_sems.at[0]).start()
    pltpu.make_async_copy(grad_in, grad_in, store_sems.at[0]).wait()
    pltpu.make_async_copy(grad_out, grad_out, store_sems.at[1]).wait()
    done(others)


def call_assemble(kept, in_shape, out_shape):
    kept = [pltpu.with_memory_space_constraint(ref, VMEM) for ref in kept]
    block = sds(kept[0].shape, BF16)
    return pl.pallas_call(
        assemble,
        name='assemble',
        out_shape=(sds(in_shape, F32), sds(out_shape, F32), block, block),
        in_specs=spaces('vvvvvv'),
        out_specs=tuple(spaces('hhhh')),
        scratch_shapes=[sems(4)],
        compiler_params=pltpu.CompilerParams(vmem_limit_bytes=VMEM_BYTES - VMEM_KEPT),
        cost_estimate=pl.CostEstimate(flops=1 << 30, bytes_accessed=1 << 25, transcendentals=0),
    )(*kept)


def solution(mesh):
    tok_spec = P(('local', 'data'), None)
    w_spec = P(None, 'local', None)

    def device_step(tokens, cotangent, w_in, w_out):
        (x1, e1, part_out, a_low, ut_low, st_low, ut_top, st_top, q_top, d_top, w1_low, w2_low) = call_upper_half(
            tokens, cotangent, w_in, w_out)
        _, _, *kept = call_lower_half(
            tokens, x1, e1, part_out, w1_low, w2_low, a_low, ut_low, st_low, ut_top, st_top, q_top, d_top)
        grad_in, grad_out, grad, x2 = call_assemble(kept, w_in.shape, w_out.shape)
        return x2, grad_in, grad_out, grad

    return jax.shard_map(device_step, mesh=mesh, in_specs=(tok_spec, tok_spec, w_spec, w_spec),
                         out_specs=(tok_spec, w_spec, w_spec, tok_spec), check_vma=False)
```

```python
import functools

import jax
import jax.numpy as jnp
from jax import lax
from jax.experimental import pallas as pl
from jax.experimental.pallas import tpu as pltpu
from jax.sharding import PartitionSpec as P

EPSILON = 1e-6
GELU_SCALE = 0.7978845608028654
GELU_CUBE = 0.044715
BF16 = jnp.bfloat16
F32 = jnp.float32
MESH = pl.DeviceIdType.MESH
HBM = pltpu.HBM
VMEM = pltpu.VMEM
VMEM_BYTES = 67043328
VMEM_KEPT = 169 << 17
UPPER = (40, 95)
LOWER = (69, 116, 34)


class Comm:
    def __init__(self, send_sems, recv_sems, local_sems):
        l = lax.axis_index('local')
        d = lax.axis_index('data')
        self.l, self.d = l, d
        self.z, self.y, self.x, self.c = l // 4, l % 4, d // 2, d % 2
        self.send_sems, self.recv_sems, self.local_sems = send_sems, recv_sems, local_sems
        self.sends = self.recvs = self.local_count = 0
        self.groups = []
        self.partner = (l, self.x * 2 + 1 - self.c)

    def pos(self, axis):
        return {'x': self.x, 'y': self.y, 'z': self.z}[axis]

    def neighbor(self, axis, delta):
        p = (self.pos(axis) + delta) % 4
        if axis == 'x':
            return (self.l, p * 2 + self.c)
        if axis == 'y':
            return (self.z * 4 + p, self.d)
        return (p * 4 + self.y, self.d)

    def peers(self, axes):
        out = [self.partner] if 'c' in axes else []
        for axis in axes.replace('c', ''):
            out += [self.neighbor(axis, 1), self.neighbor(axis, 3)]
        return out

    def signal(self, sem, axes):
        for device in self.peers(axes):
            pl.semaphore_signal(sem, inc=1, device_id=device, device_id_type=MESH)

    def wait(self, sem, axes):
        pl.semaphore_wait(sem, len(self.peers(axes)))

    def arrive(self, axes):
        self.signal(pltpu.get_barrier_semaphore(), axes)

    def meet(self, axes):
        self.wait(pltpu.get_barrier_semaphore(), axes)

    def send_sem(self):
        self.sends += 1
        return self.send_sems.at[self.sends - 1]

    def recv_sem(self):
        self.recvs += 1
        return self.recv_sems.at[self.recvs - 1]

    def copy(self, src, dst, device, send_sem, recv_sem):
        return pltpu.make_async_remote_copy(src_ref=src, dst_ref=dst, send_sem=send_sem, recv_sem=recv_sem,
                                            device_id=device, device_id_type=MESH)

    def send(self, src, dst, device, group, recv_sem):
        self.copy(src, dst, device, group.sem, recv_sem).start()

    def wait_recv(self, ref, recv_sem):
        self.copy(ref, ref, self.partner, self.send_sems.at[0], recv_sem).wait_recv()

    def push(self, src, dst):
        group, recv_sem = Sends(self, src), self.recv_sem()
        self.send(src, dst, self.partner, group, recv_sem)
        return group, lambda: self.wait_recv(dst, recv_sem)

    def local(self, *pairs):
        out = []
        for src, dst in pairs:
            copy = pltpu.make_async_copy(src, dst, self.local_sems.at[self.local_count])
            copy.start()
            self.local_count += 1
            out.append(copy)
        return out

    def end(self):
        for group in self.groups:
            group.wait()


class Sends:
    def __init__(self, comm, ref, sem=None):
        self.comm, self.ref, self.sem = comm, ref, sem or comm.send_sem()
        self.waited = False
        comm.groups.append(self)

    def wait(self):
        if not self.waited:
            self.waited = True
            c = self.comm
            c.copy(self.ref, self.ref, c.partner, self.sem, c.recv_sems.at[0]).wait_send()


def done(copies):
    for copy in copies:
        copy.wait()


class Every:
    def __init__(self, things):
        self.things = things

    def __getattr__(self, step):
        def run(*args):
            for thing in self.things:
                getattr(thing, step)(*args)
        return run


class RingGather:
    def __init__(self, comm, axis, own, slot, block, three, before=None):
        self.comm, self.own, self.slot, self.block = comm, own, slot, block
        self.me = comm.pos(axis)
        self.right, self.far, self.left = [(self.me + k) % 4 for k in (1, 2, 3)]
        self.to_right, self.to_left = comm.neighbor(axis, 1), comm.neighbor(axis, 3)
        self.group = Sends(comm, three, before and before.group.sem)
        self.sems = before.sems if before else [comm.recv_sem() for _ in range(3)]

    def both(self, k, right, right_slot, left, left_slot):
        self.comm.send(right, right_slot, self.to_right, self.group, self.sems[k])
        self.comm.send(left, left_slot, self.to_left, self.group, self.sems[k])

    def start(self):
        own, slot, me = self.own, self.slot, self.me
        self.both(0, own(0), slot(me, 0), own(1), slot(me, 1))
        self.both(1, own(1), slot(me, 1), own(0), slot(me, 0))

    def forward(self):
        self.comm.wait_recv(self.block, self.sems[0])
        right, left = self.slot(self.left, 0), self.slot(self.right, 1)
        self.both(2, right, right, left, left)

    def near(self):
        self.comm.wait_recv(self.block, self.sems[1])

    def finish(self):
        self.comm.wait_recv(self.block, self.sems[2])

    def sent(self):
        self.group.wait()


class RingReduce:
    def __init__(self, comm, axis, part, landing, before=None):
        self.comm, self.part, self.landing = comm, part, landing
        self.me = comm.pos(axis)
        self.right, self.far, self.left = [(self.me + k) % 4 for k in (1, 2, 3)]
        self.to_right, self.to_left = comm.neighbor(axis, 1), comm.neighbor(axis, 3)
        self.first = Sends(comm, landing.at[pl.ds(0, 2)], before and before.first.sem)
        self.rest = Sends(comm, landing.at[pl.ds(0, 4)], before and before.rest.sem)
        self.sems = before.sems if before else [comm.recv_sem() for _ in range(3)]
        self.right_sem, self.left_sem, self.rest_sem = self.sems
        self.pair, self.quad = landing.at[pl.ds(0, 2)], landing.at[pl.ds(0, 4)]

    def right_to(self, k, src, group, sem):
        self.comm.send(src, self.landing.at[k], self.to_right, group, sem)

    def left_to(self, k, src, group, sem):
        self.comm.send(src, self.landing.at[k], self.to_left, group, sem)

    def start_far(self, far0, far1):
        self.right_to(0, far0, self.first, self.right_sem)
        self.left_to(3, far1, self.first, self.left_sem)

    def start_near(self, right1, left0):
        self.right_to(1, right1, self.rest, self.rest_sem)
        self.left_to(4, left0, self.rest, self.rest_sem)

    def start_all(self):
        part = self.part
        self.start_far(part(self.far, 0), part(self.far, 1))
        self.start_near(part(self.right, 1), part(self.left, 0))

    def start_half(self, half):
        if half == 0:
            self.right_to(0, self.part(self.far, 0), self.first, self.right_sem)
            self.left_to(4, self.part(self.left, 0), self.rest, self.rest_sem)
        else:
            self.left_to(3, self.part(self.far, 1), self.first, self.left_sem)
            self.right_to(1, self.part(self.right, 1), self.rest, self.rest_sem)

    def wait_right(self):
        self.comm.wait_recv(self.landing.at[0], self.right_sem)

    def wait_left(self):
        self.comm.wait_recv(self.landing.at[3], self.left_sem)

    def pass_right(self):
        self.right_to(2, self.landing.at[0], self.rest, self.rest_sem)

    def pass_left(self):
        self.left_to(5, self.landing.at[3], self.rest, self.rest_sem)

    def middle_right(self):
        landing = self.landing
        self.wait_right()
        landing[0] = landing[0] + self.part(self.right, 0)[...]
        self.pass_right()

    def middle_left(self):
        landing = self.landing
        self.wait_left()
        landing[3] = landing[3] + self.part(self.left, 1)[...]
        self.pass_left()

    def finish(self):
        self.comm.wait_recv(self.quad, self.rest_sem)

    def sent(self):
        self.first.wait()
        self.rest.wait()

    def sums(self):
        landing = self.landing
        return (self.part(self.me, 0)[...] + landing[2] + landing[4],
                self.part(self.me, 1)[...] + landing[1] + landing[5])


class PlaneGather:
    def __init__(self, comm, dims, first, full, cols, before=None, out=None):
        self.comm, self.out, self.kept = comm, out, []
        c = comm.c
        lead = dims[0] == first
        second = dims.replace(first, '')
        b = comm.pos(second)
        half_rows = full.shape[3] // 2
        rows = lambda h: pl.ds(h * half_rows, half_rows)
        pair = lambda h: pl.ds(2 * h, 2)
        self.b = b
        every, three, own = slice(None), pl.ds(0, 3), comm.pos(first)
        at = lambda p, q, r: full.at[(p, q, c, r, cols) if lead else (q, p, c, r, cols)]
        slot1 = lambda p, h: at(p, b, rows(h))
        slot2 = lambda p, h: at(pair(h), p, every)
        self.ring1 = RingGather(comm, first, lambda h: slot1(own, h), slot1, at(own, b, every), at(three, b, every),
                                before and before.ring1)
        self.ring2 = RingGather(comm, second, lambda h: slot2(b, h), slot2, at(every, b, every), at(every, three, every),
                                before and before.ring2)
        self.line = lambda p, ref=full: ref.at[(every, p, c, every, cols) if lead else (p, every, c, every, cols)]
        self.whole, self.near_lines = at(every, every, every), at(every, three, every)
        self.group = Sends(comm, self.whole, before and before.group.sem)
        self.sems = before.sems if before else [comm.recv_sem(), comm.recv_sem()]

    def push(self, p, k=0):
        line = self.line(p)
        target = line if self.out is None else self.line(p, self.out)
        self.comm.send(line, target, self.comm.partner, self.group, self.sems[k])
        if self.out is not None:
            self.kept += self.comm.local((line, target))

    def start1(self):
        self.ring1.start()

    def forward1(self):
        self.ring1.forward()

    def start2(self):
        self.ring1.near()
        self.ring1.finish()
        self.ring2.start()
        self.push(self.b)

    def forward2(self):
        self.ring2.forward()

    def near2(self):
        self.ring2.near()
        self.push(self.ring2.left)
        self.push(self.ring2.right)

    def finish2(self):
        self.ring2.finish()
        self.push(self.ring2.far, 1)

    def arrived(self):
        self.comm.wait_recv(self.near_lines, self.sems[0])
        self.comm.wait_recv(self.line(self.b), self.sems[1])
        done(self.kept)

    def sent(self):
        self.ring1.sent()
        self.ring2.sent()
        self.group.wait()


def gathers(comm, dims, full, pieces, before=None, out=None):
    width = full.shape[4] // pieces
    out = [PlaneGather(comm, dims, dims[k % 2], full, pl.ds(k * width, width), before and before.things[k], out)
           for k in range(pieces)]
    return [Every(out[k:k + 2]) for k in range(0, pieces, 2)]


def own_first(comm, w_in, layer, w1):
    width = w_in.shape[2] // 64
    rows = w1.shape[3]
    own = w1.at[comm.z, comm.y, comm.c]
    sem = comm.local_sems.at[comm.local_count]
    comm.local_count += 1
    for j in range(16):
        start = (4 * (j % 4) + j // 4) * 4 * width + comm.x * width
        pltpu.make_async_copy(w_in.at[layer, pl.ds(comm.c * rows, rows), pl.ds(pl.multiple_of(start, width), width)],
                              own.at[:, pl.ds(j * width, width)], sem).start()
    return [pltpu.make_async_copy(own, own, sem)]


def own_second(comm, w_out, layer, w2):
    rows = w2.shape[3]
    start = (comm.x * 2 + comm.c) * rows
    return comm.local((w_out.at[layer, pl.ds(pl.multiple_of(start, rows), rows)], w2.at[comm.y, comm.z, comm.c]))


def own_blocks(comm, w_in, w_out, layer, w1, w2):
    return own_first(comm, w_in, layer, w1) + own_second(comm, w_out, layer, w2)


def ring_of_tokens(comm, full, before=None):
    n = full.shape[1] // 2
    slot = lambda p, h: full.at[p, pl.ds(h * n, n)]
    return RingGather(comm, 'x', lambda h: slot(comm.x, h), slot, full.at[0], full.at[pl.ds(0, 3)], before)


def token_sums(comm, part, landing, tokens, before=None):
    width = part.shape[1] // 2
    block = lambda pos, half: part.at[pl.ds(pl.multiple_of(pos * tokens, tokens), tokens), pl.ds(half * width, width)]
    return RingReduce(comm, 'x', block, landing, before)


def norm_rows(x):
    return x * lax.rsqrt(jnp.mean(x * x, axis=-1, keepdims=True) + EPSILON)


def norm_rows_vjp(x, g):
    r = lax.rsqrt(jnp.mean(x * x, axis=-1, keepdims=True) + EPSILON)
    dot = jnp.mean(x * g, axis=-1, keepdims=True)
    return r * g - x * (r * r * r * dot)


def gelu(x):
    t = jnp.tanh(GELU_SCALE * (x + GELU_CUBE * (x * x * x)))
    return x * (0.5 * (1.0 + t))


def gelu_grad(x):
    x2 = x * x
    t = jnp.tanh(GELU_SCALE * (x + GELU_CUBE * (x2 * x)))
    return 0.5 * (1.0 + t) + (0.5 * x) * (1.0 - t * t) * (GELU_SCALE * (1.0 + (3.0 * GELU_CUBE) * x2))


def dot(a, b):
    return lax.dot_general(a, b, (((1,), (0,)), ((), ())), preferred_element_type=F32)


def dot_bt(a, b):
    return lax.dot_general(a, b, (((1,), (1,)), ((), ())), preferred_element_type=F32)


def flat(value):
    return value.reshape(-1, value.shape[-1])


def tiles(n, step, tile=256):
    t = min(tile, n)

    def run(i, _):
        step(pl.ds(pl.multiple_of(i * t, t), t))
        return 0

    lax.fori_loop(0, n // t, run, 0)


def forward_acts(u, w1, a, s, st):
    def step(cols):
        acc = dot(flat(u[...]), flat(w1[:, :, :, :, cols])).astype(BF16)
        a[:, cols] = acc
        value = gelu(acc.astype(F32)).astype(BF16)
        s[:, cols] = value
        st[cols, :] = value.T

    tiles(a.shape[1], step)


def transposed(u, ut):
    def step(cols):
        ut[cols, :] = flat(u[:, :, cols]).T

    tiles(ut.shape[0], step)


def forward_part(s, w2, part, half):
    width = part.shape[1] // 2
    t = min(256, width)

    def run(i, _):
        cols = pl.ds(pl.multiple_of(half * width + i * t, t), t)
        part[:, cols] = dot(s[...], flat(w2[:, :, :, :, cols]))
        return 0

    lax.fori_loop(0, width // t, run, 0)


def row_tile(w, i):
    return flat(w[i // 2, pl.ds((i % 2) * 2, 2)])


def backward_acts(d, tile_product, a, q):
    rows = a.shape[1] // 8

    def step(i, _):
        cols = pl.ds(pl.multiple_of(i * rows, rows), rows)
        q[:, cols] = (tile_product(i) * gelu_grad(a[:, cols].astype(F32))).astype(BF16)
        return 0

    lax.fori_loop(0, 8, step, 0)


def backward_part(tile_product, part, half, which=slice(None)):
    rows = part.shape[1] // 8

    def step(j, _):
        i = half * 4 + j
        part[which, pl.ds(pl.multiple_of(i * rows, rows), rows)] = tile_product(i)
        return 0

    lax.fori_loop(0, 4, step, 0)


def backward_rows(q, w1, part, pos, tokens, half):
    rows = pl.ds(pl.multiple_of(pos * tokens, tokens), tokens)
    tile_product = lambda i: dot_bt(q[rows], row_tile(w1, i))
    backward_part(tile_product, part, half, rows)


def last_dim_half(ref, k):
    width = ref.shape[-1] // 2
    return ref.at[..., pl.ds(pl.multiple_of(k * width, width), width)]


def upper_half(x0_hbm, cot, w_in, w_out,
               x1_out, e1_out, part_out, a_low, ut_low, st_low, ut_top, st_top, q_top, d_top, w1_low, w2_low,
               p1, p2, q1, q2, uf, df, a, s, q, ut, st, x0, x1, part, landing, e1,
               send_sems, recv_sems, local_sems, credits):
    comm = Comm(send_sems, recv_sems, local_sems)
    tokens = x0.shape[0]
    x, c = comm.x, comm.c
    p_free, q1_free, q2_free = [credits.at[k] for k in range(3)]

    comm.arrive('xyzc')
    load_x = comm.local((x0_hbm, x0))
    own0 = own_blocks(comm, w_in, w_out, 0, p1, p2)
    load_d = comm.local((cot, df.at[x]))
    own1 = own_blocks(comm, w_in, w_out, 1, q1, q2)
    done(load_x)
    uf[x] = norm_rows(x0[...].astype(F32)).astype(BF16)
    comm.meet('xyzc')

    gather_u = ring_of_tokens(comm, uf)
    gather_d = ring_of_tokens(comm, df)
    g1, = gathers(comm, 'zy', p1, 2)
    g2, g3 = gathers(comm, 'yz', p2, 4)
    n1, = gathers(comm, 'zy', q1, 2)
    n2, = gathers(comm, 'yz', q2, 2)
    done(own0 + load_d)
    g2.start1()
    gather_d.start()
    g1.start1()
    gather_u.start()
    g2.forward1()
    done(own1)
    g3.start1()
    g1.forward1()
    g2.start2()
    g3.forward1()
    gather_d.forward()
    g1.start2()
    gather_d.near()
    g1.forward2()
    g2.forward2()
    gather_u.forward()
    n2.start1()
    n1.start1()
    g2.near2()
    gather_u.near()
    g3.start2()
    g1.near2()
    gather_d.finish()
    g1.finish2()
    gather_u.finish()
    g2.finish2()
    g1.arrived()
    forward_acts(uf, p1, a, s, st)
    n1.forward1()
    n2.forward1()
    g2.arrived()
    gather_u.sent()
    ring = token_sums(comm, part, landing, tokens)
    forward_part(s, p2, part, 0)
    ring.start_half(0)
    g3.forward2()
    g3.near2()
    transposed(uf, ut)
    pushed = [comm.push(ut, ut_low.at[1])]
    kept = comm.local((ut, ut_low.at[0]))
    pushed += [comm.push(st, st_low.at[1])]
    kept += comm.local((st, st_low.at[0]), (a, a_low))
    n1.start2()
    g3.finish2()
    g3.arrived()
    forward_part(s, p2, part, 1)
    ring.start_half(1)
    g1.sent()
    g2.sent()
    g3.sent()
    comm.signal(p_free, 'yzc')
    own2 = own_blocks(comm, w_in, w_out, 1, p1, p2)
    b1, = gathers(comm, 'zy', p1, 2, g1)
    b2, = gathers(comm, 'yz', p2, 2, g2)
    n1.forward2()
    done(own2)
    comm.wait(p_free, 'yzc')
    ring.middle_right()
    pushed += [comm.push(last_dim_half(df, 1 - c), d_top.at[1])]
    kept_d = comm.local((last_dim_half(df, c), d_top.at[0]))
    b2.start1()
    b1.start1()
    n1.near2()
    n1.finish2()
    n2.start2()
    b2.forward1()
    ring.middle_left()
    n1.arrived()
    b1.forward1()
    n2.forward2()
    ring.finish()
    x_next = (x0[...].astype(F32) + jnp.concatenate(ring.sums(), axis=1)).astype(BF16)
    x1[...] = x_next
    keep_x = comm.local((x1, x1_out))
    uf[x] = norm_rows(x_next.astype(F32)).astype(BF16)
    ring.sent()
    gather_v = ring_of_tokens(comm, uf, gather_u)
    gather_v.start()
    n2.near2()
    done(kept)
    pushed[0][0].wait()
    pushed[1][0].wait()
    b2.start2()
    n2.finish2()
    gather_v.forward()
    n2.arrived()
    b2.forward2()
    gather_v.near()
    b1.start2()
    b2.near2()
    gather_v.finish()
    forward_acts(uf, q1, a, s, st)
    b2.finish2()
    n1.sent()
    comm.signal(q1_free, 'yzc')
    own4 = own_first(comm, w_in, 0, q1)
    l1, = gathers(comm, 'zy', q1, 2, n1, w1_low)
    done(own4)
    comm.wait(q1_free, 'yzc')
    l1.start1()
    forward_part(s, q2, part, 0)
    forward_part(s, q2, part, 1)
    keep_part = comm.local((part, part_out))
    b1.forward2()
    n2.sent()
    comm.signal(q2_free, 'yzc')
    own3 = own_second(comm, w_out, 0, q2)
    l2, = gathers(comm, 'yz', q2, 2, n2, w2_low)
    b2.arrived()
    done(own3)
    comm.wait(q2_free, 'yzc')
    b1.near2()
    l1.forward1()
    backward_acts(df, lambda i: dot_bt(flat(df[...]), row_tile(p2, i)), a, q)
    b1.finish2()
    l2.start1()
    l1.start2()
    transposed(uf, ut)
    pushed += [comm.push(ut, ut_top.at[1]), comm.push(st, st_top.at[1])]
    kept = kept_d + comm.local((ut, ut_top.at[0]), (st, st_top.at[0]))
    b1.arrived()
    done(keep_part)
    ring = token_sums(comm, part, landing, tokens, ring)
    left, right = halves = range(2)
    tiles_of = lambda pos, half: backward_rows(q, p1, part, pos, tokens, half)
    for half in halves:
        tiles_of(ring.far, half)
    ring.start_far(*[ring.part(ring.far, half) for half in halves])
    l2.forward1()
    pushed += [comm.push(last_dim_half(q, 1 - c), q_top.at[1])]
    kept += comm.local((last_dim_half(q, c), q_top.at[0]))
    tiles_of(ring.right, right)
    tiles_of(ring.left, left)
    ring.start_near(ring.part(ring.right, right), ring.part(ring.left, left))
    l1.forward2()
    tiles_of(ring.right, left)
    tiles_of(ring.left, right)
    for half in halves:
        tiles_of(ring.me, half)
    l1.near2()
    l2.start2()
    ring.middle_right()
    ring.middle_left()
    l1.finish2()
    l2.forward2()
    l1.arrived()
    l2.near2()
    l2.finish2()
    ring.finish()
    g = jnp.concatenate(ring.sums(), axis=1)
    e = df[x].astype(F32) + norm_rows_vjp(x1[...].astype(F32), g)
    e1[...] = e
    kept += keep_x + comm.local((e1, e1_out))
    l2.arrived()
    for _, arrived in pushed:
        arrived()
    done(kept)
    comm.end()


def sds(shape, dtype):
    return jax.ShapeDtypeStruct(shape, dtype)


def sems(n):
    return pltpu.SemaphoreType.DMA((n,))


def spaces(kinds):
    return [pl.BlockSpec(memory_space=VMEM if k == 'v' else HBM) for k in kinds]


def call(kernel, ins, in_kinds, outs, out_kinds, scratch, copies, credits, collective_id, flops):
    return pl.pallas_call(
        kernel,
        name=kernel.__name__,
        out_shape=tuple(outs),
        in_specs=spaces(in_kinds),
        out_specs=tuple(spaces(out_kinds)),
        scratch_shapes=scratch + [sems(copies[0][0]), sems(copies[0][1]), sems(copies[1]),
                                  pltpu.SemaphoreType.REGULAR((credits,))],
        compiler_params=pltpu.CompilerParams(collective_id=collective_id, has_side_effects=True,
                                             vmem_limit_bytes=VMEM_BYTES),
        cost_estimate=pl.CostEstimate(flops=flops, bytes_accessed=1 << 24, transcendentals=0),
    )(*ins)


def call_upper_half(x0, cot, w_in, w_out):
    tokens, width = x0.shape
    inner = w_in.shape[2]
    group, slice_ = 4 * tokens, inner // 4
    w1 = (4, 4, 2, width // 32, slice_)
    w2 = (4, 4, 2, inner // 128, width)
    block = sds((tokens, width), BF16)
    acts = (group, slice_)
    ut, st = (width, group), (slice_, group)
    pair = lambda shape: sds((2,) + shape, BF16)
    outs = [block, sds((tokens, width), F32), sds((group, width), F32), sds(acts, BF16),
            pair(ut), pair(st), pair(ut), pair(st), pair((group, slice_ // 2)), pair((4, tokens, width // 2)),
            sds(w1, BF16), sds(w2, BF16)]
    tok = (4, tokens, width)
    scratch = [VMEM(shape, BF16) for shape in (w1, w2, w1, w2, tok, tok, acts, acts, acts, ut, st, block.shape,
                                            block.shape)]
    scratch += [VMEM((group, width), F32), VMEM((6, tokens, width // 2), F32), VMEM(block.shape, F32)]
    return call(upper_half, (x0, cot, w_in, w_out), 'hhhh', outs, 'h' * 12, scratch, (UPPER, 36), 3, 1,
                16 * group * width * slice_)


class GradReduce:
    def __init__(self, comm, axes, operands, column, sends, landing1, landing2, result, credits, before=None, unused=None):
        self.comm, self.axes, self.operands, self.column = comm, axes, operands, column
        self.sends, self.landing1, self.landing2, self.result = sends, landing1, landing2, result
        self.credits, self.before, self.unused = credits, before, unused
        self.ring = RingReduce(comm, axes[0], None, landing1, before and before.ring)
        half = sends.shape[2] // 2
        self.block = lambda pos, h: sends.at[pos // 2, pos % 2, pl.ds(h * half, half)]
        self.ring2 = RingReduce(comm, axes[1], self.block, landing2, before and before.ring2)

    def products(self, where, store):
        rows, width = self.sends.shape[2:]

        def step(n, _):
            i, j = n // 2, n % 2
            pos, half = where(i)
            start = pl.multiple_of(((pos * 2 + half) * 2 + j) * rows, rows)
            value = None
            for at, b in self.operands:
                term = dot(at[pl.ds(start, rows)], b(pl.ds(self.column, width)))
                value = term if value is None else value + term
            store(i, j, value)
            return 0

        lax.fori_loop(0, 4, step, 0)

    def take_far(self):
        me, sends = self.ring.me, self.sends
        if self.before:
            self.before.sent()
            self.comm.wait(self.credits.at[0], self.axes[0])

        def store(i, j, value):
            sends[i, j] = value

        self.products(lambda i: ((me + 2) % 4, i), store)

    def send_far(self):
        self.ring.start_far(self.sends.at[0], self.sends.at[1])

    def start_near(self):
        me, sends = self.ring.me, self.sends

        def store(i, j, value):
            sends[2 + i, j] = value

        self.products(lambda i: ((me + 1 + 2 * i) % 4, 1 - i), store)
        self.ring.start_near(sends.at[2], sends.at[3])

    def start(self):
        self.take_far()
        self.send_far()
        self.start_near()

    def middle(self):
        me, landing = self.ring.me, self.landing1
        self.ring.wait_right()
        self.ring.wait_left()

        def store(i, j, value):
            landing[3 * i, j] = landing[3 * i, j] + value

        self.products(lambda i: ((me + 1 + 2 * i) % 4, i), store)
        self.ring.pass_right()
        self.ring.pass_left()

    def turn(self):
        me, landing, sends = self.ring.me, self.landing1, self.sends
        self.ring.finish()
        self.ring.first.wait()

        def store(i, j, value):
            sends[i, j] = value + landing[2 - i, j] + landing[4 + i, j]

        self.products(lambda i: (me, i), store)
        if self.before:
            self.comm.wait(self.credits.at[1], self.axes[1])
        self.ring2.start_all()
        if self.unused is not None:
            self.ring.sent()
            self.comm.signal(self.unused, 'xc')

    def free1(self):
        self.ring.sent()
        self.comm.signal(self.credits.at[0], self.axes[0])

    def middle2(self):
        self.ring2.middle_right()
        self.ring2.middle_left()

    def finish(self):
        self.ring2.finish()
        n = self.result.shape[0] // 2
        self.result[0:n], self.result[n:2 * n] = self.ring2.sums()

    def sent(self):
        self.ring2.sent()

    def free2(self):
        self.sent()
        self.comm.signal(self.credits.at[1], self.axes[1])


CHUNKS = 4


def grad_shapes(width, slice_):
    return (width // 16, slice_ // 2 // CHUNKS), (slice_ // 16, width // 2 // CHUNKS)


def grad_chunks(comm, operands, bufs, results, credits, before=None, unused=None):
    out = []
    for k in range(CHUNKS):
        pieces = 2 if before and k == CHUNKS - 1 else 1
        for piece in range(pieces):
            both = []
            for i, axes in enumerate(('zy', 'yz')):
                width = bufs[3 * i].shape[4] // pieces
                cols = pl.ds(piece * width, width)
                sends, land1 = [ref.at[k, :, :, :, cols] for ref in bufs[3 * i:3 * i + 2]]
                land2 = bufs[3 * i + 2].at[k, :, :, cols]
                both.append(GradReduce(comm, axes, operands[i], (k * pieces + piece) * width, sends, land1, land2,
                                       results(i, k, cols), credits.at[2 * k + i],
                                       before[k].things[i] if before and piece == 0 else None,
                                       unused.at[k + piece, i] if before else None))
            out.append(Every(both))
    return out


class BlockGather:
    def __init__(self, comm, own, view, count, unused=None):
        self.comm, self.own, self.view, self.unused = comm, own, view, unused
        c = comm.c
        n = own.shape[0] // 2
        half = lambda h: pl.ds(h * n, n)
        self.ring = RingGather(comm, 'x', lambda h: own.at[half(h)], lambda p, h: view(p, c).at[half(h)], own, count(3))
        self.four = count(4)
        self.group, self.sem = Sends(comm, self.four), comm.recv_sem()
        self.kept = []

    def push(self, pos, src):
        c = self.comm
        c.send(src, self.view(pos, c.c), c.partner, self.group, self.sem)

    def start(self):
        here = self.view(self.ring.me, self.comm.c)
        if self.unused is None:
            self.kept = self.comm.local((self.own, here))
        else:
            self.comm.wait(self.unused, 'xc')
            here[...] = self.own[...]
        self.ring.start()
        self.push(self.ring.me, self.own)

    def forward(self):
        self.ring.forward()

    def near(self):
        ring, c = self.ring, self.comm.c
        ring.near()
        self.push(ring.left, self.view(ring.left, c))
        self.push(ring.right, self.view(ring.right, c))

    def finish(self):
        ring, c = self.ring, self.comm.c
        ring.finish()
        self.push(ring.far, self.view(ring.far, c))

    def arrived(self):
        self.comm.wait_recv(self.four, self.sem)
        done(self.kept)


def rows_from(src, dst, first):
    n = src.shape[1] // 4
    rows = [pl.ds(pl.multiple_of((first + k) % 4 * n, n), n) for k in range(4)]
    pairs = [(src.at[:, r], dst.at[:, r]) for r in rows]
    return pairs[0], pairs[1:]


def columns_from(src, dst):
    n = src.shape[-1] // CHUNKS
    return [(src.at[..., cols], dst.at[..., cols]) for cols in (pl.ds(0, n), pl.ds(n, src.shape[-1] - n))]


def lower_half(x0_hbm, x1_hbm, e1_hbm, part_hbm, w1_hbm, w2_hbm, a_hbm, ut_low, st_low, ut_top, st_top, q_top, d_top,
               q_low, d_low, grad, x2, landed_in, landed_out, part, landing,
               w, df, a, q, xv, e1, gut, gst, gq, gd, top_in, top_out, low_in, low_out,
               sends_in, sends_out, landing2_in, landing2_out,
               send_sems, recv_sems, local_sems, credits, x_free, in_free, out_free, unused):
    bufs = sends_in, landed_in, landing2_in, sends_out, landed_out, landing2_out
    comm = Comm(send_sems, recv_sems, local_sems)
    tokens = xv.shape[0]
    x, c = comm.x, comm.c
    group = a.shape[0]
    load_d = comm.local((e1_hbm, e1))
    far_in, rest_in = rows_from(ut_top, gut, comm.z + 2)
    far_out, rest_out = rows_from(st_top, gst, comm.y + 2)
    q_first, q_rest = columns_from(q_top, gq)
    d_first, d_rest = columns_from(d_top, gd)
    loads_in = comm.local(far_in, q_first)
    loads_out = comm.local(far_out, d_first)
    comm.arrive('xyzc')
    loads_rest = comm.local(q_rest, d_rest, *rest_in, *rest_out)
    columns = lambda ref, j: ref.at[:, pl.ds(j * group, group)]
    load_w = lambda ref: comm.local(*[(columns(ref, j), w.at[j]) for j in range(4)])
    own_b = lambda ref: lambda cols: flat(ref[..., cols])
    top = [[(at.at[k], own_b(b.at[k])) for k in (0, 1)] for at, b in ((gut, gq), (gst, gd))]
    chunk_out = low_out.shape[2]
    top_results = lambda i, k, cols: (top_out if i else top_in).at[:, pl.ds(k * chunk_out, chunk_out)]
    upper = grad_chunks(comm, top, bufs, top_results, credits)
    (t0i, t0o), (t1i, t1o), (t2i, t2o), (t3i, t3o) = [pair.things for pair in upper]
    done(loads_in)
    t0i.take_far()
    comm.meet('xyzc')

    t0i.send_far()
    gather_d = ring_of_tokens(comm, df)
    done(load_d)
    df[x] = e1[...].astype(BF16)
    gather_d.start()
    load2 = load_w(w2_hbm) + comm.local((a_hbm, a))
    load_x = comm.local((x0_hbm, xv))

    def by_columns(left):
        rows = w.shape[1] // 8

        def product(i):
            value = None
            for j in range(4):
                term = dot_bt(flat(left[..., j * group:(j + 1) * group]),
                              w[j, pl.ds(pl.multiple_of(i * rows, rows), rows)])
                value = term if value is None else value + term
            return value

        return product

    done(loads_out)
    t0o.take_far()
    t0o.send_far()
    done(loads_rest)
    t0i.start_near()
    t0o.start_near()
    t2o.start()
    t1i.start()
    gather_d.forward()
    t2i.start()
    t0o.middle()
    gather_d.near()
    t1o.start()
    gather_d.finish()
    done(load2)
    backward_acts(df, by_columns(df), a, q)
    load1 = load_w(w1_hbm)
    _, d_arrived = comm.push(last_dim_half(df, 1 - c), d_low)
    _, q_arrived = comm.push(last_dim_half(q, 1 - c), q_low)
    done(load1)
    ring = token_sums(comm, part, landing, tokens)
    product = by_columns(q)
    backward_part(product, part, 0)
    ring.start_half(0)
    t2i.middle()
    t2o.middle()
    t0o.turn()
    t0o.free1()
    t0i.middle()
    backward_part(product, part, 1)
    ring.start_half(1)
    d_arrived()
    q_arrived()
    half = a.shape[1] // 2
    loads = comm.local(*[(ut_low.at[k], w.at[k]) for k in (0, 1)], *[(st_low.at[k], w.at[2 + k]) for k in (0, 1)],
                       (q_low, a.at[:, pl.ds(0, half)]))
    loads += comm.local(*[(d_low.at[k], a.at[pl.ds(k * tokens, tokens), pl.ds(half, half)]) for k in range(4)])
    t1o.middle()
    t2i.turn()
    t0o.middle2()
    t2i.free1()
    t3i.start()
    ring.middle_right()
    t2o.turn()
    topi = BlockGather(comm, top_in, lambda p, core: landing.at[p * 2 + core], lambda n: landing.at[pl.ds(0, n)], in_free)
    rows, width = top_out.shape
    topo = BlockGather(comm, top_out, lambda p, core: part.at[pl.ds(pl.multiple_of(p * rows, rows), rows),
                                                              pl.ds(pl.multiple_of(core * width, width), width)],
                       lambda n: part.at[pl.ds(0, n * rows), pl.ds(0, width)], out_free)

    def low_gather(k, piece, pieces, i):
        res, landed = (low_out, landed_out) if i else (low_in, landed_in)
        n = res.shape[2] // pieces
        cols = pl.ds(piece * n, n)
        return BlockGather(comm, res.at[k, :, cols], lambda p, core: landed.at[k, p, core, :, cols],
                           lambda m: landed.at[k, pl.ds(0, m), 0, :, cols], unused.at[k + piece, i])

    last = CHUNKS - 1
    low = [(k, 0, 1) for k in range(last)] + [(last, 0, 2), (last, 1, 2)]
    low = [Every([low_gather(*piece, i) for i in (0, 1)]) for piece in low]
    (low0i, low0o), (low1i, low1o), (low2i, low2o), (low3i, low3o), (low4i, low4o) = [pair.things for pair in low]
    t2o.free1()
    t0i.turn()
    t0i.free1()
    t1o.turn()
    t1o.free1()
    ring.middle_left()
    t2i.middle2()
    t3o.start()
    t0i.middle2()
    done(loads)
    mine = lambda ref: lambda cols: flat(ref[..., pl.ds(pl.multiple_of(c * half + cols.start, cols.size), cols.size)])
    other = lambda first: lambda cols: a[:, pl.ds(first + cols.start, cols.size)]
    operands = [[(w.at[0], mine(q)), (w.at[1], other(0))], [(w.at[2], mine(df)), (w.at[3], other(half))]]
    low_results = lambda i, k, cols: (low_out if i else low_in).at[k, :, cols]
    lower = grad_chunks(comm, operands, bufs, low_results, credits, upper, unused)
    (g0i, g0o), (g1i, g1o), (g2i, g2o), (g3i, g3o), (g4i, g4o) = [pair.things for pair in lower]
    t0o.finish()
    t0o.free2()
    t2i.finish()
    t1i.middle()
    t2o.middle2()
    t3o.middle()
    t1o.middle2()
    t3i.middle()
    ring.finish()
    g = jnp.concatenate(ring.sums(), axis=1)
    done(load_x)
    grad[...] = (e1[...] + norm_rows_vjp(xv[...].astype(F32), g)).astype(BF16)
    load_x = comm.local((x1_hbm, xv))
    ring.sent()
    comm.signal(x_free, 'x')
    load_part = comm.local((part_hbm, part))
    comm.wait(x_free, 'x')
    done(load_part)
    ring = token_sums(comm, part, landing, tokens, ring)
    ring.start_all()
    t0i.finish()
    t1i.turn()
    t1i.free1()
    t2i.free2()
    t2o.finish()
    g0o.start()
    t1o.finish()
    t1o.free2()
    g2i.start()
    t0i.free2()
    t3o.turn()
    t3o.free1()
    t3i.turn()
    t1i.middle2()
    ring.middle_left()
    t3i.free1()
    ring.middle_right()
    g0o.middle()
    g2i.middle()
    t3i.middle2()
    t3o.middle2()
    g0i.start()
    t1i.finish()
    g1o.start()
    t2o.free2()
    g2i.turn()
    g0o.turn()
    t3o.finish()
    t3i.finish()
    t3i.free2()
    t1i.free2()
    t3o.free2()
    ring.finish()
    done(load_x)
    x2[...] = (xv[...].astype(F32) + jnp.concatenate(ring.sums(), axis=1)).astype(BF16)
    ring.sent()
    comm.signal(in_free, 'xc')
    comm.signal(out_free, 'xc')
    topo.start()
    topi.start()
    g0i.middle()
    g1o.middle()
    topo.forward()
    g2i.middle2()
    g0o.middle2()
    g1i.start()
    g2o.start()
    topo.near()
    g0i.turn()
    g0o.finish()
    g1o.turn()
    low0o.start()
    g2i.finish()
    low2i.start()
    g1i.middle()
    topi.forward()
    g2o.middle()
    g1o.middle2()
    g3i.start()
    g0i.middle2()
    g3o.start()
    topo.finish()
    g1i.turn()
    low2i.forward()
    g2o.turn()
    low0o.forward()
    g0i.finish()
    low2i.near()
    g1o.finish()
    g4i.start()
    topi.near()
    g3i.middle()
    g3o.middle()
    low1o.start()
    low0i.start()
    low0o.near()
    low2i.finish()
    g2o.middle2()
    g1i.middle2()
    g4o.start()
    low1o.forward()
    low1o.near()
    low0o.finish()
    g4i.middle()
    g1i.finish()
    low1i.start()
    low0i.forward()
    g3o.turn()
    g4o.middle()
    g3i.turn()
    g2o.finish()
    low2o.start()
    low1i.forward()
    g4i.turn()
    g3o.middle2()
    low1o.finish()
    low0i.near()
    g4o.turn()
    low2o.forward()
    g3i.middle2()
    g4i.middle2()
    g3o.finish()
    low3o.start()
    g4o.middle2()
    g3i.finish()
    low2o.near()
    low3i.start()
    low1i.near()
    low2o.finish()
    g4i.finish()
    low4i.start()
    low0i.finish()
    g4o.finish()
    low4o.start()
    topi.finish()
    low1i.finish()
    low3i.forward()
    low4i.forward()
    low4i.near()
    low3o.forward()
    low4o.forward()
    low3i.near()
    low3o.near()
    low4o.near()
    low3o.finish()
    low3i.finish()
    low4i.finish()
    low4o.finish()
    for pair in [topi, topo] + low:
        pair.arrived()
    comm.end()


def call_lower_half(x0, x1, e1, part_hbm, w1_hbm, w2_hbm, a_hbm, ut_low, st_low, ut_top, st_top, q_top, d_top):
    tokens, width = x0.shape
    group, slice_ = a_hbm.shape
    block = sds((tokens, width), BF16)
    shapes = grad_shapes(width, slice_)
    landed = [VMEM((CHUNKS, 6, 2) + shape, F32) for shape in shapes]
    (rows_in, cols_in), (rows_out, cols_out) = shapes
    kept = [VMEM(block.shape, BF16), VMEM(block.shape, BF16)] + landed
    kept += [VMEM((group, width), F32), VMEM((8, tokens, width // 2), F32)]
    outs = [sds(q_top.shape[1:], BF16), sds(d_top.shape[1:], BF16)] + kept
    acts = VMEM((group, slice_), BF16)
    scratch = [VMEM((4, width, group), BF16), VMEM((4, tokens, width), BF16), acts, acts]
    scratch += [VMEM(block.shape, BF16), VMEM(block.shape, F32)]
    scratch += [VMEM(r.shape, BF16) for r in (ut_top, st_top, q_top, d_top)]
    scratch += [VMEM(shape, F32) for shape in ((rows_in, CHUNKS * cols_in), (rows_out, CHUNKS * cols_out),
                                               (CHUNKS, rows_in, cols_in), (CHUNKS, rows_out, cols_out))]
    scratch += [VMEM((CHUNKS, 4, 2) + shape, F32) for shape in shapes]
    scratch += [VMEM((CHUNKS, 6, rows // 2, cols), F32) for rows, cols in shapes]
    ins = (x0, x1, e1, part_hbm, w1_hbm.reshape(width, slice_), w2_hbm.reshape(slice_, width), a_hbm,
           ut_low, st_low, ut_top, st_top, q_top, d_top)
    return pl.pallas_call(
        lower_half,
        name='lower_half',
        out_shape=tuple(outs),
        in_specs=spaces('h' * 13),
        out_specs=tuple(spaces('hhvvvvvv')),
        scratch_shapes=scratch + [sems(LOWER[0]), sems(LOWER[1]), sems(LOWER[2]), pltpu.SemaphoreType.REGULAR((2 * CHUNKS, 2)),
                                  pltpu.SemaphoreType.REGULAR, pltpu.SemaphoreType.REGULAR, pltpu.SemaphoreType.REGULAR,
                                  pltpu.SemaphoreType.REGULAR((CHUNKS + 1, 2))],
        compiler_params=pltpu.CompilerParams(collective_id=2, has_side_effects=True,
                                             vmem_limit_bytes=VMEM_BYTES - VMEM_KEPT),
        cost_estimate=pl.CostEstimate(flops=16 * group * width * slice_, bytes_accessed=1 << 24, transcendentals=0),
    )(*ins)


def assemble(grad, x2, landed_in, landed_out, part, landing, grad_in, grad_out, tokens_grad, tokens_out, store_sems):
    strip = grad_in.shape[2] // 64
    rows, width = landed_out.shape[-2:]
    per = landed_in.shape[-1] // strip
    others = [pltpu.make_async_copy(grad, tokens_grad, store_sems.at[2]), pltpu.make_async_copy(x2, tokens_out, store_sems.at[3])]
    for copy in others:
        copy.start()
    pltpu.make_async_copy(part, grad_out.at[1], store_sems.at[1]).start()
    for x in range(4):
        for n in range(2 * CHUNKS):
            c, k = n // CHUNKS, n % CHUNKS
            dst = grad_out.at[0, pl.ds(x * rows, rows), pl.ds(n * width, width)]
            pltpu.make_async_copy(landed_out.at[k, x, c], dst, store_sems.at[1]).start()
            for j in range(per):
                t = k * per + j
                y, z = 2 * c + t // 4, t % 4
                cols = pl.ds(((4 * z + y) * 4 + x) * strip, strip)
                low = landed_in.at[k, x, c, :, pl.ds(j * strip, strip)]
                top = landing.at[2 * x + c, :, pl.ds(t * strip, strip)]
                pltpu.make_async_copy(low, grad_in.at[0, :, cols], store_sems.at[0]).start()
                pltpu.make_async_copy(top, grad_in.at[1, :, cols], store_sems.at[0]).start()
    pltpu.make_async_copy(grad_in, grad_in, store_sems.at[0]).wait()
    pltpu.make_async_copy(grad_out, grad_out, store_sems.at[1]).wait()
    done(others)


def call_assemble(kept, in_shape, out_shape):
    kept = [pltpu.with_memory_space_constraint(ref, VMEM) for ref in kept]
    block = sds(kept[0].shape, BF16)
    return pl.pallas_call(
        assemble,
        name='assemble',
        out_shape=(sds(in_shape, F32), sds(out_shape, F32), block, block),
        in_specs=spaces('vvvvvv'),
        out_specs=tuple(spaces('hhhh')),
        scratch_shapes=[sems(4)],
        compiler_params=pltpu.CompilerParams(vmem_limit_bytes=VMEM_BYTES - VMEM_KEPT),
        cost_estimate=pl.CostEstimate(flops=1 << 30, bytes_accessed=1 << 25, transcendentals=0),
    )(*kept)


def solution(mesh):
    tok_spec = P(('local', 'data'), None)
    w_spec = P(None, 'local', None)

    def device_step(tokens, cotangent, w_in, w_out):
        (x1, e1, part_out, a_low, ut_low, st_low, ut_top, st_top, q_top, d_top, w1_low, w2_low) = call_upper_half(
            tokens, cotangent, w_in, w_out)
        _, _, *kept = call_lower_half(
            tokens, x1, e1, part_out, w1_low, w2_low, a_low, ut_low, st_low, ut_top, st_top, q_top, d_top)
        grad_in, grad_out, grad, x2 = call_assemble(kept, w_in.shape, w_out.shape)
        return x2, grad_in, grad_out, grad

    return jax.shard_map(device_step, mesh=mesh, in_specs=(tok_spec, tok_spec, w_spec, w_spec),
                         out_specs=(tok_spec, w_spec, w_spec, tok_spec), check_vma=False)
```
